8 devices in a mesh: dp: 1 (over z), cp: 8 (over y, x, core).
Axes of the slice: x: 2, y: 2, z: 1, core: 2. Of those that a mesh axis runs over, the one named last changes fastest.
Arguments:
- query: bfloat16 [32, 1024, 8, 256], P('dp', 'cp')
- keys: bfloat16 [32, 1024, 1, 256], P('dp', 'cp')
- values: bfloat16 [32, 1024, 1, 256], P('dp', 'cp')
- grad_out: bfloat16 [32, 1024, 8, 256], P('dp', 'cp')
- doc_id: int32 [32, 1024], P('dp', 'cp')
Outputs:
- output 1: bfloat16 [32, 1024, 8, 256], P('dp', 'cp')
- output 2: bfloat16 [32, 1024, 8, 256], P('dp', 'cp')
- output 3: bfloat16 [32, 1024, 1, 256], P('dp', 'cp')
- output 4: bfloat16 [32, 1024, 1, 256], P('dp', 'cp')
All inputs are finite; a program needn't handle non-finite values.
Results may differ from the reference program's by a relative error of at most 0.0107405.
Values are sent between devices in bfloat16 or wider.
A program may use at most 1 GiB of HBM per device.

```python
import jax
import jax.numpy as jnp
from jax import lax

BATCH = 32
SEQ = 1024
HEADS = 8
HEAD = 256
ROW_BLOCK = 16
DOC_CUTS = 4
NEG_BIG = -1e30


def doc_ids_row(key):
    key_cut, key_count = jax.random.split(key)
    cut_pos = jax.random.permutation(key_cut, SEQ - 1)[:DOC_CUTS] + 1
    cut_count = jax.random.randint(key_count, (), 1, DOC_CUTS + 1)
    cut_valid = jnp.arange(DOC_CUTS) < cut_count
    positions = jnp.arange(SEQ)
    cut_hits = (cut_pos[None, :] <= positions[:, None]) & cut_valid[None, :]
    return jnp.sum(cut_hits.astype(jnp.int32), axis=1).astype(jnp.int32)


def setup_inputs(seed: int = 0, part: int = 0) -> dict:
    key = jax.random.fold_in(jax.random.key(seed), part)
    key_q, key_k, key_v, key_slow, key_g, key_doc = jax.random.split(key, 6)
    query = 1.5 * jax.random.normal(key_q, (BATCH, SEQ, HEADS, HEAD), jnp.float32)
    keys = 1.5 * jax.random.normal(key_k, (BATCH, SEQ, 1, HEAD), jnp.float32)
    slow = jax.random.normal(key_slow, (BATCH, 16, 1, HEAD), jnp.float32)
    noise = jax.random.normal(key_v, (BATCH, SEQ, 1, HEAD), jnp.float32)
    values = 0.8 * jnp.repeat(slow, SEQ // 16, axis=1) + 0.6 * noise
    grad_out = 0.5 * jax.random.normal(key_g, (BATCH, SEQ, HEADS, HEAD), jnp.float32)
    doc_id = jax.vmap(doc_ids_row)(jax.random.split(key_doc, BATCH))
    return {'query': query.astype(jnp.bfloat16), 'keys': keys.astype(jnp.bfloat16), 'values': values.astype(jnp.bfloat16), 'grad_out': grad_out.astype(jnp.bfloat16), 'doc_id': doc_id}


def reference(query, keys, values, grad_out, doc_id):
    score_scale = HEAD ** -0.5
    n_blocks = SEQ // ROW_BLOCK
    key_pos = jnp.arange(SEQ)
    pos_blocks = key_pos.reshape(n_blocks, ROW_BLOCK)

    def one_row(row):
        q_row, k_row, v_row, g_row, doc_row = row
        k_mat = k_row[:, 0, :].astype(jnp.float32)
        v_mat = v_row[:, 0, :].astype(jnp.float32)
        q_blocks = q_row.reshape(n_blocks, ROW_BLOCK, HEADS, HEAD)
        g_blocks = g_row.reshape(n_blocks, ROW_BLOCK, HEADS, HEAD)
        doc_blocks = doc_row.reshape(n_blocks, ROW_BLOCK)

        def step(carry, block):
            dk_acc, dv_acc = carry
            q_block, g_block, doc_block, pos_block = block
            q_wide = q_block.astype(jnp.float32)
            g_wide = g_block.astype(jnp.float32)
            visible = (key_pos[None, :] <= pos_block[:, None]) & (doc_row[None, :] == doc_block[:, None])
            raw_scores = jnp.einsum('qhd,kd->qhk', q_wide, k_mat) * score_scale
            scores = jnp.where(visible[:, None, :], raw_scores, NEG_BIG)
            exp_scores = jnp.exp(scores - jnp.max(scores, axis=-1, keepdims=True))
            prob_f32 = exp_scores / jnp.sum(exp_scores, axis=-1, keepdims=True)
            prob_low = prob_f32.astype(jnp.bfloat16).astype(jnp.float32)
            out_block = jnp.einsum('qhk,kd->qhd', prob_low, v_mat).astype(jnp.bfloat16)
            row_delta = jnp.einsum('qhd,qhd->qh', g_wide, out_block.astype(jnp.float32))
            grad_prob = jnp.einsum('qhd,kd->qhk', g_wide, v_mat)
            grad_score = (prob_f32 * (grad_prob - row_delta[:, :, None])).astype(jnp.bfloat16).astype(jnp.float32)
            dq_block = (jnp.einsum('qhk,kd->qhd', grad_score, k_mat) * score_scale).astype(jnp.bfloat16)
            dk_acc = dk_acc + jnp.einsum('qhk,qhd->kd', grad_score, q_wide)
            dv_acc = dv_acc + jnp.einsum('qhk,qhd->kd', prob_low, g_wide)
            return (dk_acc, dv_acc), (out_block, dq_block)

        kv_zero = jnp.zeros((SEQ, HEAD), jnp.float32)
        sums, blocks = lax.scan(step, (kv_zero, kv_zero), (q_blocks, g_blocks, doc_blocks, pos_blocks))
        out_row = blocks[0].reshape(SEQ, HEADS, HEAD)
        dq_row = blocks[1].reshape(SEQ, HEADS, HEAD)
        dk_row = (sums[0] * score_scale).astype(jnp.bfloat16)[:, None, :]
        dv_row = sums[1].astype(jnp.bfloat16)[:, None, :]
        return out_row, dq_row, dk_row, dv_row

    attn_out, grad_query, grad_keys, grad_values = lax.map(one_row, (query, keys, values, grad_out, doc_id))
    return (attn_out, grad_query, grad_keys, grad_values)
```

```python
import functools

import jax
import jax.numpy as jnp
from jax import lax
from jax.experimental import pallas as pl
from jax.experimental.pallas import tpu as pltpu
from jax.sharding import PartitionSpec as P


NEG_BIG = -1e30
LOG2E = 1.4426950408889634
G = 32
NS = 16
NCH = 4
T = 4
F_CAP = ((32, 32, 32, 32),) * 3
B_CAP = ((32, 32, 32, 32),) * 3

NR, OR, NSD, OSD, DM, ST, SGO, SGR, CE, NTAB = 0, 48, 96, 144, 192, 224, 232, 256, 280, 288


def bounds(caps):
    out = [0]
    for cap in caps:
        out.append(out[-1] + cap)
    return out


F_LO = [bounds(cap) for cap in F_CAP]


def table_kernel(ks, me, tab):
    c = me[0]
    tab[CE] = c
    tab[CE + 1] = me[1]
    tab[ST] = 0
    for d in range(1, NCH):
        for s in range(NS):
            tab[NR + (d - 1) * NS + s] = 0
            tab[OR + (d - 1) * NS + s] = 0
            tab[NSD + (d - 1) * NS + s] = 0
            tab[OSD + (d - 1) * NS + s] = 0
        for v in range(T + 1):
            tab[SGO + (d - 1) * (T + 1) + v] = 0
            tab[SGR + (d - 1) * (T + 1) + v] = 0

    for s in range(NS):
        for h in range(2):
            need = jnp.maximum(256 * c - ks[s * 8 + 2 * c + h], 0)
            tab[DM + s * 2 + h] = (need + 255) >> 8

    for cc in range(NCH):
        here = cc == c

        def scan(s, carry):
            off, ready, avail = carry
            back = 256 * cc - ks[s * 8 + 2 * cc]
            nxt = []
            for d in range(1, NCH):
                if d <= cc:
                    x = jnp.clip(back - 256 * (d - 1), 0, 256)
                    n = (x + G - 1) // G
                else:
                    n = jnp.int32(0)
                nxt.append(off[d - 1] + n)

                @pl.when(here)
                def _():
                    tab[NR + (d - 1) * NS + s] = n
                    tab[OR + (d - 1) * NS + s] = off[d - 1]

                @pl.when(c + d == cc)
                def _():
                    tab[NSD + (d - 1) * NS + s] = n
                    tab[OSD + (d - 1) * NS + s] = off[d - 1]
            ready2, avail2 = [], []
            for t in range(T):
                ok = nxt[0] <= F_LO[0][t + 1]
                for d in range(2, NCH):
                    ok = ok & (nxt[d - 1] <= F_LO[d - 1][t + 1])
                one = jnp.where(ok, 1, 0)
                ready2.append(ready[t] + one)
                avail2.append(tuple(jnp.where(ok, nxt[d - 1], avail[t][d - 1]) for d in range(1, NCH)))
            return tuple(nxt), tuple(ready2), tuple(avail2)

        zero = jnp.int32(0)
        init = ((zero,) * 3, (zero,) * T, ((zero,) * 3,) * T)
        _, ready, avail = lax.fori_loop(0, NS, scan, init)

        @pl.when(here)
        def _():
            for t in range(T):
                tab[ST + t + 1] = ready[t]

        for d in range(1, NCH):
            sent = zero
            for v in range(T):
                sent = jnp.minimum(sent + B_CAP[d - 1][v], avail[v][d - 1])

                @pl.when(here)
                def _():
                    tab[SGO + (d - 1) * (T + 1) + v + 1] = sent

                @pl.when(c + d == cc)
                def _():
                    tab[SGR + (d - 1) * (T + 1) + v + 1] = sent


def pack_kernel(tab, own, mate, kvcol, *rest):
    chunks = [rest[d * T:(d + 1) * T] for d in range(3)]
    stage, sem = rest[3 * T:]
    s = pl.program_id(0)
    slot = lax.rem(s, 2)
    e = tab[CE + 1]

    def wait(ss, sl):
        for d in range(3):
            def one(k, _):
                pltpu.make_async_copy(stage.at[sl, 0], chunks[d][0].at[0], sem.at[sl]).wait()
                return 0

            lax.fori_loop(0, tab[NSD + d * NS + ss], one, 0)

    @pl.when(s >= 2)
    def _():
        wait(s - 2, slot)

    kvcol[0, e] = own[0]
    kvcol[0, 1 - e] = mate[0]
    stage[slot, pl.ds(e * 4, 4)] = own[0].reshape(4, G, 512)
    stage[slot, pl.ds(4 - e * 4, 4)] = mate[0].reshape(4, G, 512)
    for d in range(3):
        n = tab[NSD + d * NS + s]
        off = tab[OSD + d * NS + s]

        def send(k, _):
            j = off + k
            for t in range(T):
                @pl.when((j >= F_LO[d][t]) & (j < F_LO[d][t + 1]))
                def _():
                    pltpu.make_async_copy(stage.at[slot, 8 - n + k], chunks[d][t].at[j - F_LO[d][t]], sem.at[slot]).start()
            return 0

        lax.fori_loop(0, n, send, 0)

    @pl.when(s == NS - 1)
    def _():
        wait(s - 1, 1 - slot)
        wait(s, slot)


def dot_nt(a, b):
    return lax.dot_general(a, b, (((1,), (1,)), ((), ())), preferred_element_type=jnp.float32)


def dot_nn(a, b):
    return lax.dot_general(a, b, (((1,), (0,)), ((), ())), preferred_element_type=jnp.float32)


def dot_tn(a, b):
    return lax.dot_general(a, b, (((0,), (0,)), ((), ())), preferred_element_type=jnp.float32)


def compute_kernel(t, n_alias, scale, tab, docs, q_all, q_mate, g_all, g_mate, kvcol, *rest):
    fbuf = [rest[d * (t + 1):(d + 1) * (t + 1)] for d in range(3)]
    rest = rest[3 * (t + 1) + n_alias:]
    o_all, o_send, dq_all, dq_send, acc = rest[:5]
    rest = rest[5:]
    live = T - t
    bbuf = [rest[d * live:(d + 1) * live] for d in range(3)]
    qg, outb, kvs, dkv, s_scr, p_scr, m_scr, l_scr, docr, o_acc, dq_acc, isem, osem = rest[3 * live:]

    base = tab[ST + t]
    n = tab[ST + t + 1] - base
    c = tab[CE]
    e = tab[CE + 1]

    def inputs(ss, sl):
        own = e * NS + ss
        return [
            pltpu.make_async_copy(src, dst, isem.at[sl])
            for src, dst in (
                (kvcol.at[ss], kvs.at[sl, 0]),
                (q_all.at[own], qg.at[sl, 0]), (q_mate.at[ss], qg.at[sl, 1]),
                (g_all.at[own], qg.at[sl, 2]), (g_mate.at[ss], qg.at[sl, 3]),
            )
        ]

    def outputs(ss, sl):
        own = e * NS + ss
        return [
            pltpu.make_async_copy(src, dst, osem.at[sl])
            for src, dst in (
                (outb.at[sl, 0], o_all.at[own]), (outb.at[sl, 1], o_send.at[ss]),
                (outb.at[sl, 2], dq_all.at[own]), (outb.at[sl, 3], dq_send.at[ss]),
                (dkv.at[sl, 0], acc.at[ss]),
            )
        ]

    def fetch(ss, sl):
        for copy in inputs(ss, sl):
            copy.start()
        for d in range(3):
            cnt = tab[NR + d * NS + ss]
            off = tab[OR + d * NS + ss]

            def one(k, _):
                j = off + k
                for u in range(t + 1):
                    @pl.when((j >= F_LO[d][u]) & (j < F_LO[d][u + 1]))
                    def _():
                        row = pl.multiple_of((8 - cnt + k) * G, G)
                        pltpu.make_async_copy(fbuf[d][u].at[j - F_LO[d][u]], kvs.at[sl, d + 1, pl.ds(row, G)], isem.at[sl]).start()
                return 0

            lax.fori_loop(0, cnt, one, 0)

    def fetch_wait(ss, sl):
        for copy in inputs(ss, sl):
            copy.wait()
        for d in range(3):
            def one(k, _):
                pltpu.make_async_copy(fbuf[d][0].at[0], kvs.at[sl, d + 1, pl.ds(0, G)], isem.at[sl]).wait()
                return 0

            lax.fori_loop(0, tab[NR + d * NS + ss], one, 0)

    def put(ss, sl):
        for copy in outputs(ss, sl):
            copy.start()
        for d in range(3):
            cnt = tab[NR + d * NS + ss]
            off = tab[OR + d * NS + ss]

            def one(k, _):
                j = off + k
                for v in range(t, T):
                    lo = tab[SGO + d * (T + 1) + v]
                    hi = tab[SGO + d * (T + 1) + v + 1]

                    @pl.when((j >= lo) & (j < hi))
                    def _():
                        row = pl.multiple_of((8 - cnt + k) * G, G)
                        pltpu.make_async_copy(dkv.at[sl, d + 1, pl.ds(row, G)], bbuf[d][v - t].at[j - lo], osem.at[sl]).start()
                return 0

            lax.fori_loop(0, cnt, one, 0)

    def put_wait(ss, sl):
        for copy in outputs(ss, sl):
            copy.wait()
        for d in range(3):
            def one(k, _):
                pltpu.make_async_copy(dkv.at[sl, d + 1, pl.ds(0, G)], bbuf[d][0].at[0], osem.at[sl]).wait()
                return 0

            lax.fori_loop(0, tab[NR + d * NS + ss], one, 0)

    row_tok = lax.broadcasted_iota(jnp.int32, (1024, 128), 0) >> 3
    lane = lax.broadcasted_iota(jnp.int32, (1024, 128), 1)

    def attend(role, s, slot):
        q_ref, g_ref = qg.at[slot, role], qg.at[slot, 2 + role]
        h = e if role == 0 else 1 - e
        dm = tab[DM + s * 2 + h]
        dq_row = docs[s, pl.ds(2 * c + h, 1), :]
        d_t = jnp.transpose(jnp.broadcast_to(dq_row, (128, 128)))
        docr[...] = jnp.broadcast_to(d_t[:, None, :], (128, 8, 128)).reshape(1024, 128)

        def scores(d, causal):
            sc = dot_nt(q_ref[...], kvs[slot, d, :, :256]) * (scale * LOG2E)
            halves = []
            for j in range(2):
                dk = docs[s, pl.ds(2 * (c - d) + j, 1), :]
                vis = docr[...] == dk
                if causal:
                    vis = vis & (lane + 128 * j <= row_tok + 128 * h)
                x = jnp.where(vis, sc[:, 128 * j:128 * (j + 1)], NEG_BIG)
                s_scr[d, :, 128 * j:128 * (j + 1)] = x
                halves.append(x)
            return jnp.maximum(halves[0], halves[1])

        m_scr[...] = scores(0, True)

        def more_scores(d, _):
            m_scr[...] = jnp.maximum(m_scr[...], scores(d, False))
            return 0

        lax.fori_loop(1, dm + 1, more_scores, 0)
        m_scr[...] = jnp.broadcast_to(jnp.max(m_scr[...], axis=1, keepdims=True), (1024, 128))

        def exps(d):
            tot = None
            for j in range(2):
                x = jnp.exp2(s_scr[d, :, 128 * j:128 * (j + 1)] - m_scr[...])
                s_scr[d, :, 128 * j:128 * (j + 1)] = x
                tot = x if tot is None else tot + x
            return tot

        l_scr[...] = exps(0)

        def more_exps(d, _):
            l_scr[...] = l_scr[...] + exps(d)
            return 0

        lax.fori_loop(1, dm + 1, more_exps, 0)
        l_scr[...] = jnp.broadcast_to(1.0 / jnp.sum(l_scr[...], axis=1, keepdims=True), (1024, 128))

        def weighted(d):
            for j in range(2):
                p = s_scr[d, :, 128 * j:128 * (j + 1)] * l_scr[...]
                s_scr[d, :, 128 * j:128 * (j + 1)] = p
                p_scr[d, :, 128 * j:128 * (j + 1)] = p.astype(jnp.bfloat16)
            return dot_nn(p_scr[d], kvs[slot, d, :, 256:])

        o_acc[...] = weighted(0)

        def more_weighted(d, _):
            o_acc[...] = o_acc[...] + weighted(d)
            return 0

        lax.fori_loop(1, dm + 1, more_weighted, 0)
        o_low = o_acc[...].astype(jnp.bfloat16)
        outb[slot, role] = o_low
        delta = jnp.sum(g_ref[...].astype(jnp.float32) * o_low.astype(jnp.float32), axis=1, keepdims=True)
        m_scr[...] = jnp.broadcast_to(delta, (1024, 128))

        def grads(d):
            dp = dot_nt(g_ref[...], kvs[slot, d, :, 256:])
            ds = []
            for j in range(2):
                p = s_scr[d, :, 128 * j:128 * (j + 1)]
                ds.append((p * (dp[:, 128 * j:128 * (j + 1)] - m_scr[...])).astype(jnp.bfloat16))
            ds = jnp.concatenate(ds, axis=1)
            return dot_nn(ds, kvs[slot, d, :, :256]), dot_tn(ds, q_ref[...]), dot_tn(p_scr[d], g_ref[...])

        dq0, dk0, dv0 = grads(0)
        dq_acc[...] = dq0
        if role == 0:
            dkv[slot, 0, :, :256] = dk0
            dkv[slot, 0, :, 256:] = dv0
        else:
            dkv[slot, 0, :, :256] = dkv[slot, 0, :, :256] + dk0
            dkv[slot, 0, :, 256:] = dkv[slot, 0, :, 256:] + dv0

        def more_grads(d, _):
            dq1, dk1, dv1 = grads(d)
            dq_acc[...] = dq_acc[...] + dq1
            dkv[slot, d, :, :256] = dkv[slot, d, :, :256] + dk1
            dkv[slot, d, :, 256:] = dkv[slot, d, :, 256:] + dv1
            return 0

        lax.fori_loop(1, dm + 1, more_grads, 0)
        outb[slot, 2 + role] = (dq_acc[...] * scale).astype(jnp.bfloat16)

    @pl.when(n > 0)
    def _():
        kvs[...] = jnp.zeros_like(kvs)
        fetch(base, 0)

    def step(i, _):
        slot = lax.rem(i, 2)
        s = base + i

        @pl.when(i + 1 < n)
        def _():
            fetch(s + 1, 1 - slot)

        @pl.when(i >= 2)
        def _():
            put_wait(s - 2, slot)

        fetch_wait(s, slot)
        any_dm = jnp.maximum(tab[DM + s * 2], tab[DM + s * 2 + 1])

        def clear(d, _):
            dkv[slot, d] = jnp.zeros((256, 512), jnp.float32)
            return 0

        lax.fori_loop(1, any_dm + 1, clear, 0)
        attend(0, s, slot)
        attend(1, s, slot)
        put(s, slot)
        return 0

    lax.fori_loop(0, n, step, 0)

    @pl.when(n >= 2)
    def _():
        put_wait(base + n - 2, lax.rem(n, 2))

    @pl.when(n >= 1)
    def _():
        put_wait(base + n - 1, lax.rem(n + 1, 2))


def final_kernel(scale, tab, acc, *rest):
    bufs = [rest[d * T:(d + 1) * T] for d in range(3)]
    dk_own, dv_own, dkv_send, got, sem = rest[3 * T:]
    s = pl.program_id(0)
    slot = lax.rem(s, 2)
    e = tab[CE + 1]

    def fetch(ss, sl):
        for d in range(3):
            cnt = tab[NSD + d * NS + ss]
            off = tab[OSD + d * NS + ss]

            def one(k, _):
                j = off + k
                for v in range(T):
                    lo = tab[SGR + d * (T + 1) + v]
                    hi = tab[SGR + d * (T + 1) + v + 1]

                    @pl.when((j >= lo) & (j < hi))
                    def _():
                        pltpu.make_async_copy(bufs[d][v].at[j - lo], got.at[sl, d, 8 - cnt + k], sem.at[sl]).start()
                return 0

            lax.fori_loop(0, cnt, one, 0)

    @pl.when(s == 0)
    def _():
        fetch(s, 0)

    @pl.when(s + 1 < NS)
    def _():
        fetch(s + 1, 1 - slot)

    for d in range(3):
        cnt = tab[NSD + d * NS + s]

        def one(k, _):
            pltpu.make_async_copy(bufs[d][0].at[0], got.at[slot, d, 0], sem.at[slot]).wait()
            return 0

        lax.fori_loop(0, cnt, one, 0)
    for d in range(3):
        cnt = tab[NSD + d * NS + s]

        def add(k, _):
            acc[0, k] = acc[0, k] + got[slot, d, k]
            return 0

        lax.fori_loop(8 - cnt, 8, add, 0)
    mine = acc[0, pl.ds(4 * e, 4)].reshape(128, 512)
    other = acc[0, pl.ds(4 - 4 * e, 4)].reshape(128, 512)
    dk_own[0] = (mine[:, :256] * scale).astype(jnp.bfloat16)
    dv_own[0] = mine[:, 256:].astype(jnp.bfloat16)
    dkv_send[0, :, :256] = (other[:, :256] * scale).astype(jnp.bfloat16)
    dkv_send[0, :, 256:] = other[:, 256:].astype(jnp.bfloat16)


ANY = pl.BlockSpec(memory_space=pl.ANY)
SMEM = pl.BlockSpec(memory_space=pltpu.SMEM)


def solution(mesh):
    n_dev = mesh.shape['cp']
    seq_spec = P('dp', 'cp', None, None)
    id_spec = P('dp', 'cp')
    swap = [(k, k ^ 1) for k in range(n_dev)]

    def per_device(query, keys, values, grad_out, doc_id):
        nb, piece, heads, hd = query.shape
        rows = piece * heads
        scale = hd ** -0.5
        rank = lax.axis_index('cp')
        c = rank // 2
        e = rank % 2
        q3 = query.reshape(nb, rows, hd)
        g3 = grad_out.reshape(nb, rows, hd)
        kv = jnp.concatenate([keys[:, :, 0, :], values[:, :, 0, :]], axis=-1)
        other = NS * (1 - e)

        def to_mate(x):
            return lax.ppermute(lax.dynamic_slice_in_dim(x, other, NS, 0), 'cp', swap)

        kv_mate = to_mate(kv)
        docs_all = lax.all_gather(doc_id, 'cp')
        docs = lax.dynamic_slice_in_dim(docs_all, e * NS, NS, 1).transpose(1, 0, 2)
        flat = docs.reshape(NS, n_dev * piece)
        ks = jnp.sum((flat[:, None, :] < docs[:, :, :1]).astype(jnp.int32), axis=-1)
        me = jnp.stack([c, e]).astype(jnp.int32)
        tab = pl.pallas_call(
            table_kernel,
            out_shape=jax.ShapeDtypeStruct((NTAB,), jnp.int32),
            in_specs=[SMEM, SMEM],
            out_specs=SMEM,
            name="tables",
        )(ks.reshape(-1), me)

        bf = jnp.bfloat16
        f32 = jnp.float32
        fshape = [jax.ShapeDtypeStruct((F_CAP[d][t], G, 512), bf) for d in range(3) for t in range(T)]
        packed = pl.pallas_call(
            pack_kernel,
            grid_spec=pltpu.PrefetchScalarGridSpec(
                num_scalar_prefetch=1,
                grid=(NS,),
                in_specs=[
                    pl.BlockSpec((1, piece, 512), lambda s, tab: (tab[CE + 1] * NS + s, 0, 0)),
                    pl.BlockSpec((1, piece, 512), lambda s, tab: (s, 0, 0)),
                ],
                out_specs=[pl.BlockSpec((1, 2, piece, 512), lambda s, tab: (s, 0, 0, 0))] + [ANY] * (3 * T),
                scratch_shapes=[pltpu.VMEM((2, 8, G, 512), bf), pltpu.SemaphoreType.DMA((2,))],
            ),
            out_shape=[jax.ShapeDtypeStruct((NS, 2, piece, 512), bf)] + fshape,
            name="pack",
        )(tab, kv, kv_mate)
        kvcol = packed[0].reshape(NS, 2 * piece, 512)
        fsend = packed[1:]
        frecv = [None] * (3 * T)
        for t in range(T):
            for d in range(3):
                hop = 2 * (d + 1)
                frecv[d * T + t] = lax.ppermute(fsend[d * T + t], 'cp', [(k, k + hop) for k in range(n_dev - hop)])
        q_mate = to_mate(q3)
        g_mate = to_mate(g3)

        state = None
        brecv = [[None] * T for _ in range(3)]
        for t in range(T):
            live = T - t
            n_alias = 0 if state is None else 5 + 3 * live
            out_shape = [
                jax.ShapeDtypeStruct((nb, rows, hd), bf), jax.ShapeDtypeStruct((NS, rows, hd), bf),
                jax.ShapeDtypeStruct((nb, rows, hd), bf), jax.ShapeDtypeStruct((NS, rows, hd), bf),
                jax.ShapeDtypeStruct((NS, 2 * piece, 512), f32),
            ] + [jax.ShapeDtypeStruct((B_CAP[d][v], G, 512), f32) for d in range(3) for v in range(t, T)]
            n_in = 1 + 1 + 4 + 1 + 3 * (t + 1)
            outs = pl.pallas_call(
                functools.partial(compute_kernel, t, n_alias, scale),
                in_specs=[SMEM, pl.BlockSpec(memory_space=pltpu.VMEM)] + [ANY] * (5 + 3 * (t + 1) + n_alias),
                out_specs=[ANY] * (5 + 3 * live),
                scratch_shapes=[
                    pltpu.VMEM((2, 4, rows, hd), bf), pltpu.VMEM((2, 4, rows, hd), bf),
                    pltpu.VMEM((2, 4, 256, 512), bf), pltpu.VMEM((2, 4, 256, 512), f32),
                    pltpu.VMEM((4, rows, 256), f32), pltpu.VMEM((4, rows, 256), bf),
                    pltpu.VMEM((rows, 128), f32), pltpu.VMEM((rows, 128), f32), pltpu.VMEM((rows, 128), jnp.int32),
                    pltpu.VMEM((rows, hd), f32), pltpu.VMEM((rows, hd), f32),
                    pltpu.SemaphoreType.DMA((2,)), pltpu.SemaphoreType.DMA((2,)),
                ],
                out_shape=out_shape,
                input_output_aliases={n_in + k: k for k in range(n_alias)},
                compiler_params=pltpu.CompilerParams(vmem_limit_bytes=56 * 1024 * 1024),
                cost_estimate=pl.CostEstimate(flops=60_000_000_000 // T, bytes_accessed=100_000_000 // T, transcendentals=0),
            )(tab, docs, q3, q_mate, g3, g_mate, kvcol, *[frecv[d * T + u] for d in range(3) for u in range(t + 1)],
              *([] if state is None else state))
            sends = [outs[5 + d * live] for d in range(3)]
            state = list(outs[:5]) + [outs[5 + d * live + k] for d in range(3) for k in range(1, live)]
            for d in range(3):
                hop = 2 * (d + 1)
                brecv[d][t] = lax.ppermute(sends[d], 'cp', [(k + hop, k) for k in range(n_dev - hop)])

        o_own, o_send, dq_own, dq_send, acc = state[:5]
        dk_own, dv_own, dkv_send = pl.pallas_call(
            functools.partial(final_kernel, scale),
            grid_spec=pltpu.PrefetchScalarGridSpec(
                num_scalar_prefetch=1,
                grid=(NS,),
                in_specs=[pl.BlockSpec((1, 8, G, 512), lambda s, tab: (s, 0, 0, 0))] + [ANY] * (3 * T),
                out_specs=[
                    pl.BlockSpec((1, piece, hd), lambda s, tab: (tab[CE + 1] * NS + s, 0, 0)),
                    pl.BlockSpec((1, piece, hd), lambda s, tab: (tab[CE + 1] * NS + s, 0, 0)),
                    pl.BlockSpec((1, piece, 512), lambda s, tab: (s, 0, 0)),
                ],
                scratch_shapes=[pltpu.VMEM((2, 3, 8, G, 512), f32), pltpu.SemaphoreType.DMA((2,))],
            ),
            out_shape=[
                jax.ShapeDtypeStruct((nb, piece, hd), bf), jax.ShapeDtypeStruct((nb, piece, hd), bf),
                jax.ShapeDtypeStruct((NS, piece, 512), bf),
            ],
            name="finish",
        )(tab, acc.reshape(NS, 8, G, 512), *[b for row in brecv for b in row])

        def place(mine, send):
            got = lax.ppermute(send, 'cp', swap)
            return lax.dynamic_update_slice_in_dim(mine, got, other, 0)

        attn_out = place(o_own, o_send).reshape(query.shape)
        grad_query = place(dq_own, dq_send).reshape(query.shape)
        dkv_got = lax.ppermute(dkv_send, 'cp', swap)
        grad_keys = lax.dynamic_update_slice_in_dim(dk_own, dkv_got[:, :, :hd], other, 0)
        grad_values = lax.dynamic_update_slice_in_dim(dv_own, dkv_got[:, :, hd:], other, 0)
        return attn_out, grad_query, grad_keys.reshape(keys.shape), grad_values.reshape(values.shape)

    return jax.shard_map(per_device, mesh=mesh, in_specs=(seq_spec, seq_spec, seq_spec, seq_spec, id_spec),
                         out_specs=(seq_spec, seq_spec, seq_spec, seq_spec), check_vma=False)
```

```python
import functools

import jax
import jax.numpy as jnp
from jax import lax
from jax.experimental import pallas as pl
from jax.experimental.pallas import tpu as pltpu
from jax.sharding import PartitionSpec as P


NEG_BIG = -1e30
LOG2E = 1.4426950408889634
G = 32
NS = 16
NCH = 4

FAST = (
    ((24, 34, 34, 32), (20, 24, 22, 20), (12, 14, 12, 12)),
    ((20, 32, 34, 38), (12, 22, 24, 24), (6, 10, 12, 18)),
)
SLOW_SEQS = 4
SLOW = (((8 * SLOW_SEQS,),) * 3,) * 2

CNT, OFF, DM, ST, SG, CE, FIT = 0, 336, 672, 704, 712, 840, 844
NTAB = 848


def at(base, cc, d, s):
    return base + (cc * 3 + d) * NS + s


def sg(cc, d, v):
    return SG + (cc * 3 + d) * 6 + v


def bounds(caps):
    out = [0]
    for cap in caps:
        out.append(out[-1] + cap)
    return out


def gather_kernel(doc, out, ks, send_sem, recv_sem):
    me = lax.axis_index('cp')
    n = out.shape[0]
    out[me] = doc[...]
    copies = []
    for k in range(1, n):
        copy = pltpu.make_async_remote_copy(
            src_ref=doc, dst_ref=out.at[me], send_sem=send_sem.at[k], recv_sem=recv_sem.at[k],
            device_id={'cp': lax.rem(me + k, n)}, device_id_type=pl.DeviceIdType.MESH)
        copy.start()
        copies.append(copy)
    for copy in copies:
        copy.wait()
    lane = lax.broadcasted_iota(jnp.int32, ks.shape, 1)
    total = jnp.zeros(ks.shape, jnp.int32)
    for p in range(n):
        first = out[p][:, :1]
        below = jnp.zeros(ks.shape, jnp.int32)
        for j in range(n):
            below = below + (out[j] < first).astype(jnp.int32)
        total = jnp.where(lane == p, jnp.sum(below, axis=1, keepdims=True), total)
    ks[...] = total


def table_kernel(plan, ks, me, tab):
    f_cap, b_cap = plan
    n_t = len(f_cap[0])
    f_lo = [bounds(cap) for cap in f_cap]
    c, e, lo, hi = me[0], me[1], me[2], me[3]
    zero = jnp.int32(0)
    tab[CE] = c
    tab[CE + 1] = e
    tab[ST] = lo
    for cc in range(7):
        for d in range(3):
            if not 1 <= cc <= 3 or d >= cc:
                for s in range(NS):
                    tab[at(CNT, cc, d, s)] = zero
                    tab[at(OFF, cc, d, s)] = zero
                for v in range(n_t + 1):
                    tab[sg(cc, d, v)] = zero
    for s in range(NS):
        for h in range(2):
            need = jnp.maximum(256 * c - ks[e * NS + s, 2 * c + h], 0)
            tab[DM + s * 2 + h] = (need + 255) >> 8

    fit = jnp.bool_(True)
    for col in range(2):
        row0 = jnp.where(e == 0, col, 1 - col) * NS
        for cc in range(NCH):
            off = [zero] * 3
            ready = [zero] * n_t
            avail = [[zero] * 3 for _ in range(n_t)]
            for s in range(NS):
                back = 256 * cc - ks[row0 + s, 2 * cc]
                live = (lo <= s) & (s < hi)
                for d in range(min(cc, 3)):
                    x = jnp.where(live, jnp.clip(back - 256 * d, 0, 256), 0)
                    n = (x + G - 1) >> 5
                    if col == 0:
                        tab[at(CNT, cc, d, s)] = n
                        tab[at(OFF, cc, d, s)] = off[d]
                    off[d] = off[d] + n
                for t in range(n_t):
                    ok = s < hi
                    for d in range(min(cc, 3)):
                        ok = ok & (off[d] <= f_lo[d][t + 1])
                    ready[t] = ready[t] + jnp.where(ok, 1, 0)
                    for d in range(min(cc, 3)):
                        avail[t][d] = jnp.where(ok, off[d], avail[t][d])
            fit = fit & (ready[n_t - 1] == hi)
            if col == 0:
                for t in range(n_t):
                    @pl.when(cc == c)
                    def _():
                        tab[ST + t + 1] = ready[t]
            for d in range(min(cc, 3)):
                sent = zero
                if col == 0:
                    tab[sg(cc, d, 0)] = sent
                for v in range(n_t):
                    sent = jnp.minimum(sent + b_cap[d][v], avail[v][d])
                    if col == 0:
                        tab[sg(cc, d, v + 1)] = sent
                fit = fit & (sent == off[d])
    tab[FIT] = jnp.where(fit, 1, 0)


def run_copies(lo_of, n_chunks, off, n, issue):
    for v in range(n_chunks):
        lo, hi = lo_of(v), lo_of(v + 1)
        a = jnp.maximum(off, lo)
        cnt = jnp.minimum(off + n, hi) - a

        @pl.when(cnt > 0)
        def _():
            for size in (8, 4, 2, 1):
                @pl.when((cnt & size) != 0)
                def _():
                    skip = cnt & (16 - 2 * size)
                    issue(v, a - lo + skip, a - off + skip, size)


def run_waits(n, wait):
    for size in (8, 4, 2, 1):
        @pl.when((n & size) != 0)
        def _():
            wait(size)


def pack_kernel(n_t, f_lo, tab, k_all, v_all, mate, kvcol, *rest):
    chunks = [rest[d * n_t:(d + 1) * n_t] for d in range(3)]
    inb, stage, isem, sem, csem = rest[3 * n_t:]
    lo = tab[ST]
    n = tab[ST + n_t] if n_t == 1 else NS
    n = n - lo
    c, e = tab[CE], tab[CE + 1]

    def inputs(s, sl):
        return [
            pltpu.make_async_copy(k_all.at[e * NS + s], inb.at[sl, 0], isem.at[sl]),
            pltpu.make_async_copy(v_all.at[e * NS + s], inb.at[sl, 1], isem.at[sl]),
            pltpu.make_async_copy(mate.at[s], stage.at[sl, pl.ds(4 - 4 * e, 4)], isem.at[sl]),
        ]

    def out_copy(s, sl):
        return pltpu.make_async_copy(stage.at[sl], kvcol.at[s], csem.at[sl])

    def drain(s, sl):
        out_copy(s, sl).wait()
        for d in range(3):
            run_waits(tab[at(CNT, c + d + 1, d, s)],
                      lambda size: pltpu.make_async_copy(stage.at[sl, pl.ds(0, size)], kvcol.at[s, pl.ds(0, size)], sem.at[sl]).wait())

    @pl.when(n > 0)
    def _():
        for copy in inputs(lo, 0):
            copy.start()

    def step(i, _):
        s = lo + i
        sl = lax.rem(i, 3)
        nx = lax.rem(i + 1, 3)

        @pl.when(i >= 2)
        def _():
            drain(s - 2, nx)

        @pl.when(i + 1 < n)
        def _():
            for copy in inputs(s + 1, nx):
                copy.start()

        for copy in inputs(s, sl):
            copy.wait()
        stage[sl, pl.ds(4 * e, 4)] = jnp.concatenate([inb[sl, 0], inb[sl, 1]], axis=1).reshape(4, G, 512)
        out_copy(s, sl).start()
        for d in range(3):
            cnt = tab[at(CNT, c + d + 1, d, s)]
            off = tab[at(OFF, c + d + 1, d, s)]
            run_copies(lambda v: f_lo[d][v], n_t, off, cnt,
                       lambda v, slot, k, size: pltpu.make_async_copy(
                           stage.at[sl, pl.ds(8 - cnt + k, size)], chunks[d][v].at[pl.ds(slot, size)], sem.at[sl]).start())
        return 0

    lax.fori_loop(0, n, step, 0)

    @pl.when(n >= 2)
    def _():
        drain(lo + n - 2, lax.rem(n + 1, 3))

    @pl.when(n >= 1)
    def _():
        drain(lo + n - 1, lax.rem(n + 2, 3))


def dot_nt(a, b):
    return lax.dot_general(a, b, (((1,), (1,)), ((), ())), preferred_element_type=jnp.float32)


def dot_nn(a, b):
    return lax.dot_general(a, b, (((1,), (0,)), ((), ())), preferred_element_type=jnp.float32)


def dot_tn(a, b):
    return lax.dot_general(a, b, (((0,), (0,)), ((), ())), preferred_element_type=jnp.float32)


def compute_kernel(t, n_t, f_lo, n_alias, scale, tab, docs, q_all, q_mate, g_all, g_mate, kvcol, *rest):
    fbuf = [rest[d * (t + 1):(d + 1) * (t + 1)] for d in range(3)]
    rest = rest[3 * (t + 1) + n_alias:]
    o_all, o_send, dq_all, dq_send, acc = rest[:5]
    rest = rest[5:]
    live = n_t - t
    bbuf = [rest[d * live:(d + 1) * live] for d in range(3)]
    qg, outb, kvs, dkv, e_scr, p_scr, m_scr, l_scr, f_scr, docr, o_acc, dq_acc, isem, osem = rest[3 * live:]

    base = tab[ST + t]
    n = tab[ST + t + 1] - base
    c = tab[CE]
    e = tab[CE + 1]

    def inputs(ss, sl):
        own = e * NS + ss
        return [
            pltpu.make_async_copy(src, dst, isem.at[sl])
            for src, dst in (
                (kvcol.at[ss], kvs.at[sl, 0]),
                (q_all.at[own], qg.at[sl, 0]), (q_mate.at[ss], qg.at[sl, 1]),
                (g_all.at[own], qg.at[sl, 2]), (g_mate.at[ss], qg.at[sl, 3]),
            )
        ]

    def outputs(ss, sl):
        own = e * NS + ss
        return [
            pltpu.make_async_copy(src, dst, osem.at[sl])
            for src, dst in (
                (outb.at[sl, 0], o_all.at[own]), (outb.at[sl, 1], o_send.at[ss]),
                (outb.at[sl, 2], dq_all.at[own]), (outb.at[sl, 3], dq_send.at[ss]),
                (dkv.at[sl, 0], acc.at[ss]),
            )
        ]

    def fetch(ss, sl):
        for copy in inputs(ss, sl):
            copy.start()
        for d in range(3):
            cnt = tab[at(CNT, c, d, ss)]
            off = tab[at(OFF, c, d, ss)]
            run_copies(lambda v: f_lo[d][v], t + 1, off, cnt,
                       lambda v, slot, k, size: pltpu.make_async_copy(
                           fbuf[d][v].at[pl.ds(slot, size)], kvs.at[sl, d + 1, pl.ds(8 - cnt + k, size)], isem.at[sl]).start())

    def fetch_wait(ss, sl):
        for copy in inputs(ss, sl):
            copy.wait()
        for d in range(3):
            run_waits(tab[at(CNT, c, d, ss)],
                      lambda size: pltpu.make_async_copy(
                          kvcol.at[ss, pl.ds(0, size)], kvs.at[sl, d + 1, pl.ds(0, size)], isem.at[sl]).wait())

    def put(ss, sl):
        for copy in outputs(ss, sl):
            copy.start()
        for d in range(3):
            cnt = tab[at(CNT, c, d, ss)]
            off = tab[at(OFF, c, d, ss)]
            run_copies(lambda v: tab[sg(c, d, t + v)], live, off, cnt,
                       lambda v, slot, k, size: pltpu.make_async_copy(
                           dkv.at[sl, d + 1, pl.ds(8 - cnt + k, size)], bbuf[d][v].at[pl.ds(slot, size)], osem.at[sl]).start())

    def put_wait(ss, sl):
        for copy in outputs(ss, sl):
            copy.wait()
        for d in range(3):
            run_waits(tab[at(CNT, c, d, ss)],
                      lambda size: pltpu.make_async_copy(
                          dkv.at[sl, d + 1, pl.ds(0, size)], acc.at[ss, pl.ds(0, size)], osem.at[sl]).wait())

    row_tok = lax.broadcasted_iota(jnp.int32, (1024, 128), 0) >> 3
    lane = lax.broadcasted_iota(jnp.int32, (1024, 128), 1)
    cs = scale * LOG2E

    def keys_of(slot, d):
        return kvs[slot, d, :, :, :256].reshape(256, 256)

    def values_of(slot, d):
        return kvs[slot, d, :, :, 256:].reshape(256, 256)

    def attend(role, s, slot):
        q_ref, g_ref = qg.at[slot, role], qg.at[slot, 2 + role]
        h = e if role == 0 else 1 - e
        dm = tab[DM + s * 2 + h]
        row = e * NS + s
        dq_row = docs[2 * c + h, pl.ds(row, 1), :]
        d_t = jnp.transpose(jnp.broadcast_to(dq_row, (128, 128)))
        docr[...] = jnp.broadcast_to(d_t[:, None, :], (128, 8, 128)).reshape(1024, 128)

        def scores(d, causal):
            sc = dot_nt(q_ref[...], keys_of(slot, d)) * cs
            xs = []
            for j in range(2):
                dk = docs[2 * (c - d) + j, pl.ds(row, 1), :]
                vis = docr[...] == dk
                if causal:
                    vis = vis & (lane + 128 * j <= row_tok + 128 * h)
                xs.append(jnp.where(vis, sc[:, 128 * j:128 * (j + 1)], NEG_BIG))
            top = jnp.max(jnp.maximum(xs[0], xs[1]), axis=1, keepdims=True)
            es = [jnp.exp2(x - top) for x in xs]
            e_scr[d, :, :128] = es[0]
            e_scr[d, :, 128:] = es[1]
            m_scr[d] = jnp.broadcast_to(top, (1024, 128))
            l_scr[d] = es[0] + es[1]

        scores(0, True)

        def more_scores(d, _):
            scores(d, False)
            return 0

        lax.fori_loop(1, dm + 1, more_scores, 0)

        @pl.when(dm == 0)
        def _():
            f_scr[0] = jnp.broadcast_to(1.0 / jnp.sum(l_scr[0], axis=1, keepdims=True), (1024, 128))

        @pl.when(dm > 0)
        def _():
            def top_of(d, m):
                o_acc[:, :128] = jnp.maximum(o_acc[:, :128], m_scr[d])
                return m

            o_acc[:, :128] = m_scr[0]
            lax.fori_loop(1, dm + 1, top_of, 0)
            o_acc[:, 128:] = jnp.zeros((1024, 128), jnp.float32)

            def sum_of(d, x):
                f = jnp.exp2(m_scr[d] - o_acc[:, :128])
                f_scr[d] = f
                o_acc[:, 128:] = o_acc[:, 128:] + l_scr[d] * f
                return x

            lax.fori_loop(0, dm + 1, sum_of, 0)
            o_acc[:, 128:] = jnp.broadcast_to(1.0 / jnp.sum(o_acc[:, 128:], axis=1, keepdims=True), (1024, 128))

            def scale_of(d, x):
                f_scr[d] = f_scr[d] * o_acc[:, 128:]
                return x

            lax.fori_loop(0, dm + 1, scale_of, 0)

        def weighted(d):
            for j in range(2):
                p = e_scr[d, :, 128 * j:128 * (j + 1)] * f_scr[d]
                p_scr[d, :, 128 * j:128 * (j + 1)] = p.astype(jnp.bfloat16)
            return dot_nn(p_scr[d], values_of(slot, d))

        o_acc[...] = weighted(0)

        def more_weighted(d, _):
            o_acc[...] = o_acc[...] + weighted(d)
            return 0

        lax.fori_loop(1, dm + 1, more_weighted, 0)
        o_low = o_acc[...].astype(jnp.bfloat16)
        outb[slot, role] = o_low
        delta = jnp.sum(g_ref[...].astype(jnp.float32) * o_low.astype(jnp.float32), axis=1, keepdims=True)
        m_scr[0] = jnp.broadcast_to(delta, (1024, 128))

        def grads(d):
            dp = dot_nt(g_ref[...], values_of(slot, d))
            ds = []
            for j in range(2):
                p = e_scr[d, :, 128 * j:128 * (j + 1)] * f_scr[d]
                ds.append((p * (dp[:, 128 * j:128 * (j + 1)] - m_scr[0])).astype(jnp.bfloat16))
            ds = jnp.concatenate(ds, axis=1)
            dk = dot_tn(ds, q_ref[...]).reshape(8, G, 256)
            dv = dot_tn(p_scr[d], g_ref[...]).reshape(8, G, 256)
            return dot_nn(ds, keys_of(slot, d)), dk, dv

        dq0, dk0, dv0 = grads(0)
        dq_acc[...] = dq0
        if role == 0:
            dkv[slot, 0, :, :, :256] = dk0
            dkv[slot, 0, :, :, 256:] = dv0
        else:
            dkv[slot, 0, :, :, :256] = dkv[slot, 0, :, :, :256] + dk0
            dkv[slot, 0, :, :, 256:] = dkv[slot, 0, :, :, 256:] + dv0

        def more_grads(d, _):
            dq1, dk1, dv1 = grads(d)
            dq_acc[...] = dq_acc[...] + dq1
            dkv[slot, d, :, :, :256] = dkv[slot, d, :, :, :256] + dk1
            dkv[slot, d, :, :, 256:] = dkv[slot, d, :, :, 256:] + dv1
            return 0

        lax.fori_loop(1, dm + 1, more_grads, 0)
        outb[slot, 2 + role] = (dq_acc[...] * scale).astype(jnp.bfloat16)

    @pl.when(n > 0)
    def _():
        kvs[...] = jnp.zeros_like(kvs)
        fetch(base, 0)

    def step(i, _):
        slot = lax.rem(i, 2)
        s = base + i

        @pl.when(i + 1 < n)
        def _():
            fetch(s + 1, 1 - slot)

        @pl.when(i >= 2)
        def _():
            put_wait(s - 2, slot)

        fetch_wait(s, slot)
        any_dm = jnp.maximum(tab[DM + s * 2], tab[DM + s * 2 + 1])

        def clear(d, _):
            dkv[slot, d] = jnp.zeros((8, G, 512), jnp.float32)
            return 0

        lax.fori_loop(1, any_dm + 1, clear, 0)
        attend(0, s, slot)
        attend(1, s, slot)
        put(s, slot)
        return 0

    lax.fori_loop(0, n, step, 0)

    @pl.when(n >= 2)
    def _():
        put_wait(base + n - 2, lax.rem(n, 2))

    @pl.when(n >= 1)
    def _():
        put_wait(base + n - 1, lax.rem(n + 1, 2))


def finish_kernel(n_t, n_alias, scale, tab, acc, *rest):
    bufs = [rest[d * n_t:(d + 1) * n_t] for d in range(3)]
    dk_all, dv_all, dkv_send, own, got, kb, vb, sb, sem, osem = rest[3 * n_t + n_alias:]
    lo = tab[ST]
    n = tab[ST + n_t] if n_t == 1 else NS
    n = n - lo
    c, e = tab[CE], tab[CE + 1]

    def fetch(ss, sl):
        pltpu.make_async_copy(acc.at[ss], own.at[sl], sem.at[sl]).start()
        for d in range(3):
            cnt = tab[at(CNT, c + d + 1, d, ss)]
            off = tab[at(OFF, c + d + 1, d, ss)]
            run_copies(lambda v: tab[sg(c + d + 1, d, v)], n_t, off, cnt,
                       lambda v, slot, k, size: pltpu.make_async_copy(
                           bufs[d][v].at[pl.ds(slot, size)], got.at[sl, d, pl.ds(8 - cnt + k, size)], sem.at[sl]).start())

    def fetch_wait(ss, sl):
        pltpu.make_async_copy(acc.at[ss], own.at[sl], sem.at[sl]).wait()
        for d in range(3):
            run_waits(tab[at(CNT, c + d + 1, d, ss)],
                      lambda size: pltpu.make_async_copy(
                          acc.at[ss, pl.ds(0, size)], got.at[sl, d, pl.ds(0, size)], sem.at[sl]).wait())

    def outputs(ss, sl):
        row = e * NS + ss
        return [
            pltpu.make_async_copy(kb.at[sl], dk_all.at[row], osem.at[sl]),
            pltpu.make_async_copy(vb.at[sl], dv_all.at[row], osem.at[sl]),
            pltpu.make_async_copy(sb.at[sl], dkv_send.at[ss], osem.at[sl]),
        ]

    @pl.when(n > 0)
    def _():
        fetch(lo, 0)

    def step(i, _):
        s = lo + i
        sl = lax.rem(i, 2)

        @pl.when(i + 1 < n)
        def _():
            fetch(s + 1, 1 - sl)

        @pl.when(i >= 2)
        def _():
            for copy in outputs(s - 2, sl):
                copy.wait()

        fetch_wait(s, sl)
        for d in range(3):
            cnt = tab[at(CNT, c + d + 1, d, s)]

            def add(k, _):
                own[sl, k] = own[sl, k] + got[sl, d, k]
                return 0

            lax.fori_loop(8 - cnt, 8, add, 0)
        mine = own[sl, pl.ds(4 * e, 4)].reshape(128, 512)
        other = own[sl, pl.ds(4 - 4 * e, 4)].reshape(128, 512)
        kb[sl] = (mine[:, :256] * scale).astype(jnp.bfloat16)
        vb[sl] = mine[:, 256:].astype(jnp.bfloat16)
        sb[sl, :, :256] = (other[:, :256] * scale).astype(jnp.bfloat16)
        sb[sl, :, 256:] = other[:, 256:].astype(jnp.bfloat16)
        for copy in outputs(s, sl):
            copy.start()
        return 0

    lax.fori_loop(0, n, step, 0)

    @pl.when(n >= 2)
    def _():
        for copy in outputs(lo + n - 2, lax.rem(n, 2)):
            copy.wait()

    @pl.when(n >= 1)
    def _():
        for copy in outputs(lo + n - 1, lax.rem(n + 1, 2)):
            copy.wait()


ANY = pl.BlockSpec(memory_space=pl.ANY)
SMEM = pl.BlockSpec(memory_space=pltpu.SMEM)
VMEM = pl.BlockSpec(memory_space=pltpu.VMEM)
BIG = pltpu.CompilerParams(vmem_limit_bytes=58 * 1024 * 1024)


def solution(mesh):
    n_dev = mesh.shape['cp']
    seq_spec = P('dp', 'cp', None, None)
    id_spec = P('dp', 'cp')
    swap = [(k, k ^ 1) for k in range(n_dev)]
    bf, f32 = jnp.bfloat16, jnp.float32
    shape = jax.ShapeDtypeStruct

    def per_device(query, keys, values, grad_out, doc_id):
        nb, piece, heads, hd = query.shape
        rows = piece * heads
        scale = hd ** -0.5
        rank = lax.axis_index('cp')
        c = rank >> 1
        e = rank & 1
        other = NS * (1 - e)
        q3 = query.reshape(nb, rows, hd)
        g3 = grad_out.reshape(nb, rows, hd)
        k3 = keys.reshape(nb, piece, hd)
        v3 = values.reshape(nb, piece, hd)

        def half(x):
            return lax.dynamic_slice_in_dim(x, other, NS, 0)

        kv_mate = lax.ppermute(jnp.concatenate([half(k3), half(v3)], axis=-1), 'cp', swap)
        docs, ks = pl.pallas_call(
            gather_kernel,
            out_shape=[shape((n_dev, nb, piece), jnp.int32), shape((nb, 128), jnp.int32)],
            in_specs=[VMEM],
            out_specs=[VMEM, VMEM],
            scratch_shapes=[pltpu.SemaphoreType.DMA((n_dev,)), pltpu.SemaphoreType.DMA((n_dev,))],
            compiler_params=pltpu.CompilerParams(has_side_effects=True),
            name="docs",
        )(doc_id)

        def tables(plan, lo, hi):
            me = jnp.stack([c, e, lo, hi]).astype(jnp.int32)
            return pl.pallas_call(
                functools.partial(table_kernel, plan),
                out_shape=shape((NTAB,), jnp.int32),
                in_specs=[SMEM, SMEM],
                out_specs=SMEM,
                name="tables",
            )(ks, me)

        def pack(plan, tab):
            f_cap = plan[0]
            n_t = len(f_cap[0])
            return pl.pallas_call(
                functools.partial(pack_kernel, n_t, [bounds(cap) for cap in f_cap]),
                in_specs=[SMEM] + [ANY] * 3,
                out_specs=[ANY] * (1 + 3 * n_t),
                out_shape=[shape((NS, 8, G, 512), bf)] + [shape((f_cap[d][t], G, 512), bf) for d in range(3) for t in range(n_t)],
                scratch_shapes=[
                    pltpu.VMEM((3, 2, piece, hd), bf), pltpu.VMEM((3, 8, G, 512), bf),
                    pltpu.SemaphoreType.DMA((3,)), pltpu.SemaphoreType.DMA((3,)), pltpu.SemaphoreType.DMA((3,)),
                ],
                name="pack",
            )(tab, k3, v3, kv_mate.reshape(NS, 4, G, 512))

        def forward_hop(x, d):
            hop = 2 * (d + 1)
            return lax.ppermute(x, 'cp', [(k, k + hop) for k in range(n_dev - hop)])

        def backward_hop(x, d):
            hop = 2 * (d + 1)
            return lax.ppermute(x, 'cp', [(k + hop, k) for k in range(n_dev - hop)])

        def attend(plan, t, tab, q_mate, g_mate, kvcol, frecv, state):
            f_cap, b_cap = plan
            n_t = len(f_cap[0])
            live = n_t - t
            n_alias = 0 if state is None else len(state)
            n_in = 7 + 3 * (t + 1)
            return pl.pallas_call(
                functools.partial(compute_kernel, t, n_t, [bounds(cap) for cap in f_cap], n_alias, scale),
                in_specs=[SMEM, VMEM] + [ANY] * (5 + 3 * (t + 1) + n_alias),
                out_specs=[ANY] * (5 + 3 * live),
                scratch_shapes=[
                    pltpu.VMEM((2, 4, rows, hd), bf), pltpu.VMEM((2, 4, rows, hd), bf),
                    pltpu.VMEM((2, 4, 8, G, 512), bf), pltpu.VMEM((2, 4, 8, G, 512), f32),
                    pltpu.VMEM((4, rows, 256), f32), pltpu.VMEM((4, rows, 256), bf),
                    pltpu.VMEM((4, rows, 128), f32), pltpu.VMEM((4, rows, 128), f32), pltpu.VMEM((4, rows, 128), f32),
                    pltpu.VMEM((rows, 128), jnp.int32),
                    pltpu.VMEM((rows, hd), f32), pltpu.VMEM((rows, hd), f32),
                    pltpu.SemaphoreType.DMA((2,)), pltpu.SemaphoreType.DMA((2,)),
                ],
                out_shape=[
                    shape((nb, rows, hd), bf), shape((NS, rows, hd), bf),
                    shape((nb, rows, hd), bf), shape((NS, rows, hd), bf),
                    shape((NS, 8, G, 512), f32),
                ] + [shape((b_cap[d][v], G, 512), f32) for d in range(3) for v in range(t, n_t)],
                input_output_aliases={n_in + k: k for k in range(n_alias)},
                compiler_params=BIG,
                cost_estimate=pl.CostEstimate(flops=60_000_000_000 // n_t, bytes_accessed=100_000_000 // n_t, transcendentals=0),
            )(tab, docs, q3, q_mate, g3, g_mate, kvcol, *[frecv[d][u] for d in range(3) for u in range(t + 1)],
              *([] if state is None else state))

        def finish(plan, tab, acc, brecv, state):
            n_t = len(plan[0][0])
            n_alias = 0 if state is None else 3
            return pl.pallas_call(
                functools.partial(finish_kernel, n_t, n_alias, scale),
                in_specs=[SMEM] + [ANY] * (1 + 3 * n_t + n_alias),
                out_specs=[ANY] * 3,
                out_shape=[shape((nb, piece, hd), bf), shape((nb, piece, hd), bf), shape((NS, piece, 512), bf)],
                scratch_shapes=[
                    pltpu.VMEM((2, 8, G, 512), f32), pltpu.VMEM((2, 3, 8, G, 512), f32),
                    pltpu.VMEM((2, piece, hd), bf), pltpu.VMEM((2, piece, hd), bf), pltpu.VMEM((2, piece, 512), bf),
                    pltpu.SemaphoreType.DMA((2,)), pltpu.SemaphoreType.DMA((2,)),
                ],
                input_output_aliases={2 + 3 * n_t + k: k for k in range(n_alias)},
                name="finish",
            )(tab, acc, *[b for row in brecv for b in row], *([] if state is None else state))

        def place(mine, send):
            got = lax.ppermute(send, 'cp', swap)
            return lax.dynamic_update_slice_in_dim(mine, got, other, 0)

        def place_kv(dk_all, dv_all, dkv_send):
            got = lax.ppermute(dkv_send, 'cp', swap)
            return (lax.dynamic_update_slice_in_dim(dk_all, got[:, :, :hd], other, 0),
                    lax.dynamic_update_slice_in_dim(dv_all, got[:, :, hd:], other, 0))

        def mates():
            q_mate = lax.ppermute(half(q3), 'cp', swap)
            g_mate = lax.ppermute(half(g3), 'cp', swap)
            return q_mate, g_mate

        tab = tables(FAST, jnp.int32(0), jnp.int32(NS))

        def fast():
            n_t = len(FAST[0][0])
            packed = pack(FAST, tab)
            kvcol, fsend = packed[0], packed[1:]
            frecv = [[None] * n_t for _ in range(3)]
            for t in range(n_t):
                for d in range(3):
                    frecv[d][t] = forward_hop(fsend[d * n_t + t], d)
            q_mate, g_mate = mates()
            state = None
            brecv = [[None] * n_t for _ in range(3)]
            for t in range(n_t):
                live = n_t - t
                outs = attend(FAST, t, tab, q_mate, g_mate, kvcol, frecv, state)
                state = list(outs[:5]) + [outs[5 + d * live + k] for d in range(3) for k in range(1, live)]
                for d in range(3):
                    brecv[d][t] = backward_hop(outs[5 + d * live], d)
            o_all, o_send, dq_all, dq_send, acc = state
            attn_out = place(o_all, o_send)
            grad_query = place(dq_all, dq_send)
            return (attn_out, grad_query) + place_kv(*finish(FAST, tab, acc, brecv, None))

        def slow():
            q_mate, g_mate = mates()

            def blank():
                outs = [shape((nb, rows, hd), bf), shape((NS, rows, hd), bf), shape((nb, rows, hd), bf), shape((NS, rows, hd), bf),
                        shape((NS, 8, G, 512), f32), shape((nb, piece, hd), bf), shape((nb, piece, hd), bf), shape((NS, piece, 512), bf)]
                return [jnp.zeros(o.shape, o.dtype) for o in outs]

            def one_round(i, carry):
                state, grads = list(carry[:5]), list(carry[5:])
                tab = tables(SLOW, i * SLOW_SEQS, (i + 1) * SLOW_SEQS)
                packed = pack(SLOW, tab)
                frecv = [[forward_hop(packed[1 + d], d)] for d in range(3)]
                blank_b = [jnp.zeros((SLOW[1][0][0], G, 512), f32) for _ in range(3)]
                outs = attend(SLOW, 0, tab, q_mate, g_mate, packed[0], frecv, state + blank_b)
                brecv = [[backward_hop(outs[5 + d], d)] for d in range(3)]
                return tuple(outs[:5]) + tuple(finish(SLOW, tab, outs[4], brecv, grads))

            out = lax.fori_loop(0, NS // SLOW_SEQS, one_round, tuple(blank()))
            return (place(out[0], out[1]), place(out[2], out[3])) + place_kv(*out[5:])

        attn_out, grad_query, grad_keys, grad_values = lax.cond(tab[FIT] > 0, fast, slow)
        return (attn_out.reshape(query.shape), grad_query.reshape(query.shape),
                grad_keys.reshape(keys.shape), grad_values.reshape(values.shape))

    return jax.shard_map(per_device, mesh=mesh, in_specs=(seq_spec, seq_spec, seq_spec, seq_spec, id_spec),
                         out_specs=(seq_spec, seq_spec, seq_spec, seq_spec), check_vma=False)
```

```python
import functools

import jax
import jax.numpy as jnp
from jax import lax
from jax.experimental import pallas as pl
from jax.experimental.pallas import tpu as pltpu
from jax.sharding import PartitionSpec as P


NEG_BIG = -1e30
LOG2E = 1.4426950408889634
G = 32
NS = 16
NCH = 4

FAST = (
    ((28, 34, 34, 30), (22, 24, 22, 18), (14, 14, 12, 10)),
    ((20, 28, 30, 46), (12, 18, 22, 34), (6, 8, 10, 24)),
    (4, 8, 12, 16),
)
RELAY_F = (1, 2)
RELAY_B = (1, 2)
QA = 4
SLOW_SEQS = 4
SLOW = (((8 * SLOW_SEQS,),) * 3,) * 2 + ((NS,),)

CNT, OFF, DM, ST, SG, CE, FIT = 0, 336, 672, 704, 712, 840, 844
NTAB = 848


def at(base, cc, d, s):
    return base + (cc * 3 + d) * NS + s


def sg(cc, d, v):
    return SG + (cc * 3 + d) * 6 + v


def bounds(caps):
    out = [0]
    for cap in caps:
        out.append(out[-1] + cap)
    return out


def gather_kernel(doc, out, ks, send_sem, recv_sem):
    me = lax.axis_index('cp')
    n = out.shape[0]
    out[me] = doc[...]
    copies = []
    for k in range(1, n):
        copy = pltpu.make_async_remote_copy(
            src_ref=doc, dst_ref=out.at[me], send_sem=send_sem.at[k], recv_sem=recv_sem.at[k],
            device_id={'cp': lax.rem(me + k, n)}, device_id_type=pl.DeviceIdType.MESH)
        copy.start()
        copies.append(copy)
    for copy in copies:
        copy.wait()
    lane = lax.broadcasted_iota(jnp.int32, ks.shape, 1)
    total = jnp.zeros(ks.shape, jnp.int32)
    for p in range(n):
        first = out[p][:, :1]
        below = jnp.zeros(ks.shape, jnp.int32)
        for j in range(n):
            below = below + (out[j] < first).astype(jnp.int32)
        total = jnp.where(lane == p, jnp.sum(below, axis=1, keepdims=True), total)
    ks[...] = total


def table_kernel(plan, ks, me, tab):
    f_cap, b_cap, quota = plan
    n_t = len(f_cap[0])
    f_lo = [bounds(cap) for cap in f_cap]
    c, e, lo, hi = me[0], me[1], me[2], me[3]
    zero = jnp.int32(0)
    tab[CE] = c
    tab[CE + 1] = e
    tab[ST] = lo
    for cc in range(7):
        for d in range(3):
            if not 1 <= cc <= 3 or d >= cc:
                for s in range(NS):
                    tab[at(CNT, cc, d, s)] = zero
                    tab[at(OFF, cc, d, s)] = zero
                for v in range(n_t + 1):
                    tab[sg(cc, d, v)] = zero
    for s in range(NS):
        for h in range(2):
            need = jnp.maximum(256 * c - ks[e * NS + s, 2 * c + h], 0)
            tab[DM + s * 2 + h] = (need + 255) >> 8

    fit = jnp.bool_(True)
    for col in range(2):
        row0 = jnp.where(e == 0, col, 1 - col) * NS
        for cc in range(NCH):
            off = [zero] * 3
            ready = [zero] * n_t
            avail = [[zero] * 3 for _ in range(n_t)]
            for s in range(NS):
                back = 256 * cc - ks[row0 + s, 2 * cc]
                live = (lo <= s) & (s < hi)
                for d in range(min(cc, 3)):
                    x = jnp.where(live, jnp.clip(back - 256 * d, 0, 256), 0)
                    n = (x + G - 1) >> 5
                    if col == 0:
                        tab[at(CNT, cc, d, s)] = n
                        tab[at(OFF, cc, d, s)] = off[d]
                    off[d] = off[d] + n
                for t in range(n_t):
                    if s >= quota[t]:
                        continue
                    ok = s < hi
                    for d in range(min(cc, 3)):
                        ok = ok & (off[d] <= f_lo[d][t + 1])
                    ready[t] = ready[t] + jnp.where(ok, 1, 0)
                    for d in range(min(cc, 3)):
                        avail[t][d] = jnp.where(ok, off[d], avail[t][d])
            fit = fit & (ready[n_t - 1] == hi)
            if col == 0:
                for t in range(n_t):
                    @pl.when(cc == c)
                    def _():
                        tab[ST + t + 1] = ready[t]
            for d in range(min(cc, 3)):
                sent = zero
                if col == 0:
                    tab[sg(cc, d, 0)] = sent
                for v in range(n_t):
                    sent = jnp.minimum(sent + b_cap[d][v], avail[v][d])
                    if col == 0:
                        tab[sg(cc, d, v + 1)] = sent
                fit = fit & (sent == off[d])
    tab[FIT] = jnp.where(fit, 1, 0)


def run_copies(lo_of, n_chunks, off, n, issue):
    for v in range(n_chunks):
        lo, hi = lo_of(v), lo_of(v + 1)
        a = jnp.maximum(off, lo)
        cnt = jnp.minimum(off + n, hi) - a

        @pl.when(cnt > 0)
        def _():
            for size in (8, 4, 2, 1):
                @pl.when((cnt & size) != 0)
                def _():
                    skip = cnt & (16 - 2 * size)
                    issue(v, a - lo + skip, a - off + skip, size)


def run_waits(n, wait):
    for size in (8, 4, 2, 1):
        @pl.when((n & size) != 0)
        def _():
            wait(size)


def pack_kernel(n_t, n, f_lo, tab, k_all, v_all, mate, kvcol, *rest):
    chunks = [rest[d * n_t:(d + 1) * n_t] for d in range(3)]
    inb, stage, isem, sem, csem = rest[3 * n_t:]
    lo = tab[ST]
    c, e = tab[CE], tab[CE + 1]
    part = n // 4
    loads = []
    for i in range(4):
        rows = pl.ds(i * part, part)
        loads.append([
            pltpu.make_async_copy(k_all.at[pl.ds(e * NS + lo + i * part, part)], inb.at[0, rows], isem.at[i]),
            pltpu.make_async_copy(v_all.at[pl.ds(e * NS + lo + i * part, part)], inb.at[1, rows], isem.at[i]),
            pltpu.make_async_copy(mate.at[pl.ds(lo + i * part, part)], stage.at[rows, pl.ds(4 - 4 * e, 4)], isem.at[i]),
        ])
        for copy in loads[-1]:
            copy.start()
    for i in range(4):
        for copy in loads[i]:
            copy.wait()

        def step(j, _):
            s = lo + j
            stage[j, pl.ds(4 * e, 4), :, :256] = inb[0, j].reshape(4, G, 256)
            stage[j, pl.ds(4 * e, 4), :, 256:] = inb[1, j].reshape(4, G, 256)
            pltpu.make_async_copy(stage.at[j], kvcol.at[s], csem).start()
            for d in range(3):
                cnt = tab[at(CNT, c + d + 1, d, s)]
                off = tab[at(OFF, c + d + 1, d, s)]
                run_copies(lambda v: f_lo[d][v], n_t, off, cnt,
                           lambda v, slot, k, size: pltpu.make_async_copy(
                               stage.at[j, pl.ds(8 - cnt + k, size)], chunks[d][v].at[pl.ds(slot, size)], sem).start())
            return 0

        lax.fori_loop(i * part, (i + 1) * part, step, 0)

    def drain(j, _):
        pltpu.make_async_copy(stage.at[j], kvcol.at[lo + j], csem).wait()
        for d in range(3):
            run_waits(tab[at(CNT, c + d + 1, d, lo + j)],
                      lambda size: pltpu.make_async_copy(
                          stage.at[j, pl.ds(0, size)], kvcol.at[lo + j, pl.ds(0, size)], sem).wait())
        return 0

    lax.fori_loop(0, n, drain, 0)


def dot_nt(a, b):
    return lax.dot_general(a, b, (((1,), (1,)), ((), ())), preferred_element_type=jnp.float32)


def dot_nn(a, b):
    return lax.dot_general(a, b, (((1,), (0,)), ((), ())), preferred_element_type=jnp.float32)


def dot_tn(a, b):
    return lax.dot_general(a, b, (((0,), (0,)), ((), ())), preferred_element_type=jnp.float32)


def split(refs, counts):
    out = []
    for k in counts:
        out.append(refs[:k])
        refs = refs[k:]
    return out, refs


def compute_kernel(t, n_t, f_lo, n_mate, ways, n_alias, scale, tab, docs, q_all, g_all, kvcol, *rest):
    q_mates, rest = rest[:n_mate], rest[n_mate:]
    g_mates, rest = rest[:n_mate], rest[n_mate:]
    fbuf, rest = split(rest, ways)
    fbuf = [fbuf[d * (t + 1):(d + 1) * (t + 1)] for d in range(3)]
    rest = rest[n_alias:]
    o_all, o_send, dq_all, dq_send, acc = rest[:5]
    rest = rest[5:]
    live = n_t - t
    bbuf = [rest[d * live:(d + 1) * live] for d in range(3)]
    qg, outb, kvs, dkv, e_scr, p_scr, m_scr, l_scr, f_scr, docr, o_acc, dq_acc, isem, osem = rest[3 * live:]

    base = tab[ST + t]
    n = tab[ST + t + 1] - base
    c = tab[CE]
    e = tab[CE + 1]

    def inputs(ss, sl):
        own = e * NS + ss
        return [
            pltpu.make_async_copy(src, dst, isem.at[sl])
            for src, dst in (
                (kvcol.at[ss], kvs.at[sl, 0]), (q_all.at[own], qg.at[sl, 0]), (g_all.at[own], qg.at[sl, 2]),
            )
        ]

    def mate_inputs(refs, row, sl):
        return [
            pltpu.make_async_copy(refs[0].at[row], qg.at[sl, 1], isem.at[sl]),
            pltpu.make_async_copy(refs[1].at[row], qg.at[sl, 3], isem.at[sl]),
        ]

    def outputs(ss, sl):
        own = e * NS + ss
        return [
            pltpu.make_async_copy(src, dst, osem.at[sl])
            for src, dst in (
                (outb.at[sl, 0], o_all.at[own]), (outb.at[sl, 1], o_send.at[ss]),
                (outb.at[sl, 2], dq_all.at[own]), (outb.at[sl, 3], dq_send.at[ss]),
                (dkv.at[sl, 0], acc.at[ss]),
            )
        ]

    def fetch(ss, sl):
        for copy in inputs(ss, sl):
            copy.start()
        if n_mate == 1:
            for copy in mate_inputs((q_mates[0], g_mates[0]), ss, sl):
                copy.start()
        else:
            @pl.when(ss < QA)
            def _():
                for copy in mate_inputs((q_mates[0], g_mates[0]), ss, sl):
                    copy.start()

            @pl.when(ss >= QA)
            def _():
                for copy in mate_inputs((q_mates[1], g_mates[1]), ss - QA, sl):
                    copy.start()
        for d in range(3):
            cnt = tab[at(CNT, c, d, ss)]
            off = tab[at(OFF, c, d, ss)]

            def issue(v, slot, k, size):
                def go(ref):
                    pltpu.make_async_copy(ref.at[pl.ds(slot, size)], kvs.at[sl, d + 1, pl.ds(8 - cnt + k, size)], isem.at[sl]).start()

                if len(fbuf[d][v]) == 1:
                    go(fbuf[d][v][0])
                else:
                    pl.when(c != 2)(lambda: go(fbuf[d][v][0]))
                    pl.when(c == 2)(lambda: go(fbuf[d][v][1]))

            run_copies(lambda v: f_lo[d][v], t + 1, off, cnt, issue)

    def fetch_wait(ss, sl):
        for copy in inputs(ss, sl) + mate_inputs((q_mates[0], g_mates[0]), 0, sl):
            copy.wait()
        for d in range(3):
            run_waits(tab[at(CNT, c, d, ss)],
                      lambda size: pltpu.make_async_copy(
                          kvcol.at[ss, pl.ds(0, size)], kvs.at[sl, d + 1, pl.ds(0, size)], isem.at[sl]).wait())

    def put(ss, sl):
        for copy in outputs(ss, sl):
            copy.start()
        for d in range(3):
            cnt = tab[at(CNT, c, d, ss)]
            off = tab[at(OFF, c, d, ss)]
            run_copies(lambda v: tab[sg(c, d, t + v)], live, off, cnt,
                       lambda v, slot, k, size: pltpu.make_async_copy(
                           dkv.at[sl, d + 1, pl.ds(8 - cnt + k, size)], bbuf[d][v].at[pl.ds(slot, size)], osem.at[sl]).start())

    def put_wait(ss, sl):
        for copy in outputs(ss, sl):
            copy.wait()
        for d in range(3):
            run_waits(tab[at(CNT, c, d, ss)],
                      lambda size: pltpu.make_async_copy(
                          dkv.at[sl, d + 1, pl.ds(0, size)], acc.at[ss, pl.ds(0, size)], osem.at[sl]).wait())

    row_tok = lax.broadcasted_iota(jnp.int32, (1024, 128), 0) >> 3
    lane = lax.broadcasted_iota(jnp.int32, (1024, 128), 1)
    cs = scale * LOG2E

    def keys_of(slot, d):
        return kvs[slot, d, :, :, :256].reshape(256, 256)

    def values_of(slot, d):
        return kvs[slot, d, :, :, 256:].reshape(256, 256)

    def attend(role, s, slot):
        q_ref, g_ref = qg.at[slot, role], qg.at[slot, 2 + role]
        h = e if role == 0 else 1 - e
        dm = tab[DM + s * 2 + h]
        row = e * NS + s
        dq_row = docs[2 * c + h, pl.ds(row, 1), :]
        d_t = jnp.transpose(jnp.broadcast_to(dq_row, (128, 128)))
        docr[...] = jnp.broadcast_to(d_t[:, None, :], (128, 8, 128)).reshape(1024, 128)

        def scores(d, causal):
            sc = dot_nt(q_ref[...], keys_of(slot, d)) * cs
            xs = []
            for j in range(2):
                dk = docs[2 * (c - d) + j, pl.ds(row, 1), :]
                vis = docr[...] == dk
                if causal:
                    vis = vis & (lane + 128 * j <= row_tok + 128 * h)
                xs.append(jnp.where(vis, sc[:, 128 * j:128 * (j + 1)], NEG_BIG))
            top = jnp.maximum(xs[0], xs[1])
            es = [jnp.exp2(x - top) for x in xs]
            e_scr[d, :, :128] = es[0]
            e_scr[d, :, 128:] = es[1]
            m_scr[d] = top
            l_scr[d] = es[0] + es[1]

        scores(0, True)

        def more_scores(d, _):
            scores(d, False)
            return 0

        lax.fori_loop(1, dm + 1, more_scores, 0)

        @pl.when(dm == 0)
        def _():
            m = m_scr[0]
            f = jnp.exp2(m - jnp.max(m, axis=1, keepdims=True))
            f_scr[0] = f * (1.0 / jnp.sum(l_scr[0] * f, axis=1, keepdims=True))

        @pl.when(dm > 0)
        def _():
            o_acc[:, :128] = jnp.maximum(m_scr[0], m_scr[1])

            def top_of(d, x):
                o_acc[:, :128] = jnp.maximum(o_acc[:, :128], m_scr[d])
                return x

            lax.fori_loop(2, dm + 1, top_of, 0)
            top = jnp.broadcast_to(jnp.max(o_acc[:, :128], axis=1, keepdims=True), (1024, 128))
            o_acc[:, :128] = top
            f0 = jnp.exp2(m_scr[0] - top)
            f1 = jnp.exp2(m_scr[1] - top)
            f_scr[0] = f0
            f_scr[1] = f1
            o_acc[:, 128:] = l_scr[0] * f0 + l_scr[1] * f1

            def sum_of(d, x):
                f = jnp.exp2(m_scr[d] - o_acc[:, :128])
                f_scr[d] = f
                o_acc[:, 128:] = o_acc[:, 128:] + l_scr[d] * f
                return x

            lax.fori_loop(2, dm + 1, sum_of, 0)
            inv = jnp.broadcast_to(1.0 / jnp.sum(o_acc[:, 128:], axis=1, keepdims=True), (1024, 128))
            o_acc[:, 128:] = inv
            f_scr[0] = f_scr[0] * inv
            f_scr[1] = f_scr[1] * inv

            def scale_of(d, x):
                f_scr[d] = f_scr[d] * o_acc[:, 128:]
                return x

            lax.fori_loop(2, dm + 1, scale_of, 0)

        def weighted(d):
            for j in range(2):
                p = e_scr[d, :, 128 * j:128 * (j + 1)] * f_scr[d]
                p_scr[d, :, 128 * j:128 * (j + 1)] = p.astype(jnp.bfloat16)
            return dot_nn(p_scr[d], values_of(slot, d))

        o_acc[...] = weighted(0)

        def more_weighted(d, _):
            o_acc[...] = o_acc[...] + weighted(d)
            return 0

        lax.fori_loop(1, dm + 1, more_weighted, 0)
        o_low = o_acc[...].astype(jnp.bfloat16)
        outb[slot, role] = o_low
        delta = jnp.sum(g_ref[...].astype(jnp.float32) * o_low.astype(jnp.float32), axis=1, keepdims=True)
        m_scr[0] = jnp.broadcast_to(delta, (1024, 128))

        def grads(d):
            dp = dot_nt(g_ref[...], values_of(slot, d))
            ds = []
            for j in range(2):
                p = e_scr[d, :, 128 * j:128 * (j + 1)] * f_scr[d]
                ds.append((p * (dp[:, 128 * j:128 * (j + 1)] - m_scr[0])).astype(jnp.bfloat16))
            ds = jnp.concatenate(ds, axis=1)
            dk = dot_tn(ds, q_ref[...]).reshape(8, G, 256)
            dv = dot_tn(p_scr[d], g_ref[...]).reshape(8, G, 256)
            return dot_nn(ds, keys_of(slot, d)), dk, dv

        dq0, dk0, dv0 = grads(0)
        dq_acc[...] = dq0
        if role == 0:
            dkv[slot, 0, :, :, :256] = dk0
            dkv[slot, 0, :, :, 256:] = dv0
        else:
            dkv[slot, 0, :, :, :256] = dkv[slot, 0, :, :, :256] + dk0
            dkv[slot, 0, :, :, 256:] = dkv[slot, 0, :, :, 256:] + dv0

        def more_grads(d, _):
            dq1, dk1, dv1 = grads(d)
            dq_acc[...] = dq_acc[...] + dq1
            dkv[slot, d, :, :, :256] = dkv[slot, d, :, :, :256] + dk1
            dkv[slot, d, :, :, 256:] = dkv[slot, d, :, :, 256:] + dv1
            return 0

        lax.fori_loop(1, dm + 1, more_grads, 0)
        outb[slot, 2 + role] = (dq_acc[...] * scale).astype(jnp.bfloat16)

    @pl.when(n > 0)
    def _():
        kvs[...] = jnp.zeros_like(kvs)
        fetch(base, 0)

    def step(i, _):
        slot = lax.rem(i, 2)
        s = base + i

        @pl.when(i + 1 < n)
        def _():
            fetch(s + 1, 1 - slot)

        @pl.when(i >= 2)
        def _():
            put_wait(s - 2, slot)

        fetch_wait(s, slot)
        any_dm = jnp.maximum(tab[DM + s * 2], tab[DM + s * 2 + 1])

        def clear(d, _):
            dkv[slot, d] = jnp.zeros((8, G, 512), jnp.float32)
            return 0

        lax.fori_loop(1, any_dm + 1, clear, 0)
        attend(0, s, slot)
        attend(1, s, slot)
        put(s, slot)
        return 0

    lax.fori_loop(0, n, step, 0)

    @pl.when(n >= 2)
    def _():
        put_wait(base + n - 2, lax.rem(n, 2))

    @pl.when(n >= 1)
    def _():
        put_wait(base + n - 1, lax.rem(n + 1, 2))


def finish_kernel(n_t, ways, n_alias, scale, tab, acc, *rest):
    bufs, rest = split(rest, ways)
    bufs = [bufs[d * n_t:(d + 1) * n_t] for d in range(3)]
    dk_all, dv_all, dkv_send, own, got, kb, vb, sb, sem, osem = rest[n_alias:]
    lo = tab[ST]
    n = tab[ST + n_t] if n_t == 1 else NS
    n = n - lo
    c, e = tab[CE], tab[CE + 1]

    def fetch(ss, sl):
        pltpu.make_async_copy(acc.at[ss], own.at[sl], sem.at[sl]).start()
        for d in range(3):
            cnt = tab[at(CNT, c + d + 1, d, ss)]
            off = tab[at(OFF, c + d + 1, d, ss)]

            def issue(v, slot, k, size):
                def go(ref):
                    pltpu.make_async_copy(ref.at[pl.ds(slot, size)], got.at[sl, d, pl.ds(8 - cnt + k, size)], sem.at[sl]).start()

                if len(bufs[d][v]) == 1:
                    go(bufs[d][v][0])
                else:
                    pl.when(c != 1)(lambda: go(bufs[d][v][0]))
                    pl.when(c == 1)(lambda: go(bufs[d][v][1]))

            run_copies(lambda v: tab[sg(c + d + 1, d, v)], n_t, off, cnt, issue)

    def fetch_wait(ss, sl):
        pltpu.make_async_copy(acc.at[ss], own.at[sl], sem.at[sl]).wait()
        for d in range(3):
            run_waits(tab[at(CNT, c + d + 1, d, ss)],
                      lambda size: pltpu.make_async_copy(
                          acc.at[ss, pl.ds(0, size)], got.at[sl, d, pl.ds(0, size)], sem.at[sl]).wait())

    def outputs(ss, sl):
        row = e * NS + ss
        return [
            pltpu.make_async_copy(kb.at[sl], dk_all.at[row], osem.at[sl]),
            pltpu.make_async_copy(vb.at[sl], dv_all.at[row], osem.at[sl]),
            pltpu.make_async_copy(sb.at[sl], dkv_send.at[ss], osem.at[sl]),
        ]

    @pl.when(n > 0)
    def _():
        fetch(lo, 0)

    def step(i, _):
        s = lo + i
        sl = lax.rem(i, 2)

        @pl.when(i + 1 < n)
        def _():
            fetch(s + 1, 1 - sl)

        @pl.when(i >= 2)
        def _():
            for copy in outputs(s - 2, sl):
                copy.wait()

        fetch_wait(s, sl)
        for d in range(3):
            cnt = tab[at(CNT, c + d + 1, d, s)]

            def add(k, _):
                own[sl, k] = own[sl, k] + got[sl, d, k]
                return 0

            lax.fori_loop(8 - cnt, 8, add, 0)
        mine = own[sl, pl.ds(4 * e, 4)].reshape(128, 512)
        other = own[sl, pl.ds(4 - 4 * e, 4)].reshape(128, 512)
        kb[sl] = (mine[:, :256] * scale).astype(jnp.bfloat16)
        vb[sl] = mine[:, 256:].astype(jnp.bfloat16)
        sb[sl, :, :256] = (other[:, :256] * scale).astype(jnp.bfloat16)
        sb[sl, :, 256:] = other[:, 256:].astype(jnp.bfloat16)
        for copy in outputs(s, sl):
            copy.start()
        return 0

    lax.fori_loop(0, n, step, 0)

    @pl.when(n >= 2)
    def _():
        for copy in outputs(lo + n - 2, lax.rem(n, 2)):
            copy.wait()

    @pl.when(n >= 1)
    def _():
        for copy in outputs(lo + n - 1, lax.rem(n + 1, 2)):
            copy.wait()


ANY = pl.BlockSpec(memory_space=pl.ANY)
SMEM = pl.BlockSpec(memory_space=pltpu.SMEM)
VMEM = pl.BlockSpec(memory_space=pltpu.VMEM)
BIG = pltpu.CompilerParams(vmem_limit_bytes=58 * 1024 * 1024)


def solution(mesh):
    n_dev = mesh.shape['cp']
    seq_spec = P('dp', 'cp', None, None)
    id_spec = P('dp', 'cp')
    swap = [(k, k ^ 1) for k in range(n_dev)]
    bf, f32 = jnp.bfloat16, jnp.float32
    shape = jax.ShapeDtypeStruct

    def per_device(query, keys, values, grad_out, doc_id):
        nb, piece, heads, hd = query.shape
        rows = piece * heads
        scale = hd ** -0.5
        rank = lax.axis_index('cp')
        c = rank >> 1
        e = rank & 1
        other = NS * (1 - e)
        q3 = query.reshape(nb, rows, hd)
        g3 = grad_out.reshape(nb, rows, hd)
        k3 = keys.reshape(nb, piece, hd)
        v3 = values.reshape(nb, piece, hd)

        def half(x):
            return lax.dynamic_slice_in_dim(x, other, NS, 0)

        kv_mate = lax.ppermute(jnp.concatenate([half(k3), half(v3)], axis=-1), 'cp', swap)
        docs, ks = pl.pallas_call(
            gather_kernel,
            out_shape=[shape((n_dev, nb, piece), jnp.int32), shape((nb, 128), jnp.int32)],
            in_specs=[VMEM],
            out_specs=[VMEM, VMEM],
            scratch_shapes=[pltpu.SemaphoreType.DMA((n_dev,)), pltpu.SemaphoreType.DMA((n_dev,))],
            compiler_params=pltpu.CompilerParams(has_side_effects=True),
            name="docs",
        )(doc_id)

        def tables(plan, lo, hi):
            me = jnp.stack([c, e, lo, hi]).astype(jnp.int32)
            return pl.pallas_call(
                functools.partial(table_kernel, plan),
                out_shape=shape((NTAB,), jnp.int32),
                in_specs=[SMEM, SMEM],
                out_specs=SMEM,
                name="tables",
            )(ks, me)

        def pack(plan, tab, n):
            f_cap = plan[0]
            n_t = len(f_cap[0])
            return pl.pallas_call(
                functools.partial(pack_kernel, n_t, n, [bounds(cap) for cap in f_cap]),
                in_specs=[SMEM] + [ANY] * 3,
                out_specs=[ANY] * (1 + 3 * n_t),
                out_shape=[shape((NS, 8, G, 512), bf)] + [shape((f_cap[d][t], G, 512), bf) for d in range(3) for t in range(n_t)],
                scratch_shapes=[
                    pltpu.VMEM((2, n, piece, hd), bf), pltpu.VMEM((n, 8, G, 512), bf),
                    pltpu.SemaphoreType.DMA((4,)), pltpu.SemaphoreType.DMA, pltpu.SemaphoreType.DMA,
                ],
                name="pack",
            )(tab, k3, v3, kv_mate.reshape(NS, 4, G, 512))

        def chip_hop(x, *moves):
            return lax.ppermute(x, 'cp', [(2 * a + k, 2 * b + k) for a, b in moves for k in range(2)])

        def forward_hop(x, d):
            return chip_hop(x, *[(k, k + d + 1) for k in range(NCH - d - 1)])

        def backward_hop(x, d):
            return chip_hop(x, *[(k + d + 1, k) for k in range(NCH - d - 1)])

        def attend(plan, t, tab, mates, kvcol, frecv, state):
            f_cap, b_cap = plan[:2]
            n_t = len(f_cap[0])
            live = n_t - t
            n_alias = 0 if state is None else len(state)
            mates = mates[:1] if n_t > 1 and t == 0 else mates
            got = [frecv[d][u] for d in range(3) for u in range(t + 1)]
            flat = [x for way in got for x in way]
            n_in = 5 + 2 * len(mates) + len(flat)
            return pl.pallas_call(
                functools.partial(compute_kernel, t, n_t, [bounds(cap) for cap in f_cap], len(mates), [len(way) for way in got], n_alias, scale),
                in_specs=[SMEM, VMEM] + [ANY] * (n_in - 2 + n_alias),
                out_specs=[ANY] * (5 + 3 * live),
                scratch_shapes=[
                    pltpu.VMEM((2, 4, rows, hd), bf), pltpu.VMEM((2, 4, rows, hd), bf),
                    pltpu.VMEM((2, 4, 8, G, 512), bf), pltpu.VMEM((2, 4, 8, G, 512), f32),
                    pltpu.VMEM((4, rows, 256), f32), pltpu.VMEM((4, rows, 256), bf),
                    pltpu.VMEM((4, rows, 128), f32), pltpu.VMEM((4, rows, 128), f32), pltpu.VMEM((4, rows, 128), f32),
                    pltpu.VMEM((rows, 128), jnp.int32),
                    pltpu.VMEM((rows, hd), f32), pltpu.VMEM((rows, hd), f32),
                    pltpu.SemaphoreType.DMA((2,)), pltpu.SemaphoreType.DMA((2,)),
                ],
                out_shape=[
                    shape((nb, rows, hd), bf), shape((NS, rows, hd), bf),
                    shape((nb, rows, hd), bf), shape((NS, rows, hd), bf),
                    shape((NS, 8, G, 512), f32),
                ] + [shape((b_cap[d][v], G, 512), f32) for d in range(3) for v in range(t, n_t)],
                input_output_aliases={n_in + k: k for k in range(n_alias)},
                compiler_params=BIG,
                cost_estimate=pl.CostEstimate(flops=60_000_000_000 // n_t, bytes_accessed=100_000_000 // n_t, transcendentals=0),
            )(tab, docs, q3, g3, kvcol, *[m[0] for m in mates], *[m[1] for m in mates], *flat, *([] if state is None else state))

        def finish(plan, tab, acc, brecv, state):
            n_t = len(plan[0][0])
            n_alias = 0 if state is None else 3
            got = [way for row in brecv for way in row]
            flat = [x for way in got for x in way]
            return pl.pallas_call(
                functools.partial(finish_kernel, n_t, [len(way) for way in got], n_alias, scale),
                in_specs=[SMEM] + [ANY] * (1 + len(flat) + n_alias),
                out_specs=[ANY] * 3,
                out_shape=[shape((nb, piece, hd), bf), shape((nb, piece, hd), bf), shape((NS, piece, 512), bf)],
                scratch_shapes=[
                    pltpu.VMEM((2, 8, G, 512), f32), pltpu.VMEM((2, 3, 8, G, 512), f32),
                    pltpu.VMEM((2, piece, hd), bf), pltpu.VMEM((2, piece, hd), bf), pltpu.VMEM((2, piece, 512), bf),
                    pltpu.SemaphoreType.DMA((2,)), pltpu.SemaphoreType.DMA((2,)),
                ],
                input_output_aliases={2 + len(flat) + k: k for k in range(n_alias)},
                name="finish",
            )(tab, acc, *flat, *([] if state is None else state))

        def place(mine, send):
            got = lax.ppermute(send, 'cp', swap)
            return lax.dynamic_update_slice_in_dim(mine, got, other, 0)

        def place_kv(dk_all, dv_all, dkv_send):
            got = lax.ppermute(dkv_send, 'cp', swap)
            return (lax.dynamic_update_slice_in_dim(dk_all, got[:, :, :hd], other, 0),
                    lax.dynamic_update_slice_in_dim(dv_all, got[:, :, hd:], other, 0))

        def swap_part(x, lo, n):
            return lax.ppermute(lax.dynamic_slice_in_dim(x, other + lo, n, 0), 'cp', swap)

        tab = tables(FAST, jnp.int32(0), jnp.int32(NS))

        def fast():
            n_t = len(FAST[0][0])
            packed = pack(FAST, tab, NS)
            kvcol, fsend = packed[0], packed[1:]
            frecv = [[None] * n_t for _ in range(3)]
            for t in range(n_t):
                for d in range(3):
                    x = fsend[d * n_t + t]
                    if d == 0 and t in RELAY_F:
                        across = chip_hop(x, (0, 1), (2, 3))
                        mid = chip_hop(x, (1, 3))
                        frecv[0][t] = (across, chip_hop(mid, (3, 2)))
                    else:
                        frecv[d][t] = (forward_hop(x, d),)
            mates = [(swap_part(q3, 0, QA), swap_part(g3, 0, QA)),
                     (swap_part(q3, QA, NS - QA), swap_part(g3, QA, NS - QA))]
            state = None
            brecv = [[None] * n_t for _ in range(3)]
            for t in range(n_t):
                live = n_t - t
                outs = attend(FAST, t, tab, mates, kvcol, frecv, state)
                state = list(outs[:5]) + [outs[5 + d * live + k] for d in range(3) for k in range(1, live)]
                for d in range(3):
                    x = outs[5 + d * live]
                    if d == 0 and t in RELAY_B:
                        across = chip_hop(x, (1, 0), (3, 2))
                        mid = chip_hop(x, (2, 0))
                        brecv[0][t] = (across, chip_hop(mid, (0, 1)))
                    else:
                        brecv[d][t] = (backward_hop(x, d),)
            o_all, o_send, dq_all, dq_send, acc = state
            attn_out = place(o_all, o_send)
            grad_query = place(dq_all, dq_send)
            return (attn_out, grad_query) + place_kv(*finish(FAST, tab, acc, brecv, None))

        def slow():
            mates = [(swap_part(q3, 0, NS), swap_part(g3, 0, NS))]

            def blank():
                outs = [shape((nb, rows, hd), bf), shape((NS, rows, hd), bf), shape((nb, rows, hd), bf), shape((NS, rows, hd), bf),
                        shape((NS, 8, G, 512), f32), shape((nb, piece, hd), bf), shape((nb, piece, hd), bf), shape((NS, piece, 512), bf)]
                return [jnp.zeros(o.shape, o.dtype) for o in outs]

            def one_round(i, carry):
                state, grads = list(carry[:5]), list(carry[5:])
                tab = tables(SLOW, i * SLOW_SEQS, (i + 1) * SLOW_SEQS)
                packed = pack(SLOW, tab, SLOW_SEQS)
                frecv = [[(forward_hop(packed[1 + d], d),)] for d in range(3)]
                blank_b = [jnp.zeros((SLOW[1][0][0], G, 512), f32) for _ in range(3)]
                outs = attend(SLOW, 0, tab, mates, packed[0], frecv, state + blank_b)
                brecv = [[(backward_hop(outs[5 + d], d),)] for d in range(3)]
                return tuple(outs[:5]) + tuple(finish(SLOW, tab, outs[4], brecv, grads))

            out = lax.fori_loop(0, NS // SLOW_SEQS, one_round, tuple(blank()))
            return (place(out[0], out[1]), place(out[2], out[3])) + place_kv(*out[5:])

        attn_out, grad_query, grad_keys, grad_values = lax.cond(tab[FIT] > 0, fast, slow)
        return (attn_out.reshape(query.shape), grad_query.reshape(query.shape),
                grad_keys.reshape(keys.shape), grad_values.reshape(values.shape))

    return jax.shard_map(per_device, mesh=mesh, in_specs=(seq_spec, seq_spec, seq_spec, seq_spec, id_spec),
                         out_specs=(seq_spec, seq_spec, seq_spec, seq_spec), check_vma=False)
```

```python
import functools

import jax
import jax.numpy as jnp
from jax import lax
from jax.experimental import pallas as pl
from jax.experimental.pallas import tpu as pltpu
from jax.sharding import PartitionSpec as P


NEG_BIG = -1e30
LOG2E = 1.4426950408889634
G = 32
NS = 16
NCH = 4

FAST = (
    ((28, 34, 34, 30), (22, 24, 22, 18), (14, 14, 12, 10)),
    ((20, 28, 30, 46), (12, 18, 22, 34), (6, 8, 10, 24)),
    (4, 8, 12, 16),
)
RELAY_F = (1, 2)
RELAY_B = (1, 2)
QA = 4
SLOW_SEQS = 4
SLOW = (((8 * SLOW_SEQS,),) * 3,) * 2 + ((NS,),)

CNT, OFF, DM, ST, SG, CE, FIT = 0, 336, 672, 704, 712, 840, 844
NTAB = 848


def at(base, cc, d, s):
    return base + (cc * 3 + d) * NS + s


def sg(cc, d, v):
    return SG + (cc * 3 + d) * 6 + v


def bounds(caps):
    out = [0]
    for cap in caps:
        out.append(out[-1] + cap)
    return out


def gather_kernel(doc, out, ks, send_sem, recv_sem):
    me = lax.axis_index('cp')
    n = out.shape[0]
    out[me] = doc[...]
    copies = []
    for k in range(1, n):
        copy = pltpu.make_async_remote_copy(
            src_ref=doc, dst_ref=out.at[me], send_sem=send_sem.at[k], recv_sem=recv_sem.at[k],
            device_id={'cp': lax.rem(me + k, n)}, device_id_type=pl.DeviceIdType.MESH)
        copy.start()
        copies.append(copy)
    for copy in copies:
        copy.wait()
    lane = lax.broadcasted_iota(jnp.int32, ks.shape, 1)
    total = jnp.zeros(ks.shape, jnp.int32)
    for p in range(n):
        first = out[p][:, :1]
        below = jnp.zeros(ks.shape, jnp.int32)
        for j in range(n):
            below = below + (out[j] < first).astype(jnp.int32)
        total = jnp.where(lane == p, jnp.sum(below, axis=1, keepdims=True), total)
    ks[...] = total


def table_kernel(plan, ks, me, tab):
    f_cap, b_cap, quota = plan
    n_t = len(f_cap[0])
    f_lo = [bounds(cap) for cap in f_cap]
    c, e, lo, hi = me[0], me[1], me[2], me[3]
    zero = jnp.int32(0)
    tab[CE] = c
    tab[CE + 1] = e
    tab[ST] = lo
    for cc in range(7):
        for d in range(3):
            if not 1 <= cc <= 3 or d >= cc:
                for s in range(NS):
                    tab[at(CNT, cc, d, s)] = zero
                    tab[at(OFF, cc, d, s)] = zero
                for v in range(n_t + 1):
                    tab[sg(cc, d, v)] = zero
    for s in range(NS):
        for h in range(2):
            need = jnp.maximum(256 * c - ks[e * NS + s, 2 * c + h], 0)
            tab[DM + s * 2 + h] = (need + 255) >> 8

    fit = jnp.bool_(True)
    for col in range(2):
        row0 = jnp.where(e == 0, col, 1 - col) * NS
        for cc in range(NCH):
            off = [zero] * 3
            ready = [zero] * n_t
            avail = [[zero] * 3 for _ in range(n_t)]
            for s in range(NS):
                back = 256 * cc - ks[row0 + s, 2 * cc]
                live = (lo <= s) & (s < hi)
                for d in range(min(cc, 3)):
                    x = jnp.where(live, jnp.clip(back - 256 * d, 0, 256), 0)
                    n = (x + G - 1) >> 5
                    if col == 0:
                        tab[at(CNT, cc, d, s)] = n
                        tab[at(OFF, cc, d, s)] = off[d]
                    off[d] = off[d] + n
                for t in range(n_t):
                    if s >= quota[t]:
                        continue
                    ok = s < hi
                    for d in range(min(cc, 3)):
                        ok = ok & (off[d] <= f_lo[d][t + 1])
                    ready[t] = ready[t] + jnp.where(ok, 1, 0)
                    for d in range(min(cc, 3)):
                        avail[t][d] = jnp.where(ok, off[d], avail[t][d])
            fit = fit & (ready[n_t - 1] == hi)
            if col == 0:
                for t in range(n_t):
                    @pl.when(cc == c)
                    def _():
                        tab[ST + t + 1] = ready[t]
            for d in range(min(cc, 3)):
                sent = zero
                if col == 0:
                    tab[sg(cc, d, 0)] = sent
                for v in range(n_t):
                    sent = jnp.minimum(sent + b_cap[d][v], avail[v][d])
                    if col == 0:
                        tab[sg(cc, d, v + 1)] = sent
                fit = fit & (sent == off[d])
    tab[FIT] = jnp.where(fit, 1, 0)


def run_copies(lo_of, n_chunks, off, n, issue):
    for v in range(n_chunks):
        lo, hi = lo_of(v), lo_of(v + 1)
        a = jnp.maximum(off, lo)
        cnt = jnp.minimum(off + n, hi) - a

        @pl.when(cnt > 0)
        def _():
            for size in (8, 4, 2, 1):
                @pl.when((cnt & size) != 0)
                def _():
                    skip = cnt & (16 - 2 * size)
                    issue(v, a - lo + skip, a - off + skip, size)


def run_waits(n, wait):
    for size in (8, 4, 2, 1):
        @pl.when((n & size) != 0)
        def _():
            wait(size)


def pack_kernel(n_t, n, f_lo, tab, k_all, v_all, mate, kvcol, *rest):
    chunks = [rest[d * n_t:(d + 1) * n_t] for d in range(3)]
    inb, stage, isem, sem, csem = rest[3 * n_t:]
    lo = tab[ST]
    c, e = tab[CE], tab[CE + 1]
    part = n // 4
    loads = []
    for i in range(4):
        rows = pl.ds(i * part, part)
        loads.append([
            pltpu.make_async_copy(k_all.at[pl.ds(e * NS + lo + i * part, part)], inb.at[0, rows], isem.at[i]),
            pltpu.make_async_copy(v_all.at[pl.ds(e * NS + lo + i * part, part)], inb.at[1, rows], isem.at[i]),
            pltpu.make_async_copy(mate.at[pl.ds(lo + i * part, part)], stage.at[rows, pl.ds(4 - 4 * e, 4)], isem.at[i]),
        ])
        for copy in loads[-1]:
            copy.start()
    for i in range(4):
        for copy in loads[i]:
            copy.wait()

        def step(j, _):
            s = lo + j
            stage[j, pl.ds(4 * e, 4), :, :256] = inb[0, j].reshape(4, G, 256)
            stage[j, pl.ds(4 * e, 4), :, 256:] = inb[1, j].reshape(4, G, 256)
            pltpu.make_async_copy(stage.at[j], kvcol.at[s], csem).start()
            for d in range(3):
                cnt = tab[at(CNT, c + d + 1, d, s)]
                off = tab[at(OFF, c + d + 1, d, s)]
                run_copies(lambda v: f_lo[d][v], n_t, off, cnt,
                           lambda v, slot, k, size: pltpu.make_async_copy(
                               stage.at[j, pl.ds(8 - cnt + k, size)], chunks[d][v].at[pl.ds(slot, size)], sem).start())
            return 0

        lax.fori_loop(i * part, (i + 1) * part, step, 0)

    def drain(j, _):
        pltpu.make_async_copy(stage.at[j], kvcol.at[lo + j], csem).wait()
        for d in range(3):
            run_waits(tab[at(CNT, c + d + 1, d, lo + j)],
                      lambda size: pltpu.make_async_copy(
                          stage.at[j, pl.ds(0, size)], kvcol.at[lo + j, pl.ds(0, size)], sem).wait())
        return 0

    lax.fori_loop(0, n, drain, 0)


def dot_nt(a, b):
    return lax.dot_general(a, b, (((1,), (1,)), ((), ())), preferred_element_type=jnp.float32)


def dot_nn(a, b):
    return lax.dot_general(a, b, (((1,), (0,)), ((), ())), preferred_element_type=jnp.float32)


def dot_tn(a, b):
    return lax.dot_general(a, b, (((0,), (0,)), ((), ())), preferred_element_type=jnp.float32)


def split(refs, counts):
    out = []
    for k in counts:
        out.append(refs[:k])
        refs = refs[k:]
    return out, refs


def compute_kernel(t, n_t, f_lo, n_mate, ways, n_alias, scale, tab, docs, q_all, g_all, kvcol, *rest):
    q_mates, rest = rest[:n_mate], rest[n_mate:]
    g_mates, rest = rest[:n_mate], rest[n_mate:]
    fbuf, rest = split(rest, ways)
    fbuf = [fbuf[d * (t + 1):(d + 1) * (t + 1)] for d in range(3)]
    rest = rest[n_alias:]
    o_all, o_send, dq_all, dq_send, acc = rest[:5]
    rest = rest[5:]
    live = n_t - t
    bbuf = [rest[d * live:(d + 1) * live] for d in range(3)]
    qg, outb, kvs, dkv, e_scr, dp_scr, p_scr, l_scr, f_scr, t_scr, docr, o_acc, isem, osem = rest[3 * live:]

    base = tab[ST + t]
    n = tab[ST + t + 1] - base
    c = tab[CE]
    e = tab[CE + 1]

    def inputs(ss, sl):
        own = e * NS + ss
        return [
            pltpu.make_async_copy(src, dst, isem.at[sl])
            for src, dst in (
                (kvcol.at[ss], kvs.at[sl, 0]), (q_all.at[own], qg.at[sl, 0]), (g_all.at[own], qg.at[sl, 2]),
            )
        ]

    def mate_inputs(refs, row, sl):
        return [
            pltpu.make_async_copy(refs[0].at[row], qg.at[sl, 1], isem.at[sl]),
            pltpu.make_async_copy(refs[1].at[row], qg.at[sl, 3], isem.at[sl]),
        ]

    def outputs(ss, sl):
        own = e * NS + ss
        return [
            pltpu.make_async_copy(src, dst, osem.at[sl])
            for src, dst in (
                (outb.at[sl, 0], o_all.at[own]), (outb.at[sl, 1], o_send.at[ss]),
                (outb.at[sl, 2], dq_all.at[own]), (outb.at[sl, 3], dq_send.at[ss]),
                (dkv.at[sl, 0], acc.at[ss]),
            )
        ]

    def fetch(ss, sl):
        for copy in inputs(ss, sl):
            copy.start()
        if n_mate == 1:
            for copy in mate_inputs((q_mates[0], g_mates[0]), ss, sl):
                copy.start()
        else:
            @pl.when(ss < QA)
            def _():
                for copy in mate_inputs((q_mates[0], g_mates[0]), ss, sl):
                    copy.start()

            @pl.when(ss >= QA)
            def _():
                for copy in mate_inputs((q_mates[1], g_mates[1]), ss - QA, sl):
                    copy.start()
        for d in range(3):
            cnt = tab[at(CNT, c, d, ss)]
            off = tab[at(OFF, c, d, ss)]

            def issue(v, slot, k, size):
                def go(ref):
                    pltpu.make_async_copy(ref.at[pl.ds(slot, size)], kvs.at[sl, d + 1, pl.ds(8 - cnt + k, size)], isem.at[sl]).start()

                if len(fbuf[d][v]) == 1:
                    go(fbuf[d][v][0])
                else:
                    pl.when(c != 2)(lambda: go(fbuf[d][v][0]))
                    pl.when(c == 2)(lambda: go(fbuf[d][v][1]))

            run_copies(lambda v: f_lo[d][v], t + 1, off, cnt, issue)

    def fetch_wait(ss, sl):
        for copy in inputs(ss, sl) + mate_inputs((q_mates[0], g_mates[0]), 0, sl):
            copy.wait()
        for d in range(3):
            run_waits(tab[at(CNT, c, d, ss)],
                      lambda size: pltpu.make_async_copy(
                          kvcol.at[ss, pl.ds(0, size)], kvs.at[sl, d + 1, pl.ds(0, size)], isem.at[sl]).wait())

    def put(ss, sl):
        for copy in outputs(ss, sl):
            copy.start()
        for d in range(3):
            cnt = tab[at(CNT, c, d, ss)]
            off = tab[at(OFF, c, d, ss)]
            run_copies(lambda v: tab[sg(c, d, t + v)], live, off, cnt,
                       lambda v, slot, k, size: pltpu.make_async_copy(
                           dkv.at[sl, d + 1, pl.ds(8 - cnt + k, size)], bbuf[d][v].at[pl.ds(slot, size)], osem.at[sl]).start())

    def put_wait(ss, sl):
        for copy in outputs(ss, sl):
            copy.wait()
        for d in range(3):
            run_waits(tab[at(CNT, c, d, ss)],
                      lambda size: pltpu.make_async_copy(
                          dkv.at[sl, d + 1, pl.ds(0, size)], acc.at[ss, pl.ds(0, size)], osem.at[sl]).wait())

    row_tok = lax.broadcasted_iota(jnp.int32, (1024, 128), 0) >> 3
    lane = lax.broadcasted_iota(jnp.int32, (1024, 128), 1)
    cs = scale * LOG2E
    lo_half, hi_half = slice(0, 128), slice(128, 256)

    def keys_of(slot, d):
        return kvs[slot, d, :, :, :256].reshape(256, 256)

    def values_of(slot, d):
        return kvs[slot, d, :, :, 256:].reshape(256, 256)

    def attend(s, slot):
        row = e * NS + s
        dm = jnp.maximum(tab[DM + s * 2], tab[DM + s * 2 + 1])
        piece = (e, 1 - e)
        for role in range(2):
            dq_row = docs[2 * c + piece[role], pl.ds(row, 1), :]
            d_t = jnp.transpose(jnp.broadcast_to(dq_row, (128, 128)))
            docr[role] = jnp.broadcast_to(d_t[:, None, :], (128, 8, 128)).reshape(1024, 128)

        def scores(role, d, causal):
            sc = dot_nt(qg[slot, role], keys_of(slot, d)) * cs
            xs = []
            for j in range(2):
                dk = docs[2 * (c - d) + j, pl.ds(row, 1), :]
                vis = docr[role] == dk
                if causal:
                    vis = vis & (lane + 128 * j <= row_tok + 128 * piece[role])
                xs.append(jnp.where(vis, sc[:, 128 * j:128 * (j + 1)], NEG_BIG))
            top = jnp.maximum(xs[0], xs[1])
            es = [jnp.exp2(x - top) for x in xs]
            e_scr[d, role, :, lo_half] = es[0]
            e_scr[d, role, :, hi_half] = es[1]
            f_scr[d, role] = top
            l_scr[d, role] = es[0] + es[1]
            return top

        def dprob(role, d):
            dp_scr[d, role] = dot_nt(g_of(role), values_of(slot, d))

        def g_of(role):
            return qg[slot, 2 + role]

        for role in range(2):
            t_scr[role] = scores(role, 0, True)

        def far_scores(d, x):
            for role in range(2):
                t_scr[role] = jnp.maximum(t_scr[role], scores(role, d, False))
            for role in range(2):
                dprob(role, d)
            return x

        lax.fori_loop(1, dm + 1, far_scores, 0)

        for role in range(2):
            top = jnp.broadcast_to(jnp.max(t_scr[role], axis=1, keepdims=True), (1024, 128))
            t_scr[role] = top
            f = jnp.exp2(f_scr[0, role] - top)
            f_scr[0, role] = f
            l_scr[0, role] = l_scr[0, role] * f
        dprob(0, 0)

        def far_sums(d, x):
            for role in range(2):
                f = jnp.exp2(f_scr[d, role] - t_scr[role])
                f_scr[d, role] = f
                l_scr[0, role] = l_scr[0, role] + l_scr[d, role] * f
            return x

        lax.fori_loop(1, dm + 1, far_sums, 0)

        for role in range(2):
            t_scr[role] = jnp.broadcast_to(1.0 / jnp.sum(l_scr[0, role], axis=1, keepdims=True), (1024, 128))
        dprob(1, 0)

        def weighted(role, d):
            f = f_scr[d, role] * t_scr[role]
            f_scr[d, role] = f
            for half in (lo_half, hi_half):
                p_scr[d, role, :, half] = (e_scr[d, role, :, half] * f).astype(jnp.bfloat16)
            return dot_nn(p_scr[d, role], values_of(slot, d))

        def value_grads(d):
            dv = dot_tn(p_scr[d, 0], g_of(0)) + dot_tn(p_scr[d, 1], g_of(1))
            dkv[slot, d, :, :, 256:] = dv.reshape(8, G, 256)

        for role in range(2):
            o_acc[role] = weighted(role, 0)

        def far_weighted(d, x):
            for role in range(2):
                o_acc[role] = o_acc[role] + weighted(role, d)
            value_grads(d)
            return x

        lax.fori_loop(1, dm + 1, far_weighted, 0)

        for role in range(2):
            o_low = o_acc[role].astype(jnp.bfloat16)
            outb[slot, role] = o_low
            delta = jnp.sum(g_of(role).astype(jnp.float32) * o_low.astype(jnp.float32), axis=1, keepdims=True)
            t_scr[role] = jnp.broadcast_to(delta, (1024, 128))
        value_grads(0)

        def score_grads(d):
            out = []
            for role in range(2):
                ds = [
                    (e_scr[d, role, :, half] * f_scr[d, role] * (dp_scr[d, role, :, half] - t_scr[role])).astype(jnp.bfloat16)
                    for half in (lo_half, hi_half)
                ]
                out.append(jnp.concatenate(ds, axis=1))
            dk = dot_tn(out[0], qg[slot, 0]) + dot_tn(out[1], qg[slot, 1])
            dkv[slot, d, :, :, :256] = dk.reshape(8, G, 256)
            return [dot_nn(ds, keys_of(slot, d)) for ds in out]

        dq = score_grads(0)
        for role in range(2):
            o_acc[role] = dq[role]

        def far_grads(d, x):
            dq = score_grads(d)
            for role in range(2):
                o_acc[role] = o_acc[role] + dq[role]
            return x

        lax.fori_loop(1, dm + 1, far_grads, 0)
        for role in range(2):
            outb[slot, 2 + role] = (o_acc[role] * scale).astype(jnp.bfloat16)

    @pl.when(n > 0)
    def _():
        kvs[...] = jnp.zeros_like(kvs)
        fetch(base, 0)

    def step(i, _):
        slot = lax.rem(i, 2)
        s = base + i

        @pl.when(i + 1 < n)
        def _():
            fetch(s + 1, 1 - slot)

        @pl.when(i >= 2)
        def _():
            put_wait(s - 2, slot)

        fetch_wait(s, slot)
        attend(s, slot)
        put(s, slot)
        return 0

    lax.fori_loop(0, n, step, 0)

    @pl.when(n >= 2)
    def _():
        put_wait(base + n - 2, lax.rem(n, 2))

    @pl.when(n >= 1)
    def _():
        put_wait(base + n - 1, lax.rem(n + 1, 2))


def finish_kernel(n_t, ways, n_alias, scale, tab, acc, *rest):
    bufs, rest = split(rest, ways)
    bufs = [bufs[d * n_t:(d + 1) * n_t] for d in range(3)]
    dk_all, dv_all, dkv_send, own, got, kb, vb, sb, sem, osem = rest[n_alias:]
    lo = tab[ST]
    n = tab[ST + n_t] if n_t == 1 else NS
    n = n - lo
    c, e = tab[CE], tab[CE + 1]

    def fetch(ss, sl):
        pltpu.make_async_copy(acc.at[ss], own.at[sl], sem.at[sl]).start()
        for d in range(3):
            cnt = tab[at(CNT, c + d + 1, d, ss)]
            off = tab[at(OFF, c + d + 1, d, ss)]

            def issue(v, slot, k, size):
                def go(ref):
                    pltpu.make_async_copy(ref.at[pl.ds(slot, size)], got.at[sl, d, pl.ds(8 - cnt + k, size)], sem.at[sl]).start()

                if len(bufs[d][v]) == 1:
                    go(bufs[d][v][0])
                else:
                    pl.when(c != 1)(lambda: go(bufs[d][v][0]))
                    pl.when(c == 1)(lambda: go(bufs[d][v][1]))

            run_copies(lambda v: tab[sg(c + d + 1, d, v)], n_t, off, cnt, issue)

    def fetch_wait(ss, sl):
        pltpu.make_async_copy(acc.at[ss], own.at[sl], sem.at[sl]).wait()
        for d in range(3):
            run_waits(tab[at(CNT, c + d + 1, d, ss)],
                      lambda size: pltpu.make_async_copy(
                          acc.at[ss, pl.ds(0, size)], got.at[sl, d, pl.ds(0, size)], sem.at[sl]).wait())

    def outputs(ss, sl):
        row = e * NS + ss
        return [
            pltpu.make_async_copy(kb.at[sl], dk_all.at[row], osem.at[sl]),
            pltpu.make_async_copy(vb.at[sl], dv_all.at[row], osem.at[sl]),
            pltpu.make_async_copy(sb.at[sl], dkv_send.at[ss], osem.at[sl]),
        ]

    @pl.when(n > 0)
    def _():
        fetch(lo, 0)

    def step(i, _):
        s = lo + i
        sl = lax.rem(i, 2)

        @pl.when(i + 1 < n)
        def _():
            fetch(s + 1, 1 - sl)

        @pl.when(i >= 2)
        def _():
            for copy in outputs(s - 2, sl):
                copy.wait()

        fetch_wait(s, sl)
        for d in range(3):
            cnt = tab[at(CNT, c + d + 1, d, s)]

            def add(k, _):
                own[sl, k] = own[sl, k] + got[sl, d, k]
                return 0

            lax.fori_loop(8 - cnt, 8, add, 0)
        mine = own[sl, pl.ds(4 * e, 4)].reshape(128, 512)
        other = own[sl, pl.ds(4 - 4 * e, 4)].reshape(128, 512)
        kb[sl] = (mine[:, :256] * scale).astype(jnp.bfloat16)
        vb[sl] = mine[:, 256:].astype(jnp.bfloat16)
        sb[sl, :, :256] = (other[:, :256] * scale).astype(jnp.bfloat16)
        sb[sl, :, 256:] = other[:, 256:].astype(jnp.bfloat16)
        for copy in outputs(s, sl):
            copy.start()
        return 0

    lax.fori_loop(0, n, step, 0)

    @pl.when(n >= 2)
    def _():
        for copy in outputs(lo + n - 2, lax.rem(n, 2)):
            copy.wait()

    @pl.when(n >= 1)
    def _():
        for copy in outputs(lo + n - 1, lax.rem(n + 1, 2)):
            copy.wait()


ANY = pl.BlockSpec(memory_space=pl.ANY)
SMEM = pl.BlockSpec(memory_space=pltpu.SMEM)
VMEM = pl.BlockSpec(memory_space=pltpu.VMEM)
BIG = pltpu.CompilerParams(vmem_limit_bytes=58 * 1024 * 1024)


def solution(mesh):
    n_dev = mesh.shape['cp']
    seq_spec = P('dp', 'cp', None, None)
    id_spec = P('dp', 'cp')
    swap = [(k, k ^ 1) for k in range(n_dev)]
    bf, f32 = jnp.bfloat16, jnp.float32
    shape = jax.ShapeDtypeStruct

    def per_device(query, keys, values, grad_out, doc_id):
        nb, piece, heads, hd = query.shape
        rows = piece * heads
        scale = hd ** -0.5
        rank = lax.axis_index('cp')
        c = rank >> 1
        e = rank & 1
        other = NS * (1 - e)
        q3 = query.reshape(nb, rows, hd)
        g3 = grad_out.reshape(nb, rows, hd)
        k3 = keys.reshape(nb, piece, hd)
        v3 = values.reshape(nb, piece, hd)

        def half(x):
            return lax.dynamic_slice_in_dim(x, other, NS, 0)

        kv_mate = lax.ppermute(jnp.concatenate([half(k3), half(v3)], axis=-1), 'cp', swap)
        docs, ks = pl.pallas_call(
            gather_kernel,
            out_shape=[shape((n_dev, nb, piece), jnp.int32), shape((nb, 128), jnp.int32)],
            in_specs=[VMEM],
            out_specs=[VMEM, VMEM],
            scratch_shapes=[pltpu.SemaphoreType.DMA((n_dev,)), pltpu.SemaphoreType.DMA((n_dev,))],
            compiler_params=pltpu.CompilerParams(has_side_effects=True),
            name="docs",
        )(doc_id)

        def tables(plan, lo, hi):
            me = jnp.stack([c, e, lo, hi]).astype(jnp.int32)
            return pl.pallas_call(
                functools.partial(table_kernel, plan),
                out_shape=shape((NTAB,), jnp.int32),
                in_specs=[SMEM, SMEM],
                out_specs=SMEM,
                name="tables",
            )(ks, me)

        def pack(plan, tab, n):
            f_cap = plan[0]
            n_t = len(f_cap[0])
            return pl.pallas_call(
                functools.partial(pack_kernel, n_t, n, [bounds(cap) for cap in f_cap]),
                in_specs=[SMEM] + [ANY] * 3,
                out_specs=[ANY] * (1 + 3 * n_t),
                out_shape=[shape((NS, 8, G, 512), bf)] + [shape((f_cap[d][t], G, 512), bf) for d in range(3) for t in range(n_t)],
                scratch_shapes=[
                    pltpu.VMEM((2, n, piece, hd), bf), pltpu.VMEM((n, 8, G, 512), bf),
                    pltpu.SemaphoreType.DMA((4,)), pltpu.SemaphoreType.DMA, pltpu.SemaphoreType.DMA,
                ],
                name="pack",
            )(tab, k3, v3, kv_mate.reshape(NS, 4, G, 512))

        def chip_hop(x, *moves):
            return lax.ppermute(x, 'cp', [(2 * a + k, 2 * b + k) for a, b in moves for k in range(2)])

        def forward_hop(x, d):
            return chip_hop(x, *[(k, k + d + 1) for k in range(NCH - d - 1)])

        def backward_hop(x, d):
            return chip_hop(x, *[(k + d + 1, k) for k in range(NCH - d - 1)])

        def attend(plan, t, tab, mates, kvcol, frecv, state):
            f_cap, b_cap = plan[:2]
            n_t = len(f_cap[0])
            live = n_t - t
            n_alias = 0 if state is None else len(state)
            mates = mates[:1] if n_t > 1 and t == 0 else mates
            got = [frecv[d][u] for d in range(3) for u in range(t + 1)]
            flat = [x for way in got for x in way]
            n_in = 5 + 2 * len(mates) + len(flat)
            return pl.pallas_call(
                functools.partial(compute_kernel, t, n_t, [bounds(cap) for cap in f_cap], len(mates), [len(way) for way in got], n_alias, scale),
                in_specs=[SMEM, VMEM] + [ANY] * (n_in - 2 + n_alias),
                out_specs=[ANY] * (5 + 3 * live),
                scratch_shapes=[
                    pltpu.VMEM((2, 4, rows, hd), bf), pltpu.VMEM((2, 4, rows, hd), bf),
                    pltpu.VMEM((2, 4, 8, G, 512), bf), pltpu.VMEM((2, 4, 8, G, 512), f32),
                    pltpu.VMEM((4, 2, rows, 256), f32), pltpu.VMEM((4, 2, rows, 256), f32), pltpu.VMEM((4, 2, rows, 256), bf),
                    pltpu.VMEM((4, 2, rows, 128), f32), pltpu.VMEM((4, 2, rows, 128), f32), pltpu.VMEM((2, rows, 128), f32),
                    pltpu.VMEM((2, rows, 128), jnp.int32), pltpu.VMEM((2, rows, hd), f32),
                    pltpu.SemaphoreType.DMA((2,)), pltpu.SemaphoreType.DMA((2,)),
                ],
                out_shape=[
                    shape((nb, rows, hd), bf), shape((NS, rows, hd), bf),
                    shape((nb, rows, hd), bf), shape((NS, rows, hd), bf),
                    shape((NS, 8, G, 512), f32),
                ] + [shape((b_cap[d][v], G, 512), f32) for d in range(3) for v in range(t, n_t)],
                input_output_aliases={n_in + k: k for k in range(n_alias)},
                compiler_params=BIG,
                cost_estimate=pl.CostEstimate(flops=60_000_000_000 // n_t, bytes_accessed=100_000_000 // n_t, transcendentals=0),
            )(tab, docs, q3, g3, kvcol, *[m[0] for m in mates], *[m[1] for m in mates], *flat, *([] if state is None else state))

        def finish(plan, tab, acc, brecv, state):
            n_t = len(plan[0][0])
            n_alias = 0 if state is None else 3
            got = [way for row in brecv for way in row]
            flat = [x for way in got for x in way]
            return pl.pallas_call(
                functools.partial(finish_kernel, n_t, [len(way) for way in got], n_alias, scale),
                in_specs=[SMEM] + [ANY] * (1 + len(flat) + n_alias),
                out_specs=[ANY] * 3,
                out_shape=[shape((nb, piece, hd), bf), shape((nb, piece, hd), bf), shape((NS, piece, 512), bf)],
                scratch_shapes=[
                    pltpu.VMEM((2, 8, G, 512), f32), pltpu.VMEM((2, 3, 8, G, 512), f32),
                    pltpu.VMEM((2, piece, hd), bf), pltpu.VMEM((2, piece, hd), bf), pltpu.VMEM((2, piece, 512), bf),
                    pltpu.SemaphoreType.DMA((2,)), pltpu.SemaphoreType.DMA((2,)),
                ],
                input_output_aliases={2 + len(flat) + k: k for k in range(n_alias)},
                name="finish",
            )(tab, acc, *flat, *([] if state is None else state))

        def place(mine, send):
            got = lax.ppermute(send, 'cp', swap)
            return lax.dynamic_update_slice_in_dim(mine, got, other, 0)

        def place_kv(dk_all, dv_all, dkv_send):
            got = lax.ppermute(dkv_send, 'cp', swap)
            return (lax.dynamic_update_slice_in_dim(dk_all, got[:, :, :hd], other, 0),
                    lax.dynamic_update_slice_in_dim(dv_all, got[:, :, hd:], other, 0))

        def swap_part(x, lo, n):
            return lax.ppermute(lax.dynamic_slice_in_dim(x, other + lo, n, 0), 'cp', swap)

        tab = tables(FAST, jnp.int32(0), jnp.int32(NS))

        def fast():
            n_t = len(FAST[0][0])
            packed = pack(FAST, tab, NS)
            kvcol, fsend = packed[0], packed[1:]
            frecv = [[None] * n_t for _ in range(3)]
            for t in range(n_t):
                for d in range(3):
                    x = fsend[d * n_t + t]
                    if d == 0 and t in RELAY_F:
                        across = chip_hop(x, (0, 1), (2, 3))
                        mid = chip_hop(x, (1, 3))
                        frecv[0][t] = (across, chip_hop(mid, (3, 2)))
                    else:
                        frecv[d][t] = (forward_hop(x, d),)
            mates = [(swap_part(q3, 0, QA), swap_part(g3, 0, QA)),
                     (swap_part(q3, QA, NS - QA), swap_part(g3, QA, NS - QA))]
            state = None
            brecv = [[None] * n_t for _ in range(3)]
            for t in range(n_t):
                live = n_t - t
                outs = attend(FAST, t, tab, mates, kvcol, frecv, state)
                state = list(outs[:5]) + [outs[5 + d * live + k] for d in range(3) for k in range(1, live)]
                for d in range(3):
                    x = outs[5 + d * live]
                    if d == 0 and t in RELAY_B:
                        across = chip_hop(x, (1, 0), (3, 2))
                        mid = chip_hop(x, (2, 0))
                        brecv[0][t] = (across, chip_hop(mid, (0, 1)))
                    else:
                        brecv[d][t] = (backward_hop(x, d),)
            o_all, o_send, dq_all, dq_send, acc = state
            attn_out = place(o_all, o_send)
            grad_query = place(dq_all, dq_send)
            return (attn_out, grad_query) + place_kv(*finish(FAST, tab, acc, brecv, None))

        def slow():
            mates = [(swap_part(q3, 0, NS), swap_part(g3, 0, NS))]

            def blank():
                outs = [shape((nb, rows, hd), bf), shape((NS, rows, hd), bf), shape((nb, rows, hd), bf), shape((NS, rows, hd), bf),
                        shape((NS, 8, G, 512), f32), shape((nb, piece, hd), bf), shape((nb, piece, hd), bf), shape((NS, piece, 512), bf)]
                return [jnp.zeros(o.shape, o.dtype) for o in outs]

            def one_round(i, carry):
                state, grads = list(carry[:5]), list(carry[5:])
                tab = tables(SLOW, i * SLOW_SEQS, (i + 1) * SLOW_SEQS)
                packed = pack(SLOW, tab, SLOW_SEQS)
                frecv = [[(forward_hop(packed[1 + d], d),)] for d in range(3)]
                blank_b = [jnp.zeros((SLOW[1][0][0], G, 512), f32) for _ in range(3)]
                outs = attend(SLOW, 0, tab, mates, packed[0], frecv, state + blank_b)
                brecv = [[(backward_hop(outs[5 + d], d),)] for d in range(3)]
                return tuple(outs[:5]) + tuple(finish(SLOW, tab, outs[4], brecv, grads))

            out = lax.fori_loop(0, NS // SLOW_SEQS, one_round, tuple(blank()))
            return (place(out[0], out[1]), place(out[2], out[3])) + place_kv(*out[5:])

        attn_out, grad_query, grad_keys, grad_values = lax.cond(tab[FIT] > 0, fast, slow)
        return (attn_out.reshape(query.shape), grad_query.reshape(query.shape),
                grad_keys.reshape(keys.shape), grad_values.reshape(values.shape))

    return jax.shard_map(per_device, mesh=mesh, in_specs=(seq_spec, seq_spec, seq_spec, seq_spec, id_spec),
                         out_specs=(seq_spec, seq_spec, seq_spec, seq_spec), check_vma=False)
```

```python
import functools

import jax
import jax.numpy as jnp
from jax import lax
from jax.experimental import pallas as pl
from jax.experimental.pallas import tpu as pltpu
from jax.sharding import PartitionSpec as P


NEG_BIG = -1e30
LOG2E = 1.4426950408889634
G = 32
NS = 16
NCH = 4

FAST = (
    ((22, 44, 60), (18, 34, 36), (12, 20, 18)),
    ((14, 34, 34, 42), (10, 22, 24, 32), (4, 10, 12, 24)),
    (3, 8, 13, 16),
)
LEVELS = ((22, 15, 9), (28, 21, 15), (42, 32, 24))
RELAY_F = (2,)
RELAY_B = (1, 2)
QA = 3
SLOW_SEQS = 4
SLOW = (((8 * SLOW_SEQS,),) * 3,) * 2 + ((NS,),)

CNT, OFF, DM, ST, SG, CE, FIT, LEVEL, SPLIT = 0, 336, 672, 704, 712, 840, 844, 845, 846
NTAB = 848


def at(base, cc, d, s):
    return base + (cc * 3 + d) * NS + s


def sg(cc, d, v):
    return SG + (cc * 3 + d) * 6 + v


def bounds(caps):
    out = [0]
    for cap in caps:
        out.append(out[-1] + cap)
    return out


def gather_kernel(doc, out, ks, send_sem, recv_sem):
    me = lax.axis_index('cp')
    n = out.shape[0]
    out[me] = doc[...]
    copies = []
    for k in range(1, n):
        copy = pltpu.make_async_remote_copy(
            src_ref=doc, dst_ref=out.at[me], send_sem=send_sem.at[k], recv_sem=recv_sem.at[k],
            device_id={'cp': lax.rem(me + k, n)}, device_id_type=pl.DeviceIdType.MESH)
        copy.start()
        copies.append(copy)
    for copy in copies:
        copy.wait()
    lane = lax.broadcasted_iota(jnp.int32, ks.shape, 1)
    total = jnp.zeros(ks.shape, jnp.int32)
    for p in range(n):
        first = out[p][:, :1]
        below = jnp.zeros(ks.shape, jnp.int32)
        for j in range(n):
            below = below + (out[j] < first).astype(jnp.int32)
        total = jnp.where(lane == p, jnp.sum(below, axis=1, keepdims=True), total)
    ks[...] = total


def table_kernel(plan, ks, me, tab):
    f_cap, b_cap, quota = plan
    n_f, n_t = len(f_cap[0]), len(b_cap[0])
    f_lo = [bounds(cap) for cap in f_cap]
    c, e, lo, hi = me[0], me[1], me[2], me[3]
    zero = jnp.int32(0)
    tab[CE] = c
    tab[CE + 1] = e
    tab[ST] = lo
    for cc in range(7):
        for d in range(3):
            if not 1 <= cc <= 3 or d >= cc:
                for s in range(NS):
                    tab[at(CNT, cc, d, s)] = zero
                    tab[at(OFF, cc, d, s)] = zero
                for v in range(n_t + 1):
                    tab[sg(cc, d, v)] = zero
    for s in range(NS):
        for h in range(2):
            need = jnp.maximum(256 * c - ks[e * NS + s, 2 * c + h], 0)
            tab[DM + s * 2 + h] = (need + 255) >> 8

    fit = jnp.bool_(True)
    last = [zero] * 3
    for col in range(2):
        row0 = jnp.where(e == 0, col, 1 - col) * NS
        for cc in range(NCH):
            off = [zero] * 3
            ready = [zero] * n_t
            avail = [[zero] * 3 for _ in range(n_t)]
            for s in range(NS):
                back = 256 * cc - ks[row0 + s, 2 * cc]
                live = (lo <= s) & (s < hi)
                for d in range(min(cc, 3)):
                    x = jnp.where(live, jnp.clip(back - 256 * d, 0, 256), 0)
                    n = (x + G - 1) >> 5
                    if col == 0:
                        tab[at(CNT, cc, d, s)] = n
                        tab[at(OFF, cc, d, s)] = off[d]
                    off[d] = off[d] + n
                for t in range(n_t):
                    if s >= quota[t]:
                        continue
                    ok = s < hi
                    for d in range(min(cc, 3)):
                        ok = ok & (off[d] <= f_lo[d][min(t, n_f - 1) + 1])
                    ready[t] = ready[t] + jnp.where(ok, 1, 0)
                    for d in range(min(cc, 3)):
                        avail[t][d] = jnp.where(ok, off[d], avail[t][d])
            fit = fit & (ready[n_t - 1] == hi)
            if col == 0:
                for t in range(n_t):
                    @pl.when(cc == c)
                    def _():
                        tab[ST + t + 1] = ready[t]
            for d in range(min(cc, 3)):
                sent = zero
                if col == 0:
                    tab[sg(cc, d, 0)] = sent
                for v in range(n_t):
                    if v == n_t - 1:
                        last[d] = jnp.maximum(last[d], off[d] - sent)
                    sent = jnp.minimum(sent + b_cap[d][v], avail[v][d])
                    if col == 0:
                        tab[sg(cc, d, v + 1)] = sent
                fit = fit & (sent == off[d])
    tab[FIT] = jnp.where(fit, 1, 0)
    level = zero
    for size in LEVELS[:-1]:
        over = (last[0] > size[0]) | (last[1] > size[1]) | (last[2] > size[2])
        level = level + jnp.where(over, 1, 0)
    tab[LEVEL] = level
    done = zero
    for s in range(NS):
        ok = jnp.bool_(True)
        for d in range(3):
            cc = c + d + 1
            ok = ok & (tab[at(OFF, cc, d, s)] + tab[at(CNT, cc, d, s)] <= tab[sg(cc, d, n_t - 1)])
        done = done + jnp.where(ok, 1, 0)
    tab[SPLIT] = done


def run_copies(lo_of, n_chunks, off, n, issue):
    for v in range(n_chunks):
        lo, hi = lo_of(v), lo_of(v + 1)
        a = jnp.maximum(off, lo)
        cnt = jnp.minimum(off + n, hi) - a

        @pl.when(cnt > 0)
        def _():
            for size in (8, 4, 2, 1):
                @pl.when((cnt & size) != 0)
                def _():
                    skip = cnt & (16 - 2 * size)
                    issue(v, a - lo + skip, a - off + skip, size)


def run_waits(n, wait):
    for size in (8, 4, 2, 1):
        @pl.when((n & size) != 0)
        def _():
            wait(size)


def pack_kernel(n_t, n, f_lo, tab, k_all, v_all, mate, kvcol, *rest):
    chunks = [rest[d * n_t:(d + 1) * n_t] for d in range(3)]
    inb, stage, isem, sem, csem = rest[3 * n_t:]
    lo = tab[ST]
    c, e = tab[CE], tab[CE + 1]
    part = n // 4
    loads = []
    for i in range(4):
        rows = pl.ds(i * part, part)
        loads.append([
            pltpu.make_async_copy(k_all.at[pl.ds(e * NS + lo + i * part, part)], inb.at[0, rows], isem.at[i]),
            pltpu.make_async_copy(v_all.at[pl.ds(e * NS + lo + i * part, part)], inb.at[1, rows], isem.at[i]),
            pltpu.make_async_copy(mate.at[pl.ds(lo + i * part, part)], stage.at[rows, pl.ds(4 - 4 * e, 4)], isem.at[i]),
        ])
        for copy in loads[-1]:
            copy.start()
    for i in range(4):
        for copy in loads[i]:
            copy.wait()

        def step(j, _):
            s = lo + j
            stage[j, pl.ds(4 * e, 4), :, :256] = inb[0, j].reshape(4, G, 256)
            stage[j, pl.ds(4 * e, 4), :, 256:] = inb[1, j].reshape(4, G, 256)
            pltpu.make_async_copy(stage.at[j], kvcol.at[s], csem).start()
            for d in range(3):
                cnt = tab[at(CNT, c + d + 1, d, s)]
                off = tab[at(OFF, c + d + 1, d, s)]
                run_copies(lambda v: f_lo[d][v], n_t, off, cnt,
                           lambda v, slot, k, size: pltpu.make_async_copy(
                               stage.at[j, pl.ds(8 - cnt + k, size)], chunks[d][v].at[pl.ds(slot, size)], sem).start())
            return 0

        lax.fori_loop(i * part, (i + 1) * part, step, 0)

    def drain(j, _):
        pltpu.make_async_copy(stage.at[j], kvcol.at[lo + j], csem).wait()
        for d in range(3):
            run_waits(tab[at(CNT, c + d + 1, d, lo + j)],
                      lambda size: pltpu.make_async_copy(
                          stage.at[j, pl.ds(0, size)], kvcol.at[lo + j, pl.ds(0, size)], sem).wait())
        return 0

    lax.fori_loop(0, n, drain, 0)


def dot_nt(a, b):
    return lax.dot_general(a, b, (((1,), (1,)), ((), ())), preferred_element_type=jnp.float32)


def dot_nn(a, b):
    return lax.dot_general(a, b, (((1,), (0,)), ((), ())), preferred_element_type=jnp.float32)


def dot_tn(a, b):
    return lax.dot_general(a, b, (((0,), (0,)), ((), ())), preferred_element_type=jnp.float32)


def split(refs, counts):
    out = []
    for k in counts:
        out.append(refs[:k])
        refs = refs[k:]
    return out, refs


def compute_kernel(t, n_t, n_got, f_lo, n_mate, ways, n_alias, scale, tab, docs, q_all, g_all, kvcol, *rest):
    q_mates, rest = rest[:n_mate], rest[n_mate:]
    g_mates, rest = rest[:n_mate], rest[n_mate:]
    fbuf, rest = split(rest, ways)
    fbuf = [fbuf[d * n_got:(d + 1) * n_got] for d in range(3)]
    rest = rest[n_alias:]
    o_all, o_send, dq_all, dq_send, acc = rest[:5]
    rest = rest[5:]
    live = n_t - t
    bbuf = [rest[d * live:(d + 1) * live] for d in range(3)]
    qg, outb, kvs, dkv, e_scr, dp_scr, p_scr, l_scr, f_scr, t_scr, docr, o_acc, isem, osem = rest[3 * live:]

    base = tab[ST + t]
    n = tab[ST + t + 1] - base
    c = tab[CE]
    e = tab[CE + 1]

    def inputs(ss, sl):
        own = e * NS + ss
        return [
            pltpu.make_async_copy(src, dst, isem.at[sl])
            for src, dst in (
                (kvcol.at[ss], kvs.at[sl, 0]), (q_all.at[own], qg.at[sl, 0]), (g_all.at[own], qg.at[sl, 2]),
            )
        ]

    def mate_inputs(refs, row, sl):
        return [
            pltpu.make_async_copy(refs[0].at[row], qg.at[sl, 1], isem.at[sl]),
            pltpu.make_async_copy(refs[1].at[row], qg.at[sl, 3], isem.at[sl]),
        ]

    def outputs(ss, sl):
        own = e * NS + ss
        return [
            pltpu.make_async_copy(src, dst, osem.at[sl])
            for src, dst in (
                (outb.at[sl, 0], o_all.at[own]), (outb.at[sl, 1], o_send.at[ss]),
                (outb.at[sl, 2], dq_all.at[own]), (outb.at[sl, 3], dq_send.at[ss]),
                (dkv.at[sl, 0], acc.at[ss]),
            )
        ]

    def fetch(ss, sl):
        for copy in inputs(ss, sl):
            copy.start()
        if n_mate == 1:
            for copy in mate_inputs((q_mates[0], g_mates[0]), ss, sl):
                copy.start()
        else:
            @pl.when(ss < QA)
            def _():
                for copy in mate_inputs((q_mates[0], g_mates[0]), ss, sl):
                    copy.start()

            @pl.when(ss >= QA)
            def _():
                for copy in mate_inputs((q_mates[1], g_mates[1]), ss - QA, sl):
                    copy.start()
        for d in range(3):
            cnt = tab[at(CNT, c, d, ss)]
            off = tab[at(OFF, c, d, ss)]

            def issue(v, slot, k, size):
                def go(ref):
                    pltpu.make_async_copy(ref.at[pl.ds(slot, size)], kvs.at[sl, d + 1, pl.ds(8 - cnt + k, size)], isem.at[sl]).start()

                if len(fbuf[d][v]) == 1:
                    go(fbuf[d][v][0])
                else:
                    pl.when(c != 2)(lambda: go(fbuf[d][v][0]))
                    pl.when(c == 2)(lambda: go(fbuf[d][v][1]))

            run_copies(lambda v: f_lo[d][v], n_got, off, cnt, issue)

    def fetch_wait(ss, sl):
        for copy in inputs(ss, sl) + mate_inputs((q_mates[0], g_mates[0]), 0, sl):
            copy.wait()
        for d in range(3):
            run_waits(tab[at(CNT, c, d, ss)],
                      lambda size: pltpu.make_async_copy(
                          kvcol.at[ss, pl.ds(0, size)], kvs.at[sl, d + 1, pl.ds(0, size)], isem.at[sl]).wait())

    def put(ss, sl):
        for copy in outputs(ss, sl):
            copy.start()
        for d in range(3):
            cnt = tab[at(CNT, c, d, ss)]
            off = tab[at(OFF, c, d, ss)]
            run_copies(lambda v: tab[sg(c, d, t + v)], live, off, cnt,
                       lambda v, slot, k, size: pltpu.make_async_copy(
                           dkv.at[sl, d + 1, pl.ds(8 - cnt + k, size)], bbuf[d][v].at[pl.ds(slot, size)], osem.at[sl]).start())

    def put_wait(ss, sl):
        for copy in outputs(ss, sl):
            copy.wait()
        for d in range(3):
            run_waits(tab[at(CNT, c, d, ss)],
                      lambda size: pltpu.make_async_copy(
                          dkv.at[sl, d + 1, pl.ds(0, size)], acc.at[ss, pl.ds(0, size)], osem.at[sl]).wait())

    row_tok = lax.broadcasted_iota(jnp.int32, (1024, 128), 0) >> 3
    lane = lax.broadcasted_iota(jnp.int32, (1024, 128), 1)
    cs = scale * LOG2E
    lo_half, hi_half = slice(0, 128), slice(128, 256)

    def keys_of(slot, d):
        return kvs[slot, d, :, :, :256].reshape(256, 256)

    def values_of(slot, d):
        return kvs[slot, d, :, :, 256:].reshape(256, 256)

    def attend(s, slot):
        row = e * NS + s
        dm = jnp.maximum(tab[DM + s * 2], tab[DM + s * 2 + 1])
        piece = (e, 1 - e)
        for role in range(2):
            dq_row = docs[2 * c + piece[role], pl.ds(row, 1), :]
            d_t = jnp.transpose(jnp.broadcast_to(dq_row, (128, 128)))
            docr[role] = jnp.broadcast_to(d_t[:, None, :], (128, 8, 128)).reshape(1024, 128)

        def scores(role, d, causal):
            sc = dot_nt(qg[slot, role], keys_of(slot, d)) * cs
            xs = []
            for j in range(2):
                dk = docs[2 * (c - d) + j, pl.ds(row, 1), :]
                vis = docr[role] == dk
                if causal:
                    vis = vis & (lane + 128 * j <= row_tok + 128 * piece[role])
                xs.append(jnp.where(vis, sc[:, 128 * j:128 * (j + 1)], NEG_BIG))
            top = jnp.maximum(xs[0], xs[1])
            es = [jnp.exp2(x - top) for x in xs]
            e_scr[d, role, :, lo_half] = es[0]
            e_scr[d, role, :, hi_half] = es[1]
            f_scr[d, role] = top
            l_scr[d, role] = es[0] + es[1]
            return top

        def dprob(role, d):
            dp_scr[d, role] = dot_nt(g_of(role), values_of(slot, d))

        def g_of(role):
            return qg[slot, 2 + role]

        for role in range(2):
            t_scr[role] = scores(role, 0, True)

        def far_scores(d, x):
            for role in range(2):
                t_scr[role] = jnp.maximum(t_scr[role], scores(role, d, False))
            for role in range(2):
                dprob(role, d)
            return x

        lax.fori_loop(1, dm + 1, far_scores, 0)

        for role in range(2):
            top = jnp.broadcast_to(jnp.max(t_scr[role], axis=1, keepdims=True), (1024, 128))
            t_scr[role] = top
            f = jnp.exp2(f_scr[0, role] - top)
            f_scr[0, role] = f
            l_scr[0, role] = l_scr[0, role] * f
        dprob(0, 0)

        def far_sums(d, x):
            for role in range(2):
                f = jnp.exp2(f_scr[d, role] - t_scr[role])
                f_scr[d, role] = f
                l_scr[0, role] = l_scr[0, role] + l_scr[d, role] * f
            return x

        lax.fori_loop(1, dm + 1, far_sums, 0)

        for role in range(2):
            t_scr[role] = jnp.broadcast_to(1.0 / jnp.sum(l_scr[0, role], axis=1, keepdims=True), (1024, 128))
        dprob(1, 0)

        def weighted(role, d):
            f = f_scr[d, role] * t_scr[role]
            f_scr[d, role] = f
            for half in (lo_half, hi_half):
                p_scr[d, role, :, half] = (e_scr[d, role, :, half] * f).astype(jnp.bfloat16)
            return dot_nn(p_scr[d, role], values_of(slot, d))

        def value_grads(d):
            dv = dot_tn(p_scr[d, 0], g_of(0)) + dot_tn(p_scr[d, 1], g_of(1))
            dkv[slot, d, :, :, 256:] = dv.reshape(8, G, 256)

        for role in range(2):
            o_acc[role] = weighted(role, 0)

        def far_weighted(d, x):
            for role in range(2):
                o_acc[role] = o_acc[role] + weighted(role, d)
            value_grads(d)
            return x

        lax.fori_loop(1, dm + 1, far_weighted, 0)

        for role in range(2):
            o_low = o_acc[role].astype(jnp.bfloat16)
            outb[slot, role] = o_low
            delta = jnp.sum(g_of(role).astype(jnp.float32) * o_low.astype(jnp.float32), axis=1, keepdims=True)
            t_scr[role] = jnp.broadcast_to(delta, (1024, 128))
        value_grads(0)

        def score_grads(d):
            out = []
            for role in range(2):
                ds = [
                    (e_scr[d, role, :, half] * f_scr[d, role] * (dp_scr[d, role, :, half] - t_scr[role])).astype(jnp.bfloat16)
                    for half in (lo_half, hi_half)
                ]
                out.append(jnp.concatenate(ds, axis=1))
            dk = dot_tn(out[0], qg[slot, 0]) + dot_tn(out[1], qg[slot, 1])
            dkv[slot, d, :, :, :256] = dk.reshape(8, G, 256)
            return [dot_nn(ds, keys_of(slot, d)) for ds in out]

        dq = score_grads(0)
        for role in range(2):
            o_acc[role] = dq[role]

        def far_grads(d, x):
            dq = score_grads(d)
            for role in range(2):
                o_acc[role] = o_acc[role] + dq[role]
            return x

        lax.fori_loop(1, dm + 1, far_grads, 0)
        for role in range(2):
            outb[slot, 2 + role] = (o_acc[role] * scale).astype(jnp.bfloat16)

    @pl.when(n > 0)
    def _():
        kvs[...] = jnp.zeros_like(kvs)
        fetch(base, 0)

    def step(i, _):
        slot = lax.rem(i, 2)
        s = base + i

        @pl.when(i + 1 < n)
        def _():
            fetch(s + 1, 1 - slot)

        @pl.when(i >= 2)
        def _():
            put_wait(s - 2, slot)

        fetch_wait(s, slot)
        attend(s, slot)
        put(s, slot)
        return 0

    lax.fori_loop(0, n, step, 0)

    @pl.when(n >= 2)
    def _():
        put_wait(base + n - 2, lax.rem(n, 2))

    @pl.when(n >= 1)
    def _():
        put_wait(base + n - 1, lax.rem(n + 1, 2))


def finish_kernel(part, n_t, ways, n_alias, scale, tab, acc, *rest):
    bufs, rest = split(rest, ways)
    bufs = [bufs[d * n_t:(d + 1) * n_t] for d in range(3)]
    dk_all, dv_all, dkv_send, own, got, kb, vb, sb, sem, osem = rest[n_alias:]
    lo, hi = ((tab[ST], tab[ST + 1]), (0, tab[SPLIT]), (tab[SPLIT], NS))[part]
    n = hi - lo
    c, e = tab[CE], tab[CE + 1]

    def fetch(ss, sl):
        pltpu.make_async_copy(acc.at[ss], own.at[sl], sem.at[sl]).start()
        for d in range(3):
            cnt = tab[at(CNT, c + d + 1, d, ss)]
            off = tab[at(OFF, c + d + 1, d, ss)]

            def issue(v, slot, k, size):
                def go(ref):
                    pltpu.make_async_copy(ref.at[pl.ds(slot, size)], got.at[sl, d, pl.ds(8 - cnt + k, size)], sem.at[sl]).start()

                if len(bufs[d][v]) == 1:
                    go(bufs[d][v][0])
                else:
                    pl.when(c != 1)(lambda: go(bufs[d][v][0]))
                    pl.when(c == 1)(lambda: go(bufs[d][v][1]))

            run_copies(lambda v: tab[sg(c + d + 1, d, v)], n_t, off, cnt, issue)

    def fetch_wait(ss, sl):
        pltpu.make_async_copy(acc.at[ss], own.at[sl], sem.at[sl]).wait()
        for d in range(3):
            run_waits(tab[at(CNT, c + d + 1, d, ss)],
                      lambda size: pltpu.make_async_copy(
                          acc.at[ss, pl.ds(0, size)], got.at[sl, d, pl.ds(0, size)], sem.at[sl]).wait())

    def outputs(ss, sl):
        row = e * NS + ss
        return [
            pltpu.make_async_copy(kb.at[sl], dk_all.at[row], osem.at[sl]),
            pltpu.make_async_copy(vb.at[sl], dv_all.at[row], osem.at[sl]),
            pltpu.make_async_copy(sb.at[sl], dkv_send.at[ss], osem.at[sl]),
        ]

    @pl.when(n > 0)
    def _():
        fetch(lo, 0)

    def step(i, _):
        s = lo + i
        sl = lax.rem(i, 2)

        @pl.when(i + 1 < n)
        def _():
            fetch(s + 1, 1 - sl)

        @pl.when(i >= 2)
        def _():
            for copy in outputs(s - 2, sl):
                copy.wait()

        fetch_wait(s, sl)
        for d in range(3):
            cnt = tab[at(CNT, c + d + 1, d, s)]

            def add(k, _):
                own[sl, k] = own[sl, k] + got[sl, d, k]
                return 0

            lax.fori_loop(8 - cnt, 8, add, 0)
        mine = own[sl, pl.ds(4 * e, 4)].reshape(128, 512)
        other = own[sl, pl.ds(4 - 4 * e, 4)].reshape(128, 512)
        kb[sl] = (mine[:, :256] * scale).astype(jnp.bfloat16)
        vb[sl] = mine[:, 256:].astype(jnp.bfloat16)
        sb[sl, :, :256] = (other[:, :256] * scale).astype(jnp.bfloat16)
        sb[sl, :, 256:] = other[:, 256:].astype(jnp.bfloat16)
        for copy in outputs(s, sl):
            copy.start()
        return 0

    lax.fori_loop(0, n, step, 0)

    @pl.when(n >= 2)
    def _():
        for copy in outputs(lo + n - 2, lax.rem(n, 2)):
            copy.wait()

    @pl.when(n >= 1)
    def _():
        for copy in outputs(lo + n - 1, lax.rem(n + 1, 2)):
            copy.wait()


ANY = pl.BlockSpec(memory_space=pl.ANY)
SMEM = pl.BlockSpec(memory_space=pltpu.SMEM)
VMEM = pl.BlockSpec(memory_space=pltpu.VMEM)
BIG = pltpu.CompilerParams(vmem_limit_bytes=58 * 1024 * 1024)


def solution(mesh):
    n_dev = mesh.shape['cp']
    seq_spec = P('dp', 'cp', None, None)
    id_spec = P('dp', 'cp')
    swap = [(k, k ^ 1) for k in range(n_dev)]
    bf, f32 = jnp.bfloat16, jnp.float32
    shape = jax.ShapeDtypeStruct

    def per_device(query, keys, values, grad_out, doc_id):
        nb, piece, heads, hd = query.shape
        rows = piece * heads
        scale = hd ** -0.5
        rank = lax.axis_index('cp')
        c = rank >> 1
        e = rank & 1
        other = NS * (1 - e)
        q3 = query.reshape(nb, rows, hd)
        g3 = grad_out.reshape(nb, rows, hd)
        k3 = keys.reshape(nb, piece, hd)
        v3 = values.reshape(nb, piece, hd)

        def half(x):
            return lax.dynamic_slice_in_dim(x, other, NS, 0)

        kv_mate = lax.ppermute(jnp.concatenate([half(k3), half(v3)], axis=-1), 'cp', swap)
        docs, ks = pl.pallas_call(
            gather_kernel,
            out_shape=[shape((n_dev, nb, piece), jnp.int32), shape((nb, 128), jnp.int32)],
            in_specs=[VMEM],
            out_specs=[VMEM, VMEM],
            scratch_shapes=[pltpu.SemaphoreType.DMA((n_dev,)), pltpu.SemaphoreType.DMA((n_dev,))],
            compiler_params=pltpu.CompilerParams(has_side_effects=True),
            name="docs",
        )(doc_id)

        def tables(plan, lo, hi):
            me = jnp.stack([c, e, lo, hi]).astype(jnp.int32)
            return pl.pallas_call(
                functools.partial(table_kernel, plan),
                out_shape=shape((NTAB,), jnp.int32),
                in_specs=[SMEM, SMEM],
                out_specs=SMEM,
                name="tables",
            )(ks, me)

        def pack(plan, tab, n):
            f_cap = plan[0]
            n_t = len(f_cap[0])
            return pl.pallas_call(
                functools.partial(pack_kernel, n_t, n, [bounds(cap) for cap in f_cap]),
                in_specs=[SMEM] + [ANY] * 3,
                out_specs=[ANY] * (1 + 3 * n_t),
                out_shape=[shape((NS, 8, G, 512), bf)] + [shape((f_cap[d][t], G, 512), bf) for d in range(3) for t in range(n_t)],
                scratch_shapes=[
                    pltpu.VMEM((2, n, piece, hd), bf), pltpu.VMEM((n, 8, G, 512), bf),
                    pltpu.SemaphoreType.DMA((4,)), pltpu.SemaphoreType.DMA, pltpu.SemaphoreType.DMA,
                ],
                name="pack",
            )(tab, k3, v3, kv_mate.reshape(NS, 4, G, 512))

        def chip_hop(x, *moves):
            return lax.ppermute(x, 'cp', [(2 * a + k, 2 * b + k) for a, b in moves for k in range(2)])

        def forward_hop(x, d):
            return chip_hop(x, *[(k, k + d + 1) for k in range(NCH - d - 1)])

        def backward_hop(x, d):
            return chip_hop(x, *[(k + d + 1, k) for k in range(NCH - d - 1)])

        def attend(plan, t, tab, mates, kvcol, frecv, state):
            f_cap, b_cap = plan[:2]
            n_t = len(b_cap[0])
            live = n_t - t
            n_alias = 0 if state is None else len(state)
            mates = mates[:1] if n_t > 1 and t == 0 else mates
            n_got = min(t + 1, len(f_cap[0]))
            got = [frecv[d][u] for d in range(3) for u in range(n_got)]
            flat = [x for way in got for x in way]
            n_in = 5 + 2 * len(mates) + len(flat)
            return pl.pallas_call(
                functools.partial(compute_kernel, t, n_t, n_got, [bounds(cap) for cap in f_cap], len(mates), [len(way) for way in got], n_alias, scale),
                in_specs=[SMEM, VMEM] + [ANY] * (n_in - 2 + n_alias),
                out_specs=[ANY] * (5 + 3 * live),
                scratch_shapes=[
                    pltpu.VMEM((2, 4, rows, hd), bf), pltpu.VMEM((2, 4, rows, hd), bf),
                    pltpu.VMEM((2, 4, 8, G, 512), bf), pltpu.VMEM((2, 4, 8, G, 512), f32),
                    pltpu.VMEM((4, 2, rows, 256), f32), pltpu.VMEM((4, 2, rows, 256), f32), pltpu.VMEM((4, 2, rows, 256), bf),
                    pltpu.VMEM((4, 2, rows, 128), f32), pltpu.VMEM((4, 2, rows, 128), f32), pltpu.VMEM((2, rows, 128), f32),
                    pltpu.VMEM((2, rows, 128), jnp.int32), pltpu.VMEM((2, rows, hd), f32),
                    pltpu.SemaphoreType.DMA((2,)), pltpu.SemaphoreType.DMA((2,)),
                ],
                out_shape=[
                    shape((nb, rows, hd), bf), shape((NS, rows, hd), bf),
                    shape((nb, rows, hd), bf), shape((NS, rows, hd), bf),
                    shape((NS, 8, G, 512), f32),
                ] + [shape((b_cap[d][v], G, 512), f32) for d in range(3) for v in range(t, n_t)],
                input_output_aliases={n_in + k: k for k in range(n_alias)},
                compiler_params=BIG,
                cost_estimate=pl.CostEstimate(flops=60_000_000_000 // n_t, bytes_accessed=100_000_000 // n_t, transcendentals=0),
            )(tab, docs, q3, g3, kvcol, *[m[0] for m in mates], *[m[1] for m in mates], *flat, *([] if state is None else state))

        def finish(part, tab, acc, brecv, state):
            n_t = len(brecv[0])
            n_alias = 0 if state is None else 3
            got = [way for row in brecv for way in row]
            flat = [x for way in got for x in way]
            return pl.pallas_call(
                functools.partial(finish_kernel, part, n_t, [len(way) for way in got], n_alias, scale),
                in_specs=[SMEM] + [ANY] * (1 + len(flat) + n_alias),
                out_specs=[ANY] * 3,
                out_shape=[shape((nb, piece, hd), bf), shape((nb, piece, hd), bf), shape((NS, piece, 512), bf)],
                scratch_shapes=[
                    pltpu.VMEM((2, 8, G, 512), f32), pltpu.VMEM((2, 3, 8, G, 512), f32),
                    pltpu.VMEM((2, piece, hd), bf), pltpu.VMEM((2, piece, hd), bf), pltpu.VMEM((2, piece, 512), bf),
                    pltpu.SemaphoreType.DMA((2,)), pltpu.SemaphoreType.DMA((2,)),
                ],
                input_output_aliases={2 + len(flat) + k: k for k in range(n_alias)},
            )(tab, acc, *flat, *([] if state is None else state))

        def place(mine, send):
            got = lax.ppermute(send, 'cp', swap)
            return lax.dynamic_update_slice_in_dim(mine, got, other, 0)

        def place_kv(dk_all, dv_all, dkv_send):
            got = lax.ppermute(dkv_send, 'cp', swap)
            return (lax.dynamic_update_slice_in_dim(dk_all, got[:, :, :hd], other, 0),
                    lax.dynamic_update_slice_in_dim(dv_all, got[:, :, hd:], other, 0))

        def swap_part(x, lo, n):
            return lax.ppermute(lax.dynamic_slice_in_dim(x, other + lo, n, 0), 'cp', swap)

        tab = tables(FAST, jnp.int32(0), jnp.int32(NS))

        def fast():
            n_f, n_t = len(FAST[0][0]), len(FAST[1][0])
            packed = pack(FAST, tab, NS)
            kvcol, fsend = packed[0], packed[1:]
            frecv = [[None] * n_f for _ in range(3)]
            for t in range(n_f):
                for d in range(3):
                    x = fsend[d * n_f + t]
                    if d == 0 and t in RELAY_F:
                        across = chip_hop(x, (0, 1), (2, 3))
                        mid = chip_hop(x, (1, 3))
                        frecv[0][t] = (across, chip_hop(mid, (3, 2)))
                    else:
                        frecv[d][t] = (forward_hop(x, d),)
            mates = [(swap_part(q3, 0, QA), swap_part(g3, 0, QA)),
                     (swap_part(q3, QA, NS - QA), swap_part(g3, QA, NS - QA))]
            state = None
            brecv = [[None] * (n_t - 1) for _ in range(3)]
            for t in range(n_t):
                live = n_t - t
                outs = attend(FAST, t, tab, mates, kvcol, frecv, state)
                state = list(outs[:5]) + [outs[5 + d * live + k] for d in range(3) for k in range(1, live)]
                if t == n_t - 1:
                    break
                for d in range(3):
                    x = outs[5 + d * live]
                    if d == 0 and t in RELAY_B:
                        across = chip_hop(x, (1, 0), (3, 2))
                        mid = chip_hop(x, (2, 0))
                        brecv[0][t] = (across, chip_hop(mid, (0, 1)))
                    else:
                        brecv[d][t] = (backward_hop(x, d),)
            o_all, o_send, dq_all, dq_send, acc = state
            last = outs[5:]

            def tail(k):
                def run():
                    got = []
                    for d in range(3):
                        got.append((backward_hop(last[d][:LEVELS[k][d]], d),))
                    attn_out = place(o_all, o_send)
                    grad_query = place(dq_all, dq_send)
                    grads = finish(1, tab, acc, brecv, None)
                    grads = finish(2, tab, acc, [row + [x] for row, x in zip(brecv, got)], grads)
                    return (attn_out, grad_query) + place_kv(*grads)

                return run

            return lax.switch(tab[LEVEL], [tail(k) for k in range(len(LEVELS))])

        def slow():
            mates = [(swap_part(q3, 0, NS), swap_part(g3, 0, NS))]

            def blank():
                outs = [shape((nb, rows, hd), bf), shape((NS, rows, hd), bf), shape((nb, rows, hd), bf), shape((NS, rows, hd), bf),
                        shape((NS, 8, G, 512), f32), shape((nb, piece, hd), bf), shape((nb, piece, hd), bf), shape((NS, piece, 512), bf)]
                return [jnp.zeros(o.shape, o.dtype) for o in outs]

            def one_round(i, carry):
                state, grads = list(carry[:5]), list(carry[5:])
                tab = tables(SLOW, i * SLOW_SEQS, (i + 1) * SLOW_SEQS)
                packed = pack(SLOW, tab, SLOW_SEQS)
                frecv = [[(forward_hop(packed[1 + d], d),)] for d in range(3)]
                blank_b = [jnp.zeros((SLOW[1][0][0], G, 512), f32) for _ in range(3)]
                outs = attend(SLOW, 0, tab, mates, packed[0], frecv, state + blank_b)
                brecv = [[(backward_hop(outs[5 + d], d),)] for d in range(3)]
                return tuple(outs[:5]) + tuple(finish(0, tab, outs[4], brecv, grads))

            out = lax.fori_loop(0, NS // SLOW_SEQS, one_round, tuple(blank()))
            return (place(out[0], out[1]), place(out[2], out[3])) + place_kv(*out[5:])

        attn_out, grad_query, grad_keys, grad_values = lax.cond(tab[FIT] > 0, fast, slow)
        return (attn_out.reshape(query.shape), grad_query.reshape(query.shape),
                grad_keys.reshape(keys.shape), grad_values.reshape(values.shape))

    return jax.shard_map(per_device, mesh=mesh, in_specs=(seq_spec, seq_spec, seq_spec, seq_spec, id_spec),
                         out_specs=(seq_spec, seq_spec, seq_spec, seq_spec), check_vma=False)
```

```python
import functools

import jax
import jax.numpy as jnp
from jax import lax
from jax.experimental import pallas as pl
from jax.experimental.pallas import tpu as pltpu
from jax.sharding import PartitionSpec as P


NEG_BIG = -1e30
LOG2E = 1.4426950408889634
G = 32
NS = 16
NCH = 4

FAST = (
    ((28, 34, 34, 30), (22, 24, 22, 18), (14, 14, 12, 10)),
    ((22, 32, 34, 36), (14, 22, 24, 30), (8, 10, 12, 20)),
    (4, 8, 12, 16),
)
RELAY_F = ()
RELAY_B = (1, 2)
QA = 4
SLOW_SEQS = 4
SLOW = (((8 * SLOW_SEQS,),) * 3,) * 2 + ((NS,),)

CNT, OFF, DM, ST, SG, CE, FIT, SPLIT = 0, 336, 672, 704, 712, 840, 844, 845
NTAB = 848


def at(base, cc, d, s):
    return base + (cc * 3 + d) * NS + s


def sg(cc, d, v):
    return SG + (cc * 3 + d) * 6 + v


def bounds(caps):
    out = [0]
    for cap in caps:
        out.append(out[-1] + cap)
    return out


def gather_kernel(doc, out, ks, send_sem, recv_sem):
    me = lax.axis_index('cp')
    n = out.shape[0]
    out[me] = doc[...]
    copies = []
    for k in range(1, n):
        copy = pltpu.make_async_remote_copy(
            src_ref=doc, dst_ref=out.at[me], send_sem=send_sem.at[k], recv_sem=recv_sem.at[k],
            device_id={'cp': lax.rem(me + k, n)}, device_id_type=pl.DeviceIdType.MESH)
        copy.start()
        copies.append(copy)
    for copy in copies:
        copy.wait()
    lane = lax.broadcasted_iota(jnp.int32, ks.shape, 1)
    total = jnp.zeros(ks.shape, jnp.int32)
    for p in range(n):
        first = out[p][:, :1]
        below = jnp.zeros(ks.shape, jnp.int32)
        for j in range(n):
            below = below + (out[j] < first).astype(jnp.int32)
        total = jnp.where(lane == p, jnp.sum(below, axis=1, keepdims=True), total)
    ks[...] = total


def table_kernel(plan, ks, me, tab):
    f_cap, b_cap, quota = plan
    n_f, n_t = len(f_cap[0]), len(b_cap[0])
    f_lo = [bounds(cap) for cap in f_cap]
    c, e, lo, hi = me[0], me[1], me[2], me[3]
    zero = jnp.int32(0)
    tab[CE] = c
    tab[CE + 1] = e
    tab[ST] = lo
    for cc in range(7):
        for d in range(3):
            if not 1 <= cc <= 3 or d >= cc:
                for s in range(NS):
                    tab[at(CNT, cc, d, s)] = zero
                    tab[at(OFF, cc, d, s)] = zero
                for v in range(n_t + 1):
                    tab[sg(cc, d, v)] = zero
    for s in range(NS):
        for h in range(2):
            need = jnp.maximum(256 * c - ks[e * NS + s, 2 * c + h], 0)
            tab[DM + s * 2 + h] = (need + 255) >> 8

    fit = jnp.bool_(True)
    for col in range(2):
        row0 = jnp.where(e == 0, col, 1 - col) * NS
        for cc in range(NCH):
            off = [zero] * 3
            ready = [zero] * n_t
            avail = [[zero] * 3 for _ in range(n_t)]
            for s in range(NS):
                back = 256 * cc - ks[row0 + s, 2 * cc]
                live = (lo <= s) & (s < hi)
                for d in range(min(cc, 3)):
                    x = jnp.where(live, jnp.clip(back - 256 * d, 0, 256), 0)
                    n = (x + G - 1) >> 5
                    if col == 0:
                        tab[at(CNT, cc, d, s)] = n
                        tab[at(OFF, cc, d, s)] = off[d]
                    off[d] = off[d] + n
                for t in range(n_t):
                    if s >= quota[t]:
                        continue
                    ok = s < hi
                    for d in range(min(cc, 3)):
                        ok = ok & (off[d] <= f_lo[d][min(t, n_f - 1) + 1])
                    ready[t] = ready[t] + jnp.where(ok, 1, 0)
                    for d in range(min(cc, 3)):
                        avail[t][d] = jnp.where(ok, off[d], avail[t][d])
            fit = fit & (ready[n_t - 1] == hi)
            if col == 0:
                for t in range(n_t):
                    @pl.when(cc == c)
                    def _():
                        tab[ST + t + 1] = ready[t]
            for d in range(min(cc, 3)):
                sent = zero
                if col == 0:
                    tab[sg(cc, d, 0)] = sent
                for v in range(n_t):
                    sent = jnp.minimum(sent + b_cap[d][v], avail[v][d])
                    if col == 0:
                        tab[sg(cc, d, v + 1)] = sent
                fit = fit & (sent == off[d])
    tab[FIT] = jnp.where(fit, 1, 0)
    done = zero
    for s in range(NS):
        ok = jnp.bool_(True)
        for d in range(3):
            cc = c + d + 1
            ok = ok & (tab[at(OFF, cc, d, s)] + tab[at(CNT, cc, d, s)] <= tab[sg(cc, d, n_t - 1)])
        done = done + jnp.where(ok, 1, 0)
    tab[SPLIT] = done


def run_copies(lo_of, n_chunks, off, n, issue):
    for v in range(n_chunks):
        lo, hi = lo_of(v), lo_of(v + 1)
        a = jnp.maximum(off, lo)
        cnt = jnp.minimum(off + n, hi) - a

        @pl.when(cnt > 0)
        def _():
            for size in (8, 4, 2, 1):
                @pl.when((cnt & size) != 0)
                def _():
                    skip = cnt & (16 - 2 * size)
                    issue(v, a - lo + skip, a - off + skip, size)


def run_waits(n, wait):
    for size in (8, 4, 2, 1):
        @pl.when((n & size) != 0)
        def _():
            wait(size)


def pack_kernel(n_t, n, f_lo, tab, k_all, v_all, mate, kvcol, *rest):
    chunks = [rest[d * n_t:(d + 1) * n_t] for d in range(3)]
    inb, stage, isem, sem, csem = rest[3 * n_t:]
    lo = tab[ST]
    c, e = tab[CE], tab[CE + 1]
    part = n // 4
    loads = []
    for i in range(4):
        rows = pl.ds(i * part, part)
        loads.append([
            pltpu.make_async_copy(k_all.at[pl.ds(e * NS + lo + i * part, part)], inb.at[0, rows], isem.at[i]),
            pltpu.make_async_copy(v_all.at[pl.ds(e * NS + lo + i * part, part)], inb.at[1, rows], isem.at[i]),
            pltpu.make_async_copy(mate.at[pl.ds(lo + i * part, part)], stage.at[rows, pl.ds(4 - 4 * e, 4)], isem.at[i]),
        ])
        for copy in loads[-1]:
            copy.start()
    for i in range(4):
        for copy in loads[i]:
            copy.wait()

        def step(j, _):
            s = lo + j
            stage[j, pl.ds(4 * e, 4), :, :256] = inb[0, j].reshape(4, G, 256)
            stage[j, pl.ds(4 * e, 4), :, 256:] = inb[1, j].reshape(4, G, 256)
            pltpu.make_async_copy(stage.at[j], kvcol.at[s], csem).start()
            for d in range(3):
                cnt = tab[at(CNT, c + d + 1, d, s)]
                off = tab[at(OFF, c + d + 1, d, s)]
                run_copies(lambda v: f_lo[d][v], n_t, off, cnt,
                           lambda v, slot, k, size: pltpu.make_async_copy(
                               stage.at[j, pl.ds(8 - cnt + k, size)], chunks[d][v].at[pl.ds(slot, size)], sem).start())
            return 0

        lax.fori_loop(i * part, (i + 1) * part, step, 0)

    def drain(j, _):
        pltpu.make_async_copy(stage.at[j], kvcol.at[lo + j], csem).wait()
        for d in range(3):
            run_waits(tab[at(CNT, c + d + 1, d, lo + j)],
                      lambda size: pltpu.make_async_copy(
                          stage.at[j, pl.ds(0, size)], kvcol.at[lo + j, pl.ds(0, size)], sem).wait())
        return 0

    lax.fori_loop(0, n, drain, 0)


def dot_nt(a, b):
    return lax.dot_general(a, b, (((1,), (1,)), ((), ())), preferred_element_type=jnp.float32)


def dot_nn(a, b):
    return lax.dot_general(a, b, (((1,), (0,)), ((), ())), preferred_element_type=jnp.float32)


def dot_tn(a, b):
    return lax.dot_general(a, b, (((0,), (0,)), ((), ())), preferred_element_type=jnp.float32)


def split(refs, counts):
    out = []
    for k in counts:
        out.append(refs[:k])
        refs = refs[k:]
    return out, refs


def compute_kernel(t, n_t, n_got, f_lo, n_mate, ways, n_alias, scale, tab, docs, q_all, g_all, kvcol, *rest):
    q_mates, rest = rest[:n_mate], rest[n_mate:]
    g_mates, rest = rest[:n_mate], rest[n_mate:]
    fbuf, rest = split(rest, ways)
    fbuf = [fbuf[d * n_got:(d + 1) * n_got] for d in range(3)]
    rest = rest[n_alias:]
    o_all, o_send, dq_all, dq_send, acc = rest[:5]
    rest = rest[5:]
    live = n_t - t
    bbuf = [rest[d * live:(d + 1) * live] for d in range(3)]
    qg, outb, kvs, dkv, e_scr, dp_scr, p_scr, l_scr, f_scr, t_scr, docr, o_acc, isem, osem = rest[3 * live:]

    base = tab[ST + t]
    n = tab[ST + t + 1] - base
    c = tab[CE]
    e = tab[CE + 1]

    def inputs(ss, sl):
        own = e * NS + ss
        return [
            pltpu.make_async_copy(src, dst, isem.at[sl])
            for src, dst in (
                (kvcol.at[ss], kvs.at[sl, 0]), (q_all.at[own], qg.at[sl, 0]), (g_all.at[own], qg.at[sl, 2]),
            )
        ]

    def mate_inputs(refs, row, sl):
        return [
            pltpu.make_async_copy(refs[0].at[row], qg.at[sl, 1], isem.at[sl]),
            pltpu.make_async_copy(refs[1].at[row], qg.at[sl, 3], isem.at[sl]),
        ]

    def outputs(ss, sl):
        own = e * NS + ss
        return [
            pltpu.make_async_copy(src, dst, osem.at[sl])
            for src, dst in (
                (outb.at[sl, 0], o_all.at[own]), (outb.at[sl, 1], o_send.at[ss]),
                (outb.at[sl, 2], dq_all.at[own]), (outb.at[sl, 3], dq_send.at[ss]),
                (dkv.at[sl, 0], acc.at[ss]),
            )
        ]

    def fetch(ss, sl):
        for copy in inputs(ss, sl):
            copy.start()
        if n_mate == 1:
            for copy in mate_inputs((q_mates[0], g_mates[0]), ss, sl):
                copy.start()
        else:
            @pl.when(ss < QA)
            def _():
                for copy in mate_inputs((q_mates[0], g_mates[0]), ss, sl):
                    copy.start()

            @pl.when(ss >= QA)
            def _():
                for copy in mate_inputs((q_mates[1], g_mates[1]), e * NS + ss, sl):
                    copy.start()
        for d in range(3):
            cnt = tab[at(CNT, c, d, ss)]
            off = tab[at(OFF, c, d, ss)]

            def issue(v, slot, k, size):
                def go(ref):
                    pltpu.make_async_copy(ref.at[pl.ds(slot, size)], kvs.at[sl, d + 1, pl.ds(8 - cnt + k, size)], isem.at[sl]).start()

                if len(fbuf[d][v]) == 1:
                    go(fbuf[d][v][0])
                else:
                    pl.when(c != 2)(lambda: go(fbuf[d][v][0]))
                    pl.when(c == 2)(lambda: go(fbuf[d][v][1]))

            run_copies(lambda v: f_lo[d][v], n_got, off, cnt, issue)

    def fetch_wait(ss, sl):
        for copy in inputs(ss, sl) + mate_inputs((q_mates[0], g_mates[0]), 0, sl):
            copy.wait()
        for d in range(3):
            run_waits(tab[at(CNT, c, d, ss)],
                      lambda size: pltpu.make_async_copy(
                          kvcol.at[ss, pl.ds(0, size)], kvs.at[sl, d + 1, pl.ds(0, size)], isem.at[sl]).wait())

    def put(ss, sl):
        for copy in outputs(ss, sl):
            copy.start()
        for d in range(3):
            cnt = tab[at(CNT, c, d, ss)]
            off = tab[at(OFF, c, d, ss)]
            run_copies(lambda v: tab[sg(c, d, t + v)], live, off, cnt,
                       lambda v, slot, k, size: pltpu.make_async_copy(
                           dkv.at[sl, d + 1, pl.ds(8 - cnt + k, size)], bbuf[d][v].at[pl.ds(slot, size)], osem.at[sl]).start())

    def put_wait(ss, sl):
        for copy in outputs(ss, sl):
            copy.wait()
        for d in range(3):
            run_waits(tab[at(CNT, c, d, ss)],
                      lambda size: pltpu.make_async_copy(
                          dkv.at[sl, d + 1, pl.ds(0, size)], acc.at[ss, pl.ds(0, size)], osem.at[sl]).wait())

    row_tok = lax.broadcasted_iota(jnp.int32, (1024, 128), 0) >> 3
    lane = lax.broadcasted_iota(jnp.int32, (1024, 128), 1)
    cs = scale * LOG2E
    lo_half, hi_half = slice(0, 128), slice(128, 256)

    def keys_of(slot, d):
        return kvs[slot, d, :, :, :256].reshape(256, 256)

    def values_of(slot, d):
        return kvs[slot, d, :, :, 256:].reshape(256, 256)

    def attend(s, slot):
        row = e * NS + s
        dm = jnp.maximum(tab[DM + s * 2], tab[DM + s * 2 + 1])
        piece = (e, 1 - e)
        for role in range(2):
            dq_row = docs[2 * c + piece[role], pl.ds(row, 1), :]
            d_t = jnp.transpose(jnp.broadcast_to(dq_row, (128, 128)))
            docr[role] = jnp.broadcast_to(d_t[:, None, :], (128, 8, 128)).reshape(1024, 128)

        def scores(role, d, causal):
            sc = dot_nt(qg[slot, role], keys_of(slot, d)) * cs
            xs = []
            for j in range(2):
                dk = docs[2 * (c - d) + j, pl.ds(row, 1), :]
                vis = docr[role] == dk
                if causal:
                    vis = vis & (lane + 128 * j <= row_tok + 128 * piece[role])
                xs.append(jnp.where(vis, sc[:, 128 * j:128 * (j + 1)], NEG_BIG))
            top = jnp.maximum(xs[0], xs[1])
            es = [jnp.exp2(x - top) for x in xs]
            e_scr[d, role, :, lo_half] = es[0]
            e_scr[d, role, :, hi_half] = es[1]
            f_scr[d, role] = top
            l_scr[d, role] = es[0] + es[1]
            return top

        def dprob(role, d):
            dp_scr[d, role] = dot_nt(g_of(role), values_of(slot, d))

        def g_of(role):
            return qg[slot, 2 + role]

        for role in range(2):
            t_scr[role] = scores(role, 0, True)

        def far_scores(d, x):
            for role in range(2):
                t_scr[role] = jnp.maximum(t_scr[role], scores(role, d, False))
            for role in range(2):
                dprob(role, d)
            return x

        lax.fori_loop(1, dm + 1, far_scores, 0)

        for role in range(2):
            top = jnp.broadcast_to(jnp.max(t_scr[role], axis=1, keepdims=True), (1024, 128))
            t_scr[role] = top
            f = jnp.exp2(f_scr[0, role] - top)
            f_scr[0, role] = f
            l_scr[0, role] = l_scr[0, role] * f
        dprob(0, 0)

        def far_sums(d, x):
            for role in range(2):
                f = jnp.exp2(f_scr[d, role] - t_scr[role])
                f_scr[d, role] = f
                l_scr[0, role] = l_scr[0, role] + l_scr[d, role] * f
            return x

        lax.fori_loop(1, dm + 1, far_sums, 0)

        for role in range(2):
            t_scr[role] = jnp.broadcast_to(1.0 / jnp.sum(l_scr[0, role], axis=1, keepdims=True), (1024, 128))
        dprob(1, 0)

        def weighted(role, d):
            f = f_scr[d, role] * t_scr[role]
            f_scr[d, role] = f
            for half in (lo_half, hi_half):
                p_scr[d, role, :, half] = (e_scr[d, role, :, half] * f).astype(jnp.bfloat16)
            return dot_nn(p_scr[d, role], values_of(slot, d))

        def value_grads(d):
            dv = dot_tn(p_scr[d, 0], g_of(0)) + dot_tn(p_scr[d, 1], g_of(1))
            dkv[slot, d, :, :, 256:] = dv.reshape(8, G, 256)

        for role in range(2):
            o_acc[role] = weighted(role, 0)

        def far_weighted(d, x):
            for role in range(2):
                o_acc[role] = o_acc[role] + weighted(role, d)
            value_grads(d)
            return x

        lax.fori_loop(1, dm + 1, far_weighted, 0)

        for role in range(2):
            o_low = o_acc[role].astype(jnp.bfloat16)
            outb[slot, role] = o_low
            delta = jnp.sum(g_of(role).astype(jnp.float32) * o_low.astype(jnp.float32), axis=1, keepdims=True)
            t_scr[role] = jnp.broadcast_to(delta, (1024, 128))
        value_grads(0)

        def score_grads(d):
            out = []
            for role in range(2):
                ds = [
                    (e_scr[d, role, :, half] * f_scr[d, role] * (dp_scr[d, role, :, half] - t_scr[role])).astype(jnp.bfloat16)
                    for half in (lo_half, hi_half)
                ]
                out.append(jnp.concatenate(ds, axis=1))
            dk = dot_tn(out[0], qg[slot, 0]) + dot_tn(out[1], qg[slot, 1])
            dkv[slot, d, :, :, :256] = dk.reshape(8, G, 256)
            return [dot_nn(ds, keys_of(slot, d)) for ds in out]

        dq = score_grads(0)
        for role in range(2):
            o_acc[role] = dq[role]

        def far_grads(d, x):
            dq = score_grads(d)
            for role in range(2):
                o_acc[role] = o_acc[role] + dq[role]
            return x

        lax.fori_loop(1, dm + 1, far_grads, 0)
        for role in range(2):
            outb[slot, 2 + role] = (o_acc[role] * scale).astype(jnp.bfloat16)

    @pl.when(n > 0)
    def _():
        kvs[...] = jnp.zeros_like(kvs)
        fetch(base, 0)

    def step(i, _):
        slot = lax.rem(i, 2)
        s = base + i

        @pl.when(i + 1 < n)
        def _():
            fetch(s + 1, 1 - slot)

        @pl.when(i >= 2)
        def _():
            put_wait(s - 2, slot)

        fetch_wait(s, slot)
        attend(s, slot)
        put(s, slot)
        return 0

    lax.fori_loop(0, n, step, 0)

    @pl.when(n >= 2)
    def _():
        put_wait(base + n - 2, lax.rem(n, 2))

    @pl.when(n >= 1)
    def _():
        put_wait(base + n - 1, lax.rem(n + 1, 2))


def finish_kernel(part, n_t, ways, n_alias, scale, tab, acc, *rest):
    bufs, rest = split(rest, ways)
    bufs = [bufs[d * n_t:(d + 1) * n_t] for d in range(3)]
    dk_all, dv_all, dkv_send, own, got, kb, vb, sb, sem, osem = rest[n_alias:]
    lo, hi = ((tab[ST], tab[ST + 1]), (0, tab[SPLIT]), (tab[SPLIT], NS))[part]
    n = hi - lo
    c, e = tab[CE], tab[CE + 1]

    def fetch(ss, sl):
        pltpu.make_async_copy(acc.at[ss], own.at[sl], sem.at[sl]).start()
        for d in range(3):
            cnt = tab[at(CNT, c + d + 1, d, ss)]
            off = tab[at(OFF, c + d + 1, d, ss)]

            def issue(v, slot, k, size):
                def go(ref):
                    pltpu.make_async_copy(ref.at[pl.ds(slot, size)], got.at[sl, d, pl.ds(8 - cnt + k, size)], sem.at[sl]).start()

                if len(bufs[d][v]) == 1:
                    go(bufs[d][v][0])
                else:
                    pl.when(c != 1)(lambda: go(bufs[d][v][0]))
                    pl.when(c == 1)(lambda: go(bufs[d][v][1]))

            run_copies(lambda v: tab[sg(c + d + 1, d, v)], n_t, off, cnt, issue)

    def fetch_wait(ss, sl):
        pltpu.make_async_copy(acc.at[ss], own.at[sl], sem.at[sl]).wait()
        for d in range(3):
            run_waits(tab[at(CNT, c + d + 1, d, ss)],
                      lambda size: pltpu.make_async_copy(
                          acc.at[ss, pl.ds(0, size)], got.at[sl, d, pl.ds(0, size)], sem.at[sl]).wait())

    def outputs(ss, sl):
        row = e * NS + ss
        return [
            pltpu.make_async_copy(kb.at[sl], dk_all.at[row], osem.at[sl]),
            pltpu.make_async_copy(vb.at[sl], dv_all.at[row], osem.at[sl]),
            pltpu.make_async_copy(sb.at[sl], dkv_send.at[ss], osem.at[sl]),
        ]

    @pl.when(n > 0)
    def _():
        fetch(lo, 0)

    def step(i, _):
        s = lo + i
        sl = lax.rem(i, 2)

        @pl.when(i + 1 < n)
        def _():
            fetch(s + 1, 1 - sl)

        @pl.when(i >= 2)
        def _():
            for copy in outputs(s - 2, sl):
                copy.wait()

        fetch_wait(s, sl)
        for d in range(3):
            cnt = tab[at(CNT, c + d + 1, d, s)]

            def add(k, _):
                own[sl, k] = own[sl, k] + got[sl, d, k]
                return 0

            lax.fori_loop(8 - cnt, 8, add, 0)
        mine = own[sl, pl.ds(4 * e, 4)].reshape(128, 512)
        other = own[sl, pl.ds(4 - 4 * e, 4)].reshape(128, 512)
        kb[sl] = (mine[:, :256] * scale).astype(jnp.bfloat16)
        vb[sl] = mine[:, 256:].astype(jnp.bfloat16)
        sb[sl, :, :256] = (other[:, :256] * scale).astype(jnp.bfloat16)
        sb[sl, :, 256:] = other[:, 256:].astype(jnp.bfloat16)
        for copy in outputs(s, sl):
            copy.start()
        return 0

    lax.fori_loop(0, n, step, 0)

    @pl.when(n >= 2)
    def _():
        for copy in outputs(lo + n - 2, lax.rem(n, 2)):
            copy.wait()

    @pl.when(n >= 1)
    def _():
        for copy in outputs(lo + n - 1, lax.rem(n + 1, 2)):
            copy.wait()


ANY = pl.BlockSpec(memory_space=pl.ANY)
SMEM = pl.BlockSpec(memory_space=pltpu.SMEM)
VMEM = pl.BlockSpec(memory_space=pltpu.VMEM)
BIG = pltpu.CompilerParams(vmem_limit_bytes=58 * 1024 * 1024)


def solution(mesh):
    n_dev = mesh.shape['cp']
    seq_spec = P('dp', 'cp', None, None)
    id_spec = P('dp', 'cp')
    swap = [(k, k ^ 1) for k in range(n_dev)]
    bf, f32 = jnp.bfloat16, jnp.float32
    shape = jax.ShapeDtypeStruct

    def per_device(query, keys, values, grad_out, doc_id):
        nb, piece, heads, hd = query.shape
        rows = piece * heads
        scale = hd ** -0.5
        rank = lax.axis_index('cp')
        c = rank >> 1
        e = rank & 1
        other = NS * (1 - e)
        q3 = query.reshape(nb, rows, hd)
        g3 = grad_out.reshape(nb, rows, hd)
        k3 = keys.reshape(nb, piece, hd)
        v3 = values.reshape(nb, piece, hd)

        def half(x):
            return lax.dynamic_slice_in_dim(x, other, NS, 0)

        kv_mate = lax.ppermute(jnp.concatenate([half(k3), half(v3)], axis=-1), 'cp', swap)
        docs, ks = pl.pallas_call(
            gather_kernel,
            out_shape=[shape((n_dev, nb, piece), jnp.int32), shape((nb, 128), jnp.int32)],
            in_specs=[VMEM],
            out_specs=[VMEM, VMEM],
            scratch_shapes=[pltpu.SemaphoreType.DMA((n_dev,)), pltpu.SemaphoreType.DMA((n_dev,))],
            compiler_params=pltpu.CompilerParams(has_side_effects=True),
            name="docs",
        )(doc_id)

        def tables(plan, lo, hi):
            me = jnp.stack([c, e, lo, hi]).astype(jnp.int32)
            return pl.pallas_call(
                functools.partial(table_kernel, plan),
                out_shape=shape((NTAB,), jnp.int32),
                in_specs=[SMEM, SMEM],
                out_specs=SMEM,
                name="tables",
            )(ks, me)

        def pack(plan, tab, n):
            f_cap = plan[0]
            n_t = len(f_cap[0])
            return pl.pallas_call(
                functools.partial(pack_kernel, n_t, n, [bounds(cap) for cap in f_cap]),
                in_specs=[SMEM] + [ANY] * 3,
                out_specs=[ANY] * (1 + 3 * n_t),
                out_shape=[shape((NS, 8, G, 512), bf)] + [shape((f_cap[d][t], G, 512), bf) for d in range(3) for t in range(n_t)],
                scratch_shapes=[
                    pltpu.VMEM((2, n, piece, hd), bf), pltpu.VMEM((n, 8, G, 512), bf),
                    pltpu.SemaphoreType.DMA((4,)), pltpu.SemaphoreType.DMA, pltpu.SemaphoreType.DMA,
                ],
                name="pack",
            )(tab, k3, v3, kv_mate.reshape(NS, 4, G, 512))

        def chip_hop(x, *moves):
            return lax.ppermute(x, 'cp', [(2 * a + k, 2 * b + k) for a, b in moves for k in range(2)])

        def forward_hop(x, d):
            return chip_hop(x, *[(k, k + d + 1) for k in range(NCH - d - 1)])

        def backward_hop(x, d):
            return chip_hop(x, *[(k + d + 1, k) for k in range(NCH - d - 1)])

        def attend(plan, t, tab, mates, kvcol, frecv, state):
            f_cap, b_cap = plan[:2]
            n_t = len(b_cap[0])
            live = n_t - t
            n_alias = 0 if state is None else len(state)
            mates = mates[:1] if n_t > 1 and t == 0 else mates
            n_got = min(t + 1, len(f_cap[0]))
            got = [frecv[d][u] for d in range(3) for u in range(n_got)]
            flat = [x for way in got for x in way]
            n_in = 5 + 2 * len(mates) + len(flat)
            return pl.pallas_call(
                functools.partial(compute_kernel, t, n_t, n_got, [bounds(cap) for cap in f_cap], len(mates), [len(way) for way in got], n_alias, scale),
                in_specs=[SMEM, VMEM] + [ANY] * (n_in - 2 + n_alias),
                out_specs=[ANY] * (5 + 3 * live),
                scratch_shapes=[
                    pltpu.VMEM((2, 4, rows, hd), bf), pltpu.VMEM((2, 4, rows, hd), bf),
                    pltpu.VMEM((2, 4, 8, G, 512), bf), pltpu.VMEM((2, 4, 8, G, 512), f32),
                    pltpu.VMEM((4, 2, rows, 256), f32), pltpu.VMEM((4, 2, rows, 256), f32), pltpu.VMEM((4, 2, rows, 256), bf),
                    pltpu.VMEM((4, 2, rows, 128), f32), pltpu.VMEM((4, 2, rows, 128), f32), pltpu.VMEM((2, rows, 128), f32),
                    pltpu.VMEM((2, rows, 128), jnp.int32), pltpu.VMEM((2, rows, hd), f32),
                    pltpu.SemaphoreType.DMA((2,)), pltpu.SemaphoreType.DMA((2,)),
                ],
                out_shape=[
                    shape((nb, rows, hd), bf), shape((NS, rows, hd), bf),
                    shape((nb, rows, hd), bf), shape((NS, rows, hd), bf),
                    shape((NS, 8, G, 512), f32),
                ] + [shape((b_cap[d][v], G, 512), f32) for d in range(3) for v in range(t, n_t)],
                input_output_aliases={n_in + k: k for k in range(n_alias)},
                compiler_params=BIG,
                cost_estimate=pl.CostEstimate(flops=60_000_000_000 // n_t, bytes_accessed=100_000_000 // n_t, transcendentals=0),
            )(tab, docs, q3, g3, kvcol, *[m[0] for m in mates], *[m[1] for m in mates], *flat, *([] if state is None else state))

        def finish(part, tab, acc, brecv, state):
            n_t = len(brecv[0])
            n_alias = 0 if state is None else 3
            got = [way for row in brecv for way in row]
            flat = [x for way in got for x in way]
            return pl.pallas_call(
                functools.partial(finish_kernel, part, n_t, [len(way) for way in got], n_alias, scale),
                in_specs=[SMEM] + [ANY] * (1 + len(flat) + n_alias),
                out_specs=[ANY] * 3,
                out_shape=[shape((nb, piece, hd), bf), shape((nb, piece, hd), bf), shape((NS, piece, 512), bf)],
                scratch_shapes=[
                    pltpu.VMEM((2, 8, G, 512), f32), pltpu.VMEM((2, 3, 8, G, 512), f32),
                    pltpu.VMEM((2, piece, hd), bf), pltpu.VMEM((2, piece, hd), bf), pltpu.VMEM((2, piece, 512), bf),
                    pltpu.SemaphoreType.DMA((2,)), pltpu.SemaphoreType.DMA((2,)),
                ],
                input_output_aliases={2 + len(flat) + k: k for k in range(n_alias)},
            )(tab, acc, *flat, *([] if state is None else state))

        def place(mine, send):
            got = lax.ppermute(send, 'cp', swap)
            return lax.dynamic_update_slice_in_dim(mine, got, other, 0)

        def place_kv(dk_all, dv_all, dkv_send):
            got = lax.ppermute(dkv_send, 'cp', swap)
            return (lax.dynamic_update_slice_in_dim(dk_all, got[:, :, :hd], other, 0),
                    lax.dynamic_update_slice_in_dim(dv_all, got[:, :, hd:], other, 0))

        def swap_part(x, lo, n):
            return lax.ppermute(lax.dynamic_slice_in_dim(x, other + lo, n, 0), 'cp', swap)

        def swap_all(x):
            return lax.ppermute(x, 'cp', swap)

        tab = tables(FAST, jnp.int32(0), jnp.int32(NS))

        def fast():
            n_f, n_t = len(FAST[0][0]), len(FAST[1][0])
            packed = pack(FAST, tab, NS)
            kvcol, fsend = packed[0], packed[1:]
            frecv = [[None] * n_f for _ in range(3)]
            for t in range(n_f):
                for d in range(3):
                    x = fsend[d * n_f + t]
                    if d == 0 and t in RELAY_F:
                        across = chip_hop(x, (0, 1), (2, 3))
                        mid = chip_hop(x, (1, 3))
                        frecv[0][t] = (across, chip_hop(mid, (3, 2)))
                    else:
                        frecv[d][t] = (forward_hop(x, d),)
            mates = [(swap_part(q3, 0, QA), swap_part(g3, 0, QA)),
                     (swap_all(q3), swap_all(g3))]
            state = None
            brecv = [[None] * n_t for _ in range(3)]
            for t in range(n_t):
                live = n_t - t
                outs = attend(FAST, t, tab, mates, kvcol, frecv, state)
                state = list(outs[:5]) + [outs[5 + d * live + k] for d in range(3) for k in range(1, live)]
                for d in range(3):
                    x = outs[5 + d * live]
                    if d == 0 and t in RELAY_B:
                        across = chip_hop(x, (1, 0), (3, 2))
                        mid = chip_hop(x, (2, 0))
                        brecv[0][t] = (across, chip_hop(mid, (0, 1)))
                    else:
                        brecv[d][t] = (backward_hop(x, d),)
            o_all, o_send, dq_all, dq_send, acc = state
            attn_out = place(o_all, o_send)
            grad_query = place(dq_all, dq_send)
            grads = finish(1, tab, acc, [row[:-1] for row in brecv], None)
            grads = finish(2, tab, acc, brecv, grads)
            return (attn_out, grad_query) + place_kv(*grads)

        def slow():
            mates = [(swap_part(q3, 0, NS), swap_part(g3, 0, NS))]

            def blank():
                outs = [shape((nb, rows, hd), bf), shape((NS, rows, hd), bf), shape((nb, rows, hd), bf), shape((NS, rows, hd), bf),
                        shape((NS, 8, G, 512), f32), shape((nb, piece, hd), bf), shape((nb, piece, hd), bf), shape((NS, piece, 512), bf)]
                return [jnp.zeros(o.shape, o.dtype) for o in outs]

            def one_round(i, carry):
                state, grads = list(carry[:5]), list(carry[5:])
                tab = tables(SLOW, i * SLOW_SEQS, (i + 1) * SLOW_SEQS)
                packed = pack(SLOW, tab, SLOW_SEQS)
                frecv = [[(forward_hop(packed[1 + d], d),)] for d in range(3)]
                blank_b = [jnp.zeros((SLOW[1][0][0], G, 512), f32) for _ in range(3)]
                outs = attend(SLOW, 0, tab, mates, packed[0], frecv, state + blank_b)
                brecv = [[(backward_hop(outs[5 + d], d),)] for d in range(3)]
                return tuple(outs[:5]) + tuple(finish(0, tab, outs[4], brecv, grads))

            out = lax.fori_loop(0, NS // SLOW_SEQS, one_round, tuple(blank()))
            return (place(out[0], out[1]), place(out[2], out[3])) + place_kv(*out[5:])

        attn_out, grad_query, grad_keys, grad_values = lax.cond(tab[FIT] > 0, fast, slow)
        return (attn_out.reshape(query.shape), grad_query.reshape(query.shape),
                grad_keys.reshape(keys.shape), grad_values.reshape(values.shape))

    return jax.shard_map(per_device, mesh=mesh, in_specs=(seq_spec, seq_spec, seq_spec, seq_spec, id_spec),
                         out_specs=(seq_spec, seq_spec, seq_spec, seq_spec), check_vma=False)
```

```python
import functools

import jax
import jax.numpy as jnp
from jax import lax
from jax.experimental import pallas as pl
from jax.experimental.pallas import tpu as pltpu
from jax.sharding import PartitionSpec as P

NEG_BIG = -1e30
LOG2E = 1.4426950408889634
NS = 16
CH = 2
NJ = NS // CH
AHEAD = 2


def dot_nt(a, b):
    return lax.dot_general(a, b, (((1,), (1,)), ((), ())), preferred_element_type=jnp.float32)


def dot_nn(a, b):
    return lax.dot_general(a, b, (((1,), (0,)), ((), ())), preferred_element_type=jnp.float32)


def dot_tn(a, b):
    return lax.dot_general(a, b, (((0,), (0,)), ((), ())), preferred_element_type=jnp.float32)


def remote(src, dst, send, recv, dev):
    return pltpu.make_async_remote_copy(src_ref=src, dst_ref=dst, send_sem=send, recv_sem=recv,
                                        device_id={'cp': dev}, device_id_type=pl.DeviceIdType.MESH)


def fused_kernel(scale, doc, q, g, k, v, o, dq, dk, dv, qgm, kvr, part, hold,
                 docs, kvs, qg, outb, dkv, tmp, fin, e_scr, dp_scr, p_scr, l_scr, f_scr, t_scr, docr, o_acc,
                 doc_s, doc_r, isem, osem, osend_r, q_s, q_r, kv_s, kv_r, hop_s, part_r, tsem, fsem, dsend_r, lsem, xsem, rel_s):
    rank = lax.axis_index('cp')
    n_dev = docs.shape[0]
    c = rank // 2
    e = lax.rem(rank, 2)
    mate = 2 * c + 1 - e
    other = NS * (1 - e)
    mine = NS * e

    def dev(chip):
        return 2 * chip + e

    docs[rank] = doc[...]

    def doc_copy(i):
        return remote(doc, docs.at[rank], doc_s.at[i], doc_r.at[i], lax.rem(rank + i, n_dev))

    for i in range(1, n_dev):
        doc_copy(i).start()

    def kv_parts(chip, way, j, cols):
        out = []
        for col in cols:
            for which, ref in ((0, k), (1, v)):
                out.append(remote(ref.at[pl.ds(col * NS + CH * j, CH)], kvr.at[c, pl.ds(CH * j, CH), which, pl.ds(128 * e, 128)],
                                  kv_s.at[way, which], kv_r.at[c, j], 2 * chip + col))
        return out

    def send_kv(chip, way, j):
        for copy in kv_parts(chip, way, j, (0, 1)):
            copy.start()

    def kv_forward(a, chip, j):
        return remote(kvr.at[a, pl.ds(CH * j, CH)], kvr.at[a, pl.ds(CH * j, CH)], hop_s, kv_r.at[a, j], dev(chip))

    def stream_kv(j):
        @pl.when(c == 0)
        def _():
            send_kv(1, 0, j)
            send_kv(2, 1, j)

        @pl.when(c == 1)
        def _():
            send_kv(3, 0, j)
            send_kv(0, 1, j)

        @pl.when(c == 2)
        def _():
            send_kv(3, 0, j)

    def to_mate(j):
        for which, ref in ((0, k), (1, v)):
            remote(ref.at[pl.ds(other + CH * j, CH)], kvr.at[c, pl.ds(CH * j, CH), which, pl.ds(128 * e, 128)],
                   kv_s.at[2, which], kv_r.at[c, j], mate).start()

    def rows_to_mate(j):
        for which, ref in ((0, q), (1, g)):
            remote(ref.at[pl.ds(other + CH * j, CH)], qgm.at[pl.ds(CH * j, CH), which], q_s.at[which], q_r.at[j], mate).start()

    stream_kv(0)
    to_mate(0)
    rows_to_mate(0)
    for j in range(1, AHEAD):
        stream_kv(j)
    for j in range(1, NJ):
        to_mate(j)
        rows_to_mate(j)
    for i in range(1, n_dev):
        doc_copy(i).wait()

    def arrive(j):
        remote(kvr.at[c, pl.ds(CH * j, CH), :, pl.ds(0, 128)], kvr.at[c, pl.ds(CH * j, CH), :, pl.ds(0, 128)],
               hop_s, kv_r.at[c, j], mate).wait_recv()
        remote(qgm.at[pl.ds(CH * j, CH)], qgm.at[pl.ds(CH * j, CH)], hop_s, q_r.at[j], mate).wait_recv()
        for a in range(3):
            @pl.when(a < c)
            def _():
                kv_forward(a, a, j).wait_recv()

        @pl.when(c == 1)
        def _():
            kv_forward(0, 3, j).start()

        @pl.when(c == 0)
        def _():
            kv_forward(1, 1, j).wait_recv()
            kv_forward(1, 2, j).start()

        @pl.when(j + AHEAD < NJ)
        def _():
            stream_kv(j + AHEAD)

    def inputs(s, sl):
        row = mine + s
        rows = pl.ds(128 * e, 128)
        rest = pl.ds(128 - 128 * e, 128)
        pairs = [
            (q.at[row], qg.at[sl, 0]), (g.at[row], qg.at[sl, 2]), (qgm.at[s, 0], qg.at[sl, 1]), (qgm.at[s, 1], qg.at[sl, 3]),
            (k.at[row], kvs.at[sl, 0, 0, rows]), (v.at[row], kvs.at[sl, 0, 1, rows]),
            (kvr.at[c, s, :, rest], kvs.at[sl, 0, :, rest]),
        ]
        return [pltpu.make_async_copy(src, dst, isem.at[sl, i]) for i, (src, dst) in enumerate(pairs)]

    def far_input(s, sl, d):
        return pltpu.make_async_copy(kvr.at[c - d, s], kvs.at[sl, d], isem.at[sl, 6 + d])

    def fetch(s, sl):
        for copy in inputs(s, sl):
            copy.start()
        for d in range(1, 4):
            @pl.when(d <= c)
            def _():
                far_input(s, sl, d).start()

    def fetch_wait(s, sl):
        for copy in inputs(s, sl):
            copy.wait()
        for d in range(1, 4):
            @pl.when(d <= c)
            def _():
                far_input(s, sl, d).wait()

    def row_outputs(s, sl):
        row = mine + s
        here = [pltpu.make_async_copy(outb.at[sl, 0], o.at[row], osem.at[sl, 0]),
                pltpu.make_async_copy(outb.at[sl, 2], dq.at[row], osem.at[sl, 1])]
        there = [remote(outb.at[sl, 1], o.at[row], osem.at[sl, 2], osend_r.at[0], mate),
                 remote(outb.at[sl, 3], dq.at[row], osem.at[sl, 3], osend_r.at[1], mate)]
        return here, there

    def keep(sl, d, slot, s):
        return pltpu.make_async_copy(dkv.at[sl, d], hold.at[slot, s], osem.at[sl, 4 + d])

    def give(sl, d, chip, slot, s):
        return remote(dkv.at[sl, d], part.at[slot, s], osem.at[sl, 4 + d], part_r.at[slot, s], dev(chip))

    def grads_out(s, sl, start):
        even = lax.rem(s, 2) == 0

        def local(d, slot):
            copy = keep(sl, d, slot, s)
            copy.start() if start else copy.wait()

        def away(d, chip, slot):
            copy = give(sl, d, chip, slot, s)
            copy.start() if start else copy.wait_send()

        @pl.when(c < 3)
        def _():
            local(0, 1)

        @pl.when(c == 1)
        def _():
            local(1, 0)

        @pl.when(c == 2)
        def _():
            away(2, 0, 1)
            pl.when(even)(lambda: away(1, 3, 0))
            pl.when(jnp.logical_not(even))(lambda: local(1, 0))

        @pl.when(c == 3)
        def _():
            away(3, 1, 0)
            away(1, 2, 1)
            pl.when(even)(lambda: away(2, 1, 1))
            pl.when(jnp.logical_not(even))(lambda: away(2, 2, 0))

    def put(s, sl):
        here, there = row_outputs(s, sl)
        for copy in here + there:
            copy.start()
        grads_out(s, sl, True)

    def put_wait(s, sl):
        here, there = row_outputs(s, sl)
        for copy in here:
            copy.wait()
        for copy in there:
            copy.wait_send()
        grads_out(s, sl, False)

    def final_copies(s, sl):
        row = mine + s
        rows, rest = pl.ds(128 * e, 128), pl.ds(128 - 128 * e, 128)
        here = [pltpu.make_async_copy(fin.at[sl, 0, rows], dk.at[row], fsem.at[sl, 0]),
                pltpu.make_async_copy(fin.at[sl, 1, rows], dv.at[row], fsem.at[sl, 1])]
        there = [remote(fin.at[sl, 0, rest], dk.at[row], fsem.at[sl, 2], dsend_r.at[0], mate),
                 remote(fin.at[sl, 1, rest], dv.at[row], fsem.at[sl, 3], dsend_r.at[1], mate)]
        return here, there

    def final_wait(s, sl):
        here, there = final_copies(s, sl)
        for copy in here:
            copy.wait()
        for copy in there:
            copy.wait_send()

    def finalize(s, total):
        sl = lax.rem(s, 2)

        @pl.when(s >= 2)
        def _():
            final_wait(s - 2, sl)
        fin[sl, 0] = (total[:, :256] * scale).astype(jnp.bfloat16)
        fin[sl, 1] = total[:, 256:].astype(jnp.bfloat16)
        here, there = final_copies(s, sl)
        for copy in here + there:
            copy.start()

    row_tok = lax.broadcasted_iota(jnp.int32, (1024, 128), 0) >> 3
    lane = lax.broadcasted_iota(jnp.int32, (1024, 128), 1)
    cs = scale * LOG2E
    lo_half, hi_half = slice(0, 128), slice(128, 256)

    def attend(s, slot):
        row = mine + s
        piece = (e, 1 - e)
        for role in range(2):
            dq_row = docs[2 * c + piece[role], pl.ds(row, 1), :]
            d_t = jnp.transpose(jnp.broadcast_to(dq_row, (128, 128)))
            docr[role] = jnp.broadcast_to(d_t[:, None, :], (128, 8, 128)).reshape(1024, 128)

        def g_of(role):
            return qg[slot, 2 + role]

        def scores(role, d, causal):
            sc = dot_nt(qg[slot, role], kvs[slot, d, 0]) * cs
            xs = []
            for j in range(2):
                dk_row = docs[2 * (c - d) + j, pl.ds(row, 1), :]
                vis = docr[role] == dk_row
                if causal:
                    vis = vis & (lane + 128 * j <= row_tok + 128 * piece[role])
                xs.append(jnp.where(vis, sc[:, 128 * j:128 * (j + 1)], NEG_BIG))
            top = jnp.maximum(xs[0], xs[1])
            es = [jnp.exp2(x - top) for x in xs]
            e_scr[d, role, :, lo_half] = es[0]
            e_scr[d, role, :, hi_half] = es[1]
            f_scr[d, role] = top
            l_scr[d, role] = es[0] + es[1]
            return top

        def dprob(role, d):
            dp_scr[d, role] = dot_nt(g_of(role), kvs[slot, d, 1])

        for role in range(2):
            t_scr[role] = scores(role, 0, True)

        def far_scores(d, x):
            for role in range(2):
                t_scr[role] = jnp.maximum(t_scr[role], scores(role, d, False))
            for role in range(2):
                dprob(role, d)
            return x
        lax.fori_loop(1, c + 1, far_scores, 0)

        for role in range(2):
            top = jnp.broadcast_to(jnp.max(t_scr[role], axis=1, keepdims=True), (1024, 128))
            t_scr[role] = top
            f = jnp.exp2(f_scr[0, role] - top)
            f_scr[0, role] = f
            l_scr[0, role] = l_scr[0, role] * f
        dprob(0, 0)

        def far_sums(d, x):
            for role in range(2):
                f = jnp.exp2(f_scr[d, role] - t_scr[role])
                f_scr[d, role] = f
                l_scr[0, role] = l_scr[0, role] + l_scr[d, role] * f
            return x
        lax.fori_loop(1, c + 1, far_sums, 0)

        for role in range(2):
            t_scr[role] = jnp.broadcast_to(1.0 / jnp.sum(l_scr[0, role], axis=1, keepdims=True), (1024, 128))
        dprob(1, 0)

        def weighted(role, d):
            f = f_scr[d, role] * t_scr[role]
            f_scr[d, role] = f
            for half in (lo_half, hi_half):
                p_scr[d, role, :, half] = (e_scr[d, role, :, half] * f).astype(jnp.bfloat16)
            return dot_nn(p_scr[d, role], kvs[slot, d, 1])

        def value_grads(d):
            dkv[slot, d, :, 256:] = dot_tn(p_scr[d, 0], g_of(0)) + dot_tn(p_scr[d, 1], g_of(1))

        for role in range(2):
            o_acc[role] = weighted(role, 0)

        def far_weighted(d, x):
            for role in range(2):
                o_acc[role] = o_acc[role] + weighted(role, d)
            value_grads(d)
            return x
        lax.fori_loop(1, c + 1, far_weighted, 0)

        for role in range(2):
            o_low = o_acc[role].astype(jnp.bfloat16)
            outb[slot, role] = o_low
            delta = jnp.sum(g_of(role).astype(jnp.float32) * o_low.astype(jnp.float32), axis=1, keepdims=True)
            t_scr[role] = jnp.broadcast_to(delta, (1024, 128))
        value_grads(0)

        def score_grads(d):
            out = []
            for role in range(2):
                ds = [
                    (e_scr[d, role, :, half] * f_scr[d, role] * (dp_scr[d, role, :, half] - t_scr[role])).astype(jnp.bfloat16)
                    for half in (lo_half, hi_half)
                ]
                out.append(jnp.concatenate(ds, axis=1))
            dkv[slot, d, :, :256] = dot_tn(out[0], qg[slot, 0]) + dot_tn(out[1], qg[slot, 1])
            return [dot_nn(ds, kvs[slot, d, 0]) for ds in out]

        got = score_grads(0)
        for role in range(2):
            o_acc[role] = got[role]

        def far_grads(d, x):
            got = score_grads(d)
            for role in range(2):
                o_acc[role] = o_acc[role] + got[role]
            return x
        lax.fori_loop(1, c + 1, far_grads, 0)
        for role in range(2):
            outb[slot, 2 + role] = (o_acc[role] * scale).astype(jnp.bfloat16)

    def part_wait(slot, s):
        remote(part.at[slot, s], part.at[slot, s], hop_s, part_r.at[slot, s], mate).wait_recv()

    arrive(0)
    fetch(0, 0)

    def step(s, x):
        slot = lax.rem(s, 2)

        @pl.when(s + 1 < NS)
        def _():
            @pl.when(lax.rem(s + 1, CH) == 0)
            def _():
                arrive((s + 1) // CH)
            fetch(s + 1, 1 - slot)

        @pl.when(s >= 2)
        def _():
            put_wait(s - 2, slot)
        fetch_wait(s, slot)
        attend(s, slot)

        @pl.when(c == 3)
        def _():
            @pl.when(lax.rem(s, 2) == 0)
            def _():
                part_wait(0, s)
                copy = pltpu.make_async_copy(part.at[0, s], tmp, tsem)
                copy.start()
                copy.wait()
                dkv[slot, 2] = dkv[slot, 2] + tmp[...]
        put(s, slot)

        @pl.when(c == 3)
        def _():
            finalize(s, dkv[slot, 0])
        return x

    lax.fori_loop(0, NS, step, 0)
    put_wait(NS - 2, 0)
    put_wait(NS - 1, 1)

    def load(src, i):
        return pltpu.make_async_copy(src, dkv.at[0, i], lsem.at[i])

    def passed(s, sl, chip, slot):
        return remote(dkv.at[1, sl], part.at[slot, s], xsem.at[sl], part_r.at[slot, s], dev(chip))

    def relay(s):
        return remote(part.at[2, s], part.at[1, s], rel_s.at[s], part_r.at[1, s], dev(1))

    def home(i, x):
        @pl.when(c == 0)
        def _():
            @pl.when((i < NS) & (lax.rem(i, 2) == 1))
            def _():
                part_wait(2, i)
                relay(i).start()

            @pl.when(i >= 2)
            def _():
                s = i - 2
                load(hold.at[1, s], 0).start()
                part_wait(1, s)
                load(part.at[1, s], 1).start()
                part_wait(0, s)
                load(part.at[0, s], 2).start()
                for n, src in enumerate((hold.at[1, s], part.at[1, s], part.at[0, s])):
                    load(src, n).wait()
                finalize(s, dkv[0, 0] + dkv[0, 1] + dkv[0, 2])

        @pl.when(c == 1)
        def _():
            @pl.when(i < NS)
            def _():
                sl = lax.rem(i, 2)
                load(hold.at[0, i], 0).start()
                part_wait(0, i)
                load(part.at[0, i], 1).start()

                @pl.when(i >= 2)
                def _():
                    passed(i - 2, sl, 0, 0).wait_send()
                load(hold.at[0, i], 0).wait()
                load(part.at[0, i], 1).wait()
                dkv[1, sl] = dkv[0, 0] + dkv[0, 1]
                passed(i, sl, 0, 0).start()

            @pl.when(i >= 2)
            def _():
                s = i - 2
                load(hold.at[1, s], 2).start()
                part_wait(1, s)
                load(part.at[1, s], 3).start()
                load(hold.at[1, s], 2).wait()
                load(part.at[1, s], 3).wait()
                finalize(s, dkv[0, 2] + dkv[0, 3])

        @pl.when((c == 2) & (i < NS))
        def _():
            @pl.when(lax.rem(i, 2) == 1)
            def _():
                sl = lax.rem(i // 2, 2)
                load(hold.at[0, i], 0).start()
                part_wait(0, i)
                load(part.at[0, i], 1).start()

                @pl.when(i >= 4)
                def _():
                    passed(i - 4, sl, 0, 2).wait_send()
                load(hold.at[0, i], 0).wait()
                load(part.at[0, i], 1).wait()
                dkv[1, sl] = dkv[0, 0] + dkv[0, 1]
                passed(i, sl, 0, 2).start()
            load(hold.at[1, i], 2).start()
            part_wait(1, i)
            load(part.at[1, i], 3).start()
            load(hold.at[1, i], 2).wait()
            load(part.at[1, i], 3).wait()
            finalize(i, dkv[0, 2] + dkv[0, 3])
        return x

    @pl.when(c < 3)
    def _():
        lax.fori_loop(0, NS + 2, home, 0)

    @pl.when(c == 0)
    def _():
        for s in range(1, NS, 2):
            relay(s).wait_send()
        remote(kvr.at[1], kvr.at[1], hop_s, kv_r.at[0, 0], mate).wait_send()

    @pl.when(c == 1)
    def _():
        passed(NS - 2, 0, 0, 0).wait_send()
        passed(NS - 1, 1, 0, 0).wait_send()
        remote(kvr.at[0], kvr.at[0], hop_s, kv_r.at[0, 0], mate).wait_send()

    @pl.when(c == 2)
    def _():
        passed(NS - 3, (NS - 3) // 2 % 2, 0, 2).wait_send()
        passed(NS - 1, (NS - 1) // 2 % 2, 0, 2).wait_send()
    final_wait(NS - 2, 0)
    final_wait(NS - 1, 1)
    for which, ref in ((0, k), (1, v)):
        for way in range(2):
            @pl.when((c < 2) | ((c == 2) & (way == 0)))
            def _():
                remote(ref, ref, kv_s.at[way, which], kv_r.at[0, 0], mate).wait_send()
        half = ref.at[pl.ds(other, NS)]
        remote(half, half, kv_s.at[2, which], kv_r.at[0, 0], mate).wait_send()
    for which, ref in ((0, q), (1, g)):
        half = ref.at[pl.ds(other, NS)]
        remote(half, half, q_s.at[which], q_r.at[0], mate).wait_send()
    for which, ref in ((0, o), (1, dq)):
        half = ref.at[pl.ds(other, NS)]
        remote(half, half, hop_s, osend_r.at[which], mate).wait_recv()
    for which, ref in ((0, dk), (1, dv)):
        half = ref.at[pl.ds(other, NS)]
        remote(half, half, hop_s, dsend_r.at[which], mate).wait_recv()


ANY = pl.BlockSpec(memory_space=pl.ANY)
VMEM = pl.BlockSpec(memory_space=pltpu.VMEM)


def solution(mesh):
    n_dev = mesh.shape['cp']
    seq_spec = P('dp', 'cp', None, None)
    id_spec = P('dp', 'cp')
    bf, f32 = jnp.bfloat16, jnp.float32
    shape = jax.ShapeDtypeStruct
    dma = pltpu.SemaphoreType.DMA

    def per_device(query, keys, values, grad_out, doc_id):
        nb, piece, heads, hd = query.shape
        rows = piece * heads
        outs = pl.pallas_call(
            functools.partial(fused_kernel, hd ** -0.5),
            in_specs=[VMEM] + [ANY] * 4,
            out_specs=[ANY] * 8,
            out_shape=[
                shape((nb, rows, hd), bf), shape((nb, rows, hd), bf), shape((nb, piece, hd), bf), shape((nb, piece, hd), bf),
                shape((NS, 2, rows, hd), bf), shape((4, NS, 2, 256, 256), bf),
                shape((3, NS, 256, 512), f32), shape((2, NS, 256, 512), f32),
            ],
            scratch_shapes=[
                pltpu.VMEM((n_dev, nb, piece), jnp.int32), pltpu.VMEM((2, 4, 2, 256, 256), bf), pltpu.VMEM((2, 4, rows, hd), bf),
                pltpu.VMEM((2, 4, rows, hd), bf), pltpu.VMEM((2, 4, 256, 512), f32), pltpu.VMEM((256, 512), f32),
                pltpu.VMEM((2, 2, 256, 256), bf),
                pltpu.VMEM((4, 2, rows, 256), f32), pltpu.VMEM((4, 2, rows, 256), f32), pltpu.VMEM((4, 2, rows, 256), bf),
                pltpu.VMEM((4, 2, rows, 128), f32), pltpu.VMEM((4, 2, rows, 128), f32), pltpu.VMEM((2, rows, 128), f32),
                pltpu.VMEM((2, rows, 128), jnp.int32), pltpu.VMEM((2, rows, hd), f32),
                dma((n_dev,)), dma((n_dev,)), dma((2, 10)), dma((2, 8)), dma((2,)), dma((2,)), dma((NJ,)), dma((3, 2)), dma((4, NJ)),
                dma, dma((3, NS)), dma, dma((2, 4)), dma((2,)), dma((4,)), dma((2,)), dma((NS,)),
            ],
            compiler_params=pltpu.CompilerParams(has_side_effects=True, vmem_limit_bytes=62 * 1024 * 1024),
            name="attend",
        )(doc_id, query.reshape(nb, rows, hd), grad_out.reshape(nb, rows, hd), keys.reshape(nb, piece, hd), values.reshape(nb, piece, hd))
        o, dq, dk, dv = outs[:4]
        return o.reshape(query.shape), dq.reshape(query.shape), dk.reshape(keys.shape), dv.reshape(values.shape)

    return jax.shard_map(per_device, mesh=mesh, in_specs=(seq_spec, seq_spec, seq_spec, seq_spec, id_spec),
                         out_specs=(seq_spec, seq_spec, seq_spec, seq_spec), check_vma=False)
```

```python
import functools

import jax
import jax.numpy as jnp
from jax import lax
from jax.experimental import pallas as pl
from jax.experimental.pallas import tpu as pltpu
from jax.sharding import PartitionSpec as P

NEG_BIG = -1e30
LOG2E = 1.4426950408889634
NS = 16
CH = 2
NJ = NS // CH
AHEAD = 2
NG = 4
ROUND = (0, 2, 4, 6, 8, 10, 11, 12)


def dot_nt(a, b):
    return lax.dot_general(a, b, (((1,), (1,)), ((), ())), preferred_element_type=jnp.float32)


def dot_nn(a, b):
    return lax.dot_general(a, b, (((1,), (0,)), ((), ())), preferred_element_type=jnp.float32)


def dot_tn(a, b):
    return lax.dot_general(a, b, (((0,), (0,)), ((), ())), preferred_element_type=jnp.float32)


def remote(src, dst, send, recv, dev):
    return pltpu.make_async_remote_copy(src_ref=src, dst_ref=dst, send_sem=send, recv_sem=recv,
                                        device_id={'cp': dev}, device_id_type=pl.DeviceIdType.MESH)


def fused_kernel(scale, doc, q, g, k, v, o, dq, dk, dv, qgm, kvr, part, hold,
                 docs, kvs, qg, outb, dkv, tmp, fin, e_scr, dp_scr, p_scr, l_scr, f_scr, t_scr, docr, o_acc,
                 doc_s, doc_r, isem, osem, gsem, osend_r, q_s, q_r, kv_s, kv_r, hop_s, part_r, tsem, fsem, dsend_r, lsem, xsem, rel_s):
    rank = lax.axis_index('cp')
    n_dev = docs.shape[0]
    c = rank // 2
    e = lax.rem(rank, 2)
    mate = 2 * c + 1 - e
    other = NS * (1 - e)
    mine = NS * e

    def dev(chip):
        return 2 * chip + e

    docs[rank] = doc[...]

    def doc_copy(i):
        return remote(doc, docs.at[rank], doc_s.at[i], doc_r.at[i], lax.rem(rank + i, n_dev))

    for i in range(1, n_dev):
        doc_copy(i).start()

    def kv_parts(chip, way, j, cols):
        out = []
        for col in cols:
            for which, ref in ((0, k), (1, v)):
                out.append(remote(ref.at[pl.ds(col * NS + CH * j, CH)], kvr.at[c, pl.ds(CH * j, CH), which, pl.ds(128 * e, 128)],
                                  kv_s.at[way, which], kv_r.at[c, j], 2 * chip + col))
        return out

    def send_kv(chip, way, j):
        for copy in kv_parts(chip, way, j, (0, 1)):
            copy.start()

    def kv_forward(a, chip, j):
        return remote(kvr.at[a, pl.ds(CH * j, CH)], kvr.at[a, pl.ds(CH * j, CH)], hop_s, kv_r.at[a, j], dev(chip))

    def stream_kv(j):
        @pl.when(c == 0)
        def _():
            send_kv(1, 0, j)
            send_kv(2, 1, j)

        @pl.when(c == 1)
        def _():
            send_kv(3, 0, j)
            send_kv(0, 1, j)

        @pl.when(c == 2)
        def _():
            send_kv(3, 0, j)

    def to_mate(j):
        for which, ref in ((0, k), (1, v)):
            remote(ref.at[pl.ds(other + CH * j, CH)], kvr.at[c, pl.ds(CH * j, CH), which, pl.ds(128 * e, 128)],
                   kv_s.at[2, which], kv_r.at[c, j], mate).start()

    def rows_to_mate(j):
        for which, ref in ((0, q), (1, g)):
            remote(ref.at[pl.ds(other + CH * j, CH)], qgm.at[pl.ds(CH * j, CH), which], q_s.at[which], q_r.at[j], mate).start()

    stream_kv(0)
    to_mate(0)
    rows_to_mate(0)
    for j in range(1, AHEAD):
        stream_kv(j)
    for j in range(1, NJ):
        to_mate(j)
        rows_to_mate(j)
    for i in range(1, n_dev):
        doc_copy(i).wait()

    def arrive(j):
        remote(kvr.at[c, pl.ds(CH * j, CH), :, pl.ds(0, 128)], kvr.at[c, pl.ds(CH * j, CH), :, pl.ds(0, 128)],
               hop_s, kv_r.at[c, j], mate).wait_recv()
        remote(qgm.at[pl.ds(CH * j, CH)], qgm.at[pl.ds(CH * j, CH)], hop_s, q_r.at[j], mate).wait_recv()
        for a in range(3):
            @pl.when(a < c)
            def _():
                kv_forward(a, a, j).wait_recv()

        @pl.when(c == 1)
        def _():
            kv_forward(0, 3, j).start()

        @pl.when(c == 0)
        def _():
            kv_forward(1, 1, j).wait_recv()
            kv_forward(1, 2, j).start()

        @pl.when(j + AHEAD < NJ)
        def _():
            stream_kv(j + AHEAD)

    def inputs(s, sl):
        row = mine + s
        rows = pl.ds(128 * e, 128)
        rest = pl.ds(128 - 128 * e, 128)
        pairs = [
            (q.at[row], qg.at[sl, 0]), (g.at[row], qg.at[sl, 2]), (qgm.at[s, 0], qg.at[sl, 1]), (qgm.at[s, 1], qg.at[sl, 3]),
            (k.at[row], kvs.at[sl, 0, 0, rows]), (v.at[row], kvs.at[sl, 0, 1, rows]),
            (kvr.at[c, s, :, rest], kvs.at[sl, 0, :, rest]),
        ]
        return [pltpu.make_async_copy(src, dst, isem.at[sl, i]) for i, (src, dst) in enumerate(pairs)]

    def far_input(s, sl, d):
        return pltpu.make_async_copy(kvr.at[c - d, s], kvs.at[sl, d], isem.at[sl, 6 + d])

    def fetch(s, sl):
        for copy in inputs(s, sl):
            copy.start()
        for d in range(1, 4):
            @pl.when(d <= c)
            def _():
                far_input(s, sl, d).start()

    def fetch_wait(s, sl):
        for copy in inputs(s, sl):
            copy.wait()
        for d in range(1, 4):
            @pl.when(d <= c)
            def _():
                far_input(s, sl, d).wait()

    def row_outputs(s, sl):
        row = mine + s
        here = [pltpu.make_async_copy(outb.at[sl, 0], o.at[row], osem.at[sl, 0]),
                pltpu.make_async_copy(outb.at[sl, 2], dq.at[row], osem.at[sl, 1])]
        there = [remote(outb.at[sl, 1], o.at[row], osem.at[sl, 2], osend_r.at[0], mate),
                 remote(outb.at[sl, 3], dq.at[row], osem.at[sl, 3], osend_r.at[1], mate)]
        return here, there

    def keep(sl, d, slot, s):
        return pltpu.make_async_copy(dkv.at[sl, d], hold.at[slot, s], gsem.at[sl, d])

    def give(sl, d, chip, slot, s):
        return remote(dkv.at[sl, d], part.at[slot, s], gsem.at[sl, d], part_r.at[slot, s], dev(chip))

    def around(s):
        out = jnp.bool_(False)
        for one in ROUND:
            out = out | (s == one)
        return out

    def grads_out(s, start):
        even = jnp.logical_not(around(s))
        sl = lax.rem(s, NG)

        def local(d, slot):
            copy = keep(sl, d, slot, s)
            copy.start() if start else copy.wait()

        def away(d, chip, slot):
            copy = give(sl, d, chip, slot, s)
            copy.start() if start else copy.wait_send()

        @pl.when(c < 3)
        def _():
            local(0, 1)

        @pl.when(c == 1)
        def _():
            local(1, 0)

        @pl.when(c == 2)
        def _():
            away(2, 0, 1)
            pl.when(even)(lambda: away(1, 3, 0))
            pl.when(jnp.logical_not(even))(lambda: local(1, 0))

        @pl.when(c == 3)
        def _():
            away(3, 1, 0)
            away(1, 2, 1)
            pl.when(even)(lambda: away(2, 1, 1))
            pl.when(jnp.logical_not(even))(lambda: away(2, 2, 0))

    def put(s, sl):
        here, there = row_outputs(s, sl)
        for copy in here + there:
            copy.start()
        grads_out(s, True)

    def put_wait(s, sl):
        here, there = row_outputs(s, sl)
        for copy in here:
            copy.wait()
        for copy in there:
            copy.wait_send()

    def final_copies(s, sl):
        row = mine + s
        rows, rest = pl.ds(128 * e, 128), pl.ds(128 - 128 * e, 128)
        here = [pltpu.make_async_copy(fin.at[sl, 0, rows], dk.at[row], fsem.at[sl, 0]),
                pltpu.make_async_copy(fin.at[sl, 1, rows], dv.at[row], fsem.at[sl, 1])]
        there = [remote(fin.at[sl, 0, rest], dk.at[row], fsem.at[sl, 2], dsend_r.at[0], mate),
                 remote(fin.at[sl, 1, rest], dv.at[row], fsem.at[sl, 3], dsend_r.at[1], mate)]
        return here, there

    def final_wait(s, sl):
        here, there = final_copies(s, sl)
        for copy in here:
            copy.wait()
        for copy in there:
            copy.wait_send()

    def finalize(s, total):
        sl = lax.rem(s, 2)

        @pl.when(s >= 2)
        def _():
            final_wait(s - 2, sl)
        fin[sl, 0] = (total[:, :256] * scale).astype(jnp.bfloat16)
        fin[sl, 1] = total[:, 256:].astype(jnp.bfloat16)
        here, there = final_copies(s, sl)
        for copy in here + there:
            copy.start()

    row_tok = lax.broadcasted_iota(jnp.int32, (1024, 128), 0) >> 3
    lane = lax.broadcasted_iota(jnp.int32, (1024, 128), 1)
    cs = scale * LOG2E
    lo_half, hi_half = slice(0, 128), slice(128, 256)

    def attend(s, slot):
        row = mine + s
        gslot = lax.rem(s, NG)
        piece = (e, 1 - e)
        for role in range(2):
            dq_row = docs[2 * c + piece[role], pl.ds(row, 1), :]
            d_t = jnp.transpose(jnp.broadcast_to(dq_row, (128, 128)))
            docr[role] = jnp.broadcast_to(d_t[:, None, :], (128, 8, 128)).reshape(1024, 128)

        def g_of(role):
            return qg[slot, 2 + role]

        def scores(role, d, causal):
            sc = dot_nt(qg[slot, role], kvs[slot, d, 0]) * cs
            xs = []
            for j in range(2):
                dk_row = docs[2 * (c - d) + j, pl.ds(row, 1), :]
                vis = docr[role] == dk_row
                if causal:
                    vis = vis & (lane + 128 * j <= row_tok + 128 * piece[role])
                xs.append(jnp.where(vis, sc[:, 128 * j:128 * (j + 1)], NEG_BIG))
            top = jnp.maximum(xs[0], xs[1])
            es = [jnp.exp2(x - top) for x in xs]
            e_scr[d, role, :, lo_half] = es[0]
            e_scr[d, role, :, hi_half] = es[1]
            f_scr[d, role] = top
            l_scr[d, role] = es[0] + es[1]
            return top

        def dprob(role, d):
            dp_scr[d, role] = dot_nt(g_of(role), kvs[slot, d, 1])

        for role in range(2):
            t_scr[role] = scores(role, 0, True)

        def far_scores(d, x):
            for role in range(2):
                t_scr[role] = jnp.maximum(t_scr[role], scores(role, d, False))
            for role in range(2):
                dprob(role, d)
            return x
        lax.fori_loop(1, c + 1, far_scores, 0)

        for role in range(2):
            top = jnp.broadcast_to(jnp.max(t_scr[role], axis=1, keepdims=True), (1024, 128))
            t_scr[role] = top
            f = jnp.exp2(f_scr[0, role] - top)
            f_scr[0, role] = f
            l_scr[0, role] = l_scr[0, role] * f
        dprob(0, 0)

        def far_sums(d, x):
            for role in range(2):
                f = jnp.exp2(f_scr[d, role] - t_scr[role])
                f_scr[d, role] = f
                l_scr[0, role] = l_scr[0, role] + l_scr[d, role] * f
            return x
        lax.fori_loop(1, c + 1, far_sums, 0)

        for role in range(2):
            t_scr[role] = jnp.broadcast_to(1.0 / jnp.sum(l_scr[0, role], axis=1, keepdims=True), (1024, 128))
        dprob(1, 0)

        def weighted(role, d):
            f = f_scr[d, role] * t_scr[role]
            f_scr[d, role] = f
            for half in (lo_half, hi_half):
                p_scr[d, role, :, half] = (e_scr[d, role, :, half] * f).astype(jnp.bfloat16)
            return dot_nn(p_scr[d, role], kvs[slot, d, 1])

        def value_grads(d):
            dkv[gslot, d, :, 256:] = dot_tn(p_scr[d, 0], g_of(0)) + dot_tn(p_scr[d, 1], g_of(1))

        for role in range(2):
            o_acc[role] = weighted(role, 0)

        def far_weighted(d, x):
            for role in range(2):
                o_acc[role] = o_acc[role] + weighted(role, d)
            value_grads(d)
            return x
        lax.fori_loop(1, c + 1, far_weighted, 0)

        for role in range(2):
            o_low = o_acc[role].astype(jnp.bfloat16)
            outb[slot, role] = o_low
            delta = jnp.sum(g_of(role).astype(jnp.float32) * o_low.astype(jnp.float32), axis=1, keepdims=True)
            t_scr[role] = jnp.broadcast_to(delta, (1024, 128))
        value_grads(0)

        def score_grads(d):
            out = []
            for role in range(2):
                ds = [
                    (e_scr[d, role, :, half] * f_scr[d, role] * (dp_scr[d, role, :, half] - t_scr[role])).astype(jnp.bfloat16)
                    for half in (lo_half, hi_half)
                ]
                out.append(jnp.concatenate(ds, axis=1))
            dkv[gslot, d, :, :256] = dot_tn(out[0], qg[slot, 0]) + dot_tn(out[1], qg[slot, 1])
            return [dot_nn(ds, kvs[slot, d, 0]) for ds in out]

        got = score_grads(0)
        for role in range(2):
            o_acc[role] = got[role]

        def far_grads(d, x):
            got = score_grads(d)
            for role in range(2):
                o_acc[role] = o_acc[role] + got[role]
            return x
        lax.fori_loop(1, c + 1, far_grads, 0)
        for role in range(2):
            outb[slot, 2 + role] = (o_acc[role] * scale).astype(jnp.bfloat16)

    def part_wait(slot, s):
        remote(part.at[slot, s], part.at[slot, s], hop_s, part_r.at[slot, s], mate).wait_recv()

    arrive(0)
    fetch(0, 0)

    def step(s, x):
        slot = lax.rem(s, 2)

        @pl.when(s + 1 < NS)
        def _():
            @pl.when(lax.rem(s + 1, CH) == 0)
            def _():
                arrive((s + 1) // CH)
            fetch(s + 1, 1 - slot)

        @pl.when(s >= 2)
        def _():
            put_wait(s - 2, slot)

        @pl.when(s >= NG)
        def _():
            grads_out(s - NG, False)
        fetch_wait(s, slot)
        attend(s, slot)

        @pl.when(c == 3)
        def _():
            gslot = lax.rem(s, NG)

            @pl.when(jnp.logical_not(around(s)))
            def _():
                part_wait(0, s)
                copy = pltpu.make_async_copy(part.at[0, s], tmp, tsem)
                copy.start()
                copy.wait()
                dkv[gslot, 2] = dkv[gslot, 2] + tmp[...]
            finalize(s, dkv[gslot, 0])
        put(s, slot)
        return x

    lax.fori_loop(0, NS, step, 0)
    put_wait(NS - 2, 0)
    put_wait(NS - 1, 1)
    for s in range(NS - NG, NS):
        grads_out(s, False)

    def load(src, i):
        return pltpu.make_async_copy(src, dkv.at[0, i], lsem.at[i])

    def passed(s, sl, chip, slot):
        return remote(dkv.at[1, sl], part.at[slot, s], xsem.at[sl], part_r.at[slot, s], dev(chip))

    def relay(s):
        return remote(part.at[2, s], part.at[1, s], rel_s.at[s], part_r.at[1, s], dev(1))

    def home(i, x):
        @pl.when(c == 0)
        def _():
            @pl.when(around(i))
            def _():
                part_wait(2, i)
                relay(i).start()

            @pl.when(i >= 2)
            def _():
                s = i - 2
                load(hold.at[1, s], 0).start()
                part_wait(1, s)
                load(part.at[1, s], 1).start()
                part_wait(0, s)
                load(part.at[0, s], 2).start()
                for n, src in enumerate((hold.at[1, s], part.at[1, s], part.at[0, s])):
                    load(src, n).wait()
                finalize(s, dkv[0, 0] + dkv[0, 1] + dkv[0, 2])

        @pl.when(c == 1)
        def _():
            @pl.when(i < NS)
            def _():
                sl = lax.rem(i, 2)
                load(hold.at[0, i], 0).start()
                part_wait(0, i)
                load(part.at[0, i], 1).start()

                @pl.when(i >= 2)
                def _():
                    passed(i - 2, sl, 0, 0).wait_send()
                load(hold.at[0, i], 0).wait()
                load(part.at[0, i], 1).wait()
                dkv[1, sl] = dkv[0, 0] + dkv[0, 1]
                passed(i, sl, 0, 0).start()

            @pl.when(i >= 2)
            def _():
                s = i - 2
                load(hold.at[1, s], 2).start()
                part_wait(1, s)
                load(part.at[1, s], 3).start()
                load(hold.at[1, s], 2).wait()
                load(part.at[1, s], 3).wait()
                finalize(s, dkv[0, 2] + dkv[0, 3])

        @pl.when((c == 2) & (i < NS))
        def _():
            @pl.when(around(i))
            def _():
                sl = lax.rem(i, 4)
                load(hold.at[0, i], 0).start()
                part_wait(0, i)
                load(part.at[0, i], 1).start()

                @pl.when((i >= 4) & around(i - 4))
                def _():
                    passed(i - 4, sl, 0, 2).wait_send()
                load(hold.at[0, i], 0).wait()
                load(part.at[0, i], 1).wait()
                dkv[1, sl] = dkv[0, 0] + dkv[0, 1]
                passed(i, sl, 0, 2).start()
            load(hold.at[1, i], 2).start()
            part_wait(1, i)
            load(part.at[1, i], 3).start()
            load(hold.at[1, i], 2).wait()
            load(part.at[1, i], 3).wait()
            finalize(i, dkv[0, 2] + dkv[0, 3])
        return x

    @pl.when(c < 3)
    def _():
        lax.fori_loop(0, NS + 2, home, 0)

    @pl.when(c == 0)
    def _():
        for s in ROUND:
            relay(s).wait_send()
        remote(kvr.at[1], kvr.at[1], hop_s, kv_r.at[0, 0], mate).wait_send()

    @pl.when(c == 1)
    def _():
        passed(NS - 2, 0, 0, 0).wait_send()
        passed(NS - 1, 1, 0, 0).wait_send()
        remote(kvr.at[0], kvr.at[0], hop_s, kv_r.at[0, 0], mate).wait_send()

    @pl.when(c == 2)
    def _():
        for s in ROUND:
            if s + 4 not in ROUND:
                passed(s, s % 4, 0, 2).wait_send()
    final_wait(NS - 2, 0)
    final_wait(NS - 1, 1)
    for which, ref in ((0, k), (1, v)):
        for way in range(2):
            @pl.when((c < 2) | ((c == 2) & (way == 0)))
            def _():
                remote(ref, ref, kv_s.at[way, which], kv_r.at[0, 0], mate).wait_send()
        half = ref.at[pl.ds(other, NS)]
        remote(half, half, kv_s.at[2, which], kv_r.at[0, 0], mate).wait_send()
    for which, ref in ((0, q), (1, g)):
        half = ref.at[pl.ds(other, NS)]
        remote(half, half, q_s.at[which], q_r.at[0], mate).wait_send()
    for which, ref in ((0, o), (1, dq)):
        half = ref.at[pl.ds(other, NS)]
        remote(half, half, hop_s, osend_r.at[which], mate).wait_recv()
    for which, ref in ((0, dk), (1, dv)):
        half = ref.at[pl.ds(other, NS)]
        remote(half, half, hop_s, dsend_r.at[which], mate).wait_recv()


ANY = pl.BlockSpec(memory_space=pl.ANY)
VMEM = pl.BlockSpec(memory_space=pltpu.VMEM)


def solution(mesh):
    n_dev = mesh.shape['cp']
    seq_spec = P('dp', 'cp', None, None)
    id_spec = P('dp', 'cp')
    bf, f32 = jnp.bfloat16, jnp.float32
    shape = jax.ShapeDtypeStruct
    dma = pltpu.SemaphoreType.DMA

    def per_device(query, keys, values, grad_out, doc_id):
        nb, piece, heads, hd = query.shape
        rows = piece * heads
        outs = pl.pallas_call(
            functools.partial(fused_kernel, hd ** -0.5),
            in_specs=[VMEM] + [ANY] * 4,
            out_specs=[ANY] * 8,
            out_shape=[
                shape((nb, rows, hd), bf), shape((nb, rows, hd), bf), shape((nb, piece, hd), bf), shape((nb, piece, hd), bf),
                shape((NS, 2, rows, hd), bf), shape((4, NS, 2, 256, 256), bf),
                shape((3, NS, 256, 512), f32), shape((2, NS, 256, 512), f32),
            ],
            scratch_shapes=[
                pltpu.VMEM((n_dev, nb, piece), jnp.int32), pltpu.VMEM((2, 4, 2, 256, 256), bf), pltpu.VMEM((2, 4, rows, hd), bf),
                pltpu.VMEM((2, 4, rows, hd), bf), pltpu.VMEM((NG, 4, 256, 512), f32), pltpu.VMEM((256, 512), f32),
                pltpu.VMEM((2, 2, 256, 256), bf),
                pltpu.VMEM((4, 2, rows, 256), f32), pltpu.VMEM((4, 2, rows, 256), f32), pltpu.VMEM((4, 2, rows, 256), bf),
                pltpu.VMEM((4, 2, rows, 128), f32), pltpu.VMEM((4, 2, rows, 128), f32), pltpu.VMEM((2, rows, 128), f32),
                pltpu.VMEM((2, rows, 128), jnp.int32), pltpu.VMEM((2, rows, hd), f32),
                dma((n_dev,)), dma((n_dev,)), dma((2, 10)), dma((2, 4)), dma((NG, 4)), dma((2,)), dma((2,)), dma((NJ,)), dma((3, 2)), dma((4, NJ)),
                dma, dma((3, NS)), dma, dma((2, 4)), dma((2,)), dma((4,)), dma((4,)), dma((NS,)),
            ],
            compiler_params=pltpu.CompilerParams(has_side_effects=True, vmem_limit_bytes=62 * 1024 * 1024),
            name="attend",
        )(doc_id, query.reshape(nb, rows, hd), grad_out.reshape(nb, rows, hd), keys.reshape(nb, piece, hd), values.reshape(nb, piece, hd))
        o, dq, dk, dv = outs[:4]
        return o.reshape(query.shape), dq.reshape(query.shape), dk.reshape(keys.shape), dv.reshape(values.shape)

    return jax.shard_map(per_device, mesh=mesh, in_specs=(seq_spec, seq_spec, seq_spec, seq_spec, id_spec),
                         out_specs=(seq_spec, seq_spec, seq_spec, seq_spec), check_vma=False)
```

```python
import functools

import jax
import jax.numpy as jnp
from jax import lax
from jax.experimental import pallas as pl
from jax.experimental.pallas import tpu as pltpu
from jax.sharding import PartitionSpec as P

NEG_BIG = -1e30
LOG2E = 1.4426950408889634
NS = 16
NJ = NS
AHEAD = 2
NG = 4
ROUND = (0, 1, 4, 7, 8, 9, 10, 14)
EARLY_X = {12: 0, 15: 1}
EARLY_Y = {4: 0, 6: 1, 9: 4, 12: 7, 15: 8}
LAG = (2, 5, 6)


def dot_nt(a, b):
    return lax.dot_general(a, b, (((1,), (1,)), ((), ())), preferred_element_type=jnp.float32)


def dot_nn(a, b):
    return lax.dot_general(a, b, (((1,), (0,)), ((), ())), preferred_element_type=jnp.float32)


def dot_tn(a, b):
    return lax.dot_general(a, b, (((0,), (0,)), ((), ())), preferred_element_type=jnp.float32)


def remote(src, dst, send, recv, dev):
    return pltpu.make_async_remote_copy(src_ref=src, dst_ref=dst, send_sem=send, recv_sem=recv,
                                        device_id={'cp': dev}, device_id_type=pl.DeviceIdType.MESH)


def fused_kernel(scale, doc, q, g, k, v, o, dq, dk, dv, qgm, kvr, part, hold,
                 docs, kvs, qg, outb, dkv, sums, fin, e_scr, dp_scr, p_scr, l_scr, f_scr, t_scr, docr, o_acc,
                 doc_s, doc_r, isem, osem, gsem, osend_r, q_s, q_r, kv_s, kv_r, hop_s, part_r, fsem, dsend_r, lsem, xsem, rel_s):
    rank = lax.axis_index('cp')
    n_dev = docs.shape[0]
    c = rank // 2
    e = lax.rem(rank, 2)
    mate = 2 * c + 1 - e
    other = NS * (1 - e)
    mine = NS * e

    def dev(chip):
        return 2 * chip + e

    docs[rank] = doc[...]

    def doc_copy(i):
        return remote(doc, docs.at[rank], doc_s.at[i], doc_r.at[i], lax.rem(rank + i, n_dev))

    for i in range(1, n_dev):
        doc_copy(i).start()

    def kv_parts(chip, way, j, cols):
        out = []
        for col in cols:
            for which, ref in ((0, k), (1, v)):
                out.append(remote(ref.at[pl.ds(col * NS + j, 1)], kvr.at[c, pl.ds(j, 1), which, pl.ds(128 * e, 128)],
                                  kv_s.at[way, which], kv_r.at[c, j], 2 * chip + col))
        return out

    def send_kv(chip, way, j):
        for copy in kv_parts(chip, way, j, (0, 1)):
            copy.start()

    def kv_forward(a, chip, j):
        return remote(kvr.at[a, pl.ds(j, 1)], kvr.at[a, pl.ds(j, 1)], hop_s, kv_r.at[a, j], dev(chip))

    def stream_kv(j):
        @pl.when(c == 0)
        def _():
            send_kv(1, 0, j)
            send_kv(2, 1, j)

        @pl.when(c == 1)
        def _():
            send_kv(0, 1, j)

        @pl.when(c == 2)
        def _():
            send_kv(3, 0, j)

    def to_mate(j):
        for which, ref in ((0, k), (1, v)):
            remote(ref.at[pl.ds(other + j, 1)], kvr.at[c, pl.ds(j, 1), which, pl.ds(128 * e, 128)],
                   kv_s.at[2, which], kv_r.at[c, j], mate).start()

    def rows_to_mate(j):
        for which, ref in ((0, q), (1, g)):
            remote(ref.at[pl.ds(other + j, 1)], qgm.at[pl.ds(j, 1), which], q_s.at[which], q_r.at[j], mate).start()

    stream_kv(0)

    @pl.when(c == 1)
    def _():
        send_kv(3, 0, 0)
    to_mate(0)
    rows_to_mate(0)
    for j in range(1, AHEAD):
        stream_kv(j)
    for j in range(1, NJ):
        to_mate(j)
        rows_to_mate(j)
    for i in range(1, n_dev):
        doc_copy(i).wait()

    def arrive(j):
        remote(kvr.at[c, pl.ds(j, 1), :, pl.ds(0, 128)], kvr.at[c, pl.ds(j, 1), :, pl.ds(0, 128)],
               hop_s, kv_r.at[c, j], mate).wait_recv()
        remote(qgm.at[pl.ds(j, 1)], qgm.at[pl.ds(j, 1)], hop_s, q_r.at[j], mate).wait_recv()
        for a in range(3):
            @pl.when(a < c)
            def _():
                kv_forward(a, a, j).wait_recv()

        @pl.when(c == 1)
        def _():
            kv_forward(0, 3, j).start()

            @pl.when(j + 1 < NJ)
            def _():
                send_kv(3, 0, j + 1)

        @pl.when(c == 0)
        def _():
            kv_forward(1, 1, j).wait_recv()
            kv_forward(1, 2, j).start()

        @pl.when(j + AHEAD < NJ)
        def _():
            stream_kv(j + AHEAD)

    def inputs(s, sl):
        row = mine + s
        rows = pl.ds(128 * e, 128)
        rest = pl.ds(128 - 128 * e, 128)
        pairs = [
            (q.at[row], qg.at[sl, 0]), (g.at[row], qg.at[sl, 2]), (qgm.at[s, 0], qg.at[sl, 1]), (qgm.at[s, 1], qg.at[sl, 3]),
            (k.at[row], kvs.at[sl, 0, 0, rows]), (v.at[row], kvs.at[sl, 0, 1, rows]),
            (kvr.at[c, s, :, rest], kvs.at[sl, 0, :, rest]),
        ]
        return [pltpu.make_async_copy(src, dst, isem.at[sl, i]) for i, (src, dst) in enumerate(pairs)]

    def far_input(s, sl, d):
        return pltpu.make_async_copy(kvr.at[c - d, s], kvs.at[sl, d], isem.at[sl, 6 + d])

    def fetch(s, sl):
        for copy in inputs(s, sl):
            copy.start()
        for d in range(1, 4):
            @pl.when(d <= c)
            def _():
                far_input(s, sl, d).start()

    def fetch_wait(s, sl):
        for copy in inputs(s, sl):
            copy.wait()
        for d in range(1, 4):
            @pl.when(d <= c)
            def _():
                far_input(s, sl, d).wait()

    def row_outputs(s, sl):
        row = mine + s
        here = [pltpu.make_async_copy(outb.at[sl, 0], o.at[row], osem.at[sl, 0]),
                pltpu.make_async_copy(outb.at[sl, 2], dq.at[row], osem.at[sl, 1])]
        there = [remote(outb.at[sl, 1], o.at[row], osem.at[sl, 2], osend_r.at[0], mate),
                 remote(outb.at[sl, 3], dq.at[row], osem.at[sl, 3], osend_r.at[1], mate)]
        return here, there

    def keep(sl, d, slot, s):
        return pltpu.make_async_copy(dkv.at[sl, d], hold.at[slot, s], gsem.at[sl, d])

    def give(sl, d, chip, slot, s):
        return remote(dkv.at[sl, d], part.at[slot, s], gsem.at[sl, d], part_r.at[slot, s], dev(chip))

    def around(s):
        out = jnp.bool_(False)
        for one in ROUND:
            out = out | (s == one)
        return out

    def grads_out(s, start):
        even = jnp.logical_not(around(s))
        sl = lax.rem(s, NG)

        def local(d, slot):
            copy = keep(sl, d, slot, s)
            copy.start() if start else copy.wait()

        def away(d, chip, slot):
            copy = give(sl, d, chip, slot, s)
            copy.start() if start else copy.wait_send()

        @pl.when(c < 3)
        def _():
            local(0, 1)

        @pl.when(c == 1)
        def _():
            local(1, 0)

        @pl.when(c == 2)
        def _():
            away(2, 0, 1)
            pl.when(even)(lambda: away(1, 3, 0))
            pl.when(jnp.logical_not(even))(lambda: local(1, 0))

        @pl.when(c == 3)
        def _():
            if not start:
                away(3, 1, 0)
            pl.when(even)(lambda: away(2, 1, 1))
            pl.when(jnp.logical_not(even))(lambda: away(2, 2, 0))
            away(1, 2, 1)

    def put(s, sl):
        here, there = row_outputs(s, sl)
        for copy in here + there:
            copy.start()
        grads_out(s, True)

    def put_wait(s, sl):
        here, there = row_outputs(s, sl)
        for copy in here:
            copy.wait()
        for copy in there:
            copy.wait_send()

    def final_copies(s, sl):
        row = mine + s
        rows, rest = pl.ds(128 * e, 128), pl.ds(128 - 128 * e, 128)
        here = [pltpu.make_async_copy(fin.at[sl, 0, rows], dk.at[row], fsem.at[sl, 0]),
                pltpu.make_async_copy(fin.at[sl, 1, rows], dv.at[row], fsem.at[sl, 1])]
        there = [remote(fin.at[sl, 0, rest], dk.at[row], fsem.at[sl, 2], dsend_r.at[0], mate),
                 remote(fin.at[sl, 1, rest], dv.at[row], fsem.at[sl, 3], dsend_r.at[1], mate)]
        return here, there

    def final_wait(s, sl):
        here, there = final_copies(s, sl)
        for copy in here:
            copy.wait()
        for copy in there:
            copy.wait_send()

    def finalize(s, total):
        sl = lax.rem(s, 2)

        @pl.when(s >= 2)
        def _():
            final_wait(s - 2, sl)
        fin[sl, 0] = (total[:, :256] * scale).astype(jnp.bfloat16)
        fin[sl, 1] = total[:, 256:].astype(jnp.bfloat16)
        here, there = final_copies(s, sl)
        for copy in here + there:
            copy.start()

    row_tok = lax.broadcasted_iota(jnp.int32, (1024, 128), 0) >> 3
    lane = lax.broadcasted_iota(jnp.int32, (1024, 128), 1)
    cs = scale * LOG2E
    lo_half, hi_half = slice(0, 128), slice(128, 256)

    def attend(s, slot):
        row = mine + s
        gslot = lax.rem(s, NG)
        piece = (e, 1 - e)
        for role in range(2):
            dq_row = docs[2 * c + piece[role], pl.ds(row, 1), :]
            d_t = jnp.transpose(jnp.broadcast_to(dq_row, (128, 128)))
            docr[role] = jnp.broadcast_to(d_t[:, None, :], (128, 8, 128)).reshape(1024, 128)

        def g_of(role):
            return qg[slot, 2 + role]

        def scores(role, d, causal):
            sc = dot_nt(qg[slot, role], kvs[slot, d, 0]) * cs
            xs = []
            for j in range(2):
                dk_row = docs[2 * (c - d) + j, pl.ds(row, 1), :]
                vis = docr[role] == dk_row
                if causal:
                    vis = vis & (lane + 128 * j <= row_tok + 128 * piece[role])
                xs.append(jnp.where(vis, sc[:, 128 * j:128 * (j + 1)], NEG_BIG))
            top = jnp.maximum(xs[0], xs[1])
            es = [jnp.exp2(x - top) for x in xs]
            e_scr[d, role, :, lo_half] = es[0]
            e_scr[d, role, :, hi_half] = es[1]
            f_scr[d, role] = top
            l_scr[d, role] = es[0] + es[1]
            return top

        def dprob(role, d):
            dp_scr[d, role] = dot_nt(g_of(role), kvs[slot, d, 1])

        for role in range(2):
            t_scr[role] = scores(role, 0, True)

        def far_scores(d, x):
            for role in range(2):
                t_scr[role] = jnp.maximum(t_scr[role], scores(role, d, False))
            for role in range(2):
                dprob(role, d)
            return x
        lax.fori_loop(1, c + 1, far_scores, 0)

        for role in range(2):
            top = jnp.broadcast_to(jnp.max(t_scr[role], axis=1, keepdims=True), (1024, 128))
            t_scr[role] = top
            f = jnp.exp2(f_scr[0, role] - top)
            f_scr[0, role] = f
            l_scr[0, role] = l_scr[0, role] * f
        dprob(0, 0)

        def far_sums(d, x):
            for role in range(2):
                f = jnp.exp2(f_scr[d, role] - t_scr[role])
                f_scr[d, role] = f
                l_scr[0, role] = l_scr[0, role] + l_scr[d, role] * f
            return x
        lax.fori_loop(1, c + 1, far_sums, 0)

        for role in range(2):
            t_scr[role] = jnp.broadcast_to(1.0 / jnp.sum(l_scr[0, role], axis=1, keepdims=True), (1024, 128))
        dprob(1, 0)

        def weighted(role, d):
            f = f_scr[d, role] * t_scr[role]
            f_scr[d, role] = f
            for half in (lo_half, hi_half):
                p_scr[d, role, :, half] = (e_scr[d, role, :, half] * f).astype(jnp.bfloat16)
            return dot_nn(p_scr[d, role], kvs[slot, d, 1])

        def value_grads(d):
            dkv[gslot, d, :, 256:] = dot_tn(p_scr[d, 0], g_of(0)) + dot_tn(p_scr[d, 1], g_of(1))

        for role in range(2):
            o_acc[role] = weighted(role, 0)

        def far_weighted(d, x):
            for role in range(2):
                o_acc[role] = o_acc[role] + weighted(role, d)
            value_grads(d)
            return x
        lax.fori_loop(1, c + 1, far_weighted, 0)

        for role in range(2):
            o_low = o_acc[role].astype(jnp.bfloat16)
            outb[slot, role] = o_low
            delta = jnp.sum(g_of(role).astype(jnp.float32) * o_low.astype(jnp.float32), axis=1, keepdims=True)
            t_scr[role] = jnp.broadcast_to(delta, (1024, 128))
        value_grads(0)

        def score_grads(d):
            out = []
            for role in range(2):
                ds = [
                    (e_scr[d, role, :, half] * f_scr[d, role] * (dp_scr[d, role, :, half] - t_scr[role])).astype(jnp.bfloat16)
                    for half in (lo_half, hi_half)
                ]
                out.append(jnp.concatenate(ds, axis=1))
            dkv[gslot, d, :, :256] = dot_tn(out[0], qg[slot, 0]) + dot_tn(out[1], qg[slot, 1])
            return [dot_nn(ds, kvs[slot, d, 0]) for ds in out]

        got = score_grads(0)
        for role in range(2):
            o_acc[role] = got[role]

        def far_grads(d, x):
            got = score_grads(d)
            for role in range(2):
                o_acc[role] = o_acc[role] + got[role]
            return x
        lax.fori_loop(1, c + 1, far_grads, 0)
        for role in range(2):
            outb[slot, 2 + role] = (o_acc[role] * scale).astype(jnp.bfloat16)

    def part_wait(slot, s):
        remote(part.at[slot, s], part.at[slot, s], hop_s, part_r.at[slot, s], mate).wait_recv()

    def load(src, i):
        return pltpu.make_async_copy(src, sums.at[i], lsem.at[i])

    def passed(s, sl, slot):
        return remote(sums.at[4 + sl], part.at[slot, s], xsem.at[sl], part_r.at[slot, s], dev(0))

    def relay(s):
        return remote(part.at[2, s], part.at[1, s], rel_s.at[s], part_r.at[1, s], dev(1))

    def pass_on(i, count, slot):
        sl = lax.rem(count, 2)
        load(hold.at[0, i], 0).start()
        part_wait(0, i)
        load(part.at[0, i], 1).start()

        @pl.when(count >= 2)
        def _():
            passed(i, sl, slot).wait_send()
        load(hold.at[0, i], 0).wait()
        load(part.at[0, i], 1).wait()
        sums[4 + sl] = sums[0] + sums[1]
        passed(i, sl, slot).start()

    def pass_x(i):
        pass_on(i, jnp.int32(i), 0)

    def pass_y(i):
        count = jnp.int32(0)
        for one in ROUND:
            count = count + jnp.where(one < i, 1, 0)
        pass_on(i, count, 2)

    def total(s, terms):
        for n, src in enumerate(terms):
            load(src, n).start()
        for n, src in enumerate(terms):
            load(src, n).wait()
        value = sums[0]
        for n in range(1, len(terms)):
            value = value + sums[n]
        finalize(s, value)

    arrive(0)
    fetch(0, 0)

    def step(s, x):
        slot = lax.rem(s, 2)

        @pl.when(s + 1 < NS)
        def _():
            arrive(s + 1)
            fetch(s + 1, 1 - slot)

        @pl.when(s >= 2)
        def _():
            put_wait(s - 2, slot)

        @pl.when(s >= NG)
        def _():
            grads_out(s - NG, False)
        fetch_wait(s, slot)
        attend(s, slot)

        @pl.when(c == 3)
        def _():
            gslot = lax.rem(s, NG)
            give(gslot, 3, 1, 0, s).start()

            @pl.when(jnp.logical_not(around(s)))
            def _():
                part_wait(0, s)
                load(part.at[0, s], 0).start()
                load(part.at[0, s], 0).wait()
                dkv[gslot, 2] = dkv[gslot, 2] + sums[0]
            finalize(s, dkv[gslot, 0])
        put(s, slot)
        for at, i in EARLY_X.items():
            pl.when((c == 1) & (s == at))(lambda: pass_x(i))
        for at, i in EARLY_Y.items():
            pl.when((c == 2) & (s == at))(lambda: pass_y(i))
        return x

    lax.fori_loop(0, NS, step, 0)
    put_wait(NS - 2, 0)
    put_wait(NS - 1, 1)
    for s in range(NS - NG, NS):
        grads_out(s, False)

    def home(i, x):
        @pl.when(c == 0)
        def _():
            @pl.when(around(i))
            def _():
                part_wait(2, i)
                relay(i).start()
            s = i - LAG[0]

            @pl.when((s >= 0) & (s < NS))
            def _():
                part_wait(1, s)
                part_wait(0, s)
                total(s, (hold.at[1, s], part.at[1, s], part.at[0, s]))

        @pl.when(c == 1)
        def _():
            pl.when((i >= len(EARLY_X)) & (i < NS))(lambda: pass_x(i))
            s = i - LAG[1]

            @pl.when((s >= 0) & (s < NS))
            def _():
                part_wait(1, s)
                total(s, (hold.at[1, s], part.at[1, s]))

        @pl.when(c == 2)
        def _():
            pl.when(around(i) & (i > max(EARLY_Y.values())))(lambda: pass_y(i))
            s = i - LAG[2]

            @pl.when((s >= 0) & (s < NS))
            def _():
                part_wait(1, s)
                total(s, (hold.at[1, s], part.at[1, s]))
        return x

    @pl.when(c < 3)
    def _():
        lax.fori_loop(0, NS + max(LAG), home, 0)

    @pl.when(c == 0)
    def _():
        for s in ROUND:
            relay(s).wait_send()
        remote(kvr.at[1], kvr.at[1], hop_s, kv_r.at[0, 0], mate).wait_send()

    @pl.when(c == 1)
    def _():
        for sl in range(2):
            passed(0, sl, 0).wait_send()
        remote(kvr.at[0], kvr.at[0], hop_s, kv_r.at[0, 0], mate).wait_send()

    @pl.when(c == 2)
    def _():
        for sl in range(2):
            passed(0, sl, 2).wait_send()
    final_wait(NS - 2, 0)
    final_wait(NS - 1, 1)
    for which, ref in ((0, k), (1, v)):
        for way in range(2):
            @pl.when((c < 2) | ((c == 2) & (way == 0)))
            def _():
                remote(ref, ref, kv_s.at[way, which], kv_r.at[0, 0], mate).wait_send()
        half = ref.at[pl.ds(other, NS)]
        remote(half, half, kv_s.at[2, which], kv_r.at[0, 0], mate).wait_send()
    for which, ref in ((0, q), (1, g)):
        half = ref.at[pl.ds(other, NS)]
        remote(half, half, q_s.at[which], q_r.at[0], mate).wait_send()
    for which, ref in ((0, o), (1, dq)):
        half = ref.at[pl.ds(other, NS)]
        remote(half, half, hop_s, osend_r.at[which], mate).wait_recv()
    for which, ref in ((0, dk), (1, dv)):
        half = ref.at[pl.ds(other, NS)]
        remote(half, half, hop_s, dsend_r.at[which], mate).wait_recv()


ANY = pl.BlockSpec(memory_space=pl.ANY)
VMEM = pl.BlockSpec(memory_space=pltpu.VMEM)


def solution(mesh):
    n_dev = mesh.shape['cp']
    seq_spec = P('dp', 'cp', None, None)
    id_spec = P('dp', 'cp')
    bf, f32 = jnp.bfloat16, jnp.float32
    shape = jax.ShapeDtypeStruct
    dma = pltpu.SemaphoreType.DMA

    def per_device(query, keys, values, grad_out, doc_id):
        nb, piece, heads, hd = query.shape
        rows = piece * heads
        outs = pl.pallas_call(
            functools.partial(fused_kernel, hd ** -0.5),
            in_specs=[VMEM] + [ANY] * 4,
            out_specs=[ANY] * 8,
            out_shape=[
                shape((nb, rows, hd), bf), shape((nb, rows, hd), bf), shape((nb, piece, hd), bf), shape((nb, piece, hd), bf),
                shape((NS, 2, rows, hd), bf), shape((4, NS, 2, 256, 256), bf),
                shape((3, NS, 256, 512), f32), shape((2, NS, 256, 512), f32),
            ],
            scratch_shapes=[
                pltpu.VMEM((n_dev, nb, piece), jnp.int32), pltpu.VMEM((2, 4, 2, 256, 256), bf), pltpu.VMEM((2, 4, rows, hd), bf),
                pltpu.VMEM((2, 4, rows, hd), bf), pltpu.VMEM((NG, 4, 256, 512), f32), pltpu.VMEM((6, 256, 512), f32),
                pltpu.VMEM((2, 2, 256, 256), bf),
                pltpu.VMEM((4, 2, rows, 256), f32), pltpu.VMEM((4, 2, rows, 256), f32), pltpu.VMEM((4, 2, rows, 256), bf),
                pltpu.VMEM((4, 2, rows, 128), f32), pltpu.VMEM((4, 2, rows, 128), f32), pltpu.VMEM((2, rows, 128), f32),
                pltpu.VMEM((2, rows, 128), jnp.int32), pltpu.VMEM((2, rows, hd), f32),
                dma((n_dev,)), dma((n_dev,)), dma((2, 10)), dma((2, 4)), dma((NG, 4)), dma((2,)), dma((2,)), dma((NJ,)), dma((3, 2)), dma((4, NJ)),
                dma, dma((3, NS)), dma((2, 4)), dma((2,)), dma((3,)), dma((2,)), dma((NS,)),
            ],
            compiler_params=pltpu.CompilerParams(has_side_effects=True, vmem_limit_bytes=62 * 1024 * 1024),
            name="attend",
        )(doc_id, query.reshape(nb, rows, hd), grad_out.reshape(nb, rows, hd), keys.reshape(nb, piece, hd), values.reshape(nb, piece, hd))
        o, dq, dk, dv = outs[:4]
        return o.reshape(query.shape), dq.reshape(query.shape), dk.reshape(keys.shape), dv.reshape(values.shape)

    return jax.shard_map(per_device, mesh=mesh, in_specs=(seq_spec, seq_spec, seq_spec, seq_spec, id_spec),
                         out_specs=(seq_spec, seq_spec, seq_spec, seq_spec), check_vma=False)
```

```python
import functools

import jax
import jax.numpy as jnp
from jax import lax
from jax.experimental import pallas as pl
from jax.experimental.pallas import tpu as pltpu
from jax.sharding import PartitionSpec as P

NEG_BIG = -1e30
LOG2E = 1.4426950408889634
NS = 16
NJ = NS
AHEAD = 2
NG = 4
ROUND = (0, 2, 4, 8, 9, 11, 13, 14)
EARLY_X = {7: 0, 10: 1, 13: 2, 15: 3}
EARLY_Y = {7: 0, 9: 2, 12: 4, 15: 8}
LAG = (4, 5, 7)


def dot_nt(a, b):
    return lax.dot_general(a, b, (((1,), (1,)), ((), ())), preferred_element_type=jnp.float32)


def dot_nn(a, b):
    return lax.dot_general(a, b, (((1,), (0,)), ((), ())), preferred_element_type=jnp.float32)


def dot_tn(a, b):
    return lax.dot_general(a, b, (((0,), (0,)), ((), ())), preferred_element_type=jnp.float32)


def remote(src, dst, send, recv, dev):
    return pltpu.make_async_remote_copy(src_ref=src, dst_ref=dst, send_sem=send, recv_sem=recv,
                                        device_id={'cp': dev}, device_id_type=pl.DeviceIdType.MESH)


def fused_kernel(scale, doc, q, g, k, v, o, dq, dk, dv, qgm, kvr, part, hold,
                 docs, kvs, qg, outb, dkv, sums, fin, e_scr, dp_scr, p_scr, l_scr, f_scr, t_scr, docr, o_acc,
                 doc_s, doc_r, isem, osem, gsem, osend_r, q_s, q_r, kv_s, kv_r, hop_s, part_r, fsem, dsend_r, lsem, xsem, rel_s):
    rank = lax.axis_index('cp')
    n_dev = docs.shape[0]
    c = rank // 2
    e = lax.rem(rank, 2)
    mate = 2 * c + 1 - e
    other = NS * (1 - e)
    mine = NS * e

    def dev(chip):
        return 2 * chip + e

    docs[rank] = doc[...]

    def doc_copy(i):
        return remote(doc, docs.at[rank], doc_s.at[i], doc_r.at[i], lax.rem(rank + i, n_dev))

    for i in range(1, n_dev):
        doc_copy(i).start()

    def kv_parts(chip, way, j, cols):
        out = []
        for col in cols:
            for which, ref in ((0, k), (1, v)):
                out.append(remote(ref.at[pl.ds(col * NS + j, 1)], kvr.at[c, pl.ds(j, 1), which, pl.ds(128 * e, 128)],
                                  kv_s.at[way, which], kv_r.at[c, j], 2 * chip + col))
        return out

    def send_kv(chip, way, j):
        for copy in kv_parts(chip, way, j, (0, 1)):
            copy.start()

    def kv_forward(a, chip, j):
        return remote(kvr.at[a, pl.ds(j, 1)], kvr.at[a, pl.ds(j, 1)], hop_s, kv_r.at[a, j], dev(chip))

    def stream_kv(j):
        @pl.when(c == 0)
        def _():
            send_kv(1, 0, j)
            send_kv(2, 1, j)

        @pl.when(c == 1)
        def _():
            send_kv(0, 1, j)

        @pl.when(c == 2)
        def _():
            send_kv(3, 0, j)

    def to_mate(j):
        for which, ref in ((0, k), (1, v)):
            remote(ref.at[pl.ds(other + j, 1)], kvr.at[c, pl.ds(j, 1), which, pl.ds(128 * e, 128)],
                   kv_s.at[2, which], kv_r.at[c, j], mate).start()

    def rows_to_mate(j):
        for which, ref in ((0, q), (1, g)):
            remote(ref.at[pl.ds(other + j, 1)], qgm.at[pl.ds(j, 1), which], q_s.at[which], q_r.at[j], mate).start()

    stream_kv(0)

    @pl.when(c == 1)
    def _():
        send_kv(3, 0, 0)
    to_mate(0)
    rows_to_mate(0)
    for j in range(1, AHEAD):
        stream_kv(j)
    for j in range(1, NJ):
        to_mate(j)
        rows_to_mate(j)
    for i in range(1, n_dev):
        doc_copy(i).wait()

    def arrive(j):
        remote(kvr.at[c, pl.ds(j, 1), :, pl.ds(0, 128)], kvr.at[c, pl.ds(j, 1), :, pl.ds(0, 128)],
               hop_s, kv_r.at[c, j], mate).wait_recv()
        remote(qgm.at[pl.ds(j, 1)], qgm.at[pl.ds(j, 1)], hop_s, q_r.at[j], mate).wait_recv()
        for a in range(3):
            @pl.when(a < c)
            def _():
                kv_forward(a, a, j).wait_recv()

        @pl.when(c == 1)
        def _():
            kv_forward(0, 3, j).start()

            @pl.when(j + 1 < NJ)
            def _():
                send_kv(3, 0, j + 1)

        @pl.when(c == 0)
        def _():
            kv_forward(1, 1, j).wait_recv()
            kv_forward(1, 2, j).start()

        @pl.when(j + AHEAD < NJ)
        def _():
            stream_kv(j + AHEAD)

    def inputs(s, sl):
        row = mine + s
        rows = pl.ds(128 * e, 128)
        rest = pl.ds(128 - 128 * e, 128)
        pairs = [
            (q.at[row], qg.at[sl, 0]), (g.at[row], qg.at[sl, 2]), (qgm.at[s, 0], qg.at[sl, 1]), (qgm.at[s, 1], qg.at[sl, 3]),
            (k.at[row], kvs.at[sl, 0, 0, rows]), (v.at[row], kvs.at[sl, 0, 1, rows]),
            (kvr.at[c, s, :, rest], kvs.at[sl, 0, :, rest]),
        ]
        return [pltpu.make_async_copy(src, dst, isem.at[sl, i]) for i, (src, dst) in enumerate(pairs)]

    def far_input(s, sl, d):
        return pltpu.make_async_copy(kvr.at[c - d, s], kvs.at[sl, d], isem.at[sl, 6 + d])

    def fetch(s, sl):
        for copy in inputs(s, sl):
            copy.start()
        for d in range(1, 4):
            @pl.when(d <= c)
            def _():
                far_input(s, sl, d).start()

    def fetch_wait(s, sl):
        for copy in inputs(s, sl):
            copy.wait()
        for d in range(1, 4):
            @pl.when(d <= c)
            def _():
                far_input(s, sl, d).wait()

    def row_outputs(s, sl):
        row = mine + s
        here = [pltpu.make_async_copy(outb.at[sl, 0], o.at[row], osem.at[sl, 0]),
                pltpu.make_async_copy(outb.at[sl, 2], dq.at[row], osem.at[sl, 1])]
        there = [remote(outb.at[sl, 1], o.at[row], osem.at[sl, 2], osend_r.at[0], mate),
                 remote(outb.at[sl, 3], dq.at[row], osem.at[sl, 3], osend_r.at[1], mate)]
        return here, there

    def keep(sl, d, slot, s):
        return pltpu.make_async_copy(dkv.at[sl, d], hold.at[slot, s], gsem.at[sl, d])

    def give(sl, d, chip, slot, s):
        return remote(dkv.at[sl, d], part.at[slot, s], gsem.at[sl, d], part_r.at[slot, s], dev(chip))

    def around(s):
        out = jnp.bool_(False)
        for one in ROUND:
            out = out | (s == one)
        return out

    def grads_out(s, start):
        even = jnp.logical_not(around(s))
        sl = lax.rem(s, NG)

        def local(d, slot):
            copy = keep(sl, d, slot, s)
            copy.start() if start else copy.wait()

        def away(d, chip, slot):
            copy = give(sl, d, chip, slot, s)
            copy.start() if start else copy.wait_send()

        @pl.when(c < 3)
        def _():
            local(0, 1)

        @pl.when(c == 1)
        def _():
            local(1, 0)

        @pl.when(c == 2)
        def _():
            away(2, 0, 1)
            pl.when(even)(lambda: away(1, 3, 0))
            pl.when(jnp.logical_not(even))(lambda: local(1, 0))

        @pl.when(c == 3)
        def _():
            if not start:
                away(3, 1, 0)
            pl.when(even)(lambda: away(2, 1, 1))
            pl.when(jnp.logical_not(even))(lambda: away(2, 2, 0))
            away(1, 2, 1)

    def put(s, sl):
        here, there = row_outputs(s, sl)
        for copy in here + there:
            copy.start()
        grads_out(s, True)

    def put_wait(s, sl):
        here, there = row_outputs(s, sl)
        for copy in here:
            copy.wait()
        for copy in there:
            copy.wait_send()

    def final_copies(s, sl):
        row = mine + s
        rows, rest = pl.ds(128 * e, 128), pl.ds(128 - 128 * e, 128)
        here = [pltpu.make_async_copy(fin.at[sl, 0, rows], dk.at[row], fsem.at[sl, 0]),
                pltpu.make_async_copy(fin.at[sl, 1, rows], dv.at[row], fsem.at[sl, 1])]
        there = [remote(fin.at[sl, 0, rest], dk.at[row], fsem.at[sl, 2], dsend_r.at[0], mate),
                 remote(fin.at[sl, 1, rest], dv.at[row], fsem.at[sl, 3], dsend_r.at[1], mate)]
        return here, there

    def final_wait(s, sl):
        here, there = final_copies(s, sl)
        for copy in here:
            copy.wait()
        for copy in there:
            copy.wait_send()

    def finalize(s, total):
        sl = lax.rem(s, 2)

        @pl.when(s >= 2)
        def _():
            final_wait(s - 2, sl)
        fin[sl, 0] = (total[:, :256] * scale).astype(jnp.bfloat16)
        fin[sl, 1] = total[:, 256:].astype(jnp.bfloat16)
        here, there = final_copies(s, sl)
        for copy in here + there:
            copy.start()

    row_tok = lax.broadcasted_iota(jnp.int32, (1024, 128), 0) >> 3
    lane = lax.broadcasted_iota(jnp.int32, (1024, 128), 1)
    cs = scale * LOG2E
    lo_half, hi_half = slice(0, 128), slice(128, 256)

    def attend(s, slot):
        row = mine + s
        gslot = lax.rem(s, NG)
        piece = (e, 1 - e)
        for role in range(2):
            dq_row = docs[2 * c + piece[role], pl.ds(row, 1), :]
            d_t = jnp.transpose(jnp.broadcast_to(dq_row, (128, 128)))
            docr[role] = jnp.broadcast_to(d_t[:, None, :], (128, 8, 128)).reshape(1024, 128)

        def g_of(role):
            return qg[slot, 2 + role]

        def far_loop(body):
            for chip in range(1, 4):
                @pl.when(c == chip)
                def _():
                    for d in range(1, chip + 1):
                        body(d, 0)

        def scores(role, d, causal):
            sc = dot_nt(qg[slot, role], kvs[slot, d, 0]) * cs
            xs = []
            for j in range(2):
                dk_row = docs[2 * (c - d) + j, pl.ds(row, 1), :]
                vis = docr[role] == dk_row
                if causal:
                    vis = vis & (lane + 128 * j <= row_tok + 128 * piece[role])
                xs.append(jnp.where(vis, sc[:, 128 * j:128 * (j + 1)], NEG_BIG))
            top = jnp.maximum(xs[0], xs[1])
            es = [jnp.exp2(x - top) for x in xs]
            e_scr[d, role, :, lo_half] = es[0]
            e_scr[d, role, :, hi_half] = es[1]
            f_scr[d, role] = top
            l_scr[d, role] = es[0] + es[1]
            return top

        def dprob(role, d):
            dp_scr[d, role] = dot_nt(g_of(role), kvs[slot, d, 1])

        for role in range(2):
            t_scr[role] = scores(role, 0, True)

        def far_scores(d, x):
            for role in range(2):
                t_scr[role] = jnp.maximum(t_scr[role], scores(role, d, False))
            for role in range(2):
                dprob(role, d)
            return x
        far_loop(far_scores)

        for role in range(2):
            t_scr[role] = jnp.broadcast_to(jnp.max(t_scr[role], axis=1, keepdims=True), (1024, 128))
        dprob(0, 0)

        for role in range(2):
            top = t_scr[role]
            norm = l_scr[0, role] * jnp.exp2(f_scr[0, role] - top)
            for d in range(1, 4):
                norm = norm + l_scr[d, role] * jnp.exp2(f_scr[d, role] - top)
            t_scr[role] = top + jnp.log2(jnp.broadcast_to(jnp.sum(norm, axis=1, keepdims=True), (1024, 128)))
        dprob(1, 0)

        def weighted(role, d):
            f = jnp.exp2(f_scr[d, role] - t_scr[role])
            f_scr[d, role] = f
            for half in (lo_half, hi_half):
                p_scr[d, role, :, half] = (e_scr[d, role, :, half] * f).astype(jnp.bfloat16)
            return dot_nn(p_scr[d, role], kvs[slot, d, 1])

        def value_grads(d):
            dkv[gslot, d, :, 256:] = dot_tn(p_scr[d, 0], g_of(0)) + dot_tn(p_scr[d, 1], g_of(1))

        for role in range(2):
            o_acc[role] = weighted(role, 0)

        def far_weighted(d, x):
            for role in range(2):
                o_acc[role] = o_acc[role] + weighted(role, d)
            value_grads(d)
            return x
        far_loop(far_weighted)

        for role in range(2):
            o_low = o_acc[role].astype(jnp.bfloat16)
            outb[slot, role] = o_low
            delta = jnp.sum(g_of(role).astype(jnp.float32) * o_low.astype(jnp.float32), axis=1, keepdims=True)
            t_scr[role] = jnp.broadcast_to(delta, (1024, 128))
        value_grads(0)

        def score_grads(d):
            out = []
            for role in range(2):
                ds = [
                    (e_scr[d, role, :, half] * f_scr[d, role] * (dp_scr[d, role, :, half] - t_scr[role])).astype(jnp.bfloat16)
                    for half in (lo_half, hi_half)
                ]
                out.append(jnp.concatenate(ds, axis=1))
            dkv[gslot, d, :, :256] = dot_tn(out[0], qg[slot, 0]) + dot_tn(out[1], qg[slot, 1])
            return [dot_nn(ds, kvs[slot, d, 0]) for ds in out]

        got = score_grads(0)
        for role in range(2):
            o_acc[role] = got[role]

        def far_grads(d, x):
            got = score_grads(d)
            for role in range(2):
                o_acc[role] = o_acc[role] + got[role]
            return x
        far_loop(far_grads)
        for role in range(2):
            outb[slot, 2 + role] = (o_acc[role] * scale).astype(jnp.bfloat16)

    def part_wait(slot, s):
        remote(part.at[slot, s], part.at[slot, s], hop_s, part_r.at[slot, s], mate).wait_recv()

    def load(src, i):
        return pltpu.make_async_copy(src, sums.at[i], lsem.at[i])

    def passed(s, sl, slot):
        return remote(sums.at[4 + sl], part.at[slot, s], xsem.at[sl], part_r.at[slot, s], dev(0))

    def relay(s):
        return remote(part.at[2, s], part.at[1, s], rel_s.at[s], part_r.at[1, s], dev(1))

    def pass_on(i, count, slot):
        sl = lax.rem(count, 2)
        load(hold.at[0, i], 0).start()
        part_wait(0, i)
        load(part.at[0, i], 1).start()

        @pl.when(count >= 2)
        def _():
            passed(i, sl, slot).wait_send()
        load(hold.at[0, i], 0).wait()
        load(part.at[0, i], 1).wait()
        sums[4 + sl] = sums[0] + sums[1]
        passed(i, sl, slot).start()

    def pass_x(i):
        pass_on(i, jnp.int32(i), 0)

    def pass_y(i):
        count = jnp.int32(0)
        for one in ROUND:
            count = count + jnp.where(one < i, 1, 0)
        pass_on(i, count, 2)

    def total(s, terms):
        for n, src in enumerate(terms):
            load(src, n).start()
        for n, src in enumerate(terms):
            load(src, n).wait()
        value = sums[0]
        for n in range(1, len(terms)):
            value = value + sums[n]
        finalize(s, value)

    for d in range(1, 4):
        f_scr[d] = jnp.full((2, 1024, 128), NEG_BIG, jnp.float32)
        l_scr[d] = jnp.zeros((2, 1024, 128), jnp.float32)
    arrive(0)
    fetch(0, 0)

    def step(s, x):
        slot = lax.rem(s, 2)

        @pl.when(s + 1 < NS)
        def _():
            arrive(s + 1)
            fetch(s + 1, 1 - slot)

        @pl.when(s >= 2)
        def _():
            put_wait(s - 2, slot)

        @pl.when(s >= NG)
        def _():
            grads_out(s - NG, False)
        fetch_wait(s, slot)
        attend(s, slot)

        @pl.when(c == 3)
        def _():
            gslot = lax.rem(s, NG)
            give(gslot, 3, 1, 0, s).start()

            @pl.when(jnp.logical_not(around(s)))
            def _():
                part_wait(0, s)
                load(part.at[0, s], 0).start()
                load(part.at[0, s], 0).wait()
                dkv[gslot, 2] = dkv[gslot, 2] + sums[0]
            finalize(s, dkv[gslot, 0])
        put(s, slot)
        for at, i in EARLY_X.items():
            pl.when((c == 1) & (s == at))(lambda: pass_x(i))
        for at, i in EARLY_Y.items():
            pl.when((c == 2) & (s == at))(lambda: pass_y(i))
        return x

    lax.fori_loop(0, NS, step, 0)
    put_wait(NS - 2, 0)
    put_wait(NS - 1, 1)
    for s in range(NS - NG, NS):
        grads_out(s, False)

    def home(i, x):
        @pl.when(c == 0)
        def _():
            @pl.when(around(i))
            def _():
                part_wait(2, i)
                relay(i).start()
            s = i - LAG[0]

            @pl.when((s >= 0) & (s < NS))
            def _():
                part_wait(1, s)
                part_wait(0, s)
                total(s, (hold.at[1, s], part.at[1, s], part.at[0, s]))

        @pl.when(c == 1)
        def _():
            pl.when((i >= len(EARLY_X)) & (i < NS))(lambda: pass_x(i))
            s = i - LAG[1]

            @pl.when((s >= 0) & (s < NS))
            def _():
                part_wait(1, s)
                total(s, (hold.at[1, s], part.at[1, s]))

        @pl.when(c == 2)
        def _():
            pl.when(around(i) & (i > max(EARLY_Y.values())))(lambda: pass_y(i))
            s = i - LAG[2]

            @pl.when((s >= 0) & (s < NS))
            def _():
                part_wait(1, s)
                total(s, (hold.at[1, s], part.at[1, s]))
        return x

    @pl.when(c < 3)
    def _():
        lax.fori_loop(0, NS + max(LAG), home, 0)

    @pl.when(c == 0)
    def _():
        for s in ROUND:
            relay(s).wait_send()
        remote(kvr.at[1], kvr.at[1], hop_s, kv_r.at[0, 0], mate).wait_send()

    @pl.when(c == 1)
    def _():
        for sl in range(2):
            passed(0, sl, 0).wait_send()
        remote(kvr.at[0], kvr.at[0], hop_s, kv_r.at[0, 0], mate).wait_send()

    @pl.when(c == 2)
    def _():
        for sl in range(2):
            passed(0, sl, 2).wait_send()
    final_wait(NS - 2, 0)
    final_wait(NS - 1, 1)
    for which, ref in ((0, k), (1, v)):
        for way in range(2):
            @pl.when((c < 2) | ((c == 2) & (way == 0)))
            def _():
                remote(ref, ref, kv_s.at[way, which], kv_r.at[0, 0], mate).wait_send()
        half = ref.at[pl.ds(other, NS)]
        remote(half, half, kv_s.at[2, which], kv_r.at[0, 0], mate).wait_send()
    for which, ref in ((0, q), (1, g)):
        half = ref.at[pl.ds(other, NS)]
        remote(half, half, q_s.at[which], q_r.at[0], mate).wait_send()
    for which, ref in ((0, o), (1, dq)):
        half = ref.at[pl.ds(other, NS)]
        remote(half, half, hop_s, osend_r.at[which], mate).wait_recv()
    for which, ref in ((0, dk), (1, dv)):
        half = ref.at[pl.ds(other, NS)]
        remote(half, half, hop_s, dsend_r.at[which], mate).wait_recv()


ANY = pl.BlockSpec(memory_space=pl.ANY)
VMEM = pl.BlockSpec(memory_space=pltpu.VMEM)


def solution(mesh):
    n_dev = mesh.shape['cp']
    seq_spec = P('dp', 'cp', None, None)
    id_spec = P('dp', 'cp')
    bf, f32 = jnp.bfloat16, jnp.float32
    shape = jax.ShapeDtypeStruct
    dma = pltpu.SemaphoreType.DMA

    def per_device(query, keys, values, grad_out, doc_id):
        nb, piece, heads, hd = query.shape
        rows = piece * heads
        outs = pl.pallas_call(
            functools.partial(fused_kernel, hd ** -0.5),
            in_specs=[VMEM] + [ANY] * 4,
            out_specs=[ANY] * 8,
            out_shape=[
                shape((nb, rows, hd), bf), shape((nb, rows, hd), bf), shape((nb, piece, hd), bf), shape((nb, piece, hd), bf),
                shape((NS, 2, rows, hd), bf), shape((4, NS, 2, 256, 256), bf),
                shape((3, NS, 256, 512), f32), shape((2, NS, 256, 512), f32),
            ],
            scratch_shapes=[
                pltpu.VMEM((n_dev, nb, piece), jnp.int32), pltpu.VMEM((2, 4, 2, 256, 256), bf), pltpu.VMEM((2, 4, rows, hd), bf),
                pltpu.VMEM((2, 4, rows, hd), bf), pltpu.VMEM((NG, 4, 256, 512), f32), pltpu.VMEM((6, 256, 512), f32),
                pltpu.VMEM((2, 2, 256, 256), bf),
                pltpu.VMEM((4, 2, rows, 256), f32), pltpu.VMEM((4, 2, rows, 256), f32), pltpu.VMEM((4, 2, rows, 256), bf),
                pltpu.VMEM((4, 2, rows, 128), f32), pltpu.VMEM((4, 2, rows, 128), f32), pltpu.VMEM((2, rows, 128), f32),
                pltpu.VMEM((2, rows, 128), jnp.int32), pltpu.VMEM((2, rows, hd), f32),
                dma((n_dev,)), dma((n_dev,)), dma((2, 10)), dma((2, 4)), dma((NG, 4)), dma((2,)), dma((2,)), dma((NJ,)), dma((3, 2)), dma((4, NJ)),
                dma, dma((3, NS)), dma((2, 4)), dma((2,)), dma((3,)), dma((2,)), dma((NS,)),
            ],
            compiler_params=pltpu.CompilerParams(has_side_effects=True, vmem_limit_bytes=62 * 1024 * 1024),
            name="attend",
        )(doc_id, query.reshape(nb, rows, hd), grad_out.reshape(nb, rows, hd), keys.reshape(nb, piece, hd), values.reshape(nb, piece, hd))
        o, dq, dk, dv = outs[:4]
        return o.reshape(query.shape), dq.reshape(query.shape), dk.reshape(keys.shape), dv.reshape(values.shape)

    return jax.shard_map(per_device, mesh=mesh, in_specs=(seq_spec, seq_spec, seq_spec, seq_spec, id_spec),
                         out_specs=(seq_spec, seq_spec, seq_spec, seq_spec), check_vma=False)
```

```python
import functools

import jax
import jax.numpy as jnp
from jax import lax
from jax.experimental import pallas as pl
from jax.experimental.pallas import tpu as pltpu
from jax.sharding import PartitionSpec as P

NEG_BIG = -1e30
LOG2E = 1.4426950408889634
NS = 16
NJ = NS
AHEAD = 2
NG = 4
ROUND = (0, 2, 4, 8, 9, 11, 13, 14)
EARLY_X = {7: 0, 10: 1, 13: 2, 15: 3}
EARLY_Y = {7: 0, 9: 2, 12: 4, 15: 8}
LAG = (4, 5, 7)


def dot_nt(a, b):
    return lax.dot_general(a, b, (((1,), (1,)), ((), ())), preferred_element_type=jnp.float32)


def dot_nn(a, b):
    return lax.dot_general(a, b, (((1,), (0,)), ((), ())), preferred_element_type=jnp.float32)


def dot_tn(a, b):
    return lax.dot_general(a, b, (((0,), (0,)), ((), ())), preferred_element_type=jnp.float32)


def remote(src, dst, send, recv, dev):
    return pltpu.make_async_remote_copy(src_ref=src, dst_ref=dst, send_sem=send, recv_sem=recv,
                                        device_id={'cp': dev}, device_id_type=pl.DeviceIdType.MESH)


def fused_kernel(scale, doc, q, g, k, v, o, dq, dk, dv, qgm, kvr, part, hold,
                 docs, kvs, qg, outb, dkv, sums, fin, e_scr, dp_scr, p_scr, l_scr, f_scr, t_scr, docr, o_acc,
                 doc_s, doc_r, isem, osem, gsem, osend_r, q_s, q_r, kv_s, kv_r, hop_s, part_r, fsem, dsend_r, lsem, xsem, rel_s):
    rank = lax.axis_index('cp')
    n_dev = docs.shape[0]
    c = rank // 2
    e = lax.rem(rank, 2)
    mate = 2 * c + 1 - e
    other = NS * (1 - e)
    mine = NS * e

    def dev(chip):
        return 2 * chip + e

    docs[rank] = doc[...]

    def doc_copy(i):
        return remote(doc, docs.at[rank], doc_s.at[i], doc_r.at[i], lax.rem(rank + i, n_dev))

    for i in range(1, n_dev):
        doc_copy(i).start()

    def kv_parts(chip, way, j, cols):
        out = []
        for col in cols:
            for which, ref in ((0, k), (1, v)):
                out.append(remote(ref.at[pl.ds(col * NS + j, 1)], kvr.at[c, pl.ds(j, 1), which, pl.ds(128 * e, 128)],
                                  kv_s.at[way, which], kv_r.at[c, j], 2 * chip + col))
        return out

    def send_kv(chip, way, j):
        for copy in kv_parts(chip, way, j, (0, 1)):
            copy.start()

    def kv_forward(a, chip, j):
        return remote(kvr.at[a, pl.ds(j, 1)], kvr.at[a, pl.ds(j, 1)], hop_s, kv_r.at[a, j], dev(chip))

    def stream_kv(j):
        @pl.when(c == 0)
        def _():
            send_kv(1, 0, j)
            send_kv(2, 1, j)

        @pl.when(c == 1)
        def _():
            send_kv(0, 1, j)

        @pl.when(c == 2)
        def _():
            send_kv(3, 0, j)

    def to_mate(j):
        for which, ref in ((0, k), (1, v)):
            remote(ref.at[pl.ds(other + j, 1)], kvr.at[c, pl.ds(j, 1), which, pl.ds(128 * e, 128)],
                   kv_s.at[2, which], kv_r.at[c, j], mate).start()

    def rows_to_mate(j):
        for which, ref in ((0, q), (1, g)):
            remote(ref.at[pl.ds(other + j, 1)], qgm.at[pl.ds(j, 1), which], q_s.at[which], q_r.at[j], mate).start()

    stream_kv(0)

    @pl.when(c == 1)
    def _():
        send_kv(3, 0, 0)
    to_mate(0)
    rows_to_mate(0)
    for j in range(1, AHEAD):
        stream_kv(j)
    for j in range(1, NJ):
        to_mate(j)
        rows_to_mate(j)
    for i in range(1, n_dev):
        doc_copy(i).wait()

    def arrive(j):
        remote(kvr.at[c, pl.ds(j, 1), :, pl.ds(0, 128)], kvr.at[c, pl.ds(j, 1), :, pl.ds(0, 128)],
               hop_s, kv_r.at[c, j], mate).wait_recv()
        remote(qgm.at[pl.ds(j, 1)], qgm.at[pl.ds(j, 1)], hop_s, q_r.at[j], mate).wait_recv()
        for a in range(3):
            @pl.when(a < c)
            def _():
                kv_forward(a, a, j).wait_recv()

        @pl.when(c == 1)
        def _():
            kv_forward(0, 3, j).start()

            @pl.when(j + 1 < NJ)
            def _():
                send_kv(3, 0, j + 1)

        @pl.when(c == 0)
        def _():
            kv_forward(1, 1, j).wait_recv()
            kv_forward(1, 2, j).start()

        @pl.when(j + AHEAD < NJ)
        def _():
            stream_kv(j + AHEAD)

    def inputs(s, sl):
        row = mine + s
        rows = pl.ds(128 * e, 128)
        rest = pl.ds(128 - 128 * e, 128)
        pairs = [
            (q.at[row], qg.at[sl, 0]), (g.at[row], qg.at[sl, 2]), (qgm.at[s, 0], qg.at[sl, 1]), (qgm.at[s, 1], qg.at[sl, 3]),
            (k.at[row], kvs.at[sl, 0, 0, rows]), (v.at[row], kvs.at[sl, 0, 1, rows]),
            (kvr.at[c, s, :, rest], kvs.at[sl, 0, :, rest]),
        ]
        return [pltpu.make_async_copy(src, dst, isem.at[sl, i]) for i, (src, dst) in enumerate(pairs)]

    def far_input(s, sl, d):
        return pltpu.make_async_copy(kvr.at[c - d, s], kvs.at[sl, d], isem.at[sl, 6 + d])

    def fetch(s, sl):
        for copy in inputs(s, sl):
            copy.start()
        for d in range(1, 4):
            @pl.when(d <= c)
            def _():
                far_input(s, sl, d).start()

    def fetch_wait(s, sl):
        for copy in inputs(s, sl):
            copy.wait()
        for d in range(1, 4):
            @pl.when(d <= c)
            def _():
                far_input(s, sl, d).wait()

    def row_outputs(s, sl):
        row = mine + s
        here = [pltpu.make_async_copy(outb.at[sl, 0], o.at[row], osem.at[sl, 0]),
                pltpu.make_async_copy(outb.at[sl, 2], dq.at[row], osem.at[sl, 1])]
        there = [remote(outb.at[sl, 1], o.at[row], osem.at[sl, 2], osend_r.at[0], mate),
                 remote(outb.at[sl, 3], dq.at[row], osem.at[sl, 3], osend_r.at[1], mate)]
        return here, there

    def keep(sl, d, slot, s):
        return pltpu.make_async_copy(dkv.at[sl, d], hold.at[slot, s], gsem.at[sl, d])

    def give(sl, d, chip, slot, s):
        return remote(dkv.at[sl, d], part.at[slot, s], gsem.at[sl, d], part_r.at[slot, s], dev(chip))

    def around(s):
        out = jnp.bool_(False)
        for one in ROUND:
            out = out | (s == one)
        return out

    def grads_out(s, start):
        even = jnp.logical_not(around(s))
        sl = lax.rem(s, NG)

        def local(d, slot):
            copy = keep(sl, d, slot, s)
            copy.start() if start else copy.wait()

        def away(d, chip, slot):
            copy = give(sl, d, chip, slot, s)
            copy.start() if start else copy.wait_send()

        @pl.when(c < 3)
        def _():
            local(0, 1)

        @pl.when(c == 1)
        def _():
            local(1, 0)

        @pl.when(c == 2)
        def _():
            away(2, 0, 1)
            pl.when(even)(lambda: away(1, 3, 0))
            pl.when(jnp.logical_not(even))(lambda: local(1, 0))

        @pl.when(c == 3)
        def _():
            if not start:
                away(3, 1, 0)
            pl.when(even)(lambda: away(2, 1, 1))
            pl.when(jnp.logical_not(even))(lambda: away(2, 2, 0))
            away(1, 2, 1)

    def put(s, sl):
        here, there = row_outputs(s, sl)
        for copy in here + there:
            copy.start()
        grads_out(s, True)

    def put_wait(s, sl):
        here, there = row_outputs(s, sl)
        for copy in here:
            copy.wait()
        for copy in there:
            copy.wait_send()

    def final_copies(s, sl):
        row = mine + s
        rows, rest = pl.ds(128 * e, 128), pl.ds(128 - 128 * e, 128)
        here = [pltpu.make_async_copy(fin.at[sl, 0, rows], dk.at[row], fsem.at[sl, 0]),
                pltpu.make_async_copy(fin.at[sl, 1, rows], dv.at[row], fsem.at[sl, 1])]
        there = [remote(fin.at[sl, 0, rest], dk.at[row], fsem.at[sl, 2], dsend_r.at[0], mate),
                 remote(fin.at[sl, 1, rest], dv.at[row], fsem.at[sl, 3], dsend_r.at[1], mate)]
        return here, there

    def final_wait(s, sl):
        here, there = final_copies(s, sl)
        for copy in here:
            copy.wait()
        for copy in there:
            copy.wait_send()

    def finalize(s, total):
        sl = lax.rem(s, 2)

        @pl.when(s >= 2)
        def _():
            final_wait(s - 2, sl)
        fin[sl, 0] = (total[:, :256] * scale).astype(jnp.bfloat16)
        fin[sl, 1] = total[:, 256:].astype(jnp.bfloat16)
        here, there = final_copies(s, sl)
        for copy in here + there:
            copy.start()

    row_tok = lax.broadcasted_iota(jnp.int32, (1024, 128), 0) >> 3
    lane = lax.broadcasted_iota(jnp.int32, (1024, 128), 1)
    cs = scale * LOG2E
    lo_half, hi_half = slice(0, 128), slice(128, 256)

    def attend(s, slot):
        row = mine + s
        gslot = lax.rem(s, NG)
        piece = (e, 1 - e)
        for role in range(2):
            dq_row = docs[2 * c + piece[role], pl.ds(row, 1), :]
            d_t = jnp.transpose(jnp.broadcast_to(dq_row, (128, 128)))
            docr[role] = jnp.broadcast_to(d_t[:, None, :], (128, 8, 128)).reshape(1024, 128)

        def g_of(role):
            return qg[slot, 2 + role]

        def far_loop(body):
            for chip in range(1, 4):
                @pl.when(c == chip)
                def _():
                    for d in range(1, chip + 1):
                        body(d, 0)

        def scores(role, d, causal):
            sc = dot_nt(qg[slot, role], kvs[slot, d, 0]) * cs
            xs = []
            for j in range(2):
                dk_row = docs[2 * (c - d) + j, pl.ds(row, 1), :]
                vis = docr[role] == dk_row
                if causal:
                    vis = vis & (lane + 128 * j <= row_tok + 128 * piece[role])
                xs.append(jnp.where(vis, sc[:, 128 * j:128 * (j + 1)], NEG_BIG))
            top = jnp.maximum(xs[0], xs[1])
            es = [jnp.exp2(x - top) for x in xs]
            e_scr[d, role, :, lo_half] = es[0]
            e_scr[d, role, :, hi_half] = es[1]
            f_scr[d, role] = top
            l_scr[d, role] = es[0] + es[1]
            return top

        def dprob(role, d):
            dp_scr[d, role] = dot_nt(g_of(role), kvs[slot, d, 1])

        for role in range(2):
            t_scr[role] = scores(role, 0, True)

        def far_scores(d, x):
            for role in range(2):
                t_scr[role] = jnp.maximum(t_scr[role], scores(role, d, False))
            for role in range(2):
                dprob(role, d)
            return x
        far_loop(far_scores)

        for role in range(2):
            t_scr[role] = jnp.broadcast_to(jnp.max(t_scr[role], axis=1, keepdims=True), (1024, 128))
        dprob(0, 0)

        for role in range(2):
            top = t_scr[role]
            norm = l_scr[0, role] * jnp.exp2(f_scr[0, role] - top)
            for d in range(1, 4):
                norm = norm + l_scr[d, role] * jnp.exp2(f_scr[d, role] - top)
            t_scr[role] = top + jnp.log2(jnp.broadcast_to(jnp.sum(norm, axis=1, keepdims=True), (1024, 128)))
        dprob(1, 0)

        def weighted(role, d):
            f = jnp.exp2(f_scr[d, role] - t_scr[role])
            f_scr[d, role] = f
            for half in (lo_half, hi_half):
                p_scr[d, role, :, half] = (e_scr[d, role, :, half] * f).astype(jnp.bfloat16)
            return dot_nn(p_scr[d, role], kvs[slot, d, 1])

        def value_grads(d):
            dkv[gslot, d, :, 256:] = dot_tn(p_scr[d, 0], g_of(0)) + dot_tn(p_scr[d, 1], g_of(1))

        for role in range(2):
            o_acc[role] = weighted(role, 0)

        def far_weighted(d, x):
            for role in range(2):
                o_acc[role] = o_acc[role] + weighted(role, d)
            value_grads(d)
            return x
        far_loop(far_weighted)

        for role in range(2):
            o_low = o_acc[role].astype(jnp.bfloat16)
            outb[slot, role] = o_low
            delta = jnp.sum(g_of(role).astype(jnp.float32) * o_low.astype(jnp.float32), axis=1, keepdims=True)
            t_scr[role] = jnp.broadcast_to(delta, (1024, 128))
        value_grads(0)

        def score_grads(d):
            out = []
            for role in range(2):
                ds = [
                    (e_scr[d, role, :, half] * f_scr[d, role] * (dp_scr[d, role, :, half] - t_scr[role])).astype(jnp.bfloat16)
                    for half in (lo_half, hi_half)
                ]
                out.append(jnp.concatenate(ds, axis=1))
            dkv[gslot, d, :, :256] = dot_tn(out[0], qg[slot, 0]) + dot_tn(out[1], qg[slot, 1])
            return [dot_nn(ds, kvs[slot, d, 0]) for ds in out]

        got = score_grads(0)
        for role in range(2):
            o_acc[role] = got[role]

        def far_grads(d, x):
            got = score_grads(d)
            for role in range(2):
                o_acc[role] = o_acc[role] + got[role]
            return x
        far_loop(far_grads)
        for role in range(2):
            outb[slot, 2 + role] = (o_acc[role] * scale).astype(jnp.bfloat16)

    def part_wait(slot, s):
        remote(part.at[slot, s], part.at[slot, s], hop_s, part_r.at[slot, s], mate).wait_recv()

    def load(src, i):
        return [pltpu.make_async_copy(src.at[pl.ds(64 * n, 64)], sums.at[i, pl.ds(64 * n, 64)], lsem.at[i, n]) for n in range(4)]

    def start(copies):
        for copy in copies:
            copy.start()

    def finish(copies):
        for copy in copies:
            copy.wait()

    def passed(s, sl, slot):
        return remote(sums.at[4 + sl], part.at[slot, s], xsem.at[sl], part_r.at[slot, s], dev(0))

    def relay(s):
        return remote(part.at[2, s], part.at[1, s], rel_s.at[s], part_r.at[1, s], dev(1))

    def pass_on(i, count, slot):
        sl = lax.rem(count, 2)
        start(load(hold.at[0, i], 0))
        part_wait(0, i)
        start(load(part.at[0, i], 1))

        @pl.when(count >= 2)
        def _():
            passed(i, sl, slot).wait_send()
        finish(load(hold.at[0, i], 0))
        finish(load(part.at[0, i], 1))
        sums[4 + sl] = sums[0] + sums[1]
        passed(i, sl, slot).start()

    def pass_x(i):
        pass_on(i, jnp.int32(i), 0)

    def pass_y(i):
        count = jnp.int32(0)
        for one in ROUND:
            count = count + jnp.where(one < i, 1, 0)
        pass_on(i, count, 2)

    def total(s, terms):
        for n, src in enumerate(terms):
            start(load(src, n))
        for n, src in enumerate(terms):
            finish(load(src, n))
        value = sums[0]
        for n in range(1, len(terms)):
            value = value + sums[n]
        finalize(s, value)

    for d in range(1, 4):
        f_scr[d] = jnp.full((2, 1024, 128), NEG_BIG, jnp.float32)
        l_scr[d] = jnp.zeros((2, 1024, 128), jnp.float32)
    arrive(0)
    fetch(0, 0)

    def step(s, x):
        slot = lax.rem(s, 2)

        @pl.when(s + 1 < NS)
        def _():
            arrive(s + 1)
            fetch(s + 1, 1 - slot)

        @pl.when(s >= 2)
        def _():
            put_wait(s - 2, slot)

        @pl.when(s >= NG)
        def _():
            grads_out(s - NG, False)
        fetch_wait(s, slot)
        attend(s, slot)

        @pl.when(c == 3)
        def _():
            gslot = lax.rem(s, NG)
            give(gslot, 3, 1, 0, s).start()

            @pl.when(jnp.logical_not(around(s)))
            def _():
                part_wait(0, s)
                start(load(part.at[0, s], 0))
                finish(load(part.at[0, s], 0))
                dkv[gslot, 2] = dkv[gslot, 2] + sums[0]
            finalize(s, dkv[gslot, 0])
        put(s, slot)
        for at, i in EARLY_X.items():
            pl.when((c == 1) & (s == at))(lambda: pass_x(i))
        for at, i in EARLY_Y.items():
            pl.when((c == 2) & (s == at))(lambda: pass_y(i))
        return x

    lax.fori_loop(0, NS, step, 0)
    put_wait(NS - 2, 0)
    put_wait(NS - 1, 1)
    for s in range(NS - NG, NS):
        grads_out(s, False)

    def finals(i, lag):
        def end(k):
            return jnp.clip(k + 1 - lag + jnp.maximum(k - (NS - 1 - lag), 0), 0, NS)

        def deco(body):
            def one(s, x):
                body(s)
                return x
            lax.fori_loop(end(i - 1), end(i), one, 0)
        return deco

    def home(i, x):
        @pl.when(c == 0)
        def _():
            @pl.when(around(i))
            def _():
                part_wait(2, i)
                relay(i).start()
            @finals(i, LAG[0])
            def _(s):
                part_wait(1, s)
                part_wait(0, s)
                total(s, (hold.at[1, s], part.at[1, s], part.at[0, s]))

        @pl.when(c == 1)
        def _():
            pl.when((i >= len(EARLY_X)) & (i < NS))(lambda: pass_x(i))
            @finals(i, LAG[1])
            def _(s):
                part_wait(1, s)
                total(s, (hold.at[1, s], part.at[1, s]))

        @pl.when(c == 2)
        def _():
            pl.when(around(i) & (i > max(EARLY_Y.values())))(lambda: pass_y(i))
            @finals(i, LAG[2])
            def _(s):
                part_wait(1, s)
                total(s, (hold.at[1, s], part.at[1, s]))
        return x

    @pl.when(c < 3)
    def _():
        lax.fori_loop(0, NS + 1, home, 0)

    @pl.when(c == 0)
    def _():
        for s in ROUND:
            relay(s).wait_send()
        remote(kvr.at[1], kvr.at[1], hop_s, kv_r.at[0, 0], mate).wait_send()

    @pl.when(c == 1)
    def _():
        for sl in range(2):
            passed(0, sl, 0).wait_send()
        remote(kvr.at[0], kvr.at[0], hop_s, kv_r.at[0, 0], mate).wait_send()

    @pl.when(c == 2)
    def _():
        for sl in range(2):
            passed(0, sl, 2).wait_send()
    final_wait(NS - 2, 0)
    final_wait(NS - 1, 1)
    for which, ref in ((0, k), (1, v)):
        for way in range(2):
            @pl.when((c < 2) | ((c == 2) & (way == 0)))
            def _():
                remote(ref, ref, kv_s.at[way, which], kv_r.at[0, 0], mate).wait_send()
        half = ref.at[pl.ds(other, NS)]
        remote(half, half, kv_s.at[2, which], kv_r.at[0, 0], mate).wait_send()
    for which, ref in ((0, q), (1, g)):
        half = ref.at[pl.ds(other, NS)]
        remote(half, half, q_s.at[which], q_r.at[0], mate).wait_send()
    for which, ref in ((0, o), (1, dq)):
        half = ref.at[pl.ds(other, NS)]
        remote(half, half, hop_s, osend_r.at[which], mate).wait_recv()
    for which, ref in ((0, dk), (1, dv)):
        half = ref.at[pl.ds(other, NS)]
        remote(half, half, hop_s, dsend_r.at[which], mate).wait_recv()


ANY = pl.BlockSpec(memory_space=pl.ANY)
VMEM = pl.BlockSpec(memory_space=pltpu.VMEM)


def solution(mesh):
    n_dev = mesh.shape['cp']
    seq_spec = P('dp', 'cp', None, None)
    id_spec = P('dp', 'cp')
    bf, f32 = jnp.bfloat16, jnp.float32
    shape = jax.ShapeDtypeStruct
    dma = pltpu.SemaphoreType.DMA

    def per_device(query, keys, values, grad_out, doc_id):
        nb, piece, heads, hd = query.shape
        rows = piece * heads
        outs = pl.pallas_call(
            functools.partial(fused_kernel, hd ** -0.5),
            in_specs=[VMEM] + [ANY] * 4,
            out_specs=[ANY] * 8,
            out_shape=[
                shape((nb, rows, hd), bf), shape((nb, rows, hd), bf), shape((nb, piece, hd), bf), shape((nb, piece, hd), bf),
                shape((NS, 2, rows, hd), bf), shape((4, NS, 2, 256, 256), bf),
                shape((3, NS, 256, 512), f32), shape((2, NS, 256, 512), f32),
            ],
            scratch_shapes=[
                pltpu.VMEM((n_dev, nb, piece), jnp.int32), pltpu.VMEM((2, 4, 2, 256, 256), bf), pltpu.VMEM((2, 4, rows, hd), bf),
                pltpu.VMEM((2, 4, rows, hd), bf), pltpu.VMEM((NG, 4, 256, 512), f32), pltpu.VMEM((6, 256, 512), f32),
                pltpu.VMEM((2, 2, 256, 256), bf),
                pltpu.VMEM((4, 2, rows, 256), f32), pltpu.VMEM((4, 2, rows, 256), f32), pltpu.VMEM((4, 2, rows, 256), bf),
                pltpu.VMEM((4, 2, rows, 128), f32), pltpu.VMEM((4, 2, rows, 128), f32), pltpu.VMEM((2, rows, 128), f32),
                pltpu.VMEM((2, rows, 128), jnp.int32), pltpu.VMEM((2, rows, hd), f32),
                dma((n_dev,)), dma((n_dev,)), dma((2, 10)), dma((2, 4)), dma((NG, 4)), dma((2,)), dma((2,)), dma((NJ,)), dma((3, 2)), dma((4, NJ)),
                dma, dma((3, NS)), dma((2, 4)), dma((2,)), dma((3, 4)), dma((2,)), dma((NS,)),
            ],
            compiler_params=pltpu.CompilerParams(has_side_effects=True, vmem_limit_bytes=62 * 1024 * 1024),
            name="attend",
        )(doc_id, query.reshape(nb, rows, hd), grad_out.reshape(nb, rows, hd), keys.reshape(nb, piece, hd), values.reshape(nb, piece, hd))
        o, dq, dk, dv = outs[:4]
        return o.reshape(query.shape), dq.reshape(query.shape), dk.reshape(keys.shape), dv.reshape(values.shape)

    return jax.shard_map(per_device, mesh=mesh, in_specs=(seq_spec, seq_spec, seq_spec, seq_spec, id_spec),
                         out_specs=(seq_spec, seq_spec, seq_spec, seq_spec), check_vma=False)
```

```python
import functools

import jax
import jax.numpy as jnp
from jax import lax
from jax.experimental import pallas as pl
from jax.experimental.pallas import tpu as pltpu
from jax.sharding import PartitionSpec as P

NEG_BIG = -1e30
LOG2E = 1.4426950408889634
NS = 16
NJ = NS
AHEAD = 2
NG = 4
PLAN1 = 'RRMMRFRRFRFFRRMM'
PLAN0 = 'ANNNAAANCCCNNCNN'
LAST2 = (7, 8, 12)
EARLY_X = {7: 1, 9: 2, 10: 3, 12: 7, 13: 8, 14: 9, 15: 10}
EARLY_Y = {5: 0, 6: 1, 8: 4, 10: 6, 11: 7, 13: 9}
LAG = (4, 7, 7)


def where_plan(plan, kinds):
    return tuple(s for s in range(NS) if plan[s] in kinds)


ROUND, MERGE, FAR1 = (where_plan(PLAN1, x) for x in 'RMF')
HERE0, ON1, ON2 = (where_plan(PLAN0, x) for x in 'NAC')
OWN1 = where_plan(PLAN1, 'RM')
OWN2 = tuple(s for s in range(NS) if s not in LAST2)
OWN3 = tuple(range(NS))
PASS_X = where_plan(PLAN0, 'NC')
PASS_0 = where_plan(PLAN0, 'AC')


def dot_nt(a, b):
    return lax.dot_general(a, b, (((1,), (1,)), ((), ())), preferred_element_type=jnp.float32)


def dot_nn(a, b):
    return lax.dot_general(a, b, (((1,), (0,)), ((), ())), preferred_element_type=jnp.float32)


def dot_tn(a, b):
    return lax.dot_general(a, b, (((0,), (0,)), ((), ())), preferred_element_type=jnp.float32)


def remote(src, dst, send, recv, dev):
    return pltpu.make_async_remote_copy(src_ref=src, dst_ref=dst, send_sem=send, recv_sem=recv,
                                        device_id={'cp': dev}, device_id_type=pl.DeviceIdType.MESH)


def fused_kernel(scale, doc, q, g, k, v, o, dq, dk, dv, qgm, kvr, part, hold,
                 docs, kvs, qg, outb, dkv, sums, fin, e_scr, dp_scr, p_scr, l_scr, f_scr, t_scr, docr, o_acc,
                 doc_s, doc_r, isem, osem, gsem, osend_r, q_s, q_r, kv_s, kv_r, hop_s, part_r, fsem, dsend_r, lsem, xsem, rel_s, down_r):
    rank = lax.axis_index('cp')
    n_dev = docs.shape[0]
    c = rank // 2
    e = lax.rem(rank, 2)
    mate = 2 * c + 1 - e
    other = NS * (1 - e)
    mine = NS * e

    def dev(chip):
        return 2 * chip + e

    docs[rank] = doc[...]

    def doc_copy(i):
        return remote(doc, docs.at[rank], doc_s.at[i], doc_r.at[i], lax.rem(rank + i, n_dev))

    for i in range(1, n_dev):
        doc_copy(i).start()

    def kv_parts(chip, way, j, cols):
        out = []
        for col in cols:
            for which, ref in ((0, k), (1, v)):
                out.append(remote(ref.at[pl.ds(col * NS + j, 1)], kvr.at[c, pl.ds(j, 1), which, pl.ds(128 * e, 128)],
                                  kv_s.at[way, which], kv_r.at[c, j], 2 * chip + col))
        return out

    def send_kv(chip, way, j):
        for copy in kv_parts(chip, way, j, (0, 1)):
            copy.start()

    def kv_forward(a, chip, j):
        return remote(kvr.at[a, pl.ds(j, 1)], kvr.at[a, pl.ds(j, 1)], hop_s, kv_r.at[a, j], dev(chip))

    def stream_kv(j):
        @pl.when(c == 0)
        def _():
            send_kv(1, 0, j)
            send_kv(2, 1, j)

        @pl.when(c == 1)
        def _():
            send_kv(0, 1, j)

        @pl.when(c == 2)
        def _():
            send_kv(3, 0, j)

    def to_mate(j):
        for which, ref in ((0, k), (1, v)):
            remote(ref.at[pl.ds(other + j, 1)], kvr.at[c, pl.ds(j, 1), which, pl.ds(128 * e, 128)],
                   kv_s.at[2, which], kv_r.at[c, j], mate).start()

    def rows_to_mate(j):
        for which, ref in ((0, q), (1, g)):
            remote(ref.at[pl.ds(other + j, 1)], qgm.at[pl.ds(j, 1), which], q_s.at[which], q_r.at[j], mate).start()

    stream_kv(0)

    @pl.when(c == 1)
    def _():
        send_kv(3, 0, 0)
    to_mate(0)
    rows_to_mate(0)
    for j in range(1, AHEAD):
        stream_kv(j)
    for j in range(1, NJ):
        to_mate(j)
        rows_to_mate(j)
    for i in range(1, n_dev):
        doc_copy(i).wait()

    def arrive(j):
        remote(kvr.at[c, pl.ds(j, 1), :, pl.ds(0, 128)], kvr.at[c, pl.ds(j, 1), :, pl.ds(0, 128)],
               hop_s, kv_r.at[c, j], mate).wait_recv()
        remote(qgm.at[pl.ds(j, 1)], qgm.at[pl.ds(j, 1)], hop_s, q_r.at[j], mate).wait_recv()
        for a in range(3):
            @pl.when(a < c)
            def _():
                kv_forward(a, a, j).wait_recv()

        @pl.when(c == 1)
        def _():
            kv_forward(0, 3, j).start()

            @pl.when(j + 1 < NJ)
            def _():
                send_kv(3, 0, j + 1)

        @pl.when(c == 0)
        def _():
            kv_forward(1, 1, j).wait_recv()
            kv_forward(1, 2, j).start()

        @pl.when(j + AHEAD < NJ)
        def _():
            stream_kv(j + AHEAD)

    def inputs(s, sl):
        row = mine + s
        rows = pl.ds(128 * e, 128)
        rest = pl.ds(128 - 128 * e, 128)
        pairs = [
            (q.at[row], qg.at[sl, 0]), (g.at[row], qg.at[sl, 2]), (qgm.at[s, 0], qg.at[sl, 1]), (qgm.at[s, 1], qg.at[sl, 3]),
            (k.at[row], kvs.at[sl, 0, 0, rows]), (v.at[row], kvs.at[sl, 0, 1, rows]),
            (kvr.at[c, s, :, rest], kvs.at[sl, 0, :, rest]),
        ]
        return [pltpu.make_async_copy(src, dst, isem.at[sl, i]) for i, (src, dst) in enumerate(pairs)]

    def far_input(s, sl, d):
        return pltpu.make_async_copy(kvr.at[c - d, s], kvs.at[sl, d], isem.at[sl, 6 + d])

    def fetch(s, sl):
        for copy in inputs(s, sl):
            copy.start()
        for d in range(1, 4):
            @pl.when(d <= c)
            def _():
                far_input(s, sl, d).start()

    def fetch_wait(s, sl):
        for copy in inputs(s, sl):
            copy.wait()
        for d in range(1, 4):
            @pl.when(d <= c)
            def _():
                far_input(s, sl, d).wait()

    def row_outputs(s, sl):
        row = mine + s
        here = [pltpu.make_async_copy(outb.at[sl, 0], o.at[row], osem.at[sl, 0]),
                pltpu.make_async_copy(outb.at[sl, 2], dq.at[row], osem.at[sl, 1])]
        there = [remote(outb.at[sl, 1], o.at[row], osem.at[sl, 2], osend_r.at[0], mate),
                 remote(outb.at[sl, 3], dq.at[row], osem.at[sl, 3], osend_r.at[1], mate)]
        return here, there

    def keep(sl, d, slot, s):
        return pltpu.make_async_copy(dkv.at[sl, d], hold.at[slot, s], gsem.at[sl, d])

    def give(sl, d, chip, slot, s):
        return remote(dkv.at[sl, d], part.at[slot, s], gsem.at[sl, d], part_r.at[slot, s], dev(chip))

    def member(s, group):
        out = jnp.bool_(False)
        for one in group:
            out = out | (s == one)
        return out

    def rank_in(s, group):
        count = jnp.int32(0)
        for one in group:
            count = count + jnp.where(one < s, 1, 0)
        return count

    def choose(cond, yes, no):
        pl.when(cond)(yes)
        pl.when(jnp.logical_not(cond))(no)

    def grads_out(s, begin):
        sl = lax.rem(s, NG)

        def local(d, slot):
            copy = keep(sl, d, slot, s)
            copy.start() if begin else copy.wait()

        def away(d, chip, slot):
            copy = give(sl, d, chip, slot, s)
            copy.start() if begin else copy.wait_send()

        @pl.when(c == 0)
        def _():
            local(0, 1)

        @pl.when(c == 1)
        def _():
            choose(member(s, FAR1), lambda: away(0, 3, 2), lambda: local(0, 1))
            local(1, 0)

        @pl.when(c == 2)
        def _():
            choose(member(s, ROUND), lambda: local(1, 0), lambda: away(1, 3, 0))
            choose(member(s, LAST2), lambda: away(0, 3, 1), lambda: local(0, 1))
            choose(member(s, ON2), lambda: local(2, 2), lambda: away(2, 0, 1))

        if not begin:
            @pl.when(c == 3)
            def _():
                away(3, 1, 0)
                pl.when(member(s, ROUND))(lambda: away(2, 2, 0))
                pl.when(member(s, MERGE))(lambda: away(2, 1, 1))
                pl.when(jnp.logical_not(member(s, LAST2)))(lambda: away(1, 2, 1))

    def put(s, sl):
        here, there = row_outputs(s, sl)
        for copy in here + there:
            copy.start()
        grads_out(s, True)

    def put_wait(s, sl):
        here, there = row_outputs(s, sl)
        for copy in here:
            copy.wait()
        for copy in there:
            copy.wait_send()

    def final_copies(kind, sl, s, chip):
        row = mine + s
        out = []
        for which, ref in ((0, dk), (1, dv)):
            for far, rows in ((0, pl.ds(128 * e, 128)), (1, pl.ds(128 - 128 * e, 128))):
                src, sem = fin.at[kind, sl, which, rows], fsem.at[kind, sl, 2 * which + far]
                if far:
                    out.append(remote(src, ref.at[row], sem, dsend_r.at[which], mate if chip is None else 2 * chip + 1 - e))
                elif chip is None:
                    out.append(pltpu.make_async_copy(src, ref.at[row], sem))
                else:
                    out.append(remote(src, ref.at[row], sem, down_r.at[which], dev(chip)))
        return out

    def final_wait(kind, sl, chip):
        for i, copy in enumerate(final_copies(kind, sl, 0, chip)):
            if chip is None and i % 2 == 0:
                copy.wait()
            else:
                copy.wait_send()

    def finalize(kind, group, s, value, chip):
        count = rank_in(s, group)
        sl = lax.rem(count, 2)
        pl.when(count >= 2)(lambda: final_wait(kind, sl, chip))
        fin[kind, sl, 0] = (value[:, :256] * scale).astype(jnp.bfloat16)
        fin[kind, sl, 1] = value[:, 256:].astype(jnp.bfloat16)
        for copy in final_copies(kind, sl, s, chip):
            copy.start()

    def final_drain(kind, group, chip):
        for n in range(max(0, len(group) - 2), len(group)):
            final_wait(kind, n % 2, chip)

    row_tok = lax.broadcasted_iota(jnp.int32, (1024, 128), 0) >> 3
    lane = lax.broadcasted_iota(jnp.int32, (1024, 128), 1)
    cs = scale * LOG2E
    lo_half, hi_half = slice(0, 128), slice(128, 256)

    def attend(s, slot):
        row = mine + s
        gslot = lax.rem(s, NG)
        piece = (e, 1 - e)
        for role in range(2):
            dq_row = docs[2 * c + piece[role], pl.ds(row, 1), :]
            d_t = jnp.transpose(jnp.broadcast_to(dq_row, (128, 128)))
            docr[role] = jnp.broadcast_to(d_t[:, None, :], (128, 8, 128)).reshape(1024, 128)

        def g_of(role):
            return qg[slot, 2 + role]

        def far_loop(body):
            for chip in range(1, 4):
                @pl.when(c == chip)
                def _():
                    for d in range(1, chip + 1):
                        body(d, 0)

        def scores(role, d, causal):
            sc = dot_nt(qg[slot, role], kvs[slot, d, 0]) * cs
            xs = []
            for j in range(2):
                dk_row = docs[2 * (c - d) + j, pl.ds(row, 1), :]
                vis = docr[role] == dk_row
                if causal:
                    vis = vis & (lane + 128 * j <= row_tok + 128 * piece[role])
                xs.append(jnp.where(vis, sc[:, 128 * j:128 * (j + 1)], NEG_BIG))
            top = jnp.maximum(xs[0], xs[1])
            es = [jnp.exp2(x - top) for x in xs]
            e_scr[d, role, :, lo_half] = es[0]
            e_scr[d, role, :, hi_half] = es[1]
            f_scr[d, role] = top
            l_scr[d, role] = es[0] + es[1]
            return top

        def dprob(role, d):
            dp_scr[d, role] = dot_nt(g_of(role), kvs[slot, d, 1])

        for role in range(2):
            t_scr[role] = scores(role, 0, True)

        def far_scores(d, x):
            for role in range(2):
                t_scr[role] = jnp.maximum(t_scr[role], scores(role, d, False))
            for role in range(2):
                dprob(role, d)
            return x
        far_loop(far_scores)

        for role in range(2):
            t_scr[role] = jnp.broadcast_to(jnp.max(t_scr[role], axis=1, keepdims=True), (1024, 128))
        dprob(0, 0)

        for role in range(2):
            top = t_scr[role]
            norm = l_scr[0, role] * jnp.exp2(f_scr[0, role] - top)
            for d in range(1, 4):
                norm = norm + l_scr[d, role] * jnp.exp2(f_scr[d, role] - top)
            t_scr[role] = top + jnp.log2(jnp.broadcast_to(jnp.sum(norm, axis=1, keepdims=True), (1024, 128)))
        dprob(1, 0)

        def weighted(role, d):
            f = jnp.exp2(f_scr[d, role] - t_scr[role])
            f_scr[d, role] = f
            for half in (lo_half, hi_half):
                p_scr[d, role, :, half] = (e_scr[d, role, :, half] * f).astype(jnp.bfloat16)
            return dot_nn(p_scr[d, role], kvs[slot, d, 1])

        def value_grads(d):
            dkv[gslot, d, :, 256:] = dot_tn(p_scr[d, 0], g_of(0)) + dot_tn(p_scr[d, 1], g_of(1))

        for role in range(2):
            o_acc[role] = weighted(role, 0)

        def far_weighted(d, x):
            for role in range(2):
                o_acc[role] = o_acc[role] + weighted(role, d)
            value_grads(d)
            return x
        far_loop(far_weighted)

        for role in range(2):
            o_low = o_acc[role].astype(jnp.bfloat16)
            outb[slot, role] = o_low
            delta = jnp.sum(g_of(role).astype(jnp.float32) * o_low.astype(jnp.float32), axis=1, keepdims=True)
            t_scr[role] = jnp.broadcast_to(delta, (1024, 128))
        value_grads(0)

        def score_grads(d):
            out = []
            for role in range(2):
                ds = [
                    (e_scr[d, role, :, half] * f_scr[d, role] * (dp_scr[d, role, :, half] - t_scr[role])).astype(jnp.bfloat16)
                    for half in (lo_half, hi_half)
                ]
                out.append(jnp.concatenate(ds, axis=1))
            dkv[gslot, d, :, :256] = dot_tn(out[0], qg[slot, 0]) + dot_tn(out[1], qg[slot, 1])
            return [dot_nn(ds, kvs[slot, d, 0]) for ds in out]

        got = score_grads(0)
        for role in range(2):
            o_acc[role] = got[role]

        def far_grads(d, x):
            got = score_grads(d)
            for role in range(2):
                o_acc[role] = o_acc[role] + got[role]
            return x
        far_loop(far_grads)
        for role in range(2):
            outb[slot, 2 + role] = (o_acc[role] * scale).astype(jnp.bfloat16)

    def part_wait(slot, s):
        remote(part.at[slot, s], part.at[slot, s], hop_s, part_r.at[slot, s], mate).wait_recv()

    def load(src, i):
        return [pltpu.make_async_copy(src.at[pl.ds(64 * n, 64)], sums.at[i, pl.ds(64 * n, 64)], lsem.at[i, n]) for n in range(4)]

    def start(copies):
        for copy in copies:
            copy.start()

    def finish(copies):
        for copy in copies:
            copy.wait()

    def passed(s, sl, chip, slot):
        return remote(sums.at[4 + sl], part.at[slot, s], xsem.at[sl], part_r.at[slot, s], dev(chip))

    def relay(s):
        return remote(part.at[2, s], part.at[1, s], rel_s.at[s], part_r.at[1, s], dev(1))

    def pass_on(i, group, held, slot_in, chip, slot_out):
        count = rank_in(i, group)
        sl = lax.rem(count, 2)
        start(load(hold.at[held, i], 0))
        part_wait(slot_in, i)
        start(load(part.at[slot_in, i], 1))
        pl.when(count >= 2)(lambda: passed(i, sl, chip, slot_out).wait_send())
        finish(load(hold.at[held, i], 0))
        finish(load(part.at[slot_in, i], 1))
        sums[4 + sl] = sums[0] + sums[1]
        passed(i, sl, chip, slot_out).start()

    def pass_x(i):
        pass_on(i, PASS_X, 0, 0, 0, 0)

    def pass_y(i):
        pass_on(i, ROUND, 0, 0, 0, 2)

    def total(kind, group, s, held, slots, chip):
        terms = [hold.at[held, s]] + [part.at[slot, s] for slot in slots]
        for slot in slots:
            part_wait(slot, s)
        for n, src in enumerate(terms):
            start(load(src, n))
        for n, src in enumerate(terms):
            finish(load(src, n))
        value = sums[0]
        for n in range(1, len(terms)):
            value = value + sums[n]
        finalize(kind, group, s, value, chip)

    for d in range(1, 4):
        f_scr[d] = jnp.full((2, 1024, 128), NEG_BIG, jnp.float32)
        l_scr[d] = jnp.zeros((2, 1024, 128), jnp.float32)
    arrive(0)
    fetch(0, 0)

    def step(s, x):
        slot = lax.rem(s, 2)

        @pl.when(s + 1 < NS)
        def _():
            arrive(s + 1)
            fetch(s + 1, 1 - slot)

        @pl.when(s >= 2)
        def _():
            put_wait(s - 2, slot)

        @pl.when(s >= NG)
        def _():
            grads_out(s - NG, False)
        fetch_wait(s, slot)
        attend(s, slot)

        @pl.when(c == 3)
        def _():
            gslot = lax.rem(s, NG)
            give(gslot, 3, 1, 0, s).start()
            pl.when(member(s, ROUND))(lambda: give(gslot, 2, 2, 0, s).start())

            @pl.when(member(s, MERGE))
            def _():
                part_wait(0, s)
                start(load(part.at[0, s], 0))
                finish(load(part.at[0, s], 0))
                dkv[gslot, 2] = dkv[gslot, 2] + sums[0]

            @pl.when(member(s, FAR1))
            def _():
                part_wait(0, s)
                start(load(part.at[0, s], 0))
                part_wait(2, s)
                start(load(part.at[2, s], 1))
                finish(load(part.at[0, s], 0))
                finish(load(part.at[2, s], 1))
                finalize(1, FAR1, s, dkv[gslot, 2] + sums[0] + sums[1], 1)
            finalize(0, OWN3, s, dkv[gslot, 0], None)
            pl.when(member(s, MERGE))(lambda: give(gslot, 2, 1, 1, s).start())

            def last_two():
                part_wait(1, s)
                start(load(part.at[1, s], 2))
                finish(load(part.at[1, s], 2))
                finalize(2, LAST2, s, dkv[gslot, 1] + sums[2], 2)
            choose(member(s, LAST2), last_two, lambda: give(gslot, 1, 2, 1, s).start())
        put(s, slot)
        for at, i in EARLY_X.items():
            pl.when((c == 1) & (s == at))(lambda: pass_x(i))
        for at, i in EARLY_Y.items():
            pl.when((c == 2) & (s == at))(lambda: pass_y(i))
        return x

    lax.fori_loop(0, NS, step, 0)
    put_wait(NS - 2, 0)
    put_wait(NS - 1, 1)
    for s in range(NS - NG, NS):
        grads_out(s, False)

    def home(i, x):
        def behind(lag, body):
            s = i - lag
            pl.when((s >= 0) & (s < NS))(lambda: body(s))

        @pl.when(c == 0)
        def _():
            @pl.when(member(i, ROUND))
            def _():
                part_wait(2, i)
                relay(i).start()
            pl.when(member(i, ON1))(lambda: pass_on(i, PASS_0, 1, 1, 1, 2))
            pl.when(member(i, ON2))(lambda: pass_on(i, PASS_0, 1, 0, 2, 2))
            behind(LAG[0], lambda s: pl.when(member(s, HERE0))(lambda: total(0, HERE0, s, 1, (1, 0), None)))

        @pl.when(c == 1)
        def _():
            later = tuple(s for s in PASS_X if s not in EARLY_X.values())
            pl.when(member(i, later))(lambda: pass_x(i))

            def body(s):
                pl.when(member(s, ON1))(lambda: total(1, ON1, s, 0, (0, 2), 0))
                pl.when(member(s, OWN1))(lambda: total(0, OWN1, s, 1, (1,), None))
            behind(LAG[1], body)

        @pl.when(c == 2)
        def _():
            later = tuple(s for s in ROUND if s not in EARLY_Y.values())
            pl.when(member(i, later))(lambda: pass_y(i))

            def body(s):
                pl.when(member(s, ON2))(lambda: total(1, ON2, s, 2, (2,), 0))
                pl.when(member(s, OWN2))(lambda: total(0, OWN2, s, 1, (1,), None))
            behind(LAG[2], body)
        return x

    @pl.when(c < 3)
    def _():
        lax.fori_loop(0, NS + max(LAG), home, 0)

    def down_wait(n):
        for which, ref in ((0, dk), (1, dv)):
            rows = ref.at[pl.ds(0, n)]
            remote(rows, rows, hop_s, down_r.at[which], mate).wait_recv()

    @pl.when(c == 0)
    def _():
        for s in ROUND:
            relay(s).wait_send()
        for sl in range(2):
            passed(0, sl, 1, 2).wait_send()
        remote(kvr.at[1], kvr.at[1], hop_s, kv_r.at[0, 0], mate).wait_send()
        final_drain(0, HERE0, None)
        down_wait(len(PASS_0))

    @pl.when(c == 1)
    def _():
        for sl in range(2):
            passed(0, sl, 0, 0).wait_send()
        remote(kvr.at[0], kvr.at[0], hop_s, kv_r.at[0, 0], mate).wait_send()
        final_drain(0, OWN1, None)
        final_drain(1, ON1, 0)
        down_wait(len(FAR1))

    @pl.when(c == 2)
    def _():
        for sl in range(2):
            passed(0, sl, 0, 2).wait_send()
        final_drain(0, OWN2, None)
        final_drain(1, ON2, 0)
        down_wait(len(LAST2))

    @pl.when(c == 3)
    def _():
        final_drain(0, OWN3, None)
        final_drain(1, FAR1, 1)
        final_drain(2, LAST2, 2)
    for which, ref in ((0, k), (1, v)):
        for way in range(2):
            @pl.when((c < 2) | ((c == 2) & (way == 0)))
            def _():
                remote(ref, ref, kv_s.at[way, which], kv_r.at[0, 0], mate).wait_send()
        half = ref.at[pl.ds(other, NS)]
        remote(half, half, kv_s.at[2, which], kv_r.at[0, 0], mate).wait_send()
    for which, ref in ((0, q), (1, g)):
        half = ref.at[pl.ds(other, NS)]
        remote(half, half, q_s.at[which], q_r.at[0], mate).wait_send()
    for which, ref in ((0, o), (1, dq)):
        half = ref.at[pl.ds(other, NS)]
        remote(half, half, hop_s, osend_r.at[which], mate).wait_recv()
    for which, ref in ((0, dk), (1, dv)):
        half = ref.at[pl.ds(other, NS)]
        remote(half, half, hop_s, dsend_r.at[which], mate).wait_recv()


ANY = pl.BlockSpec(memory_space=pl.ANY)
VMEM = pl.BlockSpec(memory_space=pltpu.VMEM)


def solution(mesh):
    n_dev = mesh.shape['cp']
    seq_spec = P('dp', 'cp', None, None)
    id_spec = P('dp', 'cp')
    bf, f32 = jnp.bfloat16, jnp.float32
    shape = jax.ShapeDtypeStruct
    dma = pltpu.SemaphoreType.DMA

    def per_device(query, keys, values, grad_out, doc_id):
        nb, piece, heads, hd = query.shape
        rows = piece * heads
        outs = pl.pallas_call(
            functools.partial(fused_kernel, hd ** -0.5),
            in_specs=[VMEM] + [ANY] * 4,
            out_specs=[ANY] * 8,
            out_shape=[
                shape((nb, rows, hd), bf), shape((nb, rows, hd), bf), shape((nb, piece, hd), bf), shape((nb, piece, hd), bf),
                shape((NS, 2, rows, hd), bf), shape((4, NS, 2, 256, 256), bf),
                shape((3, NS, 256, 512), f32), shape((3, NS, 256, 512), f32),
            ],
            scratch_shapes=[
                pltpu.VMEM((n_dev, nb, piece), jnp.int32), pltpu.VMEM((2, 4, 2, 256, 256), bf), pltpu.VMEM((2, 4, rows, hd), bf),
                pltpu.VMEM((2, 4, rows, hd), bf), pltpu.VMEM((NG, 4, 256, 512), f32), pltpu.VMEM((6, 256, 512), f32),
                pltpu.VMEM((3, 2, 2, 256, 256), bf),
                pltpu.VMEM((4, 2, rows, 256), f32), pltpu.VMEM((4, 2, rows, 256), f32), pltpu.VMEM((4, 2, rows, 256), bf),
                pltpu.VMEM((4, 2, rows, 128), f32), pltpu.VMEM((4, 2, rows, 128), f32), pltpu.VMEM((2, rows, 128), f32),
                pltpu.VMEM((2, rows, 128), jnp.int32), pltpu.VMEM((2, rows, hd), f32),
                dma((n_dev,)), dma((n_dev,)), dma((2, 10)), dma((2, 4)), dma((NG, 4)), dma((2,)), dma((2,)), dma((NJ,)), dma((3, 2)), dma((4, NJ)),
                dma, dma((3, NS)), dma((3, 2, 4)), dma((2,)), dma((3, 4)), dma((2,)), dma((NS,)), dma((2,)),
            ],
            compiler_params=pltpu.CompilerParams(has_side_effects=True, vmem_limit_bytes=62 * 1024 * 1024),
            name="attend",
        )(doc_id, query.reshape(nb, rows, hd), grad_out.reshape(nb, rows, hd), keys.reshape(nb, piece, hd), values.reshape(nb, piece, hd))
        o, dq, dk, dv = outs[:4]
        return o.reshape(query.shape), dq.reshape(query.shape), dk.reshape(keys.shape), dv.reshape(values.shape)

    return jax.shard_map(per_device, mesh=mesh, in_specs=(seq_spec, seq_spec, seq_spec, seq_spec, id_spec),
                         out_specs=(seq_spec, seq_spec, seq_spec, seq_spec), check_vma=False)
```

```python
import functools

import jax
import jax.numpy as jnp
from jax import lax
from jax.experimental import pallas as pl
from jax.experimental.pallas import tpu as pltpu
from jax.sharding import PartitionSpec as P

NEG_BIG = -1e30
LOG2E = 1.4426950408889634
NS = 16
NJ = NS
AHEAD = 2
NG = 4
PLAN1 = 'RRMMRFRRFRFFRRMM'
PLAN0 = 'ANNNAAANCCCNNCNN'
LAST2 = (7, 8, 12)
EARLY_X = {7: 1, 9: 2, 10: 3, 12: 7, 13: 8, 14: 9, 15: 10}
EARLY_Y = {5: 0, 6: 1, 8: 4, 10: 6, 11: 7, 13: 9}
LAG = (4, 7, 7)


def where_plan(plan, kinds):
    return tuple(s for s in range(NS) if plan[s] in kinds)


ROUND, MERGE, FAR1 = (where_plan(PLAN1, x) for x in 'RMF')
HERE0, ON1, ON2 = (where_plan(PLAN0, x) for x in 'NAC')
OWN1 = where_plan(PLAN1, 'RM')
OWN2 = tuple(s for s in range(NS) if s not in LAST2)
OWN3 = tuple(range(NS))
PASS_X = where_plan(PLAN0, 'NC')
PASS_0 = where_plan(PLAN0, 'AC')


def dot_nt(a, b):
    return lax.dot_general(a, b, (((1,), (1,)), ((), ())), preferred_element_type=jnp.float32)


def dot_nn(a, b):
    return lax.dot_general(a, b, (((1,), (0,)), ((), ())), preferred_element_type=jnp.float32)


def dot_tn(a, b):
    return lax.dot_general(a, b, (((0,), (0,)), ((), ())), preferred_element_type=jnp.float32)


def remote(src, dst, send, recv, dev):
    return pltpu.make_async_remote_copy(src_ref=src, dst_ref=dst, send_sem=send, recv_sem=recv,
                                        device_id={'cp': dev}, device_id_type=pl.DeviceIdType.MESH)


def fused_kernel(scale, doc, q, g, k, v, o, dq, dk, dv, qgm, kvr, part, hold,
                 docs, kvs, qg, outb, dkv, sums, fin, e_scr, dp_scr, p_scr, l_scr, f_scr, t_scr, docr, o_acc,
                 doc_s, doc_r, isem, osem, gsem, osend_r, q_s, q_r, kv_s, kv_r, hop_s, part_r, fsem, dsend_r, lsem, xsem, rel_s, down_r):
    rank = lax.axis_index('cp')
    n_dev = docs.shape[0]
    c = rank // 2
    e = lax.rem(rank, 2)
    mate = 2 * c + 1 - e
    other = NS * (1 - e)
    mine = NS * e

    def dev(chip):
        return 2 * chip + e

    docs[rank] = doc[...]

    def doc_copy(i):
        return remote(doc, docs.at[rank], doc_s.at[i], doc_r.at[i], lax.rem(rank + i, n_dev))

    for i in range(1, n_dev):
        doc_copy(i).start()

    def kv_parts(chip, way, j, cols):
        out = []
        for col in cols:
            for which, ref in ((0, k), (1, v)):
                out.append(remote(ref.at[pl.ds(col * NS + j, 1)], kvr.at[c, pl.ds(j, 1), which, pl.ds(128 * e, 128)],
                                  kv_s.at[way, which], kv_r.at[c, j], 2 * chip + col))
        return out

    def send_kv(chip, way, j):
        for copy in kv_parts(chip, way, j, (0, 1)):
            copy.start()

    def kv_forward(a, chip, j):
        return remote(kvr.at[a, pl.ds(j, 1)], kvr.at[a, pl.ds(j, 1)], hop_s, kv_r.at[a, j], dev(chip))

    def stream_kv(j):
        @pl.when(c == 0)
        def _():
            send_kv(1, 0, j)
            send_kv(2, 1, j)

        @pl.when(c == 1)
        def _():
            send_kv(0, 1, j)

        @pl.when(c == 2)
        def _():
            send_kv(3, 0, j)

    def to_mate(j):
        for which, ref in ((0, k), (1, v)):
            remote(ref.at[pl.ds(other + j, 1)], kvr.at[c, pl.ds(j, 1), which, pl.ds(128 * e, 128)],
                   kv_s.at[2, which], kv_r.at[c, j], mate).start()

    def rows_to_mate(j):
        for which, ref in ((0, q), (1, g)):
            remote(ref.at[pl.ds(other + j, 1)], qgm.at[pl.ds(j, 1), which], q_s.at[which], q_r.at[j], mate).start()

    stream_kv(0)

    @pl.when(c == 1)
    def _():
        send_kv(3, 0, 0)
    to_mate(0)
    rows_to_mate(0)
    for j in range(1, AHEAD):
        stream_kv(j)
    for j in range(1, NJ):
        to_mate(j)
        rows_to_mate(j)
    for i in range(1, n_dev):
        doc_copy(i).wait()

    def arrive(j):
        remote(kvr.at[c, pl.ds(j, 1), :, pl.ds(0, 128)], kvr.at[c, pl.ds(j, 1), :, pl.ds(0, 128)],
               hop_s, kv_r.at[c, j], mate).wait_recv()
        remote(qgm.at[pl.ds(j, 1)], qgm.at[pl.ds(j, 1)], hop_s, q_r.at[j], mate).wait_recv()
        for a in range(3):
            @pl.when(a < c)
            def _():
                kv_forward(a, a, j).wait_recv()

        @pl.when(c == 1)
        def _():
            kv_forward(0, 3, j).start()

            @pl.when(j + 1 < NJ)
            def _():
                send_kv(3, 0, j + 1)

        @pl.when(c == 0)
        def _():
            kv_forward(1, 1, j).wait_recv()
            kv_forward(1, 2, j).start()

        @pl.when(j + AHEAD < NJ)
        def _():
            stream_kv(j + AHEAD)

    def inputs(s, sl):
        row = mine + s
        rows = pl.ds(128 * e, 128)
        rest = pl.ds(128 - 128 * e, 128)
        pairs = [
            (q.at[row], qg.at[sl, 0]), (g.at[row], qg.at[sl, 2]), (qgm.at[s, 0], qg.at[sl, 1]), (qgm.at[s, 1], qg.at[sl, 3]),
            (k.at[row], kvs.at[sl, 0, 0, rows]), (v.at[row], kvs.at[sl, 0, 1, rows]),
            (kvr.at[c, s, :, rest], kvs.at[sl, 0, :, rest]),
        ]
        return [pltpu.make_async_copy(src, dst, isem.at[sl, i]) for i, (src, dst) in enumerate(pairs)]

    def far_input(s, sl, d):
        return pltpu.make_async_copy(kvr.at[c - d, s], kvs.at[sl, d], isem.at[sl, 6 + d])

    def fetch(s, sl):
        for copy in inputs(s, sl):
            copy.start()
        for d in range(1, 4):
            @pl.when(d <= c)
            def _():
                far_input(s, sl, d).start()

    def fetch_wait(s, sl):
        for copy in inputs(s, sl):
            copy.wait()
        for d in range(1, 4):
            @pl.when(d <= c)
            def _():
                far_input(s, sl, d).wait()

    def row_outputs(s, sl):
        row = mine + s
        here = [pltpu.make_async_copy(outb.at[sl, 0], o.at[row], osem.at[sl, 0]),
                pltpu.make_async_copy(outb.at[sl, 2], dq.at[row], osem.at[sl, 1])]
        there = [remote(outb.at[sl, 1], o.at[row], osem.at[sl, 2], osend_r.at[0], mate),
                 remote(outb.at[sl, 3], dq.at[row], osem.at[sl, 3], osend_r.at[1], mate)]
        return here, there

    def keep(sl, d, slot, s):
        return pltpu.make_async_copy(dkv.at[sl, d], hold.at[slot, s], gsem.at[sl, d])

    def give(sl, d, chip, slot, s):
        return remote(dkv.at[sl, d], part.at[slot, s], gsem.at[sl, d], part_r.at[slot, s], dev(chip))

    def member(s, group):
        out = jnp.bool_(False)
        for one in group:
            out = out | (s == one)
        return out

    def rank_in(s, group):
        count = jnp.int32(0)
        for one in group:
            count = count + jnp.where(one < s, 1, 0)
        return count

    def choose(cond, yes, no):
        pl.when(cond)(yes)
        pl.when(jnp.logical_not(cond))(no)

    def grads_out(s, begin):
        sl = lax.rem(s, NG)

        def local(d, slot):
            copy = keep(sl, d, slot, s)
            copy.start() if begin else copy.wait()

        def away(d, chip, slot):
            copy = give(sl, d, chip, slot, s)
            copy.start() if begin else copy.wait_send()

        @pl.when(c == 0)
        def _():
            local(0, 1)

        @pl.when(c == 1)
        def _():
            choose(member(s, FAR1), lambda: away(0, 3, 2), lambda: local(0, 1))
            local(1, 0)

        @pl.when(c == 2)
        def _():
            choose(member(s, ROUND), lambda: local(1, 0), lambda: away(1, 3, 0))
            choose(member(s, LAST2), lambda: away(0, 3, 1), lambda: local(0, 1))
            choose(member(s, ON2), lambda: local(2, 2), lambda: away(2, 0, 1))

        if not begin:
            @pl.when(c == 3)
            def _():
                away(3, 1, 0)
                pl.when(member(s, ROUND))(lambda: away(2, 2, 0))
                pl.when(member(s, MERGE))(lambda: away(2, 1, 1))
                pl.when(jnp.logical_not(member(s, LAST2)))(lambda: away(1, 2, 1))

    def put(s, sl):
        here, there = row_outputs(s, sl)
        for copy in here + there:
            copy.start()
        grads_out(s, True)

    def put_wait(s, sl):
        here, there = row_outputs(s, sl)
        for copy in here:
            copy.wait()
        for copy in there:
            copy.wait_send()

    def final_copies(kind, sl, s, chip):
        row = mine + s
        out = []
        for which, ref in ((0, dk), (1, dv)):
            for far, rows in ((0, pl.ds(128 * e, 128)), (1, pl.ds(128 - 128 * e, 128))):
                src, sem = fin.at[kind, sl, which, rows], fsem.at[kind, sl, 2 * which + far]
                if far:
                    out.append(remote(src, ref.at[row], sem, dsend_r.at[which], mate if chip is None else 2 * chip + 1 - e))
                elif chip is None:
                    out.append(pltpu.make_async_copy(src, ref.at[row], sem))
                else:
                    out.append(remote(src, ref.at[row], sem, down_r.at[which], dev(chip)))
        return out

    def final_wait(kind, sl, chip):
        for i, copy in enumerate(final_copies(kind, sl, 0, chip)):
            if chip is None and i % 2 == 0:
                copy.wait()
            else:
                copy.wait_send()

    def finalize(kind, group, s, value, chip):
        count = rank_in(s, group)
        sl = lax.rem(count, 2)
        pl.when(count >= 2)(lambda: final_wait(kind, sl, chip))
        fin[kind, sl, 0] = (value[:, :256] * scale).astype(jnp.bfloat16)
        fin[kind, sl, 1] = value[:, 256:].astype(jnp.bfloat16)
        for copy in final_copies(kind, sl, s, chip):
            copy.start()

    def final_drain(kind, group, chip):
        for n in range(max(0, len(group) - 2), len(group)):
            final_wait(kind, n % 2, chip)

    row_tok = lax.broadcasted_iota(jnp.int32, (1024, 128), 0) >> 3
    lane = lax.broadcasted_iota(jnp.int32, (1024, 128), 1)
    cs = scale * LOG2E
    lo_half, hi_half = slice(0, 128), slice(128, 256)

    def attend(s, slot):
        row = mine + s
        gslot = lax.rem(s, NG)
        piece = (e, 1 - e)
        for role in range(2):
            dq_row = docs[2 * c + piece[role], pl.ds(row, 1), :]
            d_t = jnp.transpose(jnp.broadcast_to(dq_row, (128, 128)))
            docr[role] = jnp.broadcast_to(d_t[:, None, :], (128, 8, 128)).reshape(1024, 128)

        def g_of(role):
            return qg[slot, 2 + role]

        def far_loop(body):
            for chip in range(1, 4):
                @pl.when(c == chip)
                def _():
                    for d in range(1, chip + 1):
                        body(d, 0)

        def scores(role, d, causal):
            sc = dot_nt(qg[slot, role], kvs[slot, d, 0]) * cs
            xs = []
            for j in range(2):
                dk_row = docs[2 * (c - d) + j, pl.ds(row, 1), :]
                vis = docr[role] == dk_row
                if causal:
                    vis = vis & (lane + 128 * j <= row_tok + 128 * piece[role])
                xs.append(jnp.where(vis, sc[:, 128 * j:128 * (j + 1)], NEG_BIG))
            top = jnp.maximum(xs[0], xs[1])
            es = [jnp.exp2(x - top) for x in xs]
            e_scr[d, role, :, lo_half] = es[0]
            e_scr[d, role, :, hi_half] = es[1]
            f_scr[d, role] = top
            l_scr[d, role] = es[0] + es[1]
            return top

        def dprob(role, d):
            dp_scr[d, role] = dot_nt(g_of(role), kvs[slot, d, 1])

        for role in range(2):
            t_scr[role] = scores(role, 0, True)

        def far_scores(d, x):
            for role in range(2):
                t_scr[role] = jnp.maximum(t_scr[role], scores(role, d, False))
            for role in range(2):
                dprob(role, d)
            return x
        far_loop(far_scores)

        for role in range(2):
            t_scr[role] = jnp.broadcast_to(jnp.max(t_scr[role], axis=1, keepdims=True), (1024, 128))
        dprob(0, 0)

        for role in range(2):
            top = t_scr[role]
            norm = l_scr[0, role] * jnp.exp2(f_scr[0, role] - top)
            for d in range(1, 4):
                norm = norm + l_scr[d, role] * jnp.exp2(f_scr[d, role] - top)
            t_scr[role] = top + jnp.log2(jnp.broadcast_to(jnp.sum(norm, axis=1, keepdims=True), (1024, 128)))
        dprob(1, 0)

        def weighted(role, d):
            f = jnp.exp2(f_scr[d, role] - t_scr[role])
            f_scr[d, role] = f
            for half in (lo_half, hi_half):
                p_scr[d, role, :, half] = (e_scr[d, role, :, half] * f).astype(jnp.bfloat16)
            return dot_nn(p_scr[d, role], kvs[slot, d, 1])

        def value_grads(d):
            dkv[gslot, d, :, 256:] = dot_tn(p_scr[d, 0], g_of(0)) + dot_tn(p_scr[d, 1], g_of(1))

        for role in range(2):
            o_acc[role] = weighted(role, 0)

        def far_weighted(d, x):
            for role in range(2):
                o_acc[role] = o_acc[role] + weighted(role, d)
            value_grads(d)
            return x
        far_loop(far_weighted)

        for role in range(2):
            o_low = o_acc[role].astype(jnp.bfloat16)
            outb[slot, role] = o_low
            delta = jnp.sum(g_of(role).astype(jnp.float32) * o_low.astype(jnp.float32), axis=1, keepdims=True)
            t_scr[role] = jnp.broadcast_to(delta, (1024, 128))
        value_grads(0)

        def score_grads(d):
            out = []
            for role in range(2):
                ds = [
                    (e_scr[d, role, :, half] * f_scr[d, role] * (dp_scr[d, role, :, half] - t_scr[role])).astype(jnp.bfloat16)
                    for half in (lo_half, hi_half)
                ]
                out.append(jnp.concatenate(ds, axis=1))
            dkv[gslot, d, :, :256] = dot_tn(out[0], qg[slot, 0]) + dot_tn(out[1], qg[slot, 1])
            return [dot_nn(ds, kvs[slot, d, 0]) for ds in out]

        got = score_grads(0)
        for role in range(2):
            o_acc[role] = got[role]

        def far_grads(d, x):
            got = score_grads(d)
            for role in range(2):
                o_acc[role] = o_acc[role] + got[role]
            return x
        far_loop(far_grads)
        for role in range(2):
            outb[slot, 2 + role] = (o_acc[role] * scale).astype(jnp.bfloat16)

    def part_wait(slot, s):
        remote(part.at[slot, s], part.at[slot, s], hop_s, part_r.at[slot, s], mate).wait_recv()

    def load(src, i):
        return [pltpu.make_async_copy(src.at[pl.ds(64 * n, 64)], sums.at[i, pl.ds(64 * n, 64)], lsem.at[i, n]) for n in range(4)]

    def start(copies):
        for copy in copies:
            copy.start()

    def finish(copies):
        for copy in copies:
            copy.wait()

    def passed(s, sl, chip, slot):
        return remote(sums.at[4 + sl], part.at[slot, s], xsem.at[sl], part_r.at[slot, s], dev(chip))

    def relay(s):
        return remote(part.at[2, s], part.at[1, s], rel_s.at[s], part_r.at[1, s], dev(1))

    def pass_on(i, group, held, slot_in, chip, slot_out):
        count = rank_in(i, group)
        sl = lax.rem(count, 2)
        start(load(hold.at[held, i], 0))
        part_wait(slot_in, i)
        start(load(part.at[slot_in, i], 1))
        pl.when(count >= 2)(lambda: passed(i, sl, chip, slot_out).wait_send())
        finish(load(hold.at[held, i], 0))
        finish(load(part.at[slot_in, i], 1))
        sums[4 + sl] = sums[0] + sums[1]
        passed(i, sl, chip, slot_out).start()

    def pass_x(i):
        pass_on(i, PASS_X, 0, 0, 0, 0)

    def pass_y(i):
        pass_on(i, ROUND, 0, 0, 0, 2)

    def total(kind, group, s, held, slots, chip):
        terms = [hold.at[held, s]] + [part.at[slot, s] for slot in slots]
        for slot in slots:
            part_wait(slot, s)
        for n, src in enumerate(terms):
            start(load(src, n))
        for n, src in enumerate(terms):
            finish(load(src, n))
        value = sums[0]
        for n in range(1, len(terms)):
            value = value + sums[n]
        finalize(kind, group, s, value, chip)

    for d in range(1, 4):
        f_scr[d] = jnp.full((2, 1024, 128), NEG_BIG, jnp.float32)
        l_scr[d] = jnp.zeros((2, 1024, 128), jnp.float32)
    arrive(0)
    fetch(0, 0)

    def step(s, x):
        slot = lax.rem(s, 2)

        @pl.when(s + 1 < NS)
        def _():
            arrive(s + 1)
            fetch(s + 1, 1 - slot)

        @pl.when(s >= 2)
        def _():
            put_wait(s - 2, slot)

        @pl.when(s >= NG)
        def _():
            grads_out(s - NG, False)
        fetch_wait(s, slot)
        attend(s, slot)

        @pl.when(c == 3)
        def _():
            gslot = lax.rem(s, NG)
            give(gslot, 3, 1, 0, s).start()
            pl.when(member(s, ROUND))(lambda: give(gslot, 2, 2, 0, s).start())

            @pl.when(member(s, MERGE))
            def _():
                part_wait(0, s)
                start(load(part.at[0, s], 0))
                finish(load(part.at[0, s], 0))
                dkv[gslot, 2] = dkv[gslot, 2] + sums[0]

            @pl.when(member(s, FAR1))
            def _():
                part_wait(0, s)
                start(load(part.at[0, s], 0))
                part_wait(2, s)
                start(load(part.at[2, s], 1))
                finish(load(part.at[0, s], 0))
                finish(load(part.at[2, s], 1))
                finalize(1, FAR1, s, dkv[gslot, 2] + sums[0] + sums[1], 1)
            finalize(0, OWN3, s, dkv[gslot, 0], None)
            pl.when(member(s, MERGE))(lambda: give(gslot, 2, 1, 1, s).start())

            def last_two():
                part_wait(1, s)
                start(load(part.at[1, s], 2))
                finish(load(part.at[1, s], 2))
                finalize(2, LAST2, s, dkv[gslot, 1] + sums[2], 2)
            choose(member(s, LAST2), last_two, lambda: give(gslot, 1, 2, 1, s).start())
        put(s, slot)
        for at, i in EARLY_X.items():
            pl.when((c == 1) & (s == at))(lambda: pass_x(i))
        for at, i in EARLY_Y.items():
            pl.when((c == 2) & (s == at))(lambda: pass_y(i))
        return x

    lax.fori_loop(0, NS, step, 0)
    put_wait(NS - 2, 0)
    put_wait(NS - 1, 1)
    for s in range(NS - NG, NS):
        grads_out(s, False)

    def home(i, x):
        def behind(lag, body):
            s = i - lag
            pl.when((s >= 0) & (s < NS))(lambda: body(s))

        @pl.when(c == 0)
        def _():
            @pl.when(member(i, ROUND))
            def _():
                part_wait(2, i)
                relay(i).start()
            pl.when(member(i, ON1))(lambda: pass_on(i, PASS_0, 1, 1, 1, 2))
            pl.when(member(i, ON2))(lambda: pass_on(i, PASS_0, 1, 0, 2, 2))
            behind(LAG[0], lambda s: pl.when(member(s, HERE0))(lambda: total(0, HERE0, s, 1, (1, 0), None)))

        @pl.when(c == 1)
        def _():
            later = tuple(s for s in PASS_X if s not in EARLY_X.values())
            pl.when(member(i, later))(lambda: pass_x(i))

            def body(s):
                pl.when(member(s, ON1))(lambda: total(1, ON1, s, 0, (0, 2), 0))
                pl.when(member(s, OWN1))(lambda: total(0, OWN1, s, 1, (1,), None))
            behind(LAG[1], body)

        @pl.when(c == 2)
        def _():
            later = tuple(s for s in ROUND if s not in EARLY_Y.values())
            pl.when(member(i, later))(lambda: pass_y(i))

            def body(s):
                pl.when(member(s, ON2))(lambda: total(1, ON2, s, 2, (2,), 0))
                pl.when(member(s, OWN2))(lambda: total(0, OWN2, s, 1, (1,), None))
            behind(LAG[2], body)
        return x

    @pl.when(c < 3)
    def _():
        lax.fori_loop(0, NS + max(LAG), home, 0)

    def down_wait(n):
        for which, ref in ((0, dk), (1, dv)):
            rows = ref.at[pl.ds(0, n)]
            remote(rows, rows, hop_s, down_r.at[which], mate).wait_recv()

    @pl.when(c == 0)
    def _():
        for s in ROUND:
            relay(s).wait_send()
        for sl in range(2):
            passed(0, sl, 1, 2).wait_send()
        remote(kvr.at[1], kvr.at[1], hop_s, kv_r.at[0, 0], mate).wait_send()
        final_drain(0, HERE0, None)
        down_wait(len(PASS_0))

    @pl.when(c == 1)
    def _():
        for sl in range(2):
            passed(0, sl, 0, 0).wait_send()
        remote(kvr.at[0], kvr.at[0], hop_s, kv_r.at[0, 0], mate).wait_send()
        final_drain(0, OWN1, None)
        final_drain(1, ON1, 0)
        down_wait(len(FAR1))

    @pl.when(c == 2)
    def _():
        for sl in range(2):
            passed(0, sl, 0, 2).wait_send()
        final_drain(0, OWN2, None)
        final_drain(1, ON2, 0)
        down_wait(len(LAST2))

    @pl.when(c == 3)
    def _():
        final_drain(0, OWN3, None)
        final_drain(1, FAR1, 1)
        final_drain(2, LAST2, 2)
    for which, ref in ((0, k), (1, v)):
        for way in range(2):
            @pl.when((c < 2) | ((c == 2) & (way == 0)))
            def _():
                remote(ref, ref, kv_s.at[way, which], kv_r.at[0, 0], mate).wait_send()
        half = ref.at[pl.ds(other, NS)]
        remote(half, half, kv_s.at[2, which], kv_r.at[0, 0], mate).wait_send()
    for which, ref in ((0, q), (1, g)):
        half = ref.at[pl.ds(other, NS)]
        remote(half, half, q_s.at[which], q_r.at[0], mate).wait_send()
    for which, ref in ((0, o), (1, dq)):
        half = ref.at[pl.ds(other, NS)]
        remote(half, half, hop_s, osend_r.at[which], mate).wait_recv()
    for which, ref in ((0, dk), (1, dv)):
        half = ref.at[pl.ds(other, NS)]
        remote(half, half, hop_s, dsend_r.at[which], mate).wait_recv()


def place_kernel(slots, *refs):
    srcs, dsts, (buf, rsem, wsem) = refs[:4], refs[4:8], refs[8:]
    jobs = []
    for src, dst in zip(srcs, dsts):
        n = src.shape[0]
        size = 512 * 1024 // (src.shape[1] * src.shape[2])
        for i in range(0, n, size):
            shape = (size,) + tuple(src.shape[1:])
            jobs.append((src.at[pl.ds(i, size)], dst.at[pl.ds(i, size)], shape))

    def view(slot, shape):
        return buf.at[slot].reshape(shape)

    def read(j):
        return pltpu.make_async_copy(jobs[j][0], view(j % slots, jobs[j][2]), rsem.at[j % slots])

    def write(j):
        return pltpu.make_async_copy(view(j % slots, jobs[j][2]), jobs[j][1], wsem.at[j % slots])

    ahead = slots // 2
    for j in range(min(ahead, len(jobs))):
        read(j).start()
    for j in range(len(jobs)):
        read(j).wait()
        write(j).start()
        if j + ahead < len(jobs):
            if j + ahead >= slots:
                write(j + ahead - slots).wait()
            read(j + ahead).start()
    for j in range(max(0, len(jobs) - slots), len(jobs)):
        write(j).wait()


ANY = pl.BlockSpec(memory_space=pl.ANY)
VMEM = pl.BlockSpec(memory_space=pltpu.VMEM)


def solution(mesh):
    n_dev = mesh.shape['cp']
    seq_spec = P('dp', 'cp', None, None)
    id_spec = P('dp', 'cp')
    bf, f32 = jnp.bfloat16, jnp.float32
    shape = jax.ShapeDtypeStruct
    dma = pltpu.SemaphoreType.DMA

    def per_device(query, keys, values, grad_out, doc_id):
        nb, piece, heads, hd = query.shape
        rows = piece * heads
        outs = pl.pallas_call(
            functools.partial(fused_kernel, hd ** -0.5),
            in_specs=[VMEM] + [ANY] * 4,
            out_specs=[ANY] * 8,
            out_shape=[
                shape((nb, rows, hd), bf), shape((nb, rows, hd), bf), shape((nb, piece, hd), bf), shape((nb, piece, hd), bf),
                shape((NS, 2, rows, hd), bf), shape((4, NS, 2, 256, 256), bf),
                shape((3, NS, 256, 512), f32), shape((3, NS, 256, 512), f32),
            ],
            scratch_shapes=[
                pltpu.VMEM((n_dev, nb, piece), jnp.int32), pltpu.VMEM((2, 4, 2, 256, 256), bf), pltpu.VMEM((2, 4, rows, hd), bf),
                pltpu.VMEM((2, 4, rows, hd), bf), pltpu.VMEM((NG, 4, 256, 512), f32), pltpu.VMEM((6, 256, 512), f32),
                pltpu.VMEM((3, 2, 2, 256, 256), bf),
                pltpu.VMEM((4, 2, rows, 256), f32), pltpu.VMEM((4, 2, rows, 256), f32), pltpu.VMEM((4, 2, rows, 256), bf),
                pltpu.VMEM((4, 2, rows, 128), f32), pltpu.VMEM((4, 2, rows, 128), f32), pltpu.VMEM((2, rows, 128), f32),
                pltpu.VMEM((2, rows, 128), jnp.int32), pltpu.VMEM((2, rows, hd), f32),
                dma((n_dev,)), dma((n_dev,)), dma((2, 10)), dma((2, 4)), dma((NG, 4)), dma((2,)), dma((2,)), dma((NJ,)), dma((3, 2)), dma((4, NJ)),
                dma, dma((3, NS)), dma((3, 2, 4)), dma((2,)), dma((3, 4)), dma((2,)), dma((NS,)), dma((2,)),
            ],
            compiler_params=pltpu.CompilerParams(has_side_effects=True, vmem_limit_bytes=62 * 1024 * 1024),
            name="attend",
        )(doc_id, query.reshape(nb, rows, hd), grad_out.reshape(nb, rows, hd), keys.reshape(nb, piece, hd), values.reshape(nb, piece, hd))
        outs = [x.reshape(nb, -1, hd) for x in outs[:4]]
        o, dq, dk, dv = pl.pallas_call(
            functools.partial(place_kernel, 24),
            in_specs=[ANY] * 4,
            out_specs=[ANY] * 4,
            out_shape=[shape(x.shape, bf) for x in outs],
            scratch_shapes=[pltpu.VMEM((24, 2048, hd), bf), dma((24,)), dma((24,))],
            name="place",
        )(*outs)
        return o.reshape(query.shape), dq.reshape(query.shape), dk.reshape(keys.shape), dv.reshape(values.shape)

    return jax.shard_map(per_device, mesh=mesh, in_specs=(seq_spec, seq_spec, seq_spec, seq_spec, id_spec),
                         out_specs=(seq_spec, seq_spec, seq_spec, seq_spec), check_vma=False)
```

```python
import functools

import jax
import jax.numpy as jnp
from jax import lax
from jax.experimental import pallas as pl
from jax.experimental.pallas import tpu as pltpu
from jax.sharding import PartitionSpec as P

NEG_BIG = -1e30
LOG2E = 1.4426950408889634
NS = 16
NJ = NS
AHEAD = 2
NG = 4
PLAN1 = 'RMRMRRFRRFRFFRMM'
PLAN0 = 'NNNANCNNACCNCNNN'
LAST2 = (5, 7, 12, 14)
EARLY_X = {5: 0, 6: 1, 8: 2, 9: 4, 10: 5, 13: 6, 14: 7, 15: 9}
EARLY_Y = {4: 0, 6: 2, 9: 4, 12: 5, 13: 7, 14: 8, 15: 10}
LAG = (8, 6, 7)


def where_plan(plan, kinds):
    return tuple(s for s in range(NS) if plan[s] in kinds)


ROUND, MERGE, FAR1 = (where_plan(PLAN1, x) for x in 'RMF')
HERE0, ON1, ON2 = (where_plan(PLAN0, x) for x in 'NAC')
OWN1 = where_plan(PLAN1, 'RM')
OWN2 = tuple(s for s in range(NS) if s not in LAST2)
OWN3 = tuple(range(NS))
PASS_X = where_plan(PLAN0, 'NC')
PASS_0 = where_plan(PLAN0, 'AC')


def dot_nt(a, b):
    return lax.dot_general(a, b, (((1,), (1,)), ((), ())), preferred_element_type=jnp.float32)


def dot_nn(a, b):
    return lax.dot_general(a, b, (((1,), (0,)), ((), ())), preferred_element_type=jnp.float32)


def dot_tn(a, b):
    return lax.dot_general(a, b, (((0,), (0,)), ((), ())), preferred_element_type=jnp.float32)


def remote(src, dst, send, recv, dev):
    return pltpu.make_async_remote_copy(src_ref=src, dst_ref=dst, send_sem=send, recv_sem=recv,
                                        device_id={'cp': dev}, device_id_type=pl.DeviceIdType.MESH)


def fused_kernel(scale, doc, q, g, k, v, o, dq, dk, dv, qgm, kvr, part, hold,
                 docs, kvs, qg, outb, dkv, sums, fin, e_scr, dp_scr, p_scr, l_scr, f_scr, t_scr, docr, o_acc,
                 doc_s, doc_r, isem, osem, gsem, osend_r, q_s, q_r, kv_s, kv_r, hop_s, part_r, fsem, dsend_r, lsem, xsem, rel_s, down_r):
    rank = lax.axis_index('cp')
    n_dev = docs.shape[0]
    c = rank // 2
    e = lax.rem(rank, 2)
    mate = 2 * c + 1 - e
    other = NS * (1 - e)
    mine = NS * e

    def dev(chip):
        return 2 * chip + e

    docs[rank] = doc[...]

    def doc_copy(i):
        return remote(doc, docs.at[rank], doc_s.at[i], doc_r.at[i], lax.rem(rank + i, n_dev))

    for i in range(1, n_dev):
        doc_copy(i).start()

    def kv_parts(chip, way, j, cols):
        out = []
        for col in cols:
            for which, ref in ((0, k), (1, v)):
                out.append(remote(ref.at[pl.ds(col * NS + j, 1)], kvr.at[c, pl.ds(j, 1), which, pl.ds(128 * e, 128)],
                                  kv_s.at[way, which], kv_r.at[c, j], 2 * chip + col))
        return out

    def send_kv(chip, way, j):
        for copy in kv_parts(chip, way, j, (0, 1)):
            copy.start()

    def kv_forward(a, chip, j):
        return remote(kvr.at[a, pl.ds(j, 1)], kvr.at[a, pl.ds(j, 1)], hop_s, kv_r.at[a, j], dev(chip))

    def stream_kv(j):
        @pl.when(c == 0)
        def _():
            send_kv(1, 0, j)
            send_kv(2, 1, j)

        @pl.when(c == 1)
        def _():
            send_kv(0, 1, j)

        @pl.when(c == 2)
        def _():
            send_kv(3, 0, j)

    def to_mate(j):
        for which, ref in ((0, k), (1, v)):
            remote(ref.at[pl.ds(other + j, 1)], kvr.at[c, pl.ds(j, 1), which, pl.ds(128 * e, 128)],
                   kv_s.at[2, which], kv_r.at[c, j], mate).start()

    def rows_to_mate(j):
        for which, ref in ((0, q), (1, g)):
            remote(ref.at[pl.ds(other + j, 1)], qgm.at[pl.ds(j, 1), which], q_s.at[which], q_r.at[j], mate).start()

    stream_kv(0)

    @pl.when(c == 1)
    def _():
        send_kv(3, 0, 0)
    to_mate(0)
    rows_to_mate(0)
    for j in range(1, AHEAD):
        stream_kv(j)
    for j in range(1, NJ):
        to_mate(j)
        rows_to_mate(j)
    for i in range(1, n_dev):
        doc_copy(i).wait()

    def arrive(j):
        remote(kvr.at[c, pl.ds(j, 1), :, pl.ds(0, 128)], kvr.at[c, pl.ds(j, 1), :, pl.ds(0, 128)],
               hop_s, kv_r.at[c, j], mate).wait_recv()
        remote(qgm.at[pl.ds(j, 1)], qgm.at[pl.ds(j, 1)], hop_s, q_r.at[j], mate).wait_recv()
        for a in range(3):
            @pl.when(a < c)
            def _():
                kv_forward(a, a, j).wait_recv()

        @pl.when(c == 1)
        def _():
            kv_forward(0, 3, j).start()

            @pl.when(j + 1 < NJ)
            def _():
                send_kv(3, 0, j + 1)

        @pl.when(c == 0)
        def _():
            kv_forward(1, 1, j).wait_recv()
            kv_forward(1, 2, j).start()

        @pl.when(j + AHEAD < NJ)
        def _():
            stream_kv(j + AHEAD)

    def inputs(s, sl):
        row = mine + s
        rows = pl.ds(128 * e, 128)
        rest = pl.ds(128 - 128 * e, 128)
        pairs = [
            (q.at[row], qg.at[sl, 0]), (g.at[row], qg.at[sl, 2]), (qgm.at[s, 0], qg.at[sl, 1]), (qgm.at[s, 1], qg.at[sl, 3]),
            (k.at[row], kvs.at[sl, 0, 0, rows]), (v.at[row], kvs.at[sl, 0, 1, rows]),
            (kvr.at[c, s, :, rest], kvs.at[sl, 0, :, rest]),
        ]
        return [pltpu.make_async_copy(src, dst, isem.at[sl, i]) for i, (src, dst) in enumerate(pairs)]

    def far_input(s, sl, d):
        return pltpu.make_async_copy(kvr.at[c - d, s], kvs.at[sl, d], isem.at[sl, 6 + d])

    def fetch(s, sl):
        for copy in inputs(s, sl):
            copy.start()
        for d in range(1, 4):
            @pl.when(d <= c)
            def _():
                far_input(s, sl, d).start()

    def fetch_wait(s, sl):
        for copy in inputs(s, sl):
            copy.wait()
        for d in range(1, 4):
            @pl.when(d <= c)
            def _():
                far_input(s, sl, d).wait()

    def row_outputs(s, sl):
        row = mine + s
        here = [pltpu.make_async_copy(outb.at[sl, 0], o.at[row], osem.at[sl, 0]),
                pltpu.make_async_copy(outb.at[sl, 2], dq.at[row], osem.at[sl, 1])]
        there = [remote(outb.at[sl, 1], o.at[row], osem.at[sl, 2], osend_r.at[0], mate),
                 remote(outb.at[sl, 3], dq.at[row], osem.at[sl, 3], osend_r.at[1], mate)]
        return here, there

    def keep(sl, d, slot, s):
        return pltpu.make_async_copy(dkv.at[sl, d], hold.at[slot, s], gsem.at[sl, d])

    def give(sl, d, chip, slot, s):
        return remote(dkv.at[sl, d], part.at[slot, s], gsem.at[sl, d], part_r.at[slot, s], dev(chip))

    def member(s, group):
        out = jnp.bool_(False)
        for one in group:
            out = out | (s == one)
        return out

    def rank_in(s, group):
        count = jnp.int32(0)
        for one in group:
            count = count + jnp.where(one < s, 1, 0)
        return count

    def choose(cond, yes, no):
        pl.when(cond)(yes)
        pl.when(jnp.logical_not(cond))(no)

    def grads_out(s, begin):
        sl = lax.rem(s, NG)

        def local(d, slot):
            copy = keep(sl, d, slot, s)
            copy.start() if begin else copy.wait()

        def away(d, chip, slot):
            copy = give(sl, d, chip, slot, s)
            copy.start() if begin else copy.wait_send()

        @pl.when(c == 0)
        def _():
            local(0, 1)

        @pl.when(c == 1)
        def _():
            choose(member(s, FAR1), lambda: away(0, 3, 2), lambda: local(0, 1))
            local(1, 0)

        @pl.when(c == 2)
        def _():
            choose(member(s, ROUND), lambda: local(1, 0), lambda: away(1, 3, 0))
            choose(member(s, LAST2), lambda: away(0, 3, 1), lambda: local(0, 1))
            choose(member(s, ON2), lambda: local(2, 2), lambda: away(2, 0, 1))

        if not begin:
            @pl.when(c == 3)
            def _():
                away(3, 1, 0)
                pl.when(member(s, ROUND))(lambda: away(2, 2, 0))
                pl.when(member(s, MERGE))(lambda: away(2, 1, 1))
                pl.when(jnp.logical_not(member(s, LAST2)))(lambda: away(1, 2, 1))

    def put(s, sl):
        here, there = row_outputs(s, sl)
        for copy in here + there:
            copy.start()
        grads_out(s, True)

    def put_wait(s, sl):
        here, there = row_outputs(s, sl)
        for copy in here:
            copy.wait()
        for copy in there:
            copy.wait_send()

    def final_copies(kind, sl, s, chip):
        row = mine + s
        out = []
        for which, ref in ((0, dk), (1, dv)):
            for far, rows in ((0, pl.ds(128 * e, 128)), (1, pl.ds(128 - 128 * e, 128))):
                src, sem = fin.at[kind, sl, which, rows], fsem.at[kind, sl, 2 * which + far]
                if far:
                    out.append(remote(src, ref.at[row], sem, dsend_r.at[which], mate if chip is None else 2 * chip + 1 - e))
                elif chip is None:
                    out.append(pltpu.make_async_copy(src, ref.at[row], sem))
                else:
                    out.append(remote(src, ref.at[row], sem, down_r.at[which], dev(chip)))
        return out

    def final_wait(kind, sl, chip):
        for i, copy in enumerate(final_copies(kind, sl, 0, chip)):
            if chip is None and i % 2 == 0:
                copy.wait()
            else:
                copy.wait_send()

    def finalize(kind, group, s, value, chip):
        count = rank_in(s, group)
        sl = lax.rem(count, 2)
        pl.when(count >= 2)(lambda: final_wait(kind, sl, chip))
        fin[kind, sl, 0] = (value[:, :256] * scale).astype(jnp.bfloat16)
        fin[kind, sl, 1] = value[:, 256:].astype(jnp.bfloat16)
        for copy in final_copies(kind, sl, s, chip):
            copy.start()

    def final_drain(kind, group, chip):
        for n in range(max(0, len(group) - 2), len(group)):
            final_wait(kind, n % 2, chip)

    row_tok = lax.broadcasted_iota(jnp.int32, (1024, 128), 0) >> 3
    lane = lax.broadcasted_iota(jnp.int32, (1024, 128), 1)
    cs = scale * LOG2E
    lo_half, hi_half = slice(0, 128), slice(128, 256)

    def attend(s, slot):
        row = mine + s
        gslot = lax.rem(s, NG)
        piece = (e, 1 - e)
        for role in range(2):
            dq_row = docs[2 * c + piece[role], pl.ds(row, 1), :]
            d_t = jnp.transpose(jnp.broadcast_to(dq_row, (128, 128)))
            docr[role] = jnp.broadcast_to(d_t[:, None, :], (128, 8, 128)).reshape(1024, 128)

        def g_of(role):
            return qg[slot, 2 + role]

        def far_loop(body):
            for chip in range(1, 4):
                @pl.when(c == chip)
                def _():
                    for d in range(1, chip + 1):
                        body(d, 0)

        def scores(role, d, causal):
            sc = dot_nt(qg[slot, role], kvs[slot, d, 0]) * cs
            xs = []
            for j in range(2):
                dk_row = docs[2 * (c - d) + j, pl.ds(row, 1), :]
                vis = docr[role] == dk_row
                if causal:
                    vis = vis & (lane + 128 * j <= row_tok + 128 * piece[role])
                xs.append(jnp.where(vis, sc[:, 128 * j:128 * (j + 1)], NEG_BIG))
            top = jnp.maximum(xs[0], xs[1])
            es = [jnp.exp2(x - top) for x in xs]
            e_scr[d, role, :, lo_half] = es[0]
            e_scr[d, role, :, hi_half] = es[1]
            f_scr[d, role] = top
            l_scr[d, role] = es[0] + es[1]
            return top

        def dprob(role, d):
            dp_scr[d, role] = dot_nt(g_of(role), kvs[slot, d, 1])

        for role in range(2):
            t_scr[role] = scores(role, 0, True)

        def far_scores(d, x):
            for role in range(2):
                t_scr[role] = jnp.maximum(t_scr[role], scores(role, d, False))
            for role in range(2):
                dprob(role, d)
            return x
        far_loop(far_scores)

        for role in range(2):
            t_scr[role] = jnp.broadcast_to(jnp.max(t_scr[role], axis=1, keepdims=True), (1024, 128))
        dprob(0, 0)

        for role in range(2):
            top = t_scr[role]
            norm = l_scr[0, role] * jnp.exp2(f_scr[0, role] - top)
            for d in range(1, 4):
                norm = norm + l_scr[d, role] * jnp.exp2(f_scr[d, role] - top)
            t_scr[role] = top + jnp.log2(jnp.broadcast_to(jnp.sum(norm, axis=1, keepdims=True), (1024, 128)))
        dprob(1, 0)

        def weighted(role, d):
            f = jnp.exp2(f_scr[d, role] - t_scr[role])
            f_scr[d, role] = f
            for half in (lo_half, hi_half):
                p_scr[d, role, :, half] = (e_scr[d, role, :, half] * f).astype(jnp.bfloat16)
            return dot_nn(p_scr[d, role], kvs[slot, d, 1])

        def value_grads(d):
            dkv[gslot, d, :, 256:] = dot_tn(p_scr[d, 0], g_of(0)) + dot_tn(p_scr[d, 1], g_of(1))

        for role in range(2):
            o_acc[role] = weighted(role, 0)

        def far_weighted(d, x):
            for role in range(2):
                o_acc[role] = o_acc[role] + weighted(role, d)
            value_grads(d)
            return x
        far_loop(far_weighted)

        for role in range(2):
            o_low = o_acc[role].astype(jnp.bfloat16)
            outb[slot, role] = o_low
            delta = jnp.sum(g_of(role).astype(jnp.float32) * o_low.astype(jnp.float32), axis=1, keepdims=True)
            t_scr[role] = jnp.broadcast_to(delta, (1024, 128))
        value_grads(0)

        def score_grads(d):
            out = []
            for role in range(2):
                ds = [
                    (e_scr[d, role, :, half] * f_scr[d, role] * (dp_scr[d, role, :, half] - t_scr[role])).astype(jnp.bfloat16)
                    for half in (lo_half, hi_half)
                ]
                out.append(jnp.concatenate(ds, axis=1))
            dkv[gslot, d, :, :256] = dot_tn(out[0], qg[slot, 0]) + dot_tn(out[1], qg[slot, 1])
            return [dot_nn(ds, kvs[slot, d, 0]) for ds in out]

        got = score_grads(0)
        for role in range(2):
            o_acc[role] = got[role]

        def far_grads(d, x):
            got = score_grads(d)
            for role in range(2):
                o_acc[role] = o_acc[role] + got[role]
            return x
        far_loop(far_grads)
        for role in range(2):
            outb[slot, 2 + role] = (o_acc[role] * scale).astype(jnp.bfloat16)

    def part_wait(slot, s):
        remote(part.at[slot, s], part.at[slot, s], hop_s, part_r.at[slot, s], mate).wait_recv()

    def load(src, i):
        return [pltpu.make_async_copy(src.at[pl.ds(64 * n, 64)], sums.at[i, pl.ds(64 * n, 64)], lsem.at[i, n]) for n in range(4)]

    def start(copies):
        for copy in copies:
            copy.start()

    def finish(copies):
        for copy in copies:
            copy.wait()

    def passed(s, sl, chip, slot):
        return remote(sums.at[4 + sl], part.at[slot, s], xsem.at[sl], part_r.at[slot, s], dev(chip))

    def relay(s):
        return remote(part.at[2, s], part.at[1, s], rel_s.at[s], part_r.at[1, s], dev(1))

    def pass_on(i, group, held, slot_in, chip, slot_out):
        count = rank_in(i, group)
        sl = lax.rem(count, 2)
        start(load(hold.at[held, i], 0))
        part_wait(slot_in, i)
        start(load(part.at[slot_in, i], 1))
        pl.when(count >= 2)(lambda: passed(i, sl, chip, slot_out).wait_send())
        finish(load(hold.at[held, i], 0))
        finish(load(part.at[slot_in, i], 1))
        sums[4 + sl] = sums[0] + sums[1]
        passed(i, sl, chip, slot_out).start()

    def pass_x(i):
        pass_on(i, PASS_X, 0, 0, 0, 0)

    def pass_y(i):
        pass_on(i, ROUND, 0, 0, 0, 2)

    def total(kind, group, s, held, slots, chip):
        terms = [hold.at[held, s]] + [part.at[slot, s] for slot in slots]
        for slot in slots:
            part_wait(slot, s)
        for n, src in enumerate(terms):
            start(load(src, n))
        for n, src in enumerate(terms):
            finish(load(src, n))
        value = sums[0]
        for n in range(1, len(terms)):
            value = value + sums[n]
        finalize(kind, group, s, value, chip)

    for d in range(1, 4):
        f_scr[d] = jnp.full((2, 1024, 128), NEG_BIG, jnp.float32)
        l_scr[d] = jnp.zeros((2, 1024, 128), jnp.float32)
    arrive(0)
    fetch(0, 0)

    def step(s, x):
        slot = lax.rem(s, 2)

        @pl.when(s + 1 < NS)
        def _():
            arrive(s + 1)
            fetch(s + 1, 1 - slot)

        @pl.when(s >= 2)
        def _():
            put_wait(s - 2, slot)

        @pl.when(s >= NG)
        def _():
            grads_out(s - NG, False)
        fetch_wait(s, slot)
        attend(s, slot)

        @pl.when(c == 3)
        def _():
            gslot = lax.rem(s, NG)
            give(gslot, 3, 1, 0, s).start()
            pl.when(member(s, ROUND))(lambda: give(gslot, 2, 2, 0, s).start())

            @pl.when(member(s, MERGE))
            def _():
                part_wait(0, s)
                start(load(part.at[0, s], 0))
                finish(load(part.at[0, s], 0))
                dkv[gslot, 2] = dkv[gslot, 2] + sums[0]

            @pl.when(member(s, FAR1))
            def _():
                part_wait(0, s)
                start(load(part.at[0, s], 0))
                part_wait(2, s)
                start(load(part.at[2, s], 1))
                finish(load(part.at[0, s], 0))
                finish(load(part.at[2, s], 1))
                finalize(1, FAR1, s, dkv[gslot, 2] + sums[0] + sums[1], 1)
            finalize(0, OWN3, s, dkv[gslot, 0], None)
            pl.when(member(s, MERGE))(lambda: give(gslot, 2, 1, 1, s).start())

            def last_two():
                part_wait(1, s)
                start(load(part.at[1, s], 2))
                finish(load(part.at[1, s], 2))
                finalize(2, LAST2, s, dkv[gslot, 1] + sums[2], 2)
            choose(member(s, LAST2), last_two, lambda: give(gslot, 1, 2, 1, s).start())
        put(s, slot)
        for at, i in EARLY_X.items():
            pl.when((c == 1) & (s == at))(lambda: pass_x(i))
        for at, i in EARLY_Y.items():
            pl.when((c == 2) & (s == at))(lambda: pass_y(i))
        return x

    lax.fori_loop(0, NS, step, 0)
    put_wait(NS - 2, 0)
    put_wait(NS - 1, 1)
    for s in range(NS - NG, NS):
        grads_out(s, False)

    def home(i, x):
        def behind(lag, body):
            s = i - lag
            pl.when((s >= 0) & (s < NS))(lambda: body(s))

        @pl.when(c == 0)
        def _():
            @pl.when(member(i, ROUND))
            def _():
                part_wait(2, i)
                relay(i).start()
            pl.when(member(i, ON1))(lambda: pass_on(i, PASS_0, 1, 1, 1, 2))
            pl.when(member(i, ON2))(lambda: pass_on(i, PASS_0, 1, 0, 2, 2))
            behind(LAG[0], lambda s: pl.when(member(s, HERE0))(lambda: total(0, HERE0, s, 1, (1, 0), None)))

        @pl.when(c == 1)
        def _():
            later = tuple(s for s in PASS_X if s not in EARLY_X.values())
            pl.when(member(i, later))(lambda: pass_x(i))

            def body(s):
                pl.when(member(s, ON1))(lambda: total(1, ON1, s, 0, (0, 2), 0))
                pl.when(member(s, OWN1))(lambda: total(0, OWN1, s, 1, (1,), None))
            behind(LAG[1], body)

        @pl.when(c == 2)
        def _():
            later = tuple(s for s in ROUND if s not in EARLY_Y.values())
            pl.when(member(i, later))(lambda: pass_y(i))

            def body(s):
                pl.when(member(s, ON2))(lambda: total(1, ON2, s, 2, (2,), 0))
                pl.when(member(s, OWN2))(lambda: total(0, OWN2, s, 1, (1,), None))
            behind(LAG[2], body)
        return x

    @pl.when(c < 3)
    def _():
        lax.fori_loop(0, NS + max(LAG), home, 0)

    def down_wait(n):
        for which, ref in ((0, dk), (1, dv)):
            rows = ref.at[pl.ds(0, n)]
            remote(rows, rows, hop_s, down_r.at[which], mate).wait_recv()

    @pl.when(c == 0)
    def _():
        for s in ROUND:
            relay(s).wait_send()
        for sl in range(2):
            passed(0, sl, 1, 2).wait_send()
        remote(kvr.at[1], kvr.at[1], hop_s, kv_r.at[0, 0], mate).wait_send()
        final_drain(0, HERE0, None)
        down_wait(len(PASS_0))

    @pl.when(c == 1)
    def _():
        for sl in range(2):
            passed(0, sl, 0, 0).wait_send()
        remote(kvr.at[0], kvr.at[0], hop_s, kv_r.at[0, 0], mate).wait_send()
        final_drain(0, OWN1, None)
        final_drain(1, ON1, 0)
        down_wait(len(FAR1))

    @pl.when(c == 2)
    def _():
        for sl in range(2):
            passed(0, sl, 0, 2).wait_send()
        final_drain(0, OWN2, None)
        final_drain(1, ON2, 0)
        down_wait(len(LAST2))

    @pl.when(c == 3)
    def _():
        final_drain(0, OWN3, None)
        final_drain(1, FAR1, 1)
        final_drain(2, LAST2, 2)
    for which, ref in ((0, k), (1, v)):
        for way in range(2):
            @pl.when((c < 2) | ((c == 2) & (way == 0)))
            def _():
                remote(ref, ref, kv_s.at[way, which], kv_r.at[0, 0], mate).wait_send()
        half = ref.at[pl.ds(other, NS)]
        remote(half, half, kv_s.at[2, which], kv_r.at[0, 0], mate).wait_send()
    for which, ref in ((0, q), (1, g)):
        half = ref.at[pl.ds(other, NS)]
        remote(half, half, q_s.at[which], q_r.at[0], mate).wait_send()
    for which, ref in ((0, o), (1, dq)):
        half = ref.at[pl.ds(other, NS)]
        remote(half, half, hop_s, osend_r.at[which], mate).wait_recv()
    for which, ref in ((0, dk), (1, dv)):
        half = ref.at[pl.ds(other, NS)]
        remote(half, half, hop_s, dsend_r.at[which], mate).wait_recv()


def place_kernel(slots, *refs):
    srcs, dsts, (buf, rsem, wsem) = refs[:4], refs[4:8], refs[8:]
    jobs = []
    for src, dst in zip(srcs, dsts):
        n = src.shape[0]
        size = 512 * 1024 // (src.shape[1] * src.shape[2])
        for i in range(0, n, size):
            shape = (size,) + tuple(src.shape[1:])
            jobs.append((src.at[pl.ds(i, size)], dst.at[pl.ds(i, size)], shape))

    def view(slot, shape):
        return buf.at[slot].reshape(shape)

    def read(j):
        return pltpu.make_async_copy(jobs[j][0], view(j % slots, jobs[j][2]), rsem.at[j % slots])

    def write(j):
        return pltpu.make_async_copy(view(j % slots, jobs[j][2]), jobs[j][1], wsem.at[j % slots])

    ahead = slots
    for j in range(min(ahead, len(jobs))):
        read(j).start()
    for j in range(len(jobs)):
        read(j).wait()
        write(j).start()
        if j + ahead < len(jobs):
            if j + ahead >= slots:
                write(j + ahead - slots).wait()
            read(j + ahead).start()
    for j in range(max(0, len(jobs) - slots), len(jobs)):
        write(j).wait()


ANY = pl.BlockSpec(memory_space=pl.ANY)
VMEM = pl.BlockSpec(memory_space=pltpu.VMEM)


def solution(mesh):
    n_dev = mesh.shape['cp']
    seq_spec = P('dp', 'cp', None, None)
    id_spec = P('dp', 'cp')
    bf, f32 = jnp.bfloat16, jnp.float32
    shape = jax.ShapeDtypeStruct
    dma = pltpu.SemaphoreType.DMA

    def per_device(query, keys, values, grad_out, doc_id):
        nb, piece, heads, hd = query.shape
        rows = piece * heads
        outs = pl.pallas_call(
            functools.partial(fused_kernel, hd ** -0.5),
            in_specs=[VMEM] + [ANY] * 4,
            out_specs=[ANY] * 8,
            out_shape=[
                shape((nb, rows, hd), bf), shape((nb, rows, hd), bf), shape((nb, piece, hd), bf), shape((nb, piece, hd), bf),
                shape((NS, 2, rows, hd), bf), shape((4, NS, 2, 256, 256), bf),
                shape((3, NS, 256, 512), f32), shape((3, NS, 256, 512), f32),
            ],
            scratch_shapes=[
                pltpu.VMEM((n_dev, nb, piece), jnp.int32), pltpu.VMEM((2, 4, 2, 256, 256), bf), pltpu.VMEM((2, 4, rows, hd), bf),
                pltpu.VMEM((2, 4, rows, hd), bf), pltpu.VMEM((NG, 4, 256, 512), f32), pltpu.VMEM((6, 256, 512), f32),
                pltpu.VMEM((3, 2, 2, 256, 256), bf),
                pltpu.VMEM((4, 2, rows, 256), f32), pltpu.VMEM((4, 2, rows, 256), f32), pltpu.VMEM((4, 2, rows, 256), bf),
                pltpu.VMEM((4, 2, rows, 128), f32), pltpu.VMEM((4, 2, rows, 128), f32), pltpu.VMEM((2, rows, 128), f32),
                pltpu.VMEM((2, rows, 128), jnp.int32), pltpu.VMEM((2, rows, hd), f32),
                dma((n_dev,)), dma((n_dev,)), dma((2, 10)), dma((2, 4)), dma((NG, 4)), dma((2,)), dma((2,)), dma((NJ,)), dma((3, 2)), dma((4, NJ)),
                dma, dma((3, NS)), dma((3, 2, 4)), dma((2,)), dma((3, 4)), dma((2,)), dma((NS,)), dma((2,)),
            ],
            compiler_params=pltpu.CompilerParams(has_side_effects=True, vmem_limit_bytes=62 * 1024 * 1024),
            name="attend",
        )(doc_id, query.reshape(nb, rows, hd), grad_out.reshape(nb, rows, hd), keys.reshape(nb, piece, hd), values.reshape(nb, piece, hd))
        outs = [x.reshape(nb, -1, hd) for x in outs[:4]]
        o, dq, dk, dv = pl.pallas_call(
            functools.partial(place_kernel, 36),
            in_specs=[ANY] * 4,
            out_specs=[ANY] * 4,
            out_shape=[shape(x.shape, bf) for x in outs],
            scratch_shapes=[pltpu.VMEM((36, 2048, hd), bf), dma((36,)), dma((36,))],
            compiler_params=pltpu.CompilerParams(vmem_limit_bytes=48 * 1024 * 1024),
            name="place",
        )(*outs)
        return o.reshape(query.shape), dq.reshape(query.shape), dk.reshape(keys.shape), dv.reshape(values.shape)

    return jax.shard_map(per_device, mesh=mesh, in_specs=(seq_spec, seq_spec, seq_spec, seq_spec, id_spec),
                         out_specs=(seq_spec, seq_spec, seq_spec, seq_spec), check_vma=False)
```

```python
import functools

import jax
import jax.numpy as jnp
from jax import lax
from jax.experimental import pallas as pl
from jax.experimental.pallas import tpu as pltpu
from jax.sharding import PartitionSpec as P

NEG_BIG = -1e30
LOG2E = 1.4426950408889634
NS = 16
NJ = NS
AHEAD = 2
NG = 4
PLAN1 = 'RMRMRRFRRFRFFRMM'
PLAN0 = 'NNNANCNNACCNCNNN'
LAST2 = (5, 7, 12, 14)
EARLY_X = {5: 0, 6: 1, 8: 2, 9: 4, 10: 5, 13: 6, 14: 7, 15: 9}
EARLY_Y = {4: 0, 6: 2, 9: 4, 12: 5, 13: 7, 14: 8, 15: 10}
LAG = (8, 6, 7)


def where_plan(plan, kinds):
    return tuple(s for s in range(NS) if plan[s] in kinds)


ROUND, MERGE, FAR1 = (where_plan(PLAN1, x) for x in 'RMF')
HERE0, ON1, ON2 = (where_plan(PLAN0, x) for x in 'NAC')
OWN1 = where_plan(PLAN1, 'RM')
OWN2 = tuple(s for s in range(NS) if s not in LAST2)
OWN3 = tuple(range(NS))
PASS_X = where_plan(PLAN0, 'NC')
PASS_0 = where_plan(PLAN0, 'AC')


def dot_nt(a, b):
    return lax.dot_general(a, b, (((1,), (1,)), ((), ())), preferred_element_type=jnp.float32)


def dot_nn(a, b):
    return lax.dot_general(a, b, (((1,), (0,)), ((), ())), preferred_element_type=jnp.float32)


def dot_tn(a, b):
    return lax.dot_general(a, b, (((0,), (0,)), ((), ())), preferred_element_type=jnp.float32)


def remote(src, dst, send, recv, dev):
    return pltpu.make_async_remote_copy(src_ref=src, dst_ref=dst, send_sem=send, recv_sem=recv,
                                        device_id={'cp': dev}, device_id_type=pl.DeviceIdType.MESH)


def fused_kernel(scale, doc, q, g, k, v, o, dq, dk, dv, qgm, kvr, part, hold,
                 docs, kvs, qg, outb, dkv, sums, fin, e_scr, dp_scr, p_scr, l_scr, f_scr, t_scr, docr, o_acc,
                 doc_s, doc_r, isem, osem, gsem, osend_r, q_s, q_r, kv_s, kv_r, hop_s, part_r, fsem, dsend_r, lsem, xsem, rel_s, down_r):
    rank = lax.axis_index('cp')
    n_dev = docs.shape[0]
    c = rank // 2
    e = lax.rem(rank, 2)
    mate = 2 * c + 1 - e
    other = NS * (1 - e)
    mine = NS * e

    def dev(chip):
        return 2 * chip + e

    docs[rank] = doc[...]

    def doc_copy(i):
        return remote(doc, docs.at[rank], doc_s.at[i], doc_r.at[i], lax.rem(rank + i, n_dev))

    for i in range(1, n_dev):
        doc_copy(i).start()

    def kv_parts(chip, way, j, cols):
        out = []
        for col in cols:
            for which, ref in ((0, k), (1, v)):
                out.append(remote(ref.at[pl.ds(col * NS + j, 1)], kvr.at[c, pl.ds(j, 1), which, pl.ds(128 * e, 128)],
                                  kv_s.at[way, which], kv_r.at[c, j], 2 * chip + col))
        return out

    def send_kv(chip, way, j):
        for copy in kv_parts(chip, way, j, (0, 1)):
            copy.start()

    def kv_forward(a, chip, j):
        return remote(kvr.at[a, pl.ds(j, 1)], kvr.at[a, pl.ds(j, 1)], hop_s, kv_r.at[a, j], dev(chip))

    def stream_kv(j):
        @pl.when(c == 0)
        def _():
            send_kv(1, 0, j)
            send_kv(2, 1, j)

        @pl.when(c == 1)
        def _():
            send_kv(0, 1, j)

        @pl.when(c == 2)
        def _():
            send_kv(3, 0, j)

    def to_mate(j):
        for which, ref in ((0, k), (1, v)):
            remote(ref.at[pl.ds(other + j, 1)], kvr.at[c, pl.ds(j, 1), which, pl.ds(128 * e, 128)],
                   kv_s.at[2, which], kv_r.at[c, j], mate).start()

    def rows_to_mate(j):
        for which, ref in ((0, q), (1, g)):
            remote(ref.at[pl.ds(other + j, 1)], qgm.at[pl.ds(j, 1), which], q_s.at[which], q_r.at[j], mate).start()

    stream_kv(0)

    @pl.when(c == 1)
    def _():
        send_kv(3, 0, 0)
    to_mate(0)
    rows_to_mate(0)
    for j in range(1, AHEAD):
        stream_kv(j)
    for j in range(1, NJ):
        to_mate(j)
        rows_to_mate(j)
    for i in range(1, n_dev):
        doc_copy(i).wait()

    def arrive(j):
        remote(kvr.at[c, pl.ds(j, 1), :, pl.ds(0, 128)], kvr.at[c, pl.ds(j, 1), :, pl.ds(0, 128)],
               hop_s, kv_r.at[c, j], mate).wait_recv()
        remote(qgm.at[pl.ds(j, 1)], qgm.at[pl.ds(j, 1)], hop_s, q_r.at[j], mate).wait_recv()
        for a in range(3):
            @pl.when(a < c)
            def _():
                kv_forward(a, a, j).wait_recv()

        @pl.when(c == 1)
        def _():
            kv_forward(0, 3, j).start()

            @pl.when(j + 1 < NJ)
            def _():
                send_kv(3, 0, j + 1)

        @pl.when(c == 0)
        def _():
            kv_forward(1, 1, j).wait_recv()
            kv_forward(1, 2, j).start()

        @pl.when(j + AHEAD < NJ)
        def _():
            stream_kv(j + AHEAD)

    def inputs(s, sl):
        row = mine + s
        rows = pl.ds(128 * e, 128)
        rest = pl.ds(128 - 128 * e, 128)
        pairs = [
            (q.at[row], qg.at[sl, 0]), (g.at[row], qg.at[sl, 2]), (qgm.at[s, 0], qg.at[sl, 1]), (qgm.at[s, 1], qg.at[sl, 3]),
            (k.at[row], kvs.at[sl, 0, 0, rows]), (v.at[row], kvs.at[sl, 0, 1, rows]),
            (kvr.at[c, s, :, rest], kvs.at[sl, 0, :, rest]),
        ]
        return [pltpu.make_async_copy(src, dst, isem.at[sl, i]) for i, (src, dst) in enumerate(pairs)]

    def far_input(s, sl, d):
        return pltpu.make_async_copy(kvr.at[c - d, s], kvs.at[sl, d], isem.at[sl, 6 + d])

    def fetch(s, sl):
        for copy in inputs(s, sl):
            copy.start()
        for d in range(1, 4):
            @pl.when(d <= c)
            def _():
                far_input(s, sl, d).start()

    def fetch_wait(s, sl):
        for copy in inputs(s, sl):
            copy.wait()
        for d in range(1, 4):
            @pl.when(d <= c)
            def _():
                far_input(s, sl, d).wait()

    def row_outputs(s, sl):
        row = mine + s
        here = [pltpu.make_async_copy(outb.at[sl, 0], o.at[row], osem.at[sl, 0]),
                pltpu.make_async_copy(outb.at[sl, 2], dq.at[row], osem.at[sl, 1])]
        there = [remote(outb.at[sl, 1], o.at[row], osem.at[sl, 2], osend_r.at[0], mate),
                 remote(outb.at[sl, 3], dq.at[row], osem.at[sl, 3], osend_r.at[1], mate)]
        return here, there

    def keep(sl, d, slot, s):
        return pltpu.make_async_copy(dkv.at[sl, d], hold.at[slot, s], gsem.at[sl, d])

    def give(sl, d, chip, slot, s):
        return remote(dkv.at[sl, d], part.at[slot, s], gsem.at[sl, d], part_r.at[slot, s], dev(chip))

    def member(s, group):
        out = jnp.bool_(False)
        for one in group:
            out = out | (s == one)
        return out

    def rank_in(s, group):
        count = jnp.int32(0)
        for one in group:
            count = count + jnp.where(one < s, 1, 0)
        return count

    def choose(cond, yes, no):
        pl.when(cond)(yes)
        pl.when(jnp.logical_not(cond))(no)

    def grads_out(s, begin):
        sl = lax.rem(s, NG)

        def local(d, slot):
            copy = keep(sl, d, slot, s)
            copy.start() if begin else copy.wait()

        def away(d, chip, slot):
            copy = give(sl, d, chip, slot, s)
            copy.start() if begin else copy.wait_send()

        @pl.when(c == 0)
        def _():
            local(0, 1)

        @pl.when(c == 1)
        def _():
            choose(member(s, FAR1), lambda: away(0, 3, 2), lambda: local(0, 1))
            local(1, 0)

        @pl.when(c == 2)
        def _():
            choose(member(s, ROUND), lambda: local(1, 0), lambda: away(1, 3, 0))
            choose(member(s, LAST2), lambda: away(0, 3, 1), lambda: local(0, 1))
            choose(member(s, ON2), lambda: local(2, 2), lambda: away(2, 0, 1))

        if not begin:
            @pl.when(c == 3)
            def _():
                away(3, 1, 0)
                pl.when(member(s, ROUND))(lambda: away(2, 2, 0))
                pl.when(member(s, MERGE))(lambda: away(2, 1, 1))
                pl.when(jnp.logical_not(member(s, LAST2)))(lambda: away(1, 2, 1))

    def put(s, sl):
        here, there = row_outputs(s, sl)
        for copy in here + there:
            copy.start()
        grads_out(s, True)

    def put_wait(s, sl):
        here, there = row_outputs(s, sl)
        for copy in here:
            copy.wait()
        for copy in there:
            copy.wait_send()

    def final_copies(kind, sl, s, chip):
        row = mine + s
        out = []
        for which, ref in ((0, dk), (1, dv)):
            for far, rows in ((0, pl.ds(128 * e, 128)), (1, pl.ds(128 - 128 * e, 128))):
                src, sem = fin.at[kind, sl, which, rows], fsem.at[kind, sl, 2 * which + far]
                if far:
                    out.append(remote(src, ref.at[row], sem, dsend_r.at[which], mate if chip is None else 2 * chip + 1 - e))
                elif chip is None:
                    out.append(pltpu.make_async_copy(src, ref.at[row], sem))
                else:
                    out.append(remote(src, ref.at[row], sem, down_r.at[which], dev(chip)))
        return out

    def final_wait(kind, sl, chip):
        for i, copy in enumerate(final_copies(kind, sl, 0, chip)):
            if chip is None and i % 2 == 0:
                copy.wait()
            else:
                copy.wait_send()

    def finalize(kind, group, s, value, chip):
        count = rank_in(s, group)
        sl = lax.rem(count, 2)
        pl.when(count >= 2)(lambda: final_wait(kind, sl, chip))
        fin[kind, sl, 0] = (value[:, :256] * scale).astype(jnp.bfloat16)
        fin[kind, sl, 1] = value[:, 256:].astype(jnp.bfloat16)
        for copy in final_copies(kind, sl, s, chip):
            copy.start()

    def final_drain(kind, group, chip):
        for n in range(max(0, len(group) - 2), len(group)):
            final_wait(kind, n % 2, chip)

    row_tok = lax.broadcasted_iota(jnp.int32, (1024, 128), 0) >> 3
    lane = lax.broadcasted_iota(jnp.int32, (1024, 128), 1)
    cs = scale * LOG2E
    lo_half, hi_half = slice(0, 128), slice(128, 256)

    def attend(s, slot):
        row = mine + s
        gslot = lax.rem(s, NG)
        piece = (e, 1 - e)
        for role in range(2):
            dq_row = docs[2 * c + piece[role], pl.ds(row, 1), :]
            d_t = jnp.transpose(jnp.broadcast_to(dq_row, (128, 128)))
            docr[role] = jnp.broadcast_to(d_t[:, None, :], (128, 8, 128)).reshape(1024, 128)

        def g_of(role):
            return qg[slot, 2 + role]

        def far_loop(body):
            for chip in range(1, 4):
                @pl.when(c == chip)
                def _():
                    for d in range(1, chip + 1):
                        body(d, 0)

        def scores(role, d, causal):
            sc = dot_nt(qg[slot, role], kvs[slot, d, 0]) * cs
            xs = []
            for j in range(2):
                dk_row = docs[2 * (c - d) + j, pl.ds(row, 1), :]
                vis = docr[role] == dk_row
                if causal:
                    vis = vis & (lane + 128 * j <= row_tok + 128 * piece[role])
                xs.append(jnp.where(vis, sc[:, 128 * j:128 * (j + 1)], NEG_BIG))
            top = jnp.maximum(xs[0], xs[1])
            es = [jnp.exp2(x - top) for x in xs]
            e_scr[d, role, :, lo_half] = es[0]
            e_scr[d, role, :, hi_half] = es[1]
            f_scr[d, role] = top
            l_scr[d, role] = es[0] + es[1]
            return top

        def dprob(role, d):
            dp_scr[d, role] = dot_nt(g_of(role), kvs[slot, d, 1])

        for role in range(2):
            t_scr[role] = scores(role, 0, True)

        def far_scores(d, x):
            for role in range(2):
                t_scr[role] = jnp.maximum(t_scr[role], scores(role, d, False))
            for role in range(2):
                dprob(role, d)
            return x
        far_loop(far_scores)

        for role in range(2):
            t_scr[role] = jnp.broadcast_to(jnp.max(t_scr[role], axis=1, keepdims=True), (1024, 128))
        dprob(0, 0)

        for role in range(2):
            top = t_scr[role]
            norm = l_scr[0, role] * jnp.exp2(f_scr[0, role] - top)
            for d in range(1, 4):
                norm = norm + l_scr[d, role] * jnp.exp2(f_scr[d, role] - top)
            t_scr[role] = top + jnp.log2(jnp.broadcast_to(jnp.sum(norm, axis=1, keepdims=True), (1024, 128)))
        dprob(1, 0)

        def weighted(role, d):
            f = jnp.exp2(f_scr[d, role] - t_scr[role])
            f_scr[d, role] = f
            for half in (lo_half, hi_half):
                p_scr[d, role, :, half] = (e_scr[d, role, :, half] * f).astype(jnp.bfloat16)
            return dot_nn(p_scr[d, role], kvs[slot, d, 1])

        def value_grads(d):
            dkv[gslot, d, :, 256:] = dot_tn(p_scr[d, 0], g_of(0)) + dot_tn(p_scr[d, 1], g_of(1))

        for role in range(2):
            o_acc[role] = weighted(role, 0)

        def far_weighted(d, x):
            for role in range(2):
                o_acc[role] = o_acc[role] + weighted(role, d)
            value_grads(d)
            return x
        far_loop(far_weighted)

        for role in range(2):
            o_low = o_acc[role].astype(jnp.bfloat16)
            outb[slot, role] = o_low
            delta = jnp.sum(g_of(role).astype(jnp.float32) * o_low.astype(jnp.float32), axis=1, keepdims=True)
            t_scr[role] = jnp.broadcast_to(delta, (1024, 128))
        value_grads(0)

        def score_grads(d):
            out = []
            for role in range(2):
                ds = [
                    (e_scr[d, role, :, half] * f_scr[d, role] * (dp_scr[d, role, :, half] - t_scr[role])).astype(jnp.bfloat16)
                    for half in (lo_half, hi_half)
                ]
                out.append(jnp.concatenate(ds, axis=1))
            dkv[gslot, d, :, :256] = dot_tn(out[0], qg[slot, 0]) + dot_tn(out[1], qg[slot, 1])
            return [dot_nn(ds, kvs[slot, d, 0]) for ds in out]

        got = score_grads(0)
        for role in range(2):
            o_acc[role] = got[role]

        def far_grads(d, x):
            got = score_grads(d)
            for role in range(2):
                o_acc[role] = o_acc[role] + got[role]
            return x
        far_loop(far_grads)
        for role in range(2):
            outb[slot, 2 + role] = (o_acc[role] * scale).astype(jnp.bfloat16)

    def part_wait(slot, s):
        remote(part.at[slot, s], part.at[slot, s], hop_s, part_r.at[slot, s], mate).wait_recv()

    def load(src, i):
        return [pltpu.make_async_copy(src.at[pl.ds(64 * n, 64)], sums.at[i, pl.ds(64 * n, 64)], lsem.at[i, n]) for n in range(4)]

    def start(copies):
        for copy in copies:
            copy.start()

    def finish(copies):
        for copy in copies:
            copy.wait()

    def passed(s, sl, chip, slot):
        return remote(sums.at[4 + sl], part.at[slot, s], xsem.at[sl], part_r.at[slot, s], dev(chip))

    def relay(s):
        return remote(part.at[2, s], part.at[1, s], rel_s.at[s], part_r.at[1, s], dev(1))

    def pass_on(i, group, held, slot_in, chip, slot_out):
        count = rank_in(i, group)
        sl = lax.rem(count, 2)
        start(load(hold.at[held, i], 0))
        part_wait(slot_in, i)
        start(load(part.at[slot_in, i], 1))
        pl.when(count >= 2)(lambda: passed(i, sl, chip, slot_out).wait_send())
        finish(load(hold.at[held, i], 0))
        finish(load(part.at[slot_in, i], 1))
        sums[4 + sl] = sums[0] + sums[1]
        passed(i, sl, chip, slot_out).start()

    def pass_x(i):
        pass_on(i, PASS_X, 0, 0, 0, 0)

    def pass_y(i):
        pass_on(i, ROUND, 0, 0, 0, 2)

    def total(kind, group, s, held, slots, chip):
        terms = [hold.at[held, s]] + [part.at[slot, s] for slot in slots]
        for slot in slots:
            part_wait(slot, s)
        for n, src in enumerate(terms):
            start(load(src, n))
        for n, src in enumerate(terms):
            finish(load(src, n))
        value = sums[0]
        for n in range(1, len(terms)):
            value = value + sums[n]
        finalize(kind, group, s, value, chip)

    for d in range(1, 4):
        f_scr[d] = jnp.full((2, 1024, 128), NEG_BIG, jnp.float32)
        l_scr[d] = jnp.zeros((2, 1024, 128), jnp.float32)
    arrive(0)
    fetch(0, 0)

    def step(s, x):
        slot = lax.rem(s, 2)

        @pl.when(s + 1 < NS)
        def _():
            arrive(s + 1)
            fetch(s + 1, 1 - slot)

        @pl.when(s >= 2)
        def _():
            put_wait(s - 2, slot)

        @pl.when(s >= NG)
        def _():
            grads_out(s - NG, False)
        fetch_wait(s, slot)
        attend(s, slot)

        @pl.when(c == 3)
        def _():
            gslot = lax.rem(s, NG)
            give(gslot, 3, 1, 0, s).start()
            pl.when(member(s, ROUND))(lambda: give(gslot, 2, 2, 0, s).start())

            @pl.when(member(s, MERGE))
            def _():
                part_wait(0, s)
                start(load(part.at[0, s], 0))
                finish(load(part.at[0, s], 0))
                dkv[gslot, 2] = dkv[gslot, 2] + sums[0]

            @pl.when(member(s, FAR1))
            def _():
                part_wait(0, s)
                start(load(part.at[0, s], 0))
                part_wait(2, s)
                start(load(part.at[2, s], 1))
                finish(load(part.at[0, s], 0))
                finish(load(part.at[2, s], 1))
                finalize(1, FAR1, s, dkv[gslot, 2] + sums[0] + sums[1], 1)
            finalize(0, OWN3, s, dkv[gslot, 0], None)
            pl.when(member(s, MERGE))(lambda: give(gslot, 2, 1, 1, s).start())

            def last_two():
                part_wait(1, s)
                start(load(part.at[1, s], 2))
                finish(load(part.at[1, s], 2))
                finalize(2, LAST2, s, dkv[gslot, 1] + sums[2], 2)
            choose(member(s, LAST2), last_two, lambda: give(gslot, 1, 2, 1, s).start())
        put(s, slot)
        for at, i in EARLY_X.items():
            pl.when((c == 1) & (s == at))(lambda: pass_x(i))
        for at, i in EARLY_Y.items():
            pl.when((c == 2) & (s == at))(lambda: pass_y(i))
        return x

    lax.fori_loop(0, NS, step, 0)
    put_wait(NS - 2, 0)
    put_wait(NS - 1, 1)
    for s in range(NS - NG, NS):
        grads_out(s, False)

    def home(i, x):
        def behind(lag, body):
            s = i - lag
            pl.when((s >= 0) & (s < NS))(lambda: body(s))

        @pl.when(c == 0)
        def _():
            @pl.when(member(i, ROUND))
            def _():
                part_wait(2, i)
                relay(i).start()
            pl.when(member(i, ON1))(lambda: pass_on(i, PASS_0, 1, 1, 1, 2))
            pl.when(member(i, ON2))(lambda: pass_on(i, PASS_0, 1, 0, 2, 2))
            behind(LAG[0], lambda s: pl.when(member(s, HERE0))(lambda: total(0, HERE0, s, 1, (1, 0), None)))

        @pl.when(c == 1)
        def _():
            later = tuple(s for s in PASS_X if s not in EARLY_X.values())
            pl.when(member(i, later))(lambda: pass_x(i))

            def body(s):
                pl.when(member(s, ON1))(lambda: total(1, ON1, s, 0, (0, 2), 0))
                pl.when(member(s, OWN1))(lambda: total(0, OWN1, s, 1, (1,), None))
            behind(LAG[1], body)

        @pl.when(c == 2)
        def _():
            later = tuple(s for s in ROUND if s not in EARLY_Y.values())
            pl.when(member(i, later))(lambda: pass_y(i))

            def body(s):
                pl.when(member(s, ON2))(lambda: total(1, ON2, s, 2, (2,), 0))
                pl.when(member(s, OWN2))(lambda: total(0, OWN2, s, 1, (1,), None))
            behind(LAG[2], body)
        return x

    @pl.when(c < 3)
    def _():
        lax.fori_loop(0, NS + max(LAG), home, 0)

    def down_wait(n):
        for which, ref in ((0, dk), (1, dv)):
            rows = ref.at[pl.ds(0, n)]
            remote(rows, rows, hop_s, down_r.at[which], mate).wait_recv()

    @pl.when(c == 0)
    def _():
        for s in ROUND:
            relay(s).wait_send()
        for sl in range(2):
            passed(0, sl, 1, 2).wait_send()
        remote(kvr.at[1], kvr.at[1], hop_s, kv_r.at[0, 0], mate).wait_send()
        final_drain(0, HERE0, None)
        down_wait(len(PASS_0))

    @pl.when(c == 1)
    def _():
        for sl in range(2):
            passed(0, sl, 0, 0).wait_send()
        remote(kvr.at[0], kvr.at[0], hop_s, kv_r.at[0, 0], mate).wait_send()
        final_drain(0, OWN1, None)
        final_drain(1, ON1, 0)
        down_wait(len(FAR1))

    @pl.when(c == 2)
    def _():
        for sl in range(2):
            passed(0, sl, 0, 2).wait_send()
        final_drain(0, OWN2, None)
        final_drain(1, ON2, 0)
        down_wait(len(LAST2))

    @pl.when(c == 3)
    def _():
        final_drain(0, OWN3, None)
        final_drain(1, FAR1, 1)
        final_drain(2, LAST2, 2)
    for which, ref in ((0, k), (1, v)):
        for way in range(2):
            @pl.when((c < 2) | ((c == 2) & (way == 0)))
            def _():
                remote(ref, ref, kv_s.at[way, which], kv_r.at[0, 0], mate).wait_send()
        half = ref.at[pl.ds(other, NS)]
        remote(half, half, kv_s.at[2, which], kv_r.at[0, 0], mate).wait_send()
    for which, ref in ((0, q), (1, g)):
        half = ref.at[pl.ds(other, NS)]
        remote(half, half, q_s.at[which], q_r.at[0], mate).wait_send()
    for which, ref in ((0, o), (1, dq)):
        half = ref.at[pl.ds(other, NS)]
        remote(half, half, hop_s, osend_r.at[which], mate).wait_recv()
    for which, ref in ((0, dk), (1, dv)):
        half = ref.at[pl.ds(other, NS)]
        remote(half, half, hop_s, dsend_r.at[which], mate).wait_recv()


def place_kernel(slots, *refs):
    srcs, dsts, (buf, rsem, wsem) = refs[:4], refs[4:8], refs[8:]
    size = buf.shape[1]
    jobs = [(src.at[pl.ds(i, size)], dst.at[pl.ds(i, size)]) for src, dst in zip(srcs, dsts) for i in range(0, src.shape[0], size)]

    def read(j):
        return pltpu.make_async_copy(jobs[j][0], buf.at[j % slots], rsem.at[j % slots])

    def write(j):
        return pltpu.make_async_copy(buf.at[j % slots], jobs[j][1], wsem.at[j % slots])

    ahead = slots
    for j in range(min(ahead, len(jobs))):
        read(j).start()
    for j in range(len(jobs)):
        read(j).wait()
        write(j).start()
        if j + ahead < len(jobs):
            if j + ahead >= slots:
                write(j + ahead - slots).wait()
            read(j + ahead).start()
    for j in range(max(0, len(jobs) - slots), len(jobs)):
        write(j).wait()


ANY = pl.BlockSpec(memory_space=pl.ANY)
VMEM = pl.BlockSpec(memory_space=pltpu.VMEM)


def solution(mesh):
    n_dev = mesh.shape['cp']
    seq_spec = P('dp', 'cp', None, None)
    id_spec = P('dp', 'cp')
    bf, f32 = jnp.bfloat16, jnp.float32
    shape = jax.ShapeDtypeStruct
    dma = pltpu.SemaphoreType.DMA

    def per_device(query, keys, values, grad_out, doc_id):
        nb, piece, heads, hd = query.shape
        rows = piece * heads
        outs = pl.pallas_call(
            functools.partial(fused_kernel, hd ** -0.5),
            in_specs=[VMEM] + [ANY] * 4,
            out_specs=[ANY] * 8,
            out_shape=[
                shape((nb, rows, hd), bf), shape((nb, rows, hd), bf), shape((nb, piece, hd), bf), shape((nb, piece, hd), bf),
                shape((NS, 2, rows, hd), bf), shape((4, NS, 2, 256, 256), bf),
                shape((3, NS, 256, 512), f32), shape((3, NS, 256, 512), f32),
            ],
            scratch_shapes=[
                pltpu.VMEM((n_dev, nb, piece), jnp.int32), pltpu.VMEM((2, 4, 2, 256, 256), bf), pltpu.VMEM((2, 4, rows, hd), bf),
                pltpu.VMEM((2, 4, rows, hd), bf), pltpu.VMEM((NG, 4, 256, 512), f32), pltpu.VMEM((6, 256, 512), f32),
                pltpu.VMEM((3, 2, 2, 256, 256), bf),
                pltpu.VMEM((4, 2, rows, 256), f32), pltpu.VMEM((4, 2, rows, 256), f32), pltpu.VMEM((4, 2, rows, 256), bf),
                pltpu.VMEM((4, 2, rows, 128), f32), pltpu.VMEM((4, 2, rows, 128), f32), pltpu.VMEM((2, rows, 128), f32),
                pltpu.VMEM((2, rows, 128), jnp.int32), pltpu.VMEM((2, rows, hd), f32),
                dma((n_dev,)), dma((n_dev,)), dma((2, 10)), dma((2, 4)), dma((NG, 4)), dma((2,)), dma((2,)), dma((NJ,)), dma((3, 2)), dma((4, NJ)),
                dma, dma((3, NS)), dma((3, 2, 4)), dma((2,)), dma((3, 4)), dma((2,)), dma((NS,)), dma((2,)),
            ],
            compiler_params=pltpu.CompilerParams(has_side_effects=True, vmem_limit_bytes=62 * 1024 * 1024),
            name="attend",
        )(doc_id, query.reshape(nb, rows, hd), grad_out.reshape(nb, rows, hd), keys.reshape(nb, piece, hd), values.reshape(nb, piece, hd))
        outs = [x.reshape(-1, rows, hd) for x in outs[:4]]
        o, dq, dk, dv = pl.pallas_call(
            functools.partial(place_kernel, 36),
            in_specs=[ANY] * 4,
            out_specs=[ANY] * 4,
            out_shape=[shape(x.shape, bf) for x in outs],
            scratch_shapes=[pltpu.VMEM((36, 2, rows, hd), bf), dma((36,)), dma((36,))],
            compiler_params=pltpu.CompilerParams(vmem_limit_bytes=63 * 1024 * 1024),
            name="place",
        )(*outs)
        return o.reshape(query.shape), dq.reshape(query.shape), dk.reshape(keys.shape), dv.reshape(values.shape)

    return jax.shard_map(per_device, mesh=mesh, in_specs=(seq_spec, seq_spec, seq_spec, seq_spec, id_spec),
                         out_specs=(seq_spec, seq_spec, seq_spec, seq_spec), check_vma=False)
```

```python
import functools

import jax
import jax.numpy as jnp
from jax import lax
from jax.experimental import pallas as pl
from jax.experimental.pallas import tpu as pltpu
from jax.sharding import PartitionSpec as P

NEG_BIG = -1e30
LOG2E = 1.4426950408889634
NS = 16
NJ = NS
AHEAD = 2
NG = 4
PLAN1 = 'RRRMFMRRFRFRRMMM'
PLAN0 = 'NNANANCCNCNNCNNA'
LAST2 = (8, 9, 11)
EARLY_X = {6: 0, 8: 1, 10: 3, 12: 5, 13: 6, 14: 7}
EARLY_Y = {5: 0, 7: 1, 9: 2, 10: 6, 13: 7, 14: 9, 15: 11}
LAG = (6, 8, 7)
LATE_CHIP = 2
VIA3 = (0, 1)


def where_plan(plan, kinds):
    return tuple(s for s in range(NS) if plan[s] in kinds)


ROUND, MERGE, FAR1 = (where_plan(PLAN1, x) for x in 'RMF')
HERE0, ON1, ON2 = (where_plan(PLAN0, x) for x in 'NAC')
OWN1 = where_plan(PLAN1, 'RM')
OWN2 = tuple(s for s in range(NS) if s not in LAST2)
OWN3 = tuple(range(NS))
PASS_X = where_plan(PLAN0, 'NC')
PASS_0 = where_plan(PLAN0, 'AC')


def dot_nt(a, b):
    return lax.dot_general(a, b, (((1,), (1,)), ((), ())), preferred_element_type=jnp.float32)


def dot_nn(a, b):
    return lax.dot_general(a, b, (((1,), (0,)), ((), ())), preferred_element_type=jnp.float32)


def dot_tn(a, b):
    return lax.dot_general(a, b, (((0,), (0,)), ((), ())), preferred_element_type=jnp.float32)


def remote(src, dst, send, recv, dev):
    return pltpu.make_async_remote_copy(src_ref=src, dst_ref=dst, send_sem=send, recv_sem=recv,
                                        device_id={'cp': dev}, device_id_type=pl.DeviceIdType.MESH)


def fused_kernel(scale, doc, q, g, k, v, o, dq, dk, dv, qgm, kvr, part, hold,
                 docs, kvs, qg, outb, dkv, sums, fin, e_scr, dp_scr, p_scr, l_scr, f_scr, t_scr, docr, o_acc,
                 doc_s, doc_r, isem, osem, gsem, osend_r, q_s, q_r, kv_s, kv_r, hop_s, part_r, fsem, dsend_r, lsem, xsem, rel_s, down_r):
    rank = lax.axis_index('cp')
    n_dev = docs.shape[0]
    c = rank // 2
    e = lax.rem(rank, 2)
    mate = 2 * c + 1 - e
    other = NS * (1 - e)
    mine = NS * e

    def dev(chip):
        return 2 * chip + e

    docs[rank] = doc[...]

    def doc_copy(i):
        return remote(doc, docs.at[rank], doc_s.at[i], doc_r.at[i], lax.rem(rank + i, n_dev))

    for i in range(1, n_dev):
        doc_copy(i).start()

    def kv_parts(chip, way, j, cols):
        out = []
        for col in cols:
            for which, ref in ((0, k), (1, v)):
                out.append(remote(ref.at[pl.ds(col * NS + j, 1)], kvr.at[c, pl.ds(j, 1), which, pl.ds(128 * e, 128)],
                                  kv_s.at[way, which], kv_r.at[c, j], 2 * chip + col))
        return out

    def send_kv(chip, way, j):
        for copy in kv_parts(chip, way, j, (0, 1)):
            copy.start()

    def kv_forward(a, chip, j):
        return remote(kvr.at[a, pl.ds(j, 1)], kvr.at[a, pl.ds(j, 1)], hop_s, kv_r.at[a, j], dev(chip))

    def stream_kv(j):
        @pl.when(c == 0)
        def _():
            send_kv(1, 0, j)
            send_kv(2, 1, j)

        if not isinstance(j, int) or j not in VIA3:
            @pl.when(c == 1)
            def _():
                send_kv(0, 1, j)

        @pl.when(c == 2)
        def _():
            send_kv(3, 0, j)

    def to_mate(j):
        for which, ref in ((0, k), (1, v)):
            remote(ref.at[pl.ds(other + j, 1)], kvr.at[c, pl.ds(j, 1), which, pl.ds(128 * e, 128)],
                   kv_s.at[2, which], kv_r.at[c, j], mate).start()

    def rows_to_mate(j):
        for which, ref in ((0, q), (1, g)):
            remote(ref.at[pl.ds(other + j, 1)], qgm.at[pl.ds(j, 1), which], q_s.at[which], q_r.at[j], mate).start()

    stream_kv(0)

    @pl.when(c == 1)
    def _():
        send_kv(3, 0, 0)
    to_mate(0)
    rows_to_mate(0)
    for j in range(1, AHEAD):
        stream_kv(j)
    for j in range(1, NJ):
        to_mate(j)
        rows_to_mate(j)
    for i in range(1, n_dev):
        doc_copy(i).wait()

    def member(s, group):
        out = jnp.bool_(False)
        for one in group:
            out = out | (s == one)
        return out

    def by_way_of_3(j):
        @pl.when(c == 3)
        def _():
            kv_forward(1, 1, j).wait_recv()
            kv_forward(1, 2, j).start()

    def arrive(j):
        remote(kvr.at[c, pl.ds(j, 1), :, pl.ds(0, 128)], kvr.at[c, pl.ds(j, 1), :, pl.ds(0, 128)],
               hop_s, kv_r.at[c, j], mate).wait_recv()
        remote(qgm.at[pl.ds(j, 1)], qgm.at[pl.ds(j, 1)], hop_s, q_r.at[j], mate).wait_recv()
        for a in range(3):
            need = a < c
            if a == 1:
                need = need & jnp.logical_not((c == 3) & member(j, VIA3))

            @pl.when(need)
            def _():
                kv_forward(a, a, j).wait_recv()

        @pl.when(c == 1)
        def _():
            kv_forward(0, 3, j).start()

            @pl.when(j + 1 < NJ)
            def _():
                send_kv(3, 0, j + 1)

        @pl.when((c == 0) & jnp.logical_not(member(j, VIA3)))
        def _():
            kv_forward(1, 1, j).wait_recv()
            kv_forward(1, 2, j).start()

        @pl.when(j + AHEAD < NJ)
        def _():
            stream_kv(j + AHEAD)

    def inputs(s, sl):
        row = mine + s
        rows = pl.ds(128 * e, 128)
        rest = pl.ds(128 - 128 * e, 128)
        pairs = [
            (q.at[row], qg.at[sl, 0]), (g.at[row], qg.at[sl, 2]), (qgm.at[s, 0], qg.at[sl, 1]), (qgm.at[s, 1], qg.at[sl, 3]),
            (k.at[row], kvs.at[sl, 0, 0, rows]), (v.at[row], kvs.at[sl, 0, 1, rows]),
            (kvr.at[c, s, :, rest], kvs.at[sl, 0, :, rest]),
        ]
        return [pltpu.make_async_copy(src, dst, isem.at[sl, i]) for i, (src, dst) in enumerate(pairs)]

    def far_input(s, sl, d):
        return pltpu.make_async_copy(kvr.at[c - d, s], kvs.at[sl, d], isem.at[sl, 6 + d])

    def fetch(s, sl):
        for copy in inputs(s, sl):
            copy.start()
        for d in range(1, 4):
            @pl.when(d <= c)
            def _():
                far_input(s, sl, d).start()

    def fetch_wait(s, sl):
        for copy in inputs(s, sl):
            copy.wait()
        for d in range(1, 4):
            @pl.when(d <= c)
            def _():
                far_input(s, sl, d).wait()

    def row_outputs(s, sl):
        row = mine + s
        here = [pltpu.make_async_copy(outb.at[sl, 0], o.at[row], osem.at[sl, 0]),
                pltpu.make_async_copy(outb.at[sl, 2], dq.at[row], osem.at[sl, 1])]
        there = [remote(outb.at[sl, 1], o.at[row], osem.at[sl, 2], osend_r.at[0], mate),
                 remote(outb.at[sl, 3], dq.at[row], osem.at[sl, 3], osend_r.at[1], mate)]
        return here, there

    def keep(sl, d, slot, s):
        return pltpu.make_async_copy(dkv.at[sl, d], hold.at[slot, s], gsem.at[sl, d])

    def give(sl, d, chip, slot, s):
        return remote(dkv.at[sl, d], part.at[slot, s], gsem.at[sl, d], part_r.at[slot, s], dev(chip))

    def rank_in(s, group):
        count = jnp.int32(0)
        for one in group:
            count = count + jnp.where(one < s, 1, 0)
        return count

    def choose(cond, yes, no):
        pl.when(cond)(yes)
        pl.when(jnp.logical_not(cond))(no)

    def grads_out(s, begin):
        sl = lax.rem(s, NG)

        def local(d, slot):
            copy = keep(sl, d, slot, s)
            copy.start() if begin else copy.wait()

        def away(d, chip, slot):
            copy = give(sl, d, chip, slot, s)
            copy.start() if begin else copy.wait_send()

        @pl.when(c == 0)
        def _():
            local(0, 1)

        @pl.when(c == 1)
        def _():
            choose(member(s, FAR1), lambda: away(0, 3, 2), lambda: local(0, 1))
            local(1, 0)

        @pl.when(c == 2)
        def _():
            choose(member(s, ROUND), lambda: local(1, 0), lambda: away(1, 3, 0))
            choose(member(s, LAST2), lambda: away(0, 3, 1), lambda: local(0, 1))
            choose(member(s, ON2), lambda: local(2, 2), lambda: away(2, 0, 1))

        if not begin:
            @pl.when(c == 3)
            def _():
                away(3, 1, 0)
                pl.when(member(s, ROUND))(lambda: away(2, 2, 0))
                pl.when(member(s, MERGE))(lambda: away(2, 1, 1))
                pl.when(jnp.logical_not(member(s, LAST2)))(lambda: away(1, 2, 1))

    def put(s, sl):
        here, there = row_outputs(s, sl)
        for copy in here + there:
            copy.start()
        grads_out(s, True)

    def put_wait(s, sl):
        here, there = row_outputs(s, sl)
        for copy in here:
            copy.wait()
        for copy in there:
            copy.wait_send()

    def final_copies(kind, sl, s, chip):
        row = mine + s
        out = []
        for which, ref in ((0, dk), (1, dv)):
            for far, rows in ((0, pl.ds(128 * e, 128)), (1, pl.ds(128 - 128 * e, 128))):
                src, sem = fin.at[kind, sl, which, rows], fsem.at[kind, sl, 2 * which + far]
                if far:
                    out.append(remote(src, ref.at[row], sem, dsend_r.at[which], mate if chip is None else 2 * chip + 1 - e))
                elif chip is None:
                    out.append(pltpu.make_async_copy(src, ref.at[row], sem))
                else:
                    out.append(remote(src, ref.at[row], sem, down_r.at[which], dev(chip)))
        return out

    def final_wait(kind, sl, chip):
        for i, copy in enumerate(final_copies(kind, sl, 0, chip)):
            if chip is None and i % 2 == 0:
                copy.wait()
            else:
                copy.wait_send()

    def finalize(kind, group, s, value, chip):
        count = rank_in(s, group)
        sl = lax.rem(count, 2)
        pl.when(count >= 2)(lambda: final_wait(kind, sl, chip))
        fin[kind, sl, 0] = (value[:, :256] * scale).astype(jnp.bfloat16)
        fin[kind, sl, 1] = value[:, 256:].astype(jnp.bfloat16)
        for copy in final_copies(kind, sl, s, chip):
            copy.start()

    def final_drain(kind, group, chip):
        for n in range(max(0, len(group) - 2), len(group)):
            final_wait(kind, n % 2, chip)

    row_tok = lax.broadcasted_iota(jnp.int32, (1024, 128), 0) >> 3
    lane = lax.broadcasted_iota(jnp.int32, (1024, 128), 1)
    cs = scale * LOG2E
    lo_half, hi_half = slice(0, 128), slice(128, 256)

    def attend(s, slot):
        row = mine + s
        gslot = lax.rem(s, NG)
        piece = (e, 1 - e)
        for role in range(2):
            dq_row = docs[2 * c + piece[role], pl.ds(row, 1), :]
            d_t = jnp.transpose(jnp.broadcast_to(dq_row, (128, 128)))
            docr[role] = jnp.broadcast_to(d_t[:, None, :], (128, 8, 128)).reshape(1024, 128)

        def g_of(role):
            return qg[slot, 2 + role]

        def far_loop(body):
            for chip in range(1, 4):
                @pl.when(c == chip)
                def _():
                    for d in range(1, chip + 1):
                        body(d, 0)

        def scores(role, d, causal):
            sc = dot_nt(qg[slot, role], kvs[slot, d, 0]) * cs
            xs = []
            for j in range(2):
                dk_row = docs[2 * (c - d) + j, pl.ds(row, 1), :]
                vis = docr[role] == dk_row
                if causal:
                    vis = vis & (lane + 128 * j <= row_tok + 128 * piece[role])
                xs.append(jnp.where(vis, sc[:, 128 * j:128 * (j + 1)], NEG_BIG))
            top = jnp.maximum(xs[0], xs[1])
            es = [jnp.exp2(x - top) for x in xs]
            e_scr[d, role, :, lo_half] = es[0]
            e_scr[d, role, :, hi_half] = es[1]
            f_scr[d, role] = top
            l_scr[d, role] = es[0] + es[1]
            return top

        def dprob(role, d):
            dp_scr[d, role] = dot_nt(g_of(role), kvs[slot, d, 1])

        for role in range(2):
            t_scr[role] = scores(role, 0, True)

        def far_scores(d, x):
            for role in range(2):
                t_scr[role] = jnp.maximum(t_scr[role], scores(role, d, False))
            for role in range(2):
                dprob(role, d)
            return x
        far_loop(far_scores)

        for role in range(2):
            t_scr[role] = jnp.broadcast_to(jnp.max(t_scr[role], axis=1, keepdims=True), (1024, 128))
        dprob(0, 0)

        for role in range(2):
            top = t_scr[role]
            norm = l_scr[0, role] * jnp.exp2(f_scr[0, role] - top)
            for d in range(1, 4):
                norm = norm + l_scr[d, role] * jnp.exp2(f_scr[d, role] - top)
            t_scr[role] = top + jnp.log2(jnp.broadcast_to(jnp.sum(norm, axis=1, keepdims=True), (1024, 128)))
        dprob(1, 0)

        def weighted(role, d):
            f = jnp.exp2(f_scr[d, role] - t_scr[role])
            f_scr[d, role] = f
            for half in (lo_half, hi_half):
                p_scr[d, role, :, half] = (e_scr[d, role, :, half] * f).astype(jnp.bfloat16)
            return dot_nn(p_scr[d, role], kvs[slot, d, 1])

        def value_grads(d):
            dkv[gslot, d, :, 256:] = dot_tn(p_scr[d, 0], g_of(0)) + dot_tn(p_scr[d, 1], g_of(1))

        for role in range(2):
            o_acc[role] = weighted(role, 0)

        def far_weighted(d, x):
            for role in range(2):
                o_acc[role] = o_acc[role] + weighted(role, d)
            value_grads(d)
            return x
        far_loop(far_weighted)

        for role in range(2):
            o_low = o_acc[role].astype(jnp.bfloat16)
            outb[slot, role] = o_low
            delta = jnp.sum(g_of(role).astype(jnp.float32) * o_low.astype(jnp.float32), axis=1, keepdims=True)
            t_scr[role] = jnp.broadcast_to(delta, (1024, 128))
        value_grads(0)

        def score_grads(d):
            out = []
            for role in range(2):
                ds = [
                    (e_scr[d, role, :, half] * f_scr[d, role] * (dp_scr[d, role, :, half] - t_scr[role])).astype(jnp.bfloat16)
                    for half in (lo_half, hi_half)
                ]
                out.append(jnp.concatenate(ds, axis=1))
            dkv[gslot, d, :, :256] = dot_tn(out[0], qg[slot, 0]) + dot_tn(out[1], qg[slot, 1])
            return [dot_nn(ds, kvs[slot, d, 0]) for ds in out]

        got = score_grads(0)
        for role in range(2):
            o_acc[role] = got[role]

        def far_grads(d, x):
            got = score_grads(d)
            for role in range(2):
                o_acc[role] = o_acc[role] + got[role]
            return x
        far_loop(far_grads)
        for role in range(2):
            outb[slot, 2 + role] = (o_acc[role] * scale).astype(jnp.bfloat16)

    def part_wait(slot, s):
        remote(part.at[slot, s], part.at[slot, s], hop_s, part_r.at[slot, s], mate).wait_recv()

    def load(src, i):
        return [pltpu.make_async_copy(src.at[pl.ds(64 * n, 64)], sums.at[i, pl.ds(64 * n, 64)], lsem.at[i, n]) for n in range(4)]

    def start(copies):
        for copy in copies:
            copy.start()

    def finish(copies):
        for copy in copies:
            copy.wait()

    def passed(s, sl, chip, slot):
        return remote(sums.at[4 + sl], part.at[slot, s], xsem.at[sl], part_r.at[slot, s], dev(chip))

    def relay(s):
        return remote(part.at[2, s], part.at[1, s], rel_s.at[s], part_r.at[1, s], dev(1))

    def pass_on(i, group, held, slot_in, chip, slot_out):
        count = rank_in(i, group)
        sl = lax.rem(count, 2)
        start(load(hold.at[held, i], 0))
        part_wait(slot_in, i)
        start(load(part.at[slot_in, i], 1))
        pl.when(count >= 2)(lambda: passed(i, sl, chip, slot_out).wait_send())
        finish(load(hold.at[held, i], 0))
        finish(load(part.at[slot_in, i], 1))
        sums[4 + sl] = sums[0] + sums[1]
        passed(i, sl, chip, slot_out).start()

    def pass_x(i):
        pass_on(i, PASS_X, 0, 0, 0, 0)

    def pass_y(i):
        pass_on(i, ROUND, 0, 0, 0, 2)

    def total(kind, group, s, held, slots, chip):
        terms = [hold.at[held, s]] + [part.at[slot, s] for slot in slots]
        for slot in slots:
            part_wait(slot, s)
        for n, src in enumerate(terms):
            start(load(src, n))
        for n, src in enumerate(terms):
            finish(load(src, n))
        value = sums[0]
        for n in range(1, len(terms)):
            value = value + sums[n]
        finalize(kind, group, s, value, chip)

    for d in range(1, 4):
        f_scr[d] = jnp.full((2, 1024, 128), NEG_BIG, jnp.float32)
        l_scr[d] = jnp.zeros((2, 1024, 128), jnp.float32)
    by_way_of_3(VIA3[0])
    arrive(0)
    for j in VIA3[1:]:
        by_way_of_3(j)
    fetch(0, 0)

    def step(s, x):
        slot = lax.rem(s, 2)

        late = (c >= LATE_CHIP) & (s == 0)

        def ahead():
            arrive(s + 1)
            fetch(s + 1, 1 - slot)
        pl.when((s + 1 < NS) & jnp.logical_not(late))(ahead)

        @pl.when(s >= 2)
        def _():
            put_wait(s - 2, slot)

        @pl.when(s >= NG)
        def _():
            grads_out(s - NG, False)
        fetch_wait(s, slot)
        attend(s, slot)

        @pl.when(c == 3)
        def _():
            gslot = lax.rem(s, NG)
            give(gslot, 3, 1, 0, s).start()
            pl.when(member(s, ROUND))(lambda: give(gslot, 2, 2, 0, s).start())

            @pl.when(member(s, MERGE))
            def _():
                part_wait(0, s)
                start(load(part.at[0, s], 0))
                finish(load(part.at[0, s], 0))
                dkv[gslot, 2] = dkv[gslot, 2] + sums[0]

            @pl.when(member(s, FAR1))
            def _():
                part_wait(0, s)
                start(load(part.at[0, s], 0))
                part_wait(2, s)
                start(load(part.at[2, s], 1))
                finish(load(part.at[0, s], 0))
                finish(load(part.at[2, s], 1))
                finalize(1, FAR1, s, dkv[gslot, 2] + sums[0] + sums[1], 1)
            finalize(0, OWN3, s, dkv[gslot, 0], None)
            pl.when(member(s, MERGE))(lambda: give(gslot, 2, 1, 1, s).start())

            def last_two():
                part_wait(1, s)
                start(load(part.at[1, s], 2))
                finish(load(part.at[1, s], 2))
                finalize(2, LAST2, s, dkv[gslot, 1] + sums[2], 2)
            choose(member(s, LAST2), last_two, lambda: give(gslot, 1, 2, 1, s).start())
        put(s, slot)
        for at, i in EARLY_X.items():
            pl.when((c == 1) & (s == at))(lambda: pass_x(i))
        for at, i in EARLY_Y.items():
            pl.when((c == 2) & (s == at))(lambda: pass_y(i))
        pl.when(late)(ahead)
        return x

    lax.fori_loop(0, NS, step, 0)
    put_wait(NS - 2, 0)
    put_wait(NS - 1, 1)
    for s in range(NS - NG, NS):
        grads_out(s, False)

    def home(i, x):
        def behind(lag, body):
            s = i - lag
            pl.when((s >= 0) & (s < NS))(lambda: body(s))

        @pl.when(c == 0)
        def _():
            @pl.when(member(i, ROUND))
            def _():
                part_wait(2, i)
                relay(i).start()
            pl.when(member(i, ON1))(lambda: pass_on(i, PASS_0, 1, 1, 1, 2))
            pl.when(member(i, ON2))(lambda: pass_on(i, PASS_0, 1, 0, 2, 2))
            behind(LAG[0], lambda s: pl.when(member(s, HERE0))(lambda: total(0, HERE0, s, 1, (1, 0), None)))

        @pl.when(c == 1)
        def _():
            later = tuple(s for s in PASS_X if s not in EARLY_X.values())
            pl.when(member(i, later))(lambda: pass_x(i))

            def body(s):
                pl.when(member(s, ON1))(lambda: total(1, ON1, s, 0, (0, 2), 0))
                pl.when(member(s, OWN1))(lambda: total(0, OWN1, s, 1, (1,), None))
            behind(LAG[1], body)

        @pl.when(c == 2)
        def _():
            later = tuple(s for s in ROUND if s not in EARLY_Y.values())
            pl.when(member(i, later))(lambda: pass_y(i))

            def body(s):
                pl.when(member(s, ON2))(lambda: total(1, ON2, s, 2, (2,), 0))
                pl.when(member(s, OWN2))(lambda: total(0, OWN2, s, 1, (1,), None))
            behind(LAG[2], body)
        return x

    @pl.when(c < 3)
    def _():
        lax.fori_loop(0, NS + max(LAG), home, 0)

    def down_wait(n):
        for which, ref in ((0, dk), (1, dv)):
            rows = ref.at[pl.ds(0, n)]
            remote(rows, rows, hop_s, down_r.at[which], mate).wait_recv()

    @pl.when(c == 0)
    def _():
        for s in ROUND:
            relay(s).wait_send()
        for sl in range(2):
            passed(0, sl, 1, 2).wait_send()
        sent = kvr.at[1, pl.ds(0, NS - len(VIA3))]
        remote(sent, sent, hop_s, kv_r.at[0, 0], mate).wait_send()
        final_drain(0, HERE0, None)
        down_wait(len(PASS_0))

    @pl.when(c == 1)
    def _():
        for sl in range(2):
            passed(0, sl, 0, 0).wait_send()
        remote(kvr.at[0], kvr.at[0], hop_s, kv_r.at[0, 0], mate).wait_send()
        final_drain(0, OWN1, None)
        final_drain(1, ON1, 0)
        down_wait(len(FAR1))

    @pl.when(c == 2)
    def _():
        for sl in range(2):
            passed(0, sl, 0, 2).wait_send()
        final_drain(0, OWN2, None)
        final_drain(1, ON2, 0)
        down_wait(len(LAST2))

    @pl.when(c == 3)
    def _():
        sent = kvr.at[1, pl.ds(0, len(VIA3))]
        remote(sent, sent, hop_s, kv_r.at[0, 0], mate).wait_send()
        final_drain(0, OWN3, None)
        final_drain(1, FAR1, 1)
        final_drain(2, LAST2, 2)
    for which, ref in ((0, k), (1, v)):
        some = ref.at[pl.ds(0, 2 * (NS - len(VIA3)))]
        for way, chips, sent in ((0, c < 3, ref), (1, c == 0, ref), (1, c == 1, some)):
            @pl.when(chips)
            def _():
                remote(sent, sent, kv_s.at[way, which], kv_r.at[0, 0], mate).wait_send()
        half = ref.at[pl.ds(other, NS)]
        remote(half, half, kv_s.at[2, which], kv_r.at[0, 0], mate).wait_send()
    for which, ref in ((0, q), (1, g)):
        half = ref.at[pl.ds(other, NS)]
        remote(half, half, q_s.at[which], q_r.at[0], mate).wait_send()
    for which, ref in ((0, o), (1, dq)):
        half = ref.at[pl.ds(other, NS)]
        remote(half, half, hop_s, osend_r.at[which], mate).wait_recv()
    for which, ref in ((0, dk), (1, dv)):
        half = ref.at[pl.ds(other, NS)]
        remote(half, half, hop_s, dsend_r.at[which], mate).wait_recv()


def place_kernel(slots, *refs):
    srcs, dsts, (buf, rsem, wsem) = refs[:4], refs[4:8], refs[8:]
    size = buf.shape[1]
    jobs = [(src.at[pl.ds(i, size)], dst.at[pl.ds(i, size)]) for src, dst in zip(srcs, dsts) for i in range(0, src.shape[0], size)]

    def read(j):
        return pltpu.make_async_copy(jobs[j][0], buf.at[j % slots], rsem.at[j % slots])

    def write(j):
        return pltpu.make_async_copy(buf.at[j % slots], jobs[j][1], wsem.at[j % slots])

    ahead = slots
    for j in range(min(ahead, len(jobs))):
        read(j).start()
    for j in range(len(jobs)):
        read(j).wait()
        write(j).start()
        if j + ahead < len(jobs):
            if j + ahead >= slots:
                write(j + ahead - slots).wait()
            read(j + ahead).start()
    for j in range(max(0, len(jobs) - slots), len(jobs)):
        write(j).wait()


ANY = pl.BlockSpec(memory_space=pl.ANY)
VMEM = pl.BlockSpec(memory_space=pltpu.VMEM)


def solution(mesh):
    n_dev = mesh.shape['cp']
    seq_spec = P('dp', 'cp', None, None)
    id_spec = P('dp', 'cp')
    bf, f32 = jnp.bfloat16, jnp.float32
    shape = jax.ShapeDtypeStruct
    dma = pltpu.SemaphoreType.DMA

    def per_device(query, keys, values, grad_out, doc_id):
        nb, piece, heads, hd = query.shape
        rows = piece * heads
        outs = pl.pallas_call(
            functools.partial(fused_kernel, hd ** -0.5),
            in_specs=[VMEM] + [ANY] * 4,
            out_specs=[ANY] * 8,
            out_shape=[
                shape((nb, rows, hd), bf), shape((nb, rows, hd), bf), shape((nb, piece, hd), bf), shape((nb, piece, hd), bf),
                shape((NS, 2, rows, hd), bf), shape((4, NS, 2, 256, 256), bf),
                shape((3, NS, 256, 512), f32), shape((3, NS, 256, 512), f32),
            ],
            scratch_shapes=[
                pltpu.VMEM((n_dev, nb, piece), jnp.int32), pltpu.VMEM((2, 4, 2, 256, 256), bf), pltpu.VMEM((2, 4, rows, hd), bf),
                pltpu.VMEM((2, 4, rows, hd), bf), pltpu.VMEM((NG, 4, 256, 512), f32), pltpu.VMEM((6, 256, 512), f32),
                pltpu.VMEM((3, 2, 2, 256, 256), bf),
                pltpu.VMEM((4, 2, rows, 256), f32), pltpu.VMEM((4, 2, rows, 256), f32), pltpu.VMEM((4, 2, rows, 256), bf),
                pltpu.VMEM((4, 2, rows, 128), f32), pltpu.VMEM((4, 2, rows, 128), f32), pltpu.VMEM((2, rows, 128), f32),
                pltpu.VMEM((2, rows, 128), jnp.int32), pltpu.VMEM((2, rows, hd), f32),
                dma((n_dev,)), dma((n_dev,)), dma((2, 10)), dma((2, 4)), dma((NG, 4)), dma((2,)), dma((2,)), dma((NJ,)), dma((3, 2)), dma((4, NJ)),
                dma, dma((3, NS)), dma((3, 2, 4)), dma((2,)), dma((3, 4)), dma((2,)), dma((NS,)), dma((2,)),
            ],
            compiler_params=pltpu.CompilerParams(has_side_effects=True, vmem_limit_bytes=62 * 1024 * 1024),
            name="attend",
        )(doc_id, query.reshape(nb, rows, hd), grad_out.reshape(nb, rows, hd), keys.reshape(nb, piece, hd), values.reshape(nb, piece, hd))
        outs = [x.reshape(-1, rows, hd) for x in outs[:4]]
        o, dq, dk, dv = pl.pallas_call(
            functools.partial(place_kernel, 36),
            in_specs=[ANY] * 4,
            out_specs=[ANY] * 4,
            out_shape=[shape(x.shape, bf) for x in outs],
            scratch_shapes=[pltpu.VMEM((36, 2, rows, hd), bf), dma((36,)), dma((36,))],
            compiler_params=pltpu.CompilerParams(vmem_limit_bytes=63 * 1024 * 1024),
            name="place",
        )(*outs)
        return o.reshape(query.shape), dq.reshape(query.shape), dk.reshape(keys.shape), dv.reshape(values.shape)

    return jax.shard_map(per_device, mesh=mesh, in_specs=(seq_spec, seq_spec, seq_spec, seq_spec, id_spec),
                         out_specs=(seq_spec, seq_spec, seq_spec, seq_spec), check_vma=False)
```

```python
import functools

import jax
import jax.numpy as jnp
from jax import lax
from jax.experimental import pallas as pl
from jax.experimental.pallas import tpu as pltpu
from jax.sharding import PartitionSpec as P

NEG_BIG = -1e30
LOG2E = 1.4426950408889634
NS = 16
NJ = NS
AHEAD = 2
NG = 4
PLAN1 = 'RMRMFRRRFRFRRMMM'
PLAN0 = 'NNANANCCNCNNCNNA'
LAST2 = (8, 9, 11)
EARLY_X = {5: 0, 7: 1, 10: 3, 12: 5, 13: 6, 14: 7, 15: 8}
EARLY_Y = {5: 0, 7: 2, 9: 5, 11: 6, 13: 7, 14: 9, 15: 11}
LAG = (8, 8, 6)
LATE_CHIP = 2
VIA3 = (0, 1)


def where_plan(plan, kinds):
    return tuple(s for s in range(NS) if plan[s] in kinds)


ROUND, MERGE, FAR1 = (where_plan(PLAN1, x) for x in 'RMF')
HERE0, ON1, ON2 = (where_plan(PLAN0, x) for x in 'NAC')
OWN1 = where_plan(PLAN1, 'RM')
OWN2 = tuple(s for s in range(NS) if s not in LAST2)
OWN3 = tuple(range(NS))
PASS_X = where_plan(PLAN0, 'NC')
PASS_0 = where_plan(PLAN0, 'AC')


def dot_nt(a, b):
    return lax.dot_general(a, b, (((1,), (1,)), ((), ())), preferred_element_type=jnp.float32)


def dot_nn(a, b):
    return lax.dot_general(a, b, (((1,), (0,)), ((), ())), preferred_element_type=jnp.float32)


def dot_tn(a, b):
    return lax.dot_general(a, b, (((0,), (0,)), ((), ())), preferred_element_type=jnp.float32)


def remote(src, dst, send, recv, dev):
    return pltpu.make_async_remote_copy(src_ref=src, dst_ref=dst, send_sem=send, recv_sem=recv,
                                        device_id={'cp': dev}, device_id_type=pl.DeviceIdType.MESH)


def fused_kernel(scale, doc, q, g, k, v, o, dq, dk, dv, qgm, kvr, part, hold,
                 docs, kvs, qg, outb, dkv, sums, fin, e_scr, dp_scr, p_scr, l_scr, f_scr, t_scr, docr, o_acc,
                 doc_s, doc_r, isem, osem, gsem, osend_r, q_s, q_r, kv_s, kv_r, hop_s, part_r, fsem, dsend_r, lsem, xsem, rel_s, down_r):
    rank = lax.axis_index('cp')
    n_dev = docs.shape[0]
    c = rank // 2
    e = lax.rem(rank, 2)
    mate = 2 * c + 1 - e
    other = NS * (1 - e)
    mine = NS * e

    def dev(chip):
        return 2 * chip + e

    docs[rank] = doc[...]

    def doc_copy(i):
        return remote(doc, docs.at[rank], doc_s.at[i], doc_r.at[i], lax.rem(rank + i, n_dev))

    for i in range(1, n_dev):
        doc_copy(i).start()

    def kv_parts(chip, way, j, cols):
        out = []
        for col in cols:
            for which, ref in ((0, k), (1, v)):
                out.append(remote(ref.at[pl.ds(col * NS + j, 1)], kvr.at[c, pl.ds(j, 1), which, pl.ds(128 * e, 128)],
                                  kv_s.at[way, which], kv_r.at[c, j], 2 * chip + col))
        return out

    def send_kv(chip, way, j):
        for copy in kv_parts(chip, way, j, (0, 1)):
            copy.start()

    def kv_forward(a, chip, j):
        return remote(kvr.at[a, pl.ds(j, 1)], kvr.at[a, pl.ds(j, 1)], hop_s, kv_r.at[a, j], dev(chip))

    def stream_kv(j):
        @pl.when(c == 0)
        def _():
            send_kv(1, 0, j)
            send_kv(2, 1, j)

        if not isinstance(j, int) or j not in VIA3:
            @pl.when(c == 1)
            def _():
                send_kv(0, 1, j)

        @pl.when(c == 2)
        def _():
            send_kv(3, 0, j)

    def to_mate(j):
        for which, ref in ((0, k), (1, v)):
            remote(ref.at[pl.ds(other + j, 1)], kvr.at[c, pl.ds(j, 1), which, pl.ds(128 * e, 128)],
                   kv_s.at[2, which], kv_r.at[c, j], mate).start()

    def rows_to_mate(j):
        for which, ref in ((0, q), (1, g)):
            remote(ref.at[pl.ds(other + j, 1)], qgm.at[pl.ds(j, 1), which], q_s.at[which], q_r.at[j], mate).start()

    stream_kv(0)

    @pl.when(c == 1)
    def _():
        send_kv(3, 0, 0)
    to_mate(0)
    rows_to_mate(0)
    for j in range(1, AHEAD):
        stream_kv(j)
    for j in range(1, NJ):
        to_mate(j)
        rows_to_mate(j)
    for i in range(1, n_dev):
        doc_copy(i).wait()

    def member(s, group):
        out = jnp.bool_(False)
        for one in group:
            out = out | (s == one)
        return out

    def by_way_of_3(j):
        @pl.when(c == 3)
        def _():
            kv_forward(1, 1, j).wait_recv()
            kv_forward(1, 2, j).start()

    def arrive(j):
        remote(kvr.at[c, pl.ds(j, 1), :, pl.ds(0, 128)], kvr.at[c, pl.ds(j, 1), :, pl.ds(0, 128)],
               hop_s, kv_r.at[c, j], mate).wait_recv()
        remote(qgm.at[pl.ds(j, 1)], qgm.at[pl.ds(j, 1)], hop_s, q_r.at[j], mate).wait_recv()
        for a in range(3):
            need = a < c
            if a == 1:
                need = need & jnp.logical_not((c == 3) & member(j, VIA3))

            @pl.when(need)
            def _():
                kv_forward(a, a, j).wait_recv()

        @pl.when(c == 1)
        def _():
            kv_forward(0, 3, j).start()

            @pl.when(j + 1 < NJ)
            def _():
                send_kv(3, 0, j + 1)

        @pl.when((c == 0) & jnp.logical_not(member(j, VIA3)))
        def _():
            kv_forward(1, 1, j).wait_recv()
            kv_forward(1, 2, j).start()

        @pl.when(j + AHEAD < NJ)
        def _():
            stream_kv(j + AHEAD)

    def inputs(s, sl):
        row = mine + s
        rows = pl.ds(128 * e, 128)
        rest = pl.ds(128 - 128 * e, 128)
        pairs = [
            (q.at[row], qg.at[sl, 0]), (g.at[row], qg.at[sl, 2]), (qgm.at[s, 0], qg.at[sl, 1]), (qgm.at[s, 1], qg.at[sl, 3]),
            (k.at[row], kvs.at[sl, 0, 0, rows]), (v.at[row], kvs.at[sl, 0, 1, rows]),
            (kvr.at[c, s, :, rest], kvs.at[sl, 0, :, rest]),
        ]
        return [pltpu.make_async_copy(src, dst, isem.at[sl, i]) for i, (src, dst) in enumerate(pairs)]

    def far_input(s, sl, d):
        return pltpu.make_async_copy(kvr.at[c - d, s], kvs.at[sl, d], isem.at[sl, 6 + d])

    def fetch(s, sl):
        for copy in inputs(s, sl):
            copy.start()
        for d in range(1, 4):
            @pl.when(d <= c)
            def _():
                far_input(s, sl, d).start()

    def fetch_wait(s, sl):
        for copy in inputs(s, sl):
            copy.wait()
        for d in range(1, 4):
            @pl.when(d <= c)
            def _():
                far_input(s, sl, d).wait()

    def row_outputs(s, sl):
        row = mine + s
        here = [pltpu.make_async_copy(outb.at[sl, 0], o.at[row], osem.at[sl, 0]),
                pltpu.make_async_copy(outb.at[sl, 2], dq.at[row], osem.at[sl, 1])]
        there = [remote(outb.at[sl, 1], o.at[row], osem.at[sl, 2], osend_r.at[0], mate),
                 remote(outb.at[sl, 3], dq.at[row], osem.at[sl, 3], osend_r.at[1], mate)]
        return here, there

    def keep(sl, d, slot, s):
        return pltpu.make_async_copy(dkv.at[sl, d], hold.at[slot, s], gsem.at[sl, d])

    def give(sl, d, chip, slot, s):
        return remote(dkv.at[sl, d], part.at[slot, s], gsem.at[sl, d], part_r.at[slot, s], dev(chip))

    def rank_in(s, group):
        count = jnp.int32(0)
        for one in group:
            count = count + jnp.where(one < s, 1, 0)
        return count

    def choose(cond, yes, no):
        pl.when(cond)(yes)
        pl.when(jnp.logical_not(cond))(no)

    def grads_out(s, begin):
        sl = lax.rem(s, NG)

        def local(d, slot):
            copy = keep(sl, d, slot, s)
            copy.start() if begin else copy.wait()

        def away(d, chip, slot):
            copy = give(sl, d, chip, slot, s)
            copy.start() if begin else copy.wait_send()

        @pl.when(c == 0)
        def _():
            local(0, 1)

        @pl.when(c == 1)
        def _():
            choose(member(s, FAR1), lambda: away(0, 3, 2), lambda: local(0, 1))
            local(1, 0)

        @pl.when(c == 2)
        def _():
            choose(member(s, ROUND), lambda: local(1, 0), lambda: away(1, 3, 0))
            choose(member(s, LAST2), lambda: away(0, 3, 1), lambda: local(0, 1))
            choose(member(s, ON2), lambda: local(2, 2), lambda: away(2, 0, 1))

        if not begin:
            @pl.when(c == 3)
            def _():
                away(3, 1, 0)
                pl.when(member(s, ROUND))(lambda: away(2, 2, 0))
                pl.when(member(s, MERGE))(lambda: away(2, 1, 1))
                pl.when(jnp.logical_not(member(s, LAST2)))(lambda: away(1, 2, 1))

    def put(s, sl):
        here, there = row_outputs(s, sl)
        for copy in here + there:
            copy.start()
        grads_out(s, True)

    def put_wait(s, sl):
        here, there = row_outputs(s, sl)
        for copy in here:
            copy.wait()
        for copy in there:
            copy.wait_send()

    def final_copies(kind, sl, s, chip):
        row = mine + s
        out = []
        for which, ref in ((0, dk), (1, dv)):
            for far, rows in ((0, pl.ds(128 * e, 128)), (1, pl.ds(128 - 128 * e, 128))):
                src, sem = fin.at[kind, sl, which, rows], fsem.at[kind, sl, 2 * which + far]
                if far:
                    out.append(remote(src, ref.at[row], sem, dsend_r.at[which], mate if chip is None else 2 * chip + 1 - e))
                elif chip is None:
                    out.append(pltpu.make_async_copy(src, ref.at[row], sem))
                else:
                    out.append(remote(src, ref.at[row], sem, down_r.at[which], dev(chip)))
        return out

    def final_wait(kind, sl, chip):
        for i, copy in enumerate(final_copies(kind, sl, 0, chip)):
            if chip is None and i % 2 == 0:
                copy.wait()
            else:
                copy.wait_send()

    def finalize(kind, group, s, value, chip):
        count = rank_in(s, group)
        sl = lax.rem(count, 2)
        pl.when(count >= 2)(lambda: final_wait(kind, sl, chip))
        fin[kind, sl, 0] = (value[:, :256] * scale).astype(jnp.bfloat16)
        fin[kind, sl, 1] = value[:, 256:].astype(jnp.bfloat16)
        for copy in final_copies(kind, sl, s, chip):
            copy.start()

    def final_drain(kind, group, chip):
        for n in range(max(0, len(group) - 2), len(group)):
            final_wait(kind, n % 2, chip)

    row_tok = lax.broadcasted_iota(jnp.int32, (1024, 128), 0) >> 3
    lane = lax.broadcasted_iota(jnp.int32, (1024, 128), 1)
    cs = scale * LOG2E
    lo_half, hi_half = slice(0, 128), slice(128, 256)

    def attend(s, slot):
        row = mine + s
        gslot = lax.rem(s, NG)
        piece = (e, 1 - e)
        for role in range(2):
            dq_row = docs[2 * c + piece[role], pl.ds(row, 1), :]
            d_t = jnp.transpose(jnp.broadcast_to(dq_row, (128, 128)))
            docr[role] = jnp.broadcast_to(d_t[:, None, :], (128, 8, 128)).reshape(1024, 128)

        def g_of(role):
            return qg[slot, 2 + role]

        def far_loop(body):
            for chip in range(1, 4):
                @pl.when(c == chip)
                def _():
                    for d in range(1, chip + 1):
                        body(d, 0)

        def scores(role, d, causal):
            sc = dot_nt(qg[slot, role], kvs[slot, d, 0]) * cs
            xs = []
            for j in range(2):
                dk_row = docs[2 * (c - d) + j, pl.ds(row, 1), :]
                vis = docr[role] == dk_row
                if causal:
                    vis = vis & (lane + 128 * j <= row_tok + 128 * piece[role])
                xs.append(jnp.where(vis, sc[:, 128 * j:128 * (j + 1)], NEG_BIG))
            top = jnp.maximum(xs[0], xs[1])
            es = [jnp.exp2(x - top) for x in xs]
            e_scr[d, role, :, lo_half] = es[0]
            e_scr[d, role, :, hi_half] = es[1]
            f_scr[d, role] = top
            l_scr[d, role] = es[0] + es[1]
            return top

        def dprob(role, d):
            dp_scr[d, role] = dot_nt(g_of(role), kvs[slot, d, 1])

        for role in range(2):
            t_scr[role] = scores(role, 0, True)

        def far_scores(d, x):
            for role in range(2):
                t_scr[role] = jnp.maximum(t_scr[role], scores(role, d, False))
            for role in range(2):
                dprob(role, d)
            return x
        far_loop(far_scores)

        for role in range(2):
            t_scr[role] = jnp.broadcast_to(jnp.max(t_scr[role], axis=1, keepdims=True), (1024, 128))
        dprob(0, 0)

        for role in range(2):
            top = t_scr[role]
            norm = l_scr[0, role] * jnp.exp2(f_scr[0, role] - top)
            for d in range(1, 4):
                norm = norm + l_scr[d, role] * jnp.exp2(f_scr[d, role] - top)
            t_scr[role] = top + jnp.log2(jnp.broadcast_to(jnp.sum(norm, axis=1, keepdims=True), (1024, 128)))
        dprob(1, 0)

        def weighted(role, d):
            f = jnp.exp2(f_scr[d, role] - t_scr[role])
            f_scr[d, role] = f
            for half in (lo_half, hi_half):
                p_scr[d, role, :, half] = (e_scr[d, role, :, half] * f).astype(jnp.bfloat16)
            return dot_nn(p_scr[d, role], kvs[slot, d, 1])

        def value_grads(d):
            dkv[gslot, d, :, 256:] = dot_tn(p_scr[d, 0], g_of(0)) + dot_tn(p_scr[d, 1], g_of(1))

        for role in range(2):
            o_acc[role] = weighted(role, 0)

        def far_weighted(d, x):
            for role in range(2):
                o_acc[role] = o_acc[role] + weighted(role, d)
            value_grads(d)
            return x
        far_loop(far_weighted)

        for role in range(2):
            o_low = o_acc[role].astype(jnp.bfloat16)
            outb[slot, role] = o_low
            delta = jnp.sum(g_of(role).astype(jnp.float32) * o_low.astype(jnp.float32), axis=1, keepdims=True)
            t_scr[role] = jnp.broadcast_to(delta, (1024, 128))
        value_grads(0)

        def score_grads(d):
            out = []
            for role in range(2):
                ds = [
                    (e_scr[d, role, :, half] * f_scr[d, role] * (dp_scr[d, role, :, half] - t_scr[role])).astype(jnp.bfloat16)
                    for half in (lo_half, hi_half)
                ]
                out.append(jnp.concatenate(ds, axis=1))
            dkv[gslot, d, :, :256] = dot_tn(out[0], qg[slot, 0]) + dot_tn(out[1], qg[slot, 1])
            return [dot_nn(ds, kvs[slot, d, 0]) for ds in out]

        got = score_grads(0)
        for role in range(2):
            o_acc[role] = got[role]

        def far_grads(d, x):
            got = score_grads(d)
            for role in range(2):
                o_acc[role] = o_acc[role] + got[role]
            return x
        far_loop(far_grads)
        for role in range(2):
            outb[slot, 2 + role] = (o_acc[role] * scale).astype(jnp.bfloat16)

    def part_wait(slot, s):
        remote(part.at[slot, s], part.at[slot, s], hop_s, part_r.at[slot, s], mate).wait_recv()

    def load(src, i):
        return [pltpu.make_async_copy(src.at[pl.ds(64 * n, 64)], sums.at[i, pl.ds(64 * n, 64)], lsem.at[i, n]) for n in range(4)]

    def start(copies):
        for copy in copies:
            copy.start()

    def finish(copies):
        for copy in copies:
            copy.wait()

    def passed(s, sl, chip, slot):
        return remote(sums.at[4 + sl], part.at[slot, s], xsem.at[sl], part_r.at[slot, s], dev(chip))

    def relay(s):
        return remote(part.at[2, s], part.at[1, s], rel_s.at[s], part_r.at[1, s], dev(1))

    def pass_on(i, group, held, slot_in, chip, slot_out):
        count = rank_in(i, group)
        sl = lax.rem(count, 2)
        start(load(hold.at[held, i], 0))
        part_wait(slot_in, i)
        start(load(part.at[slot_in, i], 1))
        pl.when(count >= 2)(lambda: passed(i, sl, chip, slot_out).wait_send())
        finish(load(hold.at[held, i], 0))
        finish(load(part.at[slot_in, i], 1))
        sums[4 + sl] = sums[0] + sums[1]
        passed(i, sl, chip, slot_out).start()

    def pass_x(i):
        pass_on(i, PASS_X, 0, 0, 0, 0)

    def pass_y(i):
        pass_on(i, ROUND, 0, 0, 0, 2)

    def total(kind, group, s, held, slots, chip):
        terms = [hold.at[held, s]] + [part.at[slot, s] for slot in slots]
        for slot in slots:
            part_wait(slot, s)
        for n, src in enumerate(terms):
            start(load(src, n))
        for n, src in enumerate(terms):
            finish(load(src, n))
        value = sums[0]
        for n in range(1, len(terms)):
            value = value + sums[n]
        finalize(kind, group, s, value, chip)

    for d in range(1, 4):
        f_scr[d] = jnp.full((2, 1024, 128), NEG_BIG, jnp.float32)
        l_scr[d] = jnp.zeros((2, 1024, 128), jnp.float32)
    by_way_of_3(VIA3[0])
    arrive(0)
    for j in VIA3[1:]:
        by_way_of_3(j)
    fetch(0, 0)

    def step(s, x):
        slot = lax.rem(s, 2)

        late = (c >= LATE_CHIP) & (s == 0)

        def ahead():
            arrive(s + 1)
            fetch(s + 1, 1 - slot)
        pl.when((s + 1 < NS) & jnp.logical_not(late))(ahead)

        @pl.when(s >= 2)
        def _():
            put_wait(s - 2, slot)

        @pl.when(s >= NG)
        def _():
            grads_out(s - NG, False)
        fetch_wait(s, slot)
        attend(s, slot)

        @pl.when(c == 3)
        def _():
            gslot = lax.rem(s, NG)
            give(gslot, 3, 1, 0, s).start()
            pl.when(member(s, ROUND))(lambda: give(gslot, 2, 2, 0, s).start())

            @pl.when(member(s, MERGE))
            def _():
                part_wait(0, s)
                start(load(part.at[0, s], 0))
                finish(load(part.at[0, s], 0))
                dkv[gslot, 2] = dkv[gslot, 2] + sums[0]

            @pl.when(member(s, FAR1))
            def _():
                part_wait(0, s)
                start(load(part.at[0, s], 0))
                part_wait(2, s)
                start(load(part.at[2, s], 1))
                finish(load(part.at[0, s], 0))
                finish(load(part.at[2, s], 1))
                finalize(1, FAR1, s, dkv[gslot, 2] + sums[0] + sums[1], 1)
            finalize(0, OWN3, s, dkv[gslot, 0], None)
            pl.when(member(s, MERGE))(lambda: give(gslot, 2, 1, 1, s).start())

            def last_two():
                part_wait(1, s)
                start(load(part.at[1, s], 2))
                finish(load(part.at[1, s], 2))
                finalize(2, LAST2, s, dkv[gslot, 1] + sums[2], 2)
            choose(member(s, LAST2), last_two, lambda: give(gslot, 1, 2, 1, s).start())
        put(s, slot)
        for at, i in EARLY_X.items():
            pl.when((c == 1) & (s == at))(lambda: pass_x(i))
        for at, i in EARLY_Y.items():
            pl.when((c == 2) & (s == at))(lambda: pass_y(i))
        pl.when(late)(ahead)
        return x

    lax.fori_loop(0, NS, step, 0)
    put_wait(NS - 2, 0)
    put_wait(NS - 1, 1)
    for s in range(NS - NG, NS):
        grads_out(s, False)

    def home(i, x):
        def behind(lag, body):
            s = i - lag
            pl.when((s >= 0) & (s < NS))(lambda: body(s))

        @pl.when(c == 0)
        def _():
            @pl.when(member(i, ROUND))
            def _():
                part_wait(2, i)
                relay(i).start()
            pl.when(member(i, ON1))(lambda: pass_on(i, PASS_0, 1, 1, 1, 2))
            pl.when(member(i, ON2))(lambda: pass_on(i, PASS_0, 1, 0, 2, 2))
            behind(LAG[0], lambda s: pl.when(member(s, HERE0))(lambda: total(0, HERE0, s, 1, (1, 0), None)))

        @pl.when(c == 1)
        def _():
            later = tuple(s for s in PASS_X if s not in EARLY_X.values())
            pl.when(member(i, later))(lambda: pass_x(i))

            def body(s):
                pl.when(member(s, ON1))(lambda: total(1, ON1, s, 0, (0, 2), 0))
                pl.when(member(s, OWN1))(lambda: total(0, OWN1, s, 1, (1,), None))
            behind(LAG[1], body)

        @pl.when(c == 2)
        def _():
            later = tuple(s for s in ROUND if s not in EARLY_Y.values())
            pl.when(member(i, later))(lambda: pass_y(i))

            def body(s):
                pl.when(member(s, ON2))(lambda: total(1, ON2, s, 2, (2,), 0))
                pl.when(member(s, OWN2))(lambda: total(0, OWN2, s, 1, (1,), None))
            behind(LAG[2], body)
        return x

    @pl.when(c < 3)
    def _():
        lax.fori_loop(0, NS + max(LAG), home, 0)

    def down_wait(n):
        for which, ref in ((0, dk), (1, dv)):
            rows = ref.at[pl.ds(0, n)]
            remote(rows, rows, hop_s, down_r.at[which], mate).wait_recv()

    @pl.when(c == 0)
    def _():
        for s in ROUND:
            relay(s).wait_send()
        for sl in range(2):
            passed(0, sl, 1, 2).wait_send()
        sent = kvr.at[1, pl.ds(0, NS - len(VIA3))]
        remote(sent, sent, hop_s, kv_r.at[0, 0], mate).wait_send()
        final_drain(0, HERE0, None)
        down_wait(len(PASS_0))

    @pl.when(c == 1)
    def _():
        for sl in range(2):
            passed(0, sl, 0, 0).wait_send()
        remote(kvr.at[0], kvr.at[0], hop_s, kv_r.at[0, 0], mate).wait_send()
        final_drain(0, OWN1, None)
        final_drain(1, ON1, 0)
        down_wait(len(FAR1))

    @pl.when(c == 2)
    def _():
        for sl in range(2):
            passed(0, sl, 0, 2).wait_send()
        final_drain(0, OWN2, None)
        final_drain(1, ON2, 0)
        down_wait(len(LAST2))

    @pl.when(c == 3)
    def _():
        sent = kvr.at[1, pl.ds(0, len(VIA3))]
        remote(sent, sent, hop_s, kv_r.at[0, 0], mate).wait_send()
        final_drain(0, OWN3, None)
        final_drain(1, FAR1, 1)
        final_drain(2, LAST2, 2)
    for which, ref in ((0, k), (1, v)):
        some = ref.at[pl.ds(0, 2 * (NS - len(VIA3)))]
        for way, chips, sent in ((0, c < 3, ref), (1, c == 0, ref), (1, c == 1, some)):
            @pl.when(chips)
            def _():
                remote(sent, sent, kv_s.at[way, which], kv_r.at[0, 0], mate).wait_send()
        half = ref.at[pl.ds(other, NS)]
        remote(half, half, kv_s.at[2, which], kv_r.at[0, 0], mate).wait_send()
    for which, ref in ((0, q), (1, g)):
        half = ref.at[pl.ds(other, NS)]
        remote(half, half, q_s.at[which], q_r.at[0], mate).wait_send()
    for which, ref in ((0, o), (1, dq)):
        half = ref.at[pl.ds(other, NS)]
        remote(half, half, hop_s, osend_r.at[which], mate).wait_recv()
    for which, ref in ((0, dk), (1, dv)):
        half = ref.at[pl.ds(other, NS)]
        remote(half, half, hop_s, dsend_r.at[which], mate).wait_recv()


def place_kernel(slots, *refs):
    srcs, dsts, (buf, rsem, wsem) = refs[:4], refs[4:8], refs[8:]
    size = buf.shape[1]
    jobs = [(src.at[pl.ds(i, size)], dst.at[pl.ds(i, size)]) for src, dst in zip(srcs, dsts) for i in range(0, src.shape[0], size)]

    def read(j):
        return pltpu.make_async_copy(jobs[j][0], buf.at[j % slots], rsem.at[j % slots])

    def write(j):
        return pltpu.make_async_copy(buf.at[j % slots], jobs[j][1], wsem.at[j % slots])

    ahead = slots
    for j in range(min(ahead, len(jobs))):
        read(j).start()
    for j in range(len(jobs)):
        read(j).wait()
        write(j).start()
        if j + ahead < len(jobs):
            if j + ahead >= slots:
                write(j + ahead - slots).wait()
            read(j + ahead).start()
    for j in range(max(0, len(jobs) - slots), len(jobs)):
        write(j).wait()


ANY = pl.BlockSpec(memory_space=pl.ANY)
VMEM = pl.BlockSpec(memory_space=pltpu.VMEM)


def solution(mesh):
    n_dev = mesh.shape['cp']
    seq_spec = P('dp', 'cp', None, None)
    id_spec = P('dp', 'cp')
    bf, f32 = jnp.bfloat16, jnp.float32
    shape = jax.ShapeDtypeStruct
    dma = pltpu.SemaphoreType.DMA

    def per_device(query, keys, values, grad_out, doc_id):
        nb, piece, heads, hd = query.shape
        rows = piece * heads
        outs = pl.pallas_call(
            functools.partial(fused_kernel, hd ** -0.5),
            in_specs=[VMEM] + [ANY] * 4,
            out_specs=[ANY] * 8,
            out_shape=[
                shape((nb, rows, hd), bf), shape((nb, rows, hd), bf), shape((nb, piece, hd), bf), shape((nb, piece, hd), bf),
                shape((NS, 2, rows, hd), bf), shape((4, NS, 2, 256, 256), bf),
                shape((3, NS, 256, 512), f32), shape((3, NS, 256, 512), f32),
            ],
            scratch_shapes=[
                pltpu.VMEM((n_dev, nb, piece), jnp.int32), pltpu.VMEM((2, 4, 2, 256, 256), bf), pltpu.VMEM((2, 4, rows, hd), bf),
                pltpu.VMEM((2, 4, rows, hd), bf), pltpu.VMEM((NG, 4, 256, 512), f32), pltpu.VMEM((6, 256, 512), f32),
                pltpu.VMEM((3, 2, 2, 256, 256), bf),
                pltpu.VMEM((4, 2, rows, 256), f32), pltpu.VMEM((4, 2, rows, 256), f32), pltpu.VMEM((4, 2, rows, 256), bf),
                pltpu.VMEM((4, 2, rows, 128), f32), pltpu.VMEM((4, 2, rows, 128), f32), pltpu.VMEM((2, rows, 128), f32),
                pltpu.VMEM((2, rows, 128), jnp.int32), pltpu.VMEM((2, rows, hd), f32),
                dma((n_dev,)), dma((n_dev,)), dma((2, 10)), dma((2, 4)), dma((NG, 4)), dma((2,)), dma((2,)), dma((NJ,)), dma((3, 2)), dma((4, NJ)),
                dma, dma((3, NS)), dma((3, 2, 4)), dma((2,)), dma((3, 4)), dma((2,)), dma((NS,)), dma((2,)),
            ],
            compiler_params=pltpu.CompilerParams(has_side_effects=True, vmem_limit_bytes=62 * 1024 * 1024),
            name="attend",
        )(doc_id, query.reshape(nb, rows, hd), grad_out.reshape(nb, rows, hd), keys.reshape(nb, piece, hd), values.reshape(nb, piece, hd))
        outs = [x.reshape(-1, rows, hd) for x in outs[:4]]
        o, dq, dk, dv = pl.pallas_call(
            functools.partial(place_kernel, 36),
            in_specs=[ANY] * 4,
            out_specs=[ANY] * 4,
            out_shape=[shape(x.shape, bf) for x in outs],
            scratch_shapes=[pltpu.VMEM((36, 2, rows, hd), bf), dma((36,)), dma((36,))],
            compiler_params=pltpu.CompilerParams(vmem_limit_bytes=63 * 1024 * 1024),
            name="place",
        )(*outs)
        return o.reshape(query.shape), dq.reshape(query.shape), dk.reshape(keys.shape), dv.reshape(values.shape)

    return jax.shard_map(per_device, mesh=mesh, in_specs=(seq_spec, seq_spec, seq_spec, seq_spec, id_spec),
                         out_specs=(seq_spec, seq_spec, seq_spec, seq_spec), check_vma=False)
```

```python
import functools

import jax
import jax.numpy as jnp
from jax import lax
from jax.experimental import pallas as pl
from jax.experimental.pallas import tpu as pltpu
from jax.sharding import PartitionSpec as P

NEG_BIG = -1e30
LOG2E = 1.4426950408889634
NS = 16
NJ = NS
AHEAD = 2
NG = 4
PLAN1 = 'RRRMFMRRFRFRRMMM'
PLAN0 = 'NNANANCCNCNNCNNA'
LAST2 = (8, 9, 11)
EARLY_X = {6: 0, 8: 1, 10: 3, 12: 5, 13: 6, 14: 7}
EARLY_Y = {5: 0, 7: 1, 9: 2, 10: 6, 13: 7, 14: 9, 15: 11}
LAG = (6, 8, 7)
LATE_CHIP = 2
VIA3 = (0, 1)


def where_plan(plan, kinds):
    return tuple(s for s in range(NS) if plan[s] in kinds)


ROUND, MERGE, FAR1 = (where_plan(PLAN1, x) for x in 'RMF')
HERE0, ON1, ON2 = (where_plan(PLAN0, x) for x in 'NAC')
OWN1 = where_plan(PLAN1, 'RM')
OWN2 = tuple(s for s in range(NS) if s not in LAST2)
OWN3 = tuple(range(NS))
PASS_X = where_plan(PLAN0, 'NC')
PASS_0 = where_plan(PLAN0, 'AC')


def dot_nt(a, b):
    return lax.dot_general(a, b, (((1,), (1,)), ((), ())), preferred_element_type=jnp.float32)


def dot_nn(a, b):
    return lax.dot_general(a, b, (((1,), (0,)), ((), ())), preferred_element_type=jnp.float32)


def dot_tn(a, b):
    return lax.dot_general(a, b, (((0,), (0,)), ((), ())), preferred_element_type=jnp.float32)


def remote(src, dst, send, recv, dev):
    return pltpu.make_async_remote_copy(src_ref=src, dst_ref=dst, send_sem=send, recv_sem=recv,
                                        device_id={'cp': dev}, device_id_type=pl.DeviceIdType.MESH)


def fused_kernel(scale, doc, q, g, k, v, o, dq, dk, dv, qgm, kvr, part, hold,
                 docs, kvs, qg, outb, dkv, sums, fin, e_scr, dp_scr, p_scr, l_scr, f_scr, t_scr, docr, o_acc,
                 doc_s, doc_r, isem, osem, gsem, osend_r, q_s, q_r, kv_s, kv_r, hop_s, part_r, fsem, dsend_r, lsem, xsem, rel_s, down_r):
    rank = lax.axis_index('cp')
    n_dev = docs.shape[0]
    c = rank // 2
    e = lax.rem(rank, 2)
    mate = 2 * c + 1 - e
    other = NS * (1 - e)
    mine = NS * e

    def dev(chip):
        return 2 * chip + e

    docs[rank] = doc[...]

    def doc_copy(i):
        return remote(doc, docs.at[rank], doc_s.at[i], doc_r.at[i], lax.rem(rank + i, n_dev))

    for i in range(1, n_dev):
        doc_copy(i).start()

    def kv_parts(chip, way, j, cols):
        out = []
        for col in cols:
            for which, ref in ((0, k), (1, v)):
                out.append(remote(ref.at[pl.ds(col * NS + j, 1)], kvr.at[c, pl.ds(j, 1), which, pl.ds(128 * e, 128)],
                                  kv_s.at[way, which], kv_r.at[c, j], 2 * chip + col))
        return out

    def send_kv(chip, way, j):
        for copy in kv_parts(chip, way, j, (0, 1)):
            copy.start()

    def kv_forward(a, chip, j):
        return remote(kvr.at[a, pl.ds(j, 1)], kvr.at[a, pl.ds(j, 1)], hop_s, kv_r.at[a, j], dev(chip))

    def stream_kv(j):
        @pl.when(c == 0)
        def _():
            send_kv(1, 0, j)
            send_kv(2, 1, j)

        if not isinstance(j, int) or j not in VIA3:
            @pl.when(c == 1)
            def _():
                send_kv(0, 1, j)

        @pl.when(c == 2)
        def _():
            send_kv(3, 0, j)

    def to_mate(j):
        for which, ref in ((0, k), (1, v)):
            remote(ref.at[pl.ds(other + j, 1)], kvr.at[c, pl.ds(j, 1), which, pl.ds(128 * e, 128)],
                   kv_s.at[2, which], kv_r.at[c, j], mate).start()

    def rows_to_mate(j):
        for which, ref in ((0, q), (1, g)):
            remote(ref.at[pl.ds(other + j, 1)], qgm.at[pl.ds(j, 1), which], q_s.at[which], q_r.at[j], mate).start()

    stream_kv(0)

    @pl.when(c == 1)
    def _():
        send_kv(3, 0, 0)
    to_mate(0)
    rows_to_mate(0)
    for j in range(1, AHEAD):
        stream_kv(j)
    for j in range(1, NJ):
        to_mate(j)
        rows_to_mate(j)
    for i in range(1, n_dev):
        doc_copy(i).wait()

    def member(s, group):
        out = jnp.bool_(False)
        for one in group:
            out = out | (s == one)
        return out

    def by_way_of_3(j):
        @pl.when(c == 3)
        def _():
            kv_forward(1, 1, j).wait_recv()
            kv_forward(1, 2, j).start()

    def arrive(j):
        remote(kvr.at[c, pl.ds(j, 1), :, pl.ds(0, 128)], kvr.at[c, pl.ds(j, 1), :, pl.ds(0, 128)],
               hop_s, kv_r.at[c, j], mate).wait_recv()
        remote(qgm.at[pl.ds(j, 1)], qgm.at[pl.ds(j, 1)], hop_s, q_r.at[j], mate).wait_recv()
        for a in range(3):
            need = a < c
            if a == 1:
                need = need & jnp.logical_not((c == 3) & member(j, VIA3))

            @pl.when(need)
            def _():
                kv_forward(a, a, j).wait_recv()

        @pl.when(c == 1)
        def _():
            kv_forward(0, 3, j).start()

            @pl.when(j + 1 < NJ)
            def _():
                send_kv(3, 0, j + 1)

        @pl.when((c == 0) & jnp.logical_not(member(j, VIA3)))
        def _():
            kv_forward(1, 1, j).wait_recv()
            kv_forward(1, 2, j).start()

        @pl.when(j + AHEAD < NJ)
        def _():
            stream_kv(j + AHEAD)

    def inputs(s, sl):
        row = mine + s
        rows = pl.ds(128 * e, 128)
        rest = pl.ds(128 - 128 * e, 128)
        pairs = [
            (q.at[row], qg.at[sl, 0]), (g.at[row], qg.at[sl, 2]), (qgm.at[s, 0], qg.at[sl, 1]), (qgm.at[s, 1], qg.at[sl, 3]),
            (k.at[row], kvs.at[sl, 0, 0, rows]), (v.at[row], kvs.at[sl, 0, 1, rows]),
            (kvr.at[c, s, :, rest], kvs.at[sl, 0, :, rest]),
        ]
        return [pltpu.make_async_copy(src, dst, isem.at[sl, i]) for i, (src, dst) in enumerate(pairs)]

    def far_input(s, sl, d):
        return pltpu.make_async_copy(kvr.at[c - d, s], kvs.at[sl, d], isem.at[sl, 6 + d])

    def fetch(s, sl):
        for copy in inputs(s, sl):
            copy.start()
        for d in range(1, 4):
            @pl.when(d <= c)
            def _():
                far_input(s, sl, d).start()

    def fetch_wait(s, sl):
        for copy in inputs(s, sl):
            copy.wait()
        for d in range(1, 4):
            @pl.when(d <= c)
            def _():
                far_input(s, sl, d).wait()

    def row_outputs(s, sl):
        row = mine + s
        here = [pltpu.make_async_copy(outb.at[sl, 0], o.at[row], osem.at[sl, 0]),
                pltpu.make_async_copy(outb.at[sl, 2], dq.at[row], osem.at[sl, 1])]
        there = [remote(outb.at[sl, 1], o.at[row], osem.at[sl, 2], osend_r.at[0], mate),
                 remote(outb.at[sl, 3], dq.at[row], osem.at[sl, 3], osend_r.at[1], mate)]
        return here, there

    def keep(sl, d, slot, s):
        return pltpu.make_async_copy(dkv.at[sl, d], hold.at[slot, s], gsem.at[sl, d])

    def give(sl, d, chip, slot, s):
        return remote(dkv.at[sl, d], part.at[slot, s], gsem.at[sl, d], part_r.at[slot, s], dev(chip))

    def rank_in(s, group):
        count = jnp.int32(0)
        for one in group:
            count = count + jnp.where(one < s, 1, 0)
        return count

    def choose(cond, yes, no):
        pl.when(cond)(yes)
        pl.when(jnp.logical_not(cond))(no)

    def grads_out(s, begin):
        sl = lax.rem(s, NG)

        def local(d, slot):
            copy = keep(sl, d, slot, s)
            copy.start() if begin else copy.wait()

        def away(d, chip, slot):
            copy = give(sl, d, chip, slot, s)
            copy.start() if begin else copy.wait_send()

        @pl.when(c == 0)
        def _():
            local(0, 1)

        @pl.when(c == 1)
        def _():
            choose(member(s, FAR1), lambda: away(0, 3, 2), lambda: local(0, 1))
            local(1, 0)

        @pl.when(c == 2)
        def _():
            choose(member(s, ROUND), lambda: local(1, 0), lambda: away(1, 3, 0))
            choose(member(s, LAST2), lambda: away(0, 3, 1), lambda: local(0, 1))
            choose(member(s, ON2), lambda: local(2, 2), lambda: away(2, 0, 1))

        if not begin:
            @pl.when(c == 3)
            def _():
                away(3, 1, 0)
                pl.when(member(s, ROUND))(lambda: away(2, 2, 0))
                pl.when(member(s, MERGE))(lambda: away(2, 1, 1))
                pl.when(jnp.logical_not(member(s, LAST2)))(lambda: away(1, 2, 1))

    def put(s, sl):
        here, there = row_outputs(s, sl)
        for copy in here + there:
            copy.start()
        grads_out(s, True)

    def put_wait(s, sl):
        here, there = row_outputs(s, sl)
        for copy in here:
            copy.wait()
        for copy in there:
            copy.wait_send()

    def final_copies(kind, sl, s, chip):
        row = mine + s
        out = []
        for which, ref in ((0, dk), (1, dv)):
            for far, rows in ((0, pl.ds(128 * e, 128)), (1, pl.ds(128 - 128 * e, 128))):
                src, sem = fin.at[kind, sl, which, rows], fsem.at[kind, sl, 2 * which + far]
                if far:
                    out.append(remote(src, ref.at[row], sem, dsend_r.at[which], mate if chip is None else 2 * chip + 1 - e))
                elif chip is None:
                    out.append(pltpu.make_async_copy(src, ref.at[row], sem))
                else:
                    out.append(remote(src, ref.at[row], sem, down_r.at[which], dev(chip)))
        return out

    def final_wait(kind, sl, chip):
        for i, copy in enumerate(final_copies(kind, sl, 0, chip)):
            if chip is None and i % 2 == 0:
                copy.wait()
            else:
                copy.wait_send()

    def finalize(kind, group, s, value, chip):
        count = rank_in(s, group)
        sl = lax.rem(count, 2)
        pl.when(count >= 2)(lambda: final_wait(kind, sl, chip))
        fin[kind, sl, 0] = (value[:, :256] * scale).astype(jnp.bfloat16)
        fin[kind, sl, 1] = value[:, 256:].astype(jnp.bfloat16)
        for copy in final_copies(kind, sl, s, chip):
            copy.start()

    def final_drain(kind, group, chip):
        for n in range(max(0, len(group) - 2), len(group)):
            final_wait(kind, n % 2, chip)

    row_tok = lax.broadcasted_iota(jnp.int32, (1024, 128), 0) >> 3
    lane = lax.broadcasted_iota(jnp.int32, (1024, 128), 1)
    cs = scale * LOG2E
    lo_half, hi_half = slice(0, 128), slice(128, 256)

    def attend(s, slot):
        row = mine + s
        gslot = lax.rem(s, NG)
        piece = (e, 1 - e)
        for role in range(2):
            dq_row = docs[2 * c + piece[role], pl.ds(row, 1), :]
            d_t = jnp.transpose(jnp.broadcast_to(dq_row, (128, 128)))
            docr[role] = jnp.broadcast_to(d_t[:, None, :], (128, 8, 128)).reshape(1024, 128)

        def g_of(role):
            return qg[slot, 2 + role]

        def far_loop(body):
            for chip in range(1, 4):
                @pl.when(c == chip)
                def _():
                    for d in range(1, chip + 1):
                        body(d, 0)

        def scores(role, d, causal):
            sc = dot_nt(qg[slot, role], kvs[slot, d, 0]) * cs
            xs = []
            for j in range(2):
                dk_row = docs[2 * (c - d) + j, pl.ds(row, 1), :]
                vis = docr[role] == dk_row
                if causal:
                    vis = vis & (lane + 128 * j <= row_tok + 128 * piece[role])
                xs.append(jnp.where(vis, sc[:, 128 * j:128 * (j + 1)], NEG_BIG))
            top = jnp.maximum(xs[0], xs[1])
            es = [jnp.exp2(x - top) for x in xs]
            e_scr[d, role, :, lo_half] = es[0]
            e_scr[d, role, :, hi_half] = es[1]
            f_scr[d, role] = top
            l_scr[d, role] = es[0] + es[1]
            return top

        def dprob(role, d):
            dp_scr[d, role] = dot_nt(g_of(role), kvs[slot, d, 1])

        for role in range(2):
            t_scr[role] = scores(role, 0, True)

        def far_scores(d, x):
            for role in range(2):
                t_scr[role] = jnp.maximum(t_scr[role], scores(role, d, False))
            for role in range(2):
                dprob(role, d)
            return x
        far_loop(far_scores)

        for role in range(2):
            t_scr[role] = jnp.broadcast_to(jnp.max(t_scr[role], axis=1, keepdims=True), (1024, 128))
        dprob(0, 0)

        for role in range(2):
            top = t_scr[role]
            norm = l_scr[0, role] * jnp.exp2(f_scr[0, role] - top)
            for d in range(1, 4):
                norm = norm + l_scr[d, role] * jnp.exp2(f_scr[d, role] - top)
            t_scr[role] = top + jnp.log2(jnp.broadcast_to(jnp.sum(norm, axis=1, keepdims=True), (1024, 128)))
        dprob(1, 0)

        def weighted(role, d):
            f = jnp.exp2(f_scr[d, role] - t_scr[role])
            f_scr[d, role] = f
            for half in (lo_half, hi_half):
                p_scr[d, role, :, half] = (e_scr[d, role, :, half] * f).astype(jnp.bfloat16)
            return dot_nn(p_scr[d, role], kvs[slot, d, 1])

        def value_grads(d):
            dkv[gslot, d, :, 256:] = dot_tn(p_scr[d, 0], g_of(0)) + dot_tn(p_scr[d, 1], g_of(1))

        for role in range(2):
            o_acc[role] = weighted(role, 0)

        def far_weighted(d, x):
            for role in range(2):
                o_acc[role] = o_acc[role] + weighted(role, d)
            value_grads(d)
            return x
        far_loop(far_weighted)

        for role in range(2):
            o_low = o_acc[role].astype(jnp.bfloat16)
            outb[slot, role] = o_low
            delta = jnp.sum(g_of(role).astype(jnp.float32) * o_low.astype(jnp.float32), axis=1, keepdims=True)
            t_scr[role] = jnp.broadcast_to(delta, (1024, 128))
        value_grads(0)

        def score_grads(d):
            out = []
            for role in range(2):
                ds = [
                    (e_scr[d, role, :, half] * f_scr[d, role] * (dp_scr[d, role, :, half] - t_scr[role])).astype(jnp.bfloat16)
                    for half in (lo_half, hi_half)
                ]
                out.append(jnp.concatenate(ds, axis=1))
            dkv[gslot, d, :, :256] = dot_tn(out[0], qg[slot, 0]) + dot_tn(out[1], qg[slot, 1])
            return [dot_nn(ds, kvs[slot, d, 0]) for ds in out]

        got = score_grads(0)
        for role in range(2):
            o_acc[role] = got[role]

        def far_grads(d, x):
            got = score_grads(d)
            for role in range(2):
                o_acc[role] = o_acc[role] + got[role]
            return x
        far_loop(far_grads)
        for role in range(2):
            outb[slot, 2 + role] = (o_acc[role] * scale).astype(jnp.bfloat16)

    def part_wait(slot, s):
        remote(part.at[slot, s], part.at[slot, s], hop_s, part_r.at[slot, s], mate).wait_recv()

    def load(src, i):
        return [pltpu.make_async_copy(src.at[pl.ds(64 * n, 64)], sums.at[i, pl.ds(64 * n, 64)], lsem.at[i, n]) for n in range(4)]

    def start(copies):
        for copy in copies:
            copy.start()

    def finish(copies):
        for copy in copies:
            copy.wait()

    def passed(s, sl, chip, slot):
        return remote(sums.at[4 + sl], part.at[slot, s], xsem.at[sl], part_r.at[slot, s], dev(chip))

    def relay(s):
        return remote(part.at[2, s], part.at[1, s], rel_s.at[s], part_r.at[1, s], dev(1))

    def pass_on(i, group, held, slot_in, chip, slot_out):
        count = rank_in(i, group)
        sl = lax.rem(count, 2)
        start(load(hold.at[held, i], 0))
        part_wait(slot_in, i)
        start(load(part.at[slot_in, i], 1))
        pl.when(count >= 2)(lambda: passed(i, sl, chip, slot_out).wait_send())
        finish(load(hold.at[held, i], 0))
        finish(load(part.at[slot_in, i], 1))
        sums[4 + sl] = sums[0] + sums[1]
        passed(i, sl, chip, slot_out).start()

    def pass_x(i):
        pass_on(i, PASS_X, 0, 0, 0, 0)

    def pass_y(i):
        pass_on(i, ROUND, 0, 0, 0, 2)

    def total(kind, group, s, held, slots, chip):
        terms = [hold.at[held, s]] + [part.at[slot, s] for slot in slots]
        for slot in slots:
            part_wait(slot, s)
        for n, src in enumerate(terms):
            start(load(src, n))
        for n, src in enumerate(terms):
            finish(load(src, n))
        value = sums[0]
        for n in range(1, len(terms)):
            value = value + sums[n]
        finalize(kind, group, s, value, chip)

    for d in range(1, 4):
        f_scr[d] = jnp.full((2, 1024, 128), NEG_BIG, jnp.float32)
        l_scr[d] = jnp.zeros((2, 1024, 128), jnp.float32)
    by_way_of_3(VIA3[0])
    arrive(0)
    for j in VIA3[1:]:
        by_way_of_3(j)
    fetch(0, 0)

    def step(s, x):
        slot = lax.rem(s, 2)

        late = (c >= LATE_CHIP) & (s == 0)

        def ahead():
            arrive(s + 1)
            fetch(s + 1, 1 - slot)
        pl.when((s + 1 < NS) & jnp.logical_not(late))(ahead)

        @pl.when(s >= 2)
        def _():
            put_wait(s - 2, slot)

        @pl.when(s >= NG)
        def _():
            grads_out(s - NG, False)
        fetch_wait(s, slot)
        attend(s, slot)

        @pl.when(c == 3)
        def _():
            gslot = lax.rem(s, NG)
            give(gslot, 3, 1, 0, s).start()
            pl.when(member(s, ROUND))(lambda: give(gslot, 2, 2, 0, s).start())

            @pl.when(member(s, MERGE))
            def _():
                part_wait(0, s)
                start(load(part.at[0, s], 0))
                finish(load(part.at[0, s], 0))
                dkv[gslot, 2] = dkv[gslot, 2] + sums[0]

            @pl.when(member(s, FAR1))
            def _():
                part_wait(0, s)
                start(load(part.at[0, s], 0))
                part_wait(2, s)
                start(load(part.at[2, s], 1))
                finish(load(part.at[0, s], 0))
                finish(load(part.at[2, s], 1))
                finalize(1, FAR1, s, dkv[gslot, 2] + sums[0] + sums[1], 1)
            finalize(0, OWN3, s, dkv[gslot, 0], None)
            pl.when(member(s, MERGE))(lambda: give(gslot, 2, 1, 1, s).start())

            def last_two():
                part_wait(1, s)
                start(load(part.at[1, s], 2))
                finish(load(part.at[1, s], 2))
                finalize(2, LAST2, s, dkv[gslot, 1] + sums[2], 2)
            choose(member(s, LAST2), last_two, lambda: give(gslot, 1, 2, 1, s).start())
        put(s, slot)
        for at, i in EARLY_X.items():
            pl.when((c == 1) & (s == at))(lambda: pass_x(i))
        for at, i in EARLY_Y.items():
            pl.when((c == 2) & (s == at))(lambda: pass_y(i))
        pl.when(late)(ahead)
        return x

    lax.fori_loop(0, NS, step, 0)
    put_wait(NS - 2, 0)
    put_wait(NS - 1, 1)
    for s in range(NS - NG, NS):
        grads_out(s, False)

    def home(i, x):
        def behind(lag, body):
            s = i - lag
            pl.when((s >= 0) & (s < NS))(lambda: body(s))

        @pl.when(c == 0)
        def _():
            @pl.when(member(i, ROUND))
            def _():
                part_wait(2, i)
                relay(i).start()
            pl.when(member(i, ON1))(lambda: pass_on(i, PASS_0, 1, 1, 1, 2))
            pl.when(member(i, ON2))(lambda: pass_on(i, PASS_0, 1, 0, 2, 2))
            behind(LAG[0], lambda s: pl.when(member(s, HERE0))(lambda: total(0, HERE0, s, 1, (1, 0), None)))

        @pl.when(c == 1)
        def _():
            later = tuple(s for s in PASS_X if s not in EARLY_X.values())
            pl.when(member(i, later))(lambda: pass_x(i))

            def body(s):
                pl.when(member(s, ON1))(lambda: total(1, ON1, s, 0, (0, 2), 0))
                pl.when(member(s, OWN1))(lambda: total(0, OWN1, s, 1, (1,), None))
            behind(LAG[1], body)

        @pl.when(c == 2)
        def _():
            later = tuple(s for s in ROUND if s not in EARLY_Y.values())
            pl.when(member(i, later))(lambda: pass_y(i))

            def body(s):
                pl.when(member(s, ON2))(lambda: total(1, ON2, s, 2, (2,), 0))
                pl.when(member(s, OWN2))(lambda: total(0, OWN2, s, 1, (1,), None))
            behind(LAG[2], body)
        return x

    @pl.when(c < 3)
    def _():
        lax.fori_loop(0, NS + max(LAG), home, 0)

    def down_wait(n):
        for which, ref in ((0, dk), (1, dv)):
            rows = ref.at[pl.ds(0, n)]
            remote(rows, rows, hop_s, down_r.at[which], mate).wait_recv()

    @pl.when(c == 0)
    def _():
        for s in ROUND:
            relay(s).wait_send()
        for sl in range(2):
            passed(0, sl, 1, 2).wait_send()
        sent = kvr.at[1, pl.ds(0, NS - len(VIA3))]
        remote(sent, sent, hop_s, kv_r.at[0, 0], mate).wait_send()
        final_drain(0, HERE0, None)
        down_wait(len(PASS_0))

    @pl.when(c == 1)
    def _():
        for sl in range(2):
            passed(0, sl, 0, 0).wait_send()
        remote(kvr.at[0], kvr.at[0], hop_s, kv_r.at[0, 0], mate).wait_send()
        final_drain(0, OWN1, None)
        final_drain(1, ON1, 0)
        down_wait(len(FAR1))

    @pl.when(c == 2)
    def _():
        for sl in range(2):
            passed(0, sl, 0, 2).wait_send()
        final_drain(0, OWN2, None)
        final_drain(1, ON2, 0)
        down_wait(len(LAST2))

    @pl.when(c == 3)
    def _():
        sent = kvr.at[1, pl.ds(0, len(VIA3))]
        remote(sent, sent, hop_s, kv_r.at[0, 0], mate).wait_send()
        final_drain(0, OWN3, None)
        final_drain(1, FAR1, 1)
        final_drain(2, LAST2, 2)
    for which, ref in ((0, k), (1, v)):
        some = ref.at[pl.ds(0, 2 * (NS - len(VIA3)))]
        for way, chips, sent in ((0, c < 3, ref), (1, c == 0, ref), (1, c == 1, some)):
            @pl.when(chips)
            def _():
                remote(sent, sent, kv_s.at[way, which], kv_r.at[0, 0], mate).wait_send()
        half = ref.at[pl.ds(other, NS)]
        remote(half, half, kv_s.at[2, which], kv_r.at[0, 0], mate).wait_send()
    for which, ref in ((0, q), (1, g)):
        half = ref.at[pl.ds(other, NS)]
        remote(half, half, q_s.at[which], q_r.at[0], mate).wait_send()
    for which, ref in ((0, o), (1, dq)):
        half = ref.at[pl.ds(other, NS)]
        remote(half, half, hop_s, osend_r.at[which], mate).wait_recv()
    for which, ref in ((0, dk), (1, dv)):
        half = ref.at[pl.ds(other, NS)]
        remote(half, half, hop_s, dsend_r.at[which], mate).wait_recv()


def place_kernel(slots, *refs):
    srcs, dsts, (buf, rsem, wsem) = refs[:4], refs[4:8], refs[8:]
    size = buf.shape[1]
    jobs = [(src.at[pl.ds(i, size)], dst.at[pl.ds(i, size)]) for src, dst in zip(srcs, dsts) for i in range(0, src.shape[0], size)]

    def read(j):
        return pltpu.make_async_copy(jobs[j][0], buf.at[j % slots], rsem.at[j % slots])

    def write(j):
        return pltpu.make_async_copy(buf.at[j % slots], jobs[j][1], wsem.at[j % slots])

    ahead = 10
    for j in range(min(ahead, len(jobs))):
        read(j).start()
    for j in range(len(jobs)):
        read(j).wait()
        write(j).start()
        if j + ahead < len(jobs):
            if j + ahead >= slots:
                write(j + ahead - slots).wait()
            read(j + ahead).start()
    for j in range(max(0, len(jobs) - slots), len(jobs)):
        write(j).wait()


ANY = pl.BlockSpec(memory_space=pl.ANY)
VMEM = pl.BlockSpec(memory_space=pltpu.VMEM)


def solution(mesh):
    n_dev = mesh.shape['cp']
    seq_spec = P('dp', 'cp', None, None)
    id_spec = P('dp', 'cp')
    bf, f32 = jnp.bfloat16, jnp.float32
    shape = jax.ShapeDtypeStruct
    dma = pltpu.SemaphoreType.DMA

    def per_device(query, keys, values, grad_out, doc_id):
        nb, piece, heads, hd = query.shape
        rows = piece * heads
        outs = pl.pallas_call(
            functools.partial(fused_kernel, hd ** -0.5),
            in_specs=[VMEM] + [ANY] * 4,
            out_specs=[ANY] * 8,
            out_shape=[
                shape((nb, rows, hd), bf), shape((nb, rows, hd), bf), shape((nb, piece, hd), bf), shape((nb, piece, hd), bf),
                shape((NS, 2, rows, hd), bf), shape((4, NS, 2, 256, 256), bf),
                shape((3, NS, 256, 512), f32), shape((3, NS, 256, 512), f32),
            ],
            scratch_shapes=[
                pltpu.VMEM((n_dev, nb, piece), jnp.int32), pltpu.VMEM((2, 4, 2, 256, 256), bf), pltpu.VMEM((2, 4, rows, hd), bf),
                pltpu.VMEM((2, 4, rows, hd), bf), pltpu.VMEM((NG, 4, 256, 512), f32), pltpu.VMEM((6, 256, 512), f32),
                pltpu.VMEM((3, 2, 2, 256, 256), bf),
                pltpu.VMEM((4, 2, rows, 256), f32), pltpu.VMEM((4, 2, rows, 256), f32), pltpu.VMEM((4, 2, rows, 256), bf),
                pltpu.VMEM((4, 2, rows, 128), f32), pltpu.VMEM((4, 2, rows, 128), f32), pltpu.VMEM((2, rows, 128), f32),
                pltpu.VMEM((2, rows, 128), jnp.int32), pltpu.VMEM((2, rows, hd), f32),
                dma((n_dev,)), dma((n_dev,)), dma((2, 10)), dma((2, 4)), dma((NG, 4)), dma((2,)), dma((2,)), dma((NJ,)), dma((3, 2)), dma((4, NJ)),
                dma, dma((3, NS)), dma((3, 2, 4)), dma((2,)), dma((3, 4)), dma((2,)), dma((NS,)), dma((2,)),
            ],
            compiler_params=pltpu.CompilerParams(has_side_effects=True, vmem_limit_bytes=62 * 1024 * 1024),
            name="attend",
        )(doc_id, query.reshape(nb, rows, hd), grad_out.reshape(nb, rows, hd), keys.reshape(nb, piece, hd), values.reshape(nb, piece, hd))
        outs = [x.reshape(-1, rows, hd) for x in outs[:4]]
        o, dq, dk, dv = pl.pallas_call(
            functools.partial(place_kernel, 14),
            in_specs=[ANY] * 4,
            out_specs=[ANY] * 4,
            out_shape=[shape(x.shape, bf) for x in outs],
            scratch_shapes=[pltpu.VMEM((14, 4, rows, hd), bf), dma((14,)), dma((14,))],
            compiler_params=pltpu.CompilerParams(vmem_limit_bytes=63 * 1024 * 1024),
            name="place",
        )(*outs)
        return o.reshape(query.shape), dq.reshape(query.shape), dk.reshape(keys.shape), dv.reshape(values.shape)

    return jax.shard_map(per_device, mesh=mesh, in_specs=(seq_spec, seq_spec, seq_spec, seq_spec, id_spec),
                         out_specs=(seq_spec, seq_spec, seq_spec, seq_spec), check_vma=False)
```

```python
import functools

import jax
import jax.numpy as jnp
from jax import lax
from jax.experimental import pallas as pl
from jax.experimental.pallas import tpu as pltpu
from jax.sharding import PartitionSpec as P

NEG_BIG = -1e30
LOG2E = 1.4426950408889634
NS = 16
NJ = NS
AHEAD = 2
NG = 4
PLAN1 = 'RRRMFMRRFRFRRMMM'
PLAN0 = 'NNANANCCNCNNCNNA'
LAST2 = (8, 9, 11)
EARLY_X = {6: 0, 8: 1, 10: 3, 12: 5, 13: 6, 14: 7}
EARLY_Y = {5: 0, 7: 1, 9: 2, 10: 6, 13: 7, 14: 9, 15: 11}
LAG = (6, 8, 7)
LATE_CHIP = 2
VIA3 = (0, 1)


def where_plan(plan, kinds):
    return tuple(s for s in range(NS) if plan[s] in kinds)


ROUND, MERGE, FAR1 = (where_plan(PLAN1, x) for x in 'RMF')
HERE0, ON1, ON2 = (where_plan(PLAN0, x) for x in 'NAC')
OWN1 = where_plan(PLAN1, 'RM')
OWN2 = tuple(s for s in range(NS) if s not in LAST2)
OWN3 = tuple(range(NS))
PASS_X = where_plan(PLAN0, 'NC')
PASS_0 = where_plan(PLAN0, 'AC')


def dot_nt(a, b):
    return lax.dot_general(a, b, (((1,), (1,)), ((), ())), preferred_element_type=jnp.float32)


def dot_nn(a, b):
    return lax.dot_general(a, b, (((1,), (0,)), ((), ())), preferred_element_type=jnp.float32)


def dot_tn(a, b):
    return lax.dot_general(a, b, (((0,), (0,)), ((), ())), preferred_element_type=jnp.float32)


def remote(src, dst, send, recv, dev):
    return pltpu.make_async_remote_copy(src_ref=src, dst_ref=dst, send_sem=send, recv_sem=recv,
                                        device_id={'cp': dev}, device_id_type=pl.DeviceIdType.MESH)


def fused_kernel(scale, doc, q, g, k, v, o, dq, dk, dv, qgm, kvr, part, hold,
                 docs, kvs, qg, outb, dkv, sums, fin, e_scr, dp_scr, p_scr, l_scr, f_scr, t_scr, docr, o_acc,
                 doc_s, doc_r, isem, osem, gsem, osend_r, q_s, q_r, kv_s, kv_r, hop_s, part_r, fsem, dsend_r, lsem, xsem, rel_s, down_r):
    rank = lax.axis_index('cp')
    n_dev = docs.shape[0]
    c = rank // 2
    e = lax.rem(rank, 2)
    mate = 2 * c + 1 - e
    other = NS * (1 - e)
    mine = NS * e

    def dev(chip):
        return 2 * chip + e

    docs[rank] = doc[...]

    def doc_copy(i):
        return remote(doc, docs.at[rank], doc_s.at[i], doc_r.at[i], lax.rem(rank + i, n_dev))

    for i in range(1, n_dev):
        doc_copy(i).start()

    def kv_parts(chip, way, j, cols):
        out = []
        for col in cols:
            for which, ref in ((0, k), (1, v)):
                out.append(remote(ref.at[pl.ds(col * NS + j, 1)], kvr.at[c, pl.ds(j, 1), which, pl.ds(128 * e, 128)],
                                  kv_s.at[way, which], kv_r.at[c, j], 2 * chip + col))
        return out

    def send_kv(chip, way, j):
        for copy in kv_parts(chip, way, j, (0, 1)):
            copy.start()

    def kv_forward(a, chip, j):
        return remote(kvr.at[a, pl.ds(j, 1)], kvr.at[a, pl.ds(j, 1)], hop_s, kv_r.at[a, j], dev(chip))

    def stream_kv(j):
        @pl.when(c == 0)
        def _():
            send_kv(1, 0, j)
            send_kv(2, 1, j)

        if not isinstance(j, int) or j not in VIA3:
            @pl.when(c == 1)
            def _():
                send_kv(0, 1, j)

        @pl.when(c == 2)
        def _():
            send_kv(3, 0, j)

    def to_mate(j):
        for which, ref in ((0, k), (1, v)):
            remote(ref.at[pl.ds(other + j, 1)], kvr.at[c, pl.ds(j, 1), which, pl.ds(128 * e, 128)],
                   kv_s.at[2, which], kv_r.at[c, j], mate).start()

    def rows_to_mate(j):
        for which, ref in ((0, q), (1, g)):
            remote(ref.at[pl.ds(other + j, 1)], qgm.at[pl.ds(j, 1), which], q_s.at[which], q_r.at[j], mate).start()

    stream_kv(0)

    @pl.when(c == 1)
    def _():
        send_kv(3, 0, 0)
    to_mate(0)
    rows_to_mate(0)
    for j in range(1, AHEAD):
        stream_kv(j)
    for j in range(1, NJ):
        to_mate(j)
        rows_to_mate(j)
    for i in range(1, n_dev):
        doc_copy(i).wait()

    def member(s, group):
        out = jnp.bool_(False)
        for one in group:
            out = out | (s == one)
        return out

    def by_way_of_3(j):
        @pl.when(c == 3)
        def _():
            kv_forward(1, 1, j).wait_recv()
            kv_forward(1, 2, j).start()

    def arrive(j):
        remote(kvr.at[c, pl.ds(j, 1), :, pl.ds(0, 128)], kvr.at[c, pl.ds(j, 1), :, pl.ds(0, 128)],
               hop_s, kv_r.at[c, j], mate).wait_recv()
        remote(qgm.at[pl.ds(j, 1)], qgm.at[pl.ds(j, 1)], hop_s, q_r.at[j], mate).wait_recv()
        for a in range(3):
            need = a < c
            if a == 1:
                need = need & jnp.logical_not((c == 3) & member(j, VIA3))

            @pl.when(need)
            def _():
                kv_forward(a, a, j).wait_recv()

        @pl.when(c == 1)
        def _():
            kv_forward(0, 3, j).start()

            @pl.when(j + 1 < NJ)
            def _():
                send_kv(3, 0, j + 1)

        @pl.when((c == 0) & jnp.logical_not(member(j, VIA3)))
        def _():
            kv_forward(1, 1, j).wait_recv()
            kv_forward(1, 2, j).start()

        @pl.when(j + AHEAD < NJ)
        def _():
            stream_kv(j + AHEAD)

    def inputs(s, sl):
        row = mine + s
        rows = pl.ds(128 * e, 128)
        rest = pl.ds(128 - 128 * e, 128)
        pairs = [
            (q.at[row], qg.at[sl, 0]), (g.at[row], qg.at[sl, 2]), (qgm.at[s, 0], qg.at[sl, 1]), (qgm.at[s, 1], qg.at[sl, 3]),
            (k.at[row], kvs.at[sl, 0, 0, rows]), (v.at[row], kvs.at[sl, 0, 1, rows]),
            (kvr.at[c, s, :, rest], kvs.at[sl, 0, :, rest]),
        ]
        return [pltpu.make_async_copy(src, dst, isem.at[sl, i]) for i, (src, dst) in enumerate(pairs)]

    def far_input(s, sl, d):
        return pltpu.make_async_copy(kvr.at[c - d, s], kvs.at[sl, d], isem.at[sl, 6 + d])

    def fetch(s, sl):
        for copy in inputs(s, sl):
            copy.start()
        for d in range(1, 4):
            @pl.when(d <= c)
            def _():
                far_input(s, sl, d).start()

    def fetch_wait(s, sl):
        for copy in inputs(s, sl):
            copy.wait()
        for d in range(1, 4):
            @pl.when(d <= c)
            def _():
                far_input(s, sl, d).wait()

    def row_outputs(s, sl):
        row = mine + s
        here = [pltpu.make_async_copy(outb.at[sl, 0], o.at[row], osem.at[sl, 0]),
                pltpu.make_async_copy(outb.at[sl, 2], dq.at[row], osem.at[sl, 1])]
        there = [remote(outb.at[sl, 1], o.at[row], osem.at[sl, 2], osend_r.at[0], mate),
                 remote(outb.at[sl, 3], dq.at[row], osem.at[sl, 3], osend_r.at[1], mate)]
        return here, there

    def keep(sl, d, slot, s):
        return pltpu.make_async_copy(dkv.at[sl, d], hold.at[slot, s], gsem.at[sl, d])

    def give(sl, d, chip, slot, s):
        return remote(dkv.at[sl, d], part.at[slot, s], gsem.at[sl, d], part_r.at[slot, s], dev(chip))

    def rank_in(s, group):
        count = jnp.int32(0)
        for one in group:
            count = count + jnp.where(one < s, 1, 0)
        return count

    def choose(cond, yes, no):
        pl.when(cond)(yes)
        pl.when(jnp.logical_not(cond))(no)

    def grads_out(s, begin):
        sl = lax.rem(s, NG)

        def local(d, slot):
            copy = keep(sl, d, slot, s)
            copy.start() if begin else copy.wait()

        def away(d, chip, slot):
            copy = give(sl, d, chip, slot, s)
            copy.start() if begin else copy.wait_send()

        @pl.when(c == 0)
        def _():
            local(0, 1)

        @pl.when(c == 1)
        def _():
            choose(member(s, FAR1), lambda: away(0, 3, 2), lambda: local(0, 1))
            local(1, 0)

        @pl.when(c == 2)
        def _():
            choose(member(s, ROUND), lambda: local(1, 0), lambda: away(1, 3, 0))
            choose(member(s, LAST2), lambda: away(0, 3, 1), lambda: local(0, 1))
            pl.when(member(s, ON2))(lambda: local(2, 2))
            if not begin:
                pl.when(jnp.logical_not(member(s, ON2)))(lambda: away(2, 0, 1))

        if not begin:
            @pl.when(c == 3)
            def _():
                away(3, 1, 0)
                pl.when(member(s, ROUND))(lambda: away(2, 2, 0))
                pl.when(member(s, MERGE))(lambda: away(2, 1, 1))
                pl.when(jnp.logical_not(member(s, LAST2)))(lambda: away(1, 2, 1))

    def put(s, sl):
        here, there = row_outputs(s, sl)
        for copy in here + there:
            copy.start()
        grads_out(s, True)

    def put_wait(s, sl):
        here, there = row_outputs(s, sl)
        for copy in here:
            copy.wait()
        for copy in there:
            copy.wait_send()

    def final_copies(kind, sl, s, chip):
        row = mine + s
        out = []
        for which, ref in ((0, dk), (1, dv)):
            for far, rows in ((0, pl.ds(128 * e, 128)), (1, pl.ds(128 - 128 * e, 128))):
                src, sem = fin.at[kind, sl, which, rows], fsem.at[kind, sl, 2 * which + far]
                if far:
                    out.append(remote(src, ref.at[row], sem, dsend_r.at[which], mate if chip is None else 2 * chip + 1 - e))
                elif chip is None:
                    out.append(pltpu.make_async_copy(src, ref.at[row], sem))
                else:
                    out.append(remote(src, ref.at[row], sem, down_r.at[which], dev(chip)))
        return out

    def final_wait(kind, sl, chip):
        for i, copy in enumerate(final_copies(kind, sl, 0, chip)):
            if chip is None and i % 2 == 0:
                copy.wait()
            else:
                copy.wait_send()

    def finalize(kind, group, s, value, chip):
        count = rank_in(s, group)
        sl = lax.rem(count, 2)
        pl.when(count >= 2)(lambda: final_wait(kind, sl, chip))
        fin[kind, sl, 0] = (value[:, :256] * scale).astype(jnp.bfloat16)
        fin[kind, sl, 1] = value[:, 256:].astype(jnp.bfloat16)
        for copy in final_copies(kind, sl, s, chip):
            copy.start()

    def final_drain(kind, group, chip):
        for n in range(max(0, len(group) - 2), len(group)):
            final_wait(kind, n % 2, chip)

    row_tok = lax.broadcasted_iota(jnp.int32, (1024, 128), 0) >> 3
    lane = lax.broadcasted_iota(jnp.int32, (1024, 128), 1)
    cs = scale * LOG2E
    lo_half, hi_half = slice(0, 128), slice(128, 256)

    def attend(s, slot):
        row = mine + s
        gslot = lax.rem(s, NG)
        piece = (e, 1 - e)
        for role in range(2):
            dq_row = docs[2 * c + piece[role], pl.ds(row, 1), :]
            d_t = jnp.transpose(jnp.broadcast_to(dq_row, (128, 128)))
            docr[role] = jnp.broadcast_to(d_t[:, None, :], (128, 8, 128)).reshape(1024, 128)

        def g_of(role):
            return qg[slot, 2 + role]

        def far_loop(body, down=False):
            for chip in range(1, 4):
                @pl.when(c == chip)
                def _():
                    for d in (range(chip, 0, -1) if down else range(1, chip + 1)):
                        body(d, d == chip)

        def scores(role, d, causal):
            sc = dot_nt(qg[slot, role], kvs[slot, d, 0]) * cs
            xs = []
            for j in range(2):
                dk_row = docs[2 * (c - d) + j, pl.ds(row, 1), :]
                vis = docr[role] == dk_row
                if causal:
                    vis = vis & (lane + 128 * j <= row_tok + 128 * piece[role])
                xs.append(jnp.where(vis, sc[:, 128 * j:128 * (j + 1)], NEG_BIG))
            top = jnp.maximum(xs[0], xs[1])
            es = [jnp.exp2(x - top) for x in xs]
            e_scr[d, role, :, lo_half] = es[0]
            e_scr[d, role, :, hi_half] = es[1]
            f_scr[d, role] = top
            l_scr[d, role] = es[0] + es[1]
            return top

        def dprob(role, d):
            dp_scr[d, role] = dot_nt(g_of(role), kvs[slot, d, 1])

        for role in range(2):
            t_scr[role] = scores(role, 0, True)

        def far_scores(d, x):
            for role in range(2):
                t_scr[role] = jnp.maximum(t_scr[role], scores(role, d, False))
            for role in range(2):
                dprob(role, d)
            return x
        far_loop(far_scores)

        for role in range(2):
            t_scr[role] = jnp.broadcast_to(jnp.max(t_scr[role], axis=1, keepdims=True), (1024, 128))
        dprob(0, 0)

        for role in range(2):
            top = t_scr[role]
            norm = l_scr[0, role] * jnp.exp2(f_scr[0, role] - top)
            for d in range(1, 4):
                norm = norm + l_scr[d, role] * jnp.exp2(f_scr[d, role] - top)
            t_scr[role] = top + jnp.log2(jnp.broadcast_to(jnp.sum(norm, axis=1, keepdims=True), (1024, 128)))
        dprob(1, 0)

        def weighted(role, d):
            f = jnp.exp2(f_scr[d, role] - t_scr[role])
            f_scr[d, role] = f
            for half in (lo_half, hi_half):
                p_scr[d, role, :, half] = (e_scr[d, role, :, half] * f).astype(jnp.bfloat16)
            return dot_nn(p_scr[d, role], kvs[slot, d, 1])

        def value_grads(d):
            dkv[gslot, d, :, 256:] = dot_tn(p_scr[d, 0], g_of(0)) + dot_tn(p_scr[d, 1], g_of(1))

        for role in range(2):
            o_acc[role] = weighted(role, 0)

        def far_weighted(d, x):
            for role in range(2):
                o_acc[role] = o_acc[role] + weighted(role, d)
            value_grads(d)
            return x
        far_loop(far_weighted)

        for role in range(2):
            o_low = o_acc[role].astype(jnp.bfloat16)
            outb[slot, role] = o_low
            delta = jnp.sum(g_of(role).astype(jnp.float32) * o_low.astype(jnp.float32), axis=1, keepdims=True)
            t_scr[role] = jnp.broadcast_to(delta, (1024, 128))
        value_grads(0)

        def score_grads(d):
            out = []
            for role in range(2):
                ds = [
                    (e_scr[d, role, :, half] * f_scr[d, role] * (dp_scr[d, role, :, half] - t_scr[role])).astype(jnp.bfloat16)
                    for half in (lo_half, hi_half)
                ]
                out.append(jnp.concatenate(ds, axis=1))
            dkv[gslot, d, :, :256] = dot_tn(out[0], qg[slot, 0]) + dot_tn(out[1], qg[slot, 1])
            return [dot_nn(ds, kvs[slot, d, 0]) for ds in out]

        def far_grads(d, farthest):
            got = score_grads(d)
            for role in range(2):
                o_acc[role] = got[role] if farthest else o_acc[role] + got[role]
            if farthest and d == 3:
                give(gslot, 3, 1, 0, s).start()
            if farthest and d == 2:
                pl.when(jnp.logical_not(member(s, ON2)))(lambda: give(gslot, 2, 0, 1, s).start())
        far_loop(far_grads, down=True)

        @pl.when(c == 0)
        def _():
            o_acc[...] = jnp.zeros_like(o_acc)
        got = score_grads(0)
        for role in range(2):
            o_acc[role] = o_acc[role] + got[role]
        for role in range(2):
            outb[slot, 2 + role] = (o_acc[role] * scale).astype(jnp.bfloat16)

    def part_wait(slot, s):
        remote(part.at[slot, s], part.at[slot, s], hop_s, part_r.at[slot, s], mate).wait_recv()

    def load(src, i):
        return [pltpu.make_async_copy(src.at[pl.ds(64 * n, 64)], sums.at[i, pl.ds(64 * n, 64)], lsem.at[i, n]) for n in range(4)]

    def start(copies):
        for copy in copies:
            copy.start()

    def finish(copies):
        for copy in copies:
            copy.wait()

    def passed(s, sl, chip, slot):
        return remote(sums.at[4 + sl], part.at[slot, s], xsem.at[sl], part_r.at[slot, s], dev(chip))

    def relay(s):
        return remote(part.at[2, s], part.at[1, s], rel_s.at[s], part_r.at[1, s], dev(1))

    def pass_on(i, group, held, slot_in, chip, slot_out):
        count = rank_in(i, group)
        sl = lax.rem(count, 2)
        start(load(hold.at[held, i], 0))
        part_wait(slot_in, i)
        start(load(part.at[slot_in, i], 1))
        pl.when(count >= 2)(lambda: passed(i, sl, chip, slot_out).wait_send())
        finish(load(hold.at[held, i], 0))
        finish(load(part.at[slot_in, i], 1))
        sums[4 + sl] = sums[0] + sums[1]
        passed(i, sl, chip, slot_out).start()

    def pass_x(i):
        pass_on(i, PASS_X, 0, 0, 0, 0)

    def pass_y(i):
        pass_on(i, ROUND, 0, 0, 0, 2)

    def total(kind, group, s, held, slots, chip):
        terms = [hold.at[held, s]] + [part.at[slot, s] for slot in slots]
        for slot in slots:
            part_wait(slot, s)
        for n, src in enumerate(terms):
            start(load(src, n))
        for n, src in enumerate(terms):
            finish(load(src, n))
        value = sums[0]
        for n in range(1, len(terms)):
            value = value + sums[n]
        finalize(kind, group, s, value, chip)

    for d in range(1, 4):
        f_scr[d] = jnp.full((2, 1024, 128), NEG_BIG, jnp.float32)
        l_scr[d] = jnp.zeros((2, 1024, 128), jnp.float32)
    by_way_of_3(VIA3[0])
    arrive(0)
    for j in VIA3[1:]:
        by_way_of_3(j)
    fetch(0, 0)

    def step(s, x):
        slot = lax.rem(s, 2)

        late = (c >= LATE_CHIP) & (s == 0)

        def ahead():
            arrive(s + 1)
            fetch(s + 1, 1 - slot)
        pl.when((s + 1 < NS) & jnp.logical_not(late))(ahead)

        @pl.when(s >= 2)
        def _():
            put_wait(s - 2, slot)

        @pl.when(s >= NG)
        def _():
            grads_out(s - NG, False)
        fetch_wait(s, slot)
        attend(s, slot)

        @pl.when(c == 3)
        def _():
            gslot = lax.rem(s, NG)
            pl.when(member(s, ROUND))(lambda: give(gslot, 2, 2, 0, s).start())

            @pl.when(member(s, MERGE))
            def _():
                part_wait(0, s)
                start(load(part.at[0, s], 0))
                finish(load(part.at[0, s], 0))
                dkv[gslot, 2] = dkv[gslot, 2] + sums[0]

            @pl.when(member(s, FAR1))
            def _():
                part_wait(0, s)
                start(load(part.at[0, s], 0))
                part_wait(2, s)
                start(load(part.at[2, s], 1))
                finish(load(part.at[0, s], 0))
                finish(load(part.at[2, s], 1))
                finalize(1, FAR1, s, dkv[gslot, 2] + sums[0] + sums[1], 1)
            finalize(0, OWN3, s, dkv[gslot, 0], None)
            pl.when(member(s, MERGE))(lambda: give(gslot, 2, 1, 1, s).start())

            def last_two():
                part_wait(1, s)
                start(load(part.at[1, s], 2))
                finish(load(part.at[1, s], 2))
                finalize(2, LAST2, s, dkv[gslot, 1] + sums[2], 2)
            choose(member(s, LAST2), last_two, lambda: give(gslot, 1, 2, 1, s).start())
        put(s, slot)
        for at, i in EARLY_X.items():
            pl.when((c == 1) & (s == at))(lambda: pass_x(i))
        for at, i in EARLY_Y.items():
            pl.when((c == 2) & (s == at))(lambda: pass_y(i))
        pl.when(late)(ahead)
        return x

    lax.fori_loop(0, NS, step, 0)
    put_wait(NS - 2, 0)
    put_wait(NS - 1, 1)
    for s in range(NS - NG, NS):
        grads_out(s, False)

    def home(i, x):
        def behind(lag, body):
            s = i - lag
            pl.when((s >= 0) & (s < NS))(lambda: body(s))

        @pl.when(c == 0)
        def _():
            @pl.when(member(i, ROUND))
            def _():
                part_wait(2, i)
                relay(i).start()
            pl.when(member(i, ON1))(lambda: pass_on(i, PASS_0, 1, 1, 1, 2))
            pl.when(member(i, ON2))(lambda: pass_on(i, PASS_0, 1, 0, 2, 2))
            behind(LAG[0], lambda s: pl.when(member(s, HERE0))(lambda: total(0, HERE0, s, 1, (1, 0), None)))

        @pl.when(c == 1)
        def _():
            later = tuple(s for s in PASS_X if s not in EARLY_X.values())
            pl.when(member(i, later))(lambda: pass_x(i))

            def body(s):
                pl.when(member(s, ON1))(lambda: total(1, ON1, s, 0, (0, 2), 0))
                pl.when(member(s, OWN1))(lambda: total(0, OWN1, s, 1, (1,), None))
            behind(LAG[1], body)

        @pl.when(c == 2)
        def _():
            later = tuple(s for s in ROUND if s not in EARLY_Y.values())
            pl.when(member(i, later))(lambda: pass_y(i))

            def body(s):
                pl.when(member(s, ON2))(lambda: total(1, ON2, s, 2, (2,), 0))
                pl.when(member(s, OWN2))(lambda: total(0, OWN2, s, 1, (1,), None))
            behind(LAG[2], body)
        return x

    @pl.when(c < 3)
    def _():
        lax.fori_loop(0, NS + max(LAG), home, 0)

    def down_wait(n):
        for which, ref in ((0, dk), (1, dv)):
            rows = ref.at[pl.ds(0, n)]
            remote(rows, rows, hop_s, down_r.at[which], mate).wait_recv()

    @pl.when(c == 0)
    def _():
        for s in ROUND:
            relay(s).wait_send()
        for sl in range(2):
            passed(0, sl, 1, 2).wait_send()
        sent = kvr.at[1, pl.ds(0, NS - len(VIA3))]
        remote(sent, sent, hop_s, kv_r.at[0, 0], mate).wait_send()
        final_drain(0, HERE0, None)
        down_wait(len(PASS_0))

    @pl.when(c == 1)
    def _():
        for sl in range(2):
            passed(0, sl, 0, 0).wait_send()
        remote(kvr.at[0], kvr.at[0], hop_s, kv_r.at[0, 0], mate).wait_send()
        final_drain(0, OWN1, None)
        final_drain(1, ON1, 0)
        down_wait(len(FAR1))

    @pl.when(c == 2)
    def _():
        for sl in range(2):
            passed(0, sl, 0, 2).wait_send()
        final_drain(0, OWN2, None)
        final_drain(1, ON2, 0)
        down_wait(len(LAST2))

    @pl.when(c == 3)
    def _():
        sent = kvr.at[1, pl.ds(0, len(VIA3))]
        remote(sent, sent, hop_s, kv_r.at[0, 0], mate).wait_send()
        final_drain(0, OWN3, None)
        final_drain(1, FAR1, 1)
        final_drain(2, LAST2, 2)
    for which, ref in ((0, k), (1, v)):
        some = ref.at[pl.ds(0, 2 * (NS - len(VIA3)))]
        for way, chips, sent in ((0, c < 3, ref), (1, c == 0, ref), (1, c == 1, some)):
            @pl.when(chips)
            def _():
                remote(sent, sent, kv_s.at[way, which], kv_r.at[0, 0], mate).wait_send()
        half = ref.at[pl.ds(other, NS)]
        remote(half, half, kv_s.at[2, which], kv_r.at[0, 0], mate).wait_send()
    for which, ref in ((0, q), (1, g)):
        half = ref.at[pl.ds(other, NS)]
        remote(half, half, q_s.at[which], q_r.at[0], mate).wait_send()
    for which, ref in ((0, o), (1, dq)):
        half = ref.at[pl.ds(other, NS)]
        remote(half, half, hop_s, osend_r.at[which], mate).wait_recv()
    for which, ref in ((0, dk), (1, dv)):
        half = ref.at[pl.ds(other, NS)]
        remote(half, half, hop_s, dsend_r.at[which], mate).wait_recv()


def place_kernel(slots, *refs):
    srcs, dsts, (buf, rsem, wsem) = refs[:4], refs[4:8], refs[8:]
    size = buf.shape[1]
    jobs = [(src.at[pl.ds(i, size)], dst.at[pl.ds(i, size)]) for src, dst in zip(srcs, dsts) for i in range(0, src.shape[0], size)]

    def read(j):
        return pltpu.make_async_copy(jobs[j][0], buf.at[j % slots], rsem.at[j % slots])

    def write(j):
        return pltpu.make_async_copy(buf.at[j % slots], jobs[j][1], wsem.at[j % slots])

    ahead = 10
    for j in range(min(ahead, len(jobs))):
        read(j).start()
    for j in range(len(jobs)):
        read(j).wait()
        write(j).start()
        if j + ahead < len(jobs):
            if j + ahead >= slots:
                write(j + ahead - slots).wait()
            read(j + ahead).start()
    for j in range(max(0, len(jobs) - slots), len(jobs)):
        write(j).wait()


ANY = pl.BlockSpec(memory_space=pl.ANY)
VMEM = pl.BlockSpec(memory_space=pltpu.VMEM)


def solution(mesh):
    n_dev = mesh.shape['cp']
    seq_spec = P('dp', 'cp', None, None)
    id_spec = P('dp', 'cp')
    bf, f32 = jnp.bfloat16, jnp.float32
    shape = jax.ShapeDtypeStruct
    dma = pltpu.SemaphoreType.DMA

    def per_device(query, keys, values, grad_out, doc_id):
        nb, piece, heads, hd = query.shape
        rows = piece * heads
        outs = pl.pallas_call(
            functools.partial(fused_kernel, hd ** -0.5),
            in_specs=[VMEM] + [ANY] * 4,
            out_specs=[ANY] * 8,
            out_shape=[
                shape((nb, rows, hd), bf), shape((nb, rows, hd), bf), shape((nb, piece, hd), bf), shape((nb, piece, hd), bf),
                shape((NS, 2, rows, hd), bf), shape((4, NS, 2, 256, 256), bf),
                shape((3, NS, 256, 512), f32), shape((3, NS, 256, 512), f32),
            ],
            scratch_shapes=[
                pltpu.VMEM((n_dev, nb, piece), jnp.int32), pltpu.VMEM((2, 4, 2, 256, 256), bf), pltpu.VMEM((2, 4, rows, hd), bf),
                pltpu.VMEM((2, 4, rows, hd), bf), pltpu.VMEM((NG, 4, 256, 512), f32), pltpu.VMEM((6, 256, 512), f32),
                pltpu.VMEM((3, 2, 2, 256, 256), bf),
                pltpu.VMEM((4, 2, rows, 256), f32), pltpu.VMEM((4, 2, rows, 256), f32), pltpu.VMEM((4, 2, rows, 256), bf),
                pltpu.VMEM((4, 2, rows, 128), f32), pltpu.VMEM((4, 2, rows, 128), f32), pltpu.VMEM((2, rows, 128), f32),
                pltpu.VMEM((2, rows, 128), jnp.int32), pltpu.VMEM((2, rows, hd), f32),
                dma((n_dev,)), dma((n_dev,)), dma((2, 10)), dma((2, 4)), dma((NG, 4)), dma((2,)), dma((2,)), dma((NJ,)), dma((3, 2)), dma((4, NJ)),
                dma, dma((3, NS)), dma((3, 2, 4)), dma((2,)), dma((3, 4)), dma((2,)), dma((NS,)), dma((2,)),
            ],
            compiler_params=pltpu.CompilerParams(has_side_effects=True, vmem_limit_bytes=62 * 1024 * 1024),
            name="attend",
        )(doc_id, query.reshape(nb, rows, hd), grad_out.reshape(nb, rows, hd), keys.reshape(nb, piece, hd), values.reshape(nb, piece, hd))
        outs = [x.reshape(-1, rows, hd) for x in outs[:4]]
        o, dq, dk, dv = pl.pallas_call(
            functools.partial(place_kernel, 14),
            in_specs=[ANY] * 4,
            out_specs=[ANY] * 4,
            out_shape=[shape(x.shape, bf) for x in outs],
            scratch_shapes=[pltpu.VMEM((14, 4, rows, hd), bf), dma((14,)), dma((14,))],
            compiler_params=pltpu.CompilerParams(vmem_limit_bytes=63 * 1024 * 1024),
            name="place",
        )(*outs)
        return o.reshape(query.shape), dq.reshape(query.shape), dk.reshape(keys.shape), dv.reshape(values.shape)

    return jax.shard_map(per_device, mesh=mesh, in_specs=(seq_spec, seq_spec, seq_spec, seq_spec, id_spec),
                         out_specs=(seq_spec, seq_spec, seq_spec, seq_spec), check_vma=False)
```

```python
import functools

import jax
import jax.numpy as jnp
from jax import lax
from jax.experimental import pallas as pl
from jax.experimental.pallas import tpu as pltpu
from jax.sharding import PartitionSpec as P

NEG_BIG = -1e30
LOG2E = 1.4426950408889634
NS = 16
NJ = NS
AHEAD = 2
NG = 4
PLAN1 = 'RMRMFRRRFRFRRMMM'
PLAN0 = 'NNANANCCNCNNCNNA'
LAST2 = (8, 9, 11)
EARLY_X = {5: 0, 7: 1, 10: 3, 12: 5, 13: 6, 14: 7, 15: 8}
EARLY_Y = {5: 0, 7: 2, 9: 5, 11: 6, 13: 7, 14: 9, 15: 11}
LAG = (2, 8, 7)
LATE_CHIP = 2
VIA3 = (0, 1)


def where_plan(plan, kinds):
    return tuple(s for s in range(NS) if plan[s] in kinds)


ROUND, MERGE, FAR1 = (where_plan(PLAN1, x) for x in 'RMF')
HERE0, ON1, ON2 = (where_plan(PLAN0, x) for x in 'NAC')
OWN1 = where_plan(PLAN1, 'RM')
OWN2 = tuple(s for s in range(NS) if s not in LAST2)
OWN3 = tuple(range(NS))
PASS_X = where_plan(PLAN0, 'NC')
PASS_0 = where_plan(PLAN0, 'AC')


def dot_nt(a, b):
    return lax.dot_general(a, b, (((1,), (1,)), ((), ())), preferred_element_type=jnp.float32)


def dot_nn(a, b):
    return lax.dot_general(a, b, (((1,), (0,)), ((), ())), preferred_element_type=jnp.float32)


def dot_tn(a, b):
    return lax.dot_general(a, b, (((0,), (0,)), ((), ())), preferred_element_type=jnp.float32)


def remote(src, dst, send, recv, dev):
    return pltpu.make_async_remote_copy(src_ref=src, dst_ref=dst, send_sem=send, recv_sem=recv,
                                        device_id={'cp': dev}, device_id_type=pl.DeviceIdType.MESH)


def fused_kernel(scale, doc, q, g, k, v, o, dq, dk, dv, qgm, kvr, part, hold,
                 docs, kvs, qg, outb, dkv, sums, fin, e_scr, dp_scr, p_scr, l_scr, f_scr, t_scr, docr, o_acc,
                 doc_s, doc_r, isem, osem, gsem, osend_r, q_s, q_r, kv_s, kv_r, hop_s, part_r, fsem, dsend_r, lsem, xsem, rel_s, down_r):
    rank = lax.axis_index('cp')
    n_dev = docs.shape[0]
    c = rank // 2
    e = lax.rem(rank, 2)
    mate = 2 * c + 1 - e
    other = NS * (1 - e)
    mine = NS * e

    def dev(chip):
        return 2 * chip + e

    docs[rank] = doc[...]

    def doc_copy(i):
        return remote(doc, docs.at[rank], doc_s.at[i], doc_r.at[i], lax.rem(rank + i, n_dev))

    for i in range(1, n_dev):
        doc_copy(i).start()

    def kv_parts(chip, way, j, cols):
        out = []
        for col in cols:
            for which, ref in ((0, k), (1, v)):
                out.append(remote(ref.at[pl.ds(col * NS + j, 1)], kvr.at[c, pl.ds(j, 1), which, pl.ds(128 * e, 128)],
                                  kv_s.at[way, which], kv_r.at[c, j], 2 * chip + col))
        return out

    def send_kv(chip, way, j):
        for copy in kv_parts(chip, way, j, (0, 1)):
            copy.start()

    def kv_forward(a, chip, j):
        return remote(kvr.at[a, pl.ds(j, 1)], kvr.at[a, pl.ds(j, 1)], hop_s, kv_r.at[a, j], dev(chip))

    def stream_kv(j):
        @pl.when(c == 0)
        def _():
            send_kv(1, 0, j)
            send_kv(2, 1, j)

        if not isinstance(j, int) or j not in VIA3:
            @pl.when(c == 1)
            def _():
                send_kv(0, 1, j)

        @pl.when(c == 2)
        def _():
            send_kv(3, 0, j)

    def to_mate(j):
        for which, ref in ((0, k), (1, v)):
            remote(ref.at[pl.ds(other + j, 1)], kvr.at[c, pl.ds(j, 1), which, pl.ds(128 * e, 128)],
                   kv_s.at[2, which], kv_r.at[c, j], mate).start()

    def rows_to_mate(j):
        for which, ref in ((0, q), (1, g)):
            remote(ref.at[pl.ds(other + j, 1)], qgm.at[pl.ds(j, 1), which], q_s.at[which], q_r.at[j], mate).start()

    stream_kv(0)

    @pl.when(c == 1)
    def _():
        send_kv(3, 0, 0)
    to_mate(0)
    rows_to_mate(0)
    for j in range(1, AHEAD):
        stream_kv(j)
    for j in range(1, NJ):
        to_mate(j)
        rows_to_mate(j)
    for i in range(1, n_dev):
        doc_copy(i).wait()

    def member(s, group):
        out = jnp.bool_(False)
        for one in group:
            out = out | (s == one)
        return out

    def by_way_of_3(j):
        @pl.when(c == 3)
        def _():
            kv_forward(1, 1, j).wait_recv()
            kv_forward(1, 2, j).start()

    def arrive(j):
        remote(kvr.at[c, pl.ds(j, 1), :, pl.ds(0, 128)], kvr.at[c, pl.ds(j, 1), :, pl.ds(0, 128)],
               hop_s, kv_r.at[c, j], mate).wait_recv()
        remote(qgm.at[pl.ds(j, 1)], qgm.at[pl.ds(j, 1)], hop_s, q_r.at[j], mate).wait_recv()
        for a in range(3):
            need = a < c
            if a == 1:
                need = need & jnp.logical_not((c == 3) & member(j, VIA3))

            @pl.when(need)
            def _():
                kv_forward(a, a, j).wait_recv()

        @pl.when(c == 1)
        def _():
            kv_forward(0, 3, j).start()

            @pl.when(j + 1 < NJ)
            def _():
                send_kv(3, 0, j + 1)

        @pl.when((c == 0) & jnp.logical_not(member(j, VIA3)))
        def _():
            kv_forward(1, 1, j).wait_recv()
            kv_forward(1, 2, j).start()

        @pl.when(j + AHEAD < NJ)
        def _():
            stream_kv(j + AHEAD)

    def inputs(s, sl):
        row = mine + s
        rows = pl.ds(128 * e, 128)
        rest = pl.ds(128 - 128 * e, 128)
        pairs = [
            (q.at[row], qg.at[sl, 0]), (g.at[row], qg.at[sl, 2]), (qgm.at[s, 0], qg.at[sl, 1]), (qgm.at[s, 1], qg.at[sl, 3]),
            (k.at[row], kvs.at[sl, 0, 0, rows]), (v.at[row], kvs.at[sl, 0, 1, rows]),
            (kvr.at[c, s, :, rest], kvs.at[sl, 0, :, rest]),
        ]
        return [pltpu.make_async_copy(src, dst, isem.at[sl, i]) for i, (src, dst) in enumerate(pairs)]

    def far_input(s, sl, d):
        return pltpu.make_async_copy(kvr.at[c - d, s], kvs.at[sl, d], isem.at[sl, 6 + d])

    def fetch(s, sl):
        for copy in inputs(s, sl):
            copy.start()
        for d in range(1, 4):
            @pl.when(d <= c)
            def _():
                far_input(s, sl, d).start()

    def fetch_wait(s, sl):
        for copy in inputs(s, sl):
            copy.wait()
        for d in range(1, 4):
            @pl.when(d <= c)
            def _():
                far_input(s, sl, d).wait()

    def row_outputs(s, sl):
        row = mine + s
        here = [pltpu.make_async_copy(outb.at[sl, 0], o.at[row], osem.at[sl, 0]),
                pltpu.make_async_copy(outb.at[sl, 2], dq.at[row], osem.at[sl, 1])]
        there = [remote(outb.at[sl, 1], o.at[row], osem.at[sl, 2], osend_r.at[0], mate),
                 remote(outb.at[sl, 3], dq.at[row], osem.at[sl, 3], osend_r.at[1], mate)]
        return here, there

    def keep(sl, d, slot, s):
        return pltpu.make_async_copy(dkv.at[sl, d], hold.at[slot, s], gsem.at[sl, d])

    def give(sl, d, chip, slot, s):
        return remote(dkv.at[sl, d], part.at[slot, s], gsem.at[sl, d], part_r.at[slot, s], dev(chip))

    def rank_in(s, group):
        count = jnp.int32(0)
        for one in group:
            count = count + jnp.where(one < s, 1, 0)
        return count

    def choose(cond, yes, no):
        pl.when(cond)(yes)
        pl.when(jnp.logical_not(cond))(no)

    def grads_out(s, begin):
        sl = lax.rem(s, NG)

        def local(d, slot):
            copy = keep(sl, d, slot, s)
            copy.start() if begin else copy.wait()

        def away(d, chip, slot):
            copy = give(sl, d, chip, slot, s)
            copy.start() if begin else copy.wait_send()

        @pl.when(c == 0)
        def _():
            local(0, 1)

        @pl.when(c == 1)
        def _():
            choose(member(s, FAR1), lambda: away(0, 3, 2), lambda: local(0, 1))
            local(1, 0)

        @pl.when(c == 2)
        def _():
            choose(member(s, ROUND), lambda: local(1, 0), lambda: away(1, 3, 0))
            choose(member(s, LAST2), lambda: away(0, 3, 1), lambda: local(0, 1))
            pl.when(member(s, ON2))(lambda: local(2, 2))
            if not begin:
                pl.when(jnp.logical_not(member(s, ON2)))(lambda: away(2, 0, 1))

        if not begin:
            @pl.when(c == 3)
            def _():
                away(3, 1, 0)
                pl.when(member(s, ROUND))(lambda: away(2, 2, 0))
                pl.when(member(s, MERGE))(lambda: away(2, 1, 1))
                pl.when(jnp.logical_not(member(s, LAST2)))(lambda: away(1, 2, 1))

    def put(s, sl):
        here, there = row_outputs(s, sl)
        for copy in here + there:
            copy.start()
        grads_out(s, True)

    def put_wait(s, sl):
        here, there = row_outputs(s, sl)
        for copy in here:
            copy.wait()
        for copy in there:
            copy.wait_send()

    def final_copies(kind, sl, s, chip):
        row = mine + s
        out = []
        for which, ref in ((0, dk), (1, dv)):
            for far, rows in ((0, pl.ds(128 * e, 128)), (1, pl.ds(128 - 128 * e, 128))):
                src, sem = fin.at[kind, sl, which, rows], fsem.at[kind, sl, 2 * which + far]
                if far:
                    out.append(remote(src, ref.at[row], sem, dsend_r.at[which], mate if chip is None else 2 * chip + 1 - e))
                elif chip is None:
                    out.append(pltpu.make_async_copy(src, ref.at[row], sem))
                else:
                    out.append(remote(src, ref.at[row], sem, down_r.at[which], dev(chip)))
        return out

    def final_wait(kind, sl, chip):
        for i, copy in enumerate(final_copies(kind, sl, 0, chip)):
            if chip is None and i % 2 == 0:
                copy.wait()
            else:
                copy.wait_send()

    def finalize(kind, group, s, value, chip):
        count = rank_in(s, group)
        sl = lax.rem(count, 2)
        pl.when(count >= 2)(lambda: final_wait(kind, sl, chip))
        fin[kind, sl, 0] = (value[:, :256] * scale).astype(jnp.bfloat16)
        fin[kind, sl, 1] = value[:, 256:].astype(jnp.bfloat16)
        for copy in final_copies(kind, sl, s, chip):
            copy.start()

    def final_drain(kind, group, chip):
        for n in range(max(0, len(group) - 2), len(group)):
            final_wait(kind, n % 2, chip)

    row_tok = lax.broadcasted_iota(jnp.int32, (1024, 128), 0) >> 3
    lane = lax.broadcasted_iota(jnp.int32, (1024, 128), 1)
    cs = scale * LOG2E
    lo_half, hi_half = slice(0, 128), slice(128, 256)

    def attend(s, slot):
        row = mine + s
        gslot = lax.rem(s, NG)
        piece = (e, 1 - e)
        for role in range(2):
            dq_row = docs[2 * c + piece[role], pl.ds(row, 1), :]
            d_t = jnp.transpose(jnp.broadcast_to(dq_row, (128, 128)))
            docr[role] = jnp.broadcast_to(d_t[:, None, :], (128, 8, 128)).reshape(1024, 128)

        def g_of(role):
            return qg[slot, 2 + role]

        def far_loop(body, down=False):
            for chip in range(1, 4):
                @pl.when(c == chip)
                def _():
                    for d in (range(chip, 0, -1) if down else range(1, chip + 1)):
                        body(d, d == chip)

        def scores(role, d, causal):
            sc = dot_nt(qg[slot, role], kvs[slot, d, 0]) * cs
            xs = []
            for j in range(2):
                dk_row = docs[2 * (c - d) + j, pl.ds(row, 1), :]
                vis = docr[role] == dk_row
                if causal:
                    vis = vis & (lane + 128 * j <= row_tok + 128 * piece[role])
                xs.append(jnp.where(vis, sc[:, 128 * j:128 * (j + 1)], NEG_BIG))
            top = jnp.maximum(xs[0], xs[1])
            es = [jnp.exp2(x - top) for x in xs]
            e_scr[d, role, :, lo_half] = es[0]
            e_scr[d, role, :, hi_half] = es[1]
            f_scr[d, role] = top
            l_scr[d, role] = es[0] + es[1]
            return top

        def dprob(role, d):
            dp_scr[d, role] = dot_nt(g_of(role), kvs[slot, d, 1])

        for role in range(2):
            t_scr[role] = scores(role, 0, True)

        def far_scores(d, x):
            for role in range(2):
                t_scr[role] = jnp.maximum(t_scr[role], scores(role, d, False))
            for role in range(2):
                dprob(role, d)
            return x
        far_loop(far_scores)

        for role in range(2):
            t_scr[role] = jnp.broadcast_to(jnp.max(t_scr[role], axis=1, keepdims=True), (1024, 128))
        dprob(0, 0)

        for role in range(2):
            top = t_scr[role]
            norm = l_scr[0, role] * jnp.exp2(f_scr[0, role] - top)
            for d in range(1, 4):
                norm = norm + l_scr[d, role] * jnp.exp2(f_scr[d, role] - top)
            t_scr[role] = top + jnp.log2(jnp.broadcast_to(jnp.sum(norm, axis=1, keepdims=True), (1024, 128)))
        dprob(1, 0)

        def weighted(role, d):
            f = jnp.exp2(f_scr[d, role] - t_scr[role])
            f_scr[d, role] = f
            for half in (lo_half, hi_half):
                p_scr[d, role, :, half] = (e_scr[d, role, :, half] * f).astype(jnp.bfloat16)
            return dot_nn(p_scr[d, role], kvs[slot, d, 1])

        def value_grads(d):
            dkv[gslot, d, :, 256:] = dot_tn(p_scr[d, 0], g_of(0)) + dot_tn(p_scr[d, 1], g_of(1))

        for role in range(2):
            o_acc[role] = weighted(role, 0)

        def far_weighted(d, x):
            for role in range(2):
                o_acc[role] = o_acc[role] + weighted(role, d)
            value_grads(d)
            return x
        far_loop(far_weighted)

        for role in range(2):
            o_low = o_acc[role].astype(jnp.bfloat16)
            outb[slot, role] = o_low
            delta = jnp.sum(g_of(role).astype(jnp.float32) * o_low.astype(jnp.float32), axis=1, keepdims=True)
            t_scr[role] = jnp.broadcast_to(delta, (1024, 128))
        value_grads(0)

        def score_grads(d):
            out = []
            for role in range(2):
                ds = [
                    (e_scr[d, role, :, half] * f_scr[d, role] * (dp_scr[d, role, :, half] - t_scr[role])).astype(jnp.bfloat16)
                    for half in (lo_half, hi_half)
                ]
                out.append(jnp.concatenate(ds, axis=1))
            dkv[gslot, d, :, :256] = dot_tn(out[0], qg[slot, 0]) + dot_tn(out[1], qg[slot, 1])
            return [dot_nn(ds, kvs[slot, d, 0]) for ds in out]

        def far_grads(d, farthest):
            got = score_grads(d)
            for role in range(2):
                o_acc[role] = got[role] if farthest else o_acc[role] + got[role]
            if farthest and d == 3:
                give(gslot, 3, 1, 0, s).start()
            if farthest and d == 2:
                pl.when(jnp.logical_not(member(s, ON2)))(lambda: give(gslot, 2, 0, 1, s).start())
        far_loop(far_grads, down=True)

        @pl.when(c == 0)
        def _():
            o_acc[...] = jnp.zeros_like(o_acc)
        got = score_grads(0)
        for role in range(2):
            o_acc[role] = o_acc[role] + got[role]
        for role in range(2):
            outb[slot, 2 + role] = (o_acc[role] * scale).astype(jnp.bfloat16)

    def part_wait(slot, s):
        remote(part.at[slot, s], part.at[slot, s], hop_s, part_r.at[slot, s], mate).wait_recv()

    def load(src, i):
        return [pltpu.make_async_copy(src.at[pl.ds(64 * n, 64)], sums.at[i, pl.ds(64 * n, 64)], lsem.at[i, n]) for n in range(4)]

    def start(copies):
        for copy in copies:
            copy.start()

    def finish(copies):
        for copy in copies:
            copy.wait()

    def passed(s, sl, chip, slot):
        return remote(sums.at[4 + sl], part.at[slot, s], xsem.at[sl], part_r.at[slot, s], dev(chip))

    def relay(s):
        return remote(part.at[2, s], part.at[1, s], rel_s.at[s], part_r.at[1, s], dev(1))

    def pass_on(i, group, held, slot_in, chip, slot_out):
        count = rank_in(i, group)
        sl = lax.rem(count, 2)
        start(load(hold.at[held, i], 0))
        part_wait(slot_in, i)
        start(load(part.at[slot_in, i], 1))
        pl.when(count >= 2)(lambda: passed(i, sl, chip, slot_out).wait_send())
        finish(load(hold.at[held, i], 0))
        finish(load(part.at[slot_in, i], 1))
        sums[4 + sl] = sums[0] + sums[1]
        passed(i, sl, chip, slot_out).start()

    def pass_x(i):
        pass_on(i, PASS_X, 0, 0, 0, 0)

    def pass_y(i):
        pass_on(i, ROUND, 0, 0, 0, 2)

    def total(kind, group, s, held, slots, chip):
        terms = [hold.at[held, s]] + [part.at[slot, s] for slot in slots]
        for slot in slots:
            part_wait(slot, s)
        for n, src in enumerate(terms):
            start(load(src, n))
        for n, src in enumerate(terms):
            finish(load(src, n))
        value = sums[0]
        for n in range(1, len(terms)):
            value = value + sums[n]
        finalize(kind, group, s, value, chip)

    for d in range(1, 4):
        f_scr[d] = jnp.full((2, 1024, 128), NEG_BIG, jnp.float32)
        l_scr[d] = jnp.zeros((2, 1024, 128), jnp.float32)
    by_way_of_3(VIA3[0])
    arrive(0)
    for j in VIA3[1:]:
        by_way_of_3(j)
    fetch(0, 0)

    def step(s, x):
        slot = lax.rem(s, 2)

        late = (c >= LATE_CHIP) & (s == 0)

        def ahead():
            arrive(s + 1)
            fetch(s + 1, 1 - slot)
        pl.when((s + 1 < NS) & jnp.logical_not(late))(ahead)

        @pl.when(s >= 2)
        def _():
            put_wait(s - 2, slot)

        @pl.when(s >= NG)
        def _():
            grads_out(s - NG, False)
        fetch_wait(s, slot)
        attend(s, slot)

        @pl.when(c == 3)
        def _():
            gslot = lax.rem(s, NG)
            pl.when(member(s, ROUND))(lambda: give(gslot, 2, 2, 0, s).start())

            @pl.when(member(s, MERGE))
            def _():
                part_wait(0, s)
                start(load(part.at[0, s], 0))
                finish(load(part.at[0, s], 0))
                dkv[gslot, 2] = dkv[gslot, 2] + sums[0]

            @pl.when(member(s, FAR1))
            def _():
                part_wait(0, s)
                start(load(part.at[0, s], 0))
                part_wait(2, s)
                start(load(part.at[2, s], 1))
                finish(load(part.at[0, s], 0))
                finish(load(part.at[2, s], 1))
                finalize(1, FAR1, s, dkv[gslot, 2] + sums[0] + sums[1], 1)
            finalize(0, OWN3, s, dkv[gslot, 0], None)
            pl.when(member(s, MERGE))(lambda: give(gslot, 2, 1, 1, s).start())

            def last_two():
                part_wait(1, s)
                start(load(part.at[1, s], 2))
                finish(load(part.at[1, s], 2))
                finalize(2, LAST2, s, dkv[gslot, 1] + sums[2], 2)
            choose(member(s, LAST2), last_two, lambda: give(gslot, 1, 2, 1, s).start())
        put(s, slot)
        for at, i in EARLY_X.items():
            pl.when((c == 1) & (s == at))(lambda: pass_x(i))
        for at, i in EARLY_Y.items():
            pl.when((c == 2) & (s == at))(lambda: pass_y(i))
        pl.when(late)(ahead)
        return x

    lax.fori_loop(0, NS, step, 0)
    put_wait(NS - 2, 0)
    put_wait(NS - 1, 1)
    for s in range(NS - NG, NS):
        grads_out(s, False)

    def home(i, x):
        def behind(lag, body):
            s = i - lag
            pl.when((s >= 0) & (s < NS))(lambda: body(s))

        @pl.when(c == 0)
        def _():
            @pl.when(member(i, ROUND))
            def _():
                part_wait(2, i)
                relay(i).start()
            pl.when(member(i, ON1))(lambda: pass_on(i, PASS_0, 1, 1, 1, 2))
            pl.when(member(i, ON2))(lambda: pass_on(i, PASS_0, 1, 0, 2, 2))
            behind(LAG[0], lambda s: pl.when(member(s, HERE0))(lambda: total(0, HERE0, s, 1, (1, 0), None)))

        @pl.when(c == 1)
        def _():
            later = tuple(s for s in PASS_X if s not in EARLY_X.values())
            pl.when(member(i, later))(lambda: pass_x(i))

            def body(s):
                pl.when(member(s, ON1))(lambda: total(1, ON1, s, 0, (0, 2), 0))
                pl.when(member(s, OWN1))(lambda: total(0, OWN1, s, 1, (1,), None))
            behind(LAG[1], body)

        @pl.when(c == 2)
        def _():
            later = tuple(s for s in ROUND if s not in EARLY_Y.values())
            pl.when(member(i, later))(lambda: pass_y(i))

            def body(s):
                pl.when(member(s, ON2))(lambda: total(1, ON2, s, 2, (2,), 0))
                pl.when(member(s, OWN2))(lambda: total(0, OWN2, s, 1, (1,), None))
            behind(LAG[2], body)
        return x

    @pl.when(c < 3)
    def _():
        lax.fori_loop(0, NS + max(LAG), home, 0)

    def down_wait(n):
        for which, ref in ((0, dk), (1, dv)):
            rows = ref.at[pl.ds(0, n)]
            remote(rows, rows, hop_s, down_r.at[which], mate).wait_recv()

    @pl.when(c == 0)
    def _():
        for s in ROUND:
            relay(s).wait_send()
        for sl in range(2):
            passed(0, sl, 1, 2).wait_send()
        sent = kvr.at[1, pl.ds(0, NS - len(VIA3))]
        remote(sent, sent, hop_s, kv_r.at[0, 0], mate).wait_send()
        final_drain(0, HERE0, None)
        down_wait(len(PASS_0))

    @pl.when(c == 1)
    def _():
        for sl in range(2):
            passed(0, sl, 0, 0).wait_send()
        remote(kvr.at[0], kvr.at[0], hop_s, kv_r.at[0, 0], mate).wait_send()
        final_drain(0, OWN1, None)
        final_drain(1, ON1, 0)
        down_wait(len(FAR1))

    @pl.when(c == 2)
    def _():
        for sl in range(2):
            passed(0, sl, 0, 2).wait_send()
        final_drain(0, OWN2, None)
        final_drain(1, ON2, 0)
        down_wait(len(LAST2))

    @pl.when(c == 3)
    def _():
        sent = kvr.at[1, pl.ds(0, len(VIA3))]
        remote(sent, sent, hop_s, kv_r.at[0, 0], mate).wait_send()
        final_drain(0, OWN3, None)
        final_drain(1, FAR1, 1)
        final_drain(2, LAST2, 2)
    for which, ref in ((0, k), (1, v)):
        some = ref.at[pl.ds(0, 2 * (NS - len(VIA3)))]
        for way, chips, sent in ((0, c < 3, ref), (1, c == 0, ref), (1, c == 1, some)):
            @pl.when(chips)
            def _():
                remote(sent, sent, kv_s.at[way, which], kv_r.at[0, 0], mate).wait_send()
        half = ref.at[pl.ds(other, NS)]
        remote(half, half, kv_s.at[2, which], kv_r.at[0, 0], mate).wait_send()
    for which, ref in ((0, q), (1, g)):
        half = ref.at[pl.ds(other, NS)]
        remote(half, half, q_s.at[which], q_r.at[0], mate).wait_send()
    for which, ref in ((0, o), (1, dq)):
        half = ref.at[pl.ds(other, NS)]
        remote(half, half, hop_s, osend_r.at[which], mate).wait_recv()
    for which, ref in ((0, dk), (1, dv)):
        half = ref.at[pl.ds(other, NS)]
        remote(half, half, hop_s, dsend_r.at[which], mate).wait_recv()


def place_kernel(slots, *refs):
    srcs, dsts, (buf, rsem, wsem) = refs[:4], refs[4:8], refs[8:]
    size = buf.shape[1]
    jobs = [(src.at[pl.ds(i, size)], dst.at[pl.ds(i, size)]) for src, dst in zip(srcs, dsts) for i in range(0, src.shape[0], size)]

    def read(j):
        return pltpu.make_async_copy(jobs[j][0], buf.at[j % slots], rsem.at[j % slots])

    def write(j):
        return pltpu.make_async_copy(buf.at[j % slots], jobs[j][1], wsem.at[j % slots])

    ahead = 10
    for j in range(min(ahead, len(jobs))):
        read(j).start()
    for j in range(len(jobs)):
        read(j).wait()
        write(j).start()
        if j + ahead < len(jobs):
            if j + ahead >= slots:
                write(j + ahead - slots).wait()
            read(j + ahead).start()
    for j in range(max(0, len(jobs) - slots), len(jobs)):
        write(j).wait()


ANY = pl.BlockSpec(memory_space=pl.ANY)
VMEM = pl.BlockSpec(memory_space=pltpu.VMEM)


def solution(mesh):
    n_dev = mesh.shape['cp']
    seq_spec = P('dp', 'cp', None, None)
    id_spec = P('dp', 'cp')
    bf, f32 = jnp.bfloat16, jnp.float32
    shape = jax.ShapeDtypeStruct
    dma = pltpu.SemaphoreType.DMA

    def per_device(query, keys, values, grad_out, doc_id):
        nb, piece, heads, hd = query.shape
        rows = piece * heads
        outs = pl.pallas_call(
            functools.partial(fused_kernel, hd ** -0.5),
            in_specs=[VMEM] + [ANY] * 4,
            out_specs=[ANY] * 8,
            out_shape=[
                shape((nb, rows, hd), bf), shape((nb, rows, hd), bf), shape((nb, piece, hd), bf), shape((nb, piece, hd), bf),
                shape((NS, 2, rows, hd), bf), shape((4, NS, 2, 256, 256), bf),
                shape((3, NS, 256, 512), f32), shape((3, NS, 256, 512), f32),
            ],
            scratch_shapes=[
                pltpu.VMEM((n_dev, nb, piece), jnp.int32), pltpu.VMEM((2, 4, 2, 256, 256), bf), pltpu.VMEM((2, 4, rows, hd), bf),
                pltpu.VMEM((2, 4, rows, hd), bf), pltpu.VMEM((NG, 4, 256, 512), f32), pltpu.VMEM((6, 256, 512), f32),
                pltpu.VMEM((3, 2, 2, 256, 256), bf),
                pltpu.VMEM((4, 2, rows, 256), f32), pltpu.VMEM((4, 2, rows, 256), f32), pltpu.VMEM((4, 2, rows, 256), bf),
                pltpu.VMEM((4, 2, rows, 128), f32), pltpu.VMEM((4, 2, rows, 128), f32), pltpu.VMEM((2, rows, 128), f32),
                pltpu.VMEM((2, rows, 128), jnp.int32), pltpu.VMEM((2, rows, hd), f32),
                dma((n_dev,)), dma((n_dev,)), dma((2, 10)), dma((2, 4)), dma((NG, 4)), dma((2,)), dma((2,)), dma((NJ,)), dma((3, 2)), dma((4, NJ)),
                dma, dma((3, NS)), dma((3, 2, 4)), dma((2,)), dma((3, 4)), dma((2,)), dma((NS,)), dma((2,)),
            ],
            compiler_params=pltpu.CompilerParams(has_side_effects=True, vmem_limit_bytes=62 * 1024 * 1024),
            name="attend",
        )(doc_id, query.reshape(nb, rows, hd), grad_out.reshape(nb, rows, hd), keys.reshape(nb, piece, hd), values.reshape(nb, piece, hd))
        outs = [x.reshape(-1, rows, hd) for x in outs[:4]]
        o, dq, dk, dv = pl.pallas_call(
            functools.partial(place_kernel, 14),
            in_specs=[ANY] * 4,
            out_specs=[ANY] * 4,
            out_shape=[shape(x.shape, bf) for x in outs],
            scratch_shapes=[pltpu.VMEM((14, 4, rows, hd), bf), dma((14,)), dma((14,))],
            compiler_params=pltpu.CompilerParams(vmem_limit_bytes=63 * 1024 * 1024),
            name="place",
        )(*outs)
        return o.reshape(query.shape), dq.reshape(query.shape), dk.reshape(keys.shape), dv.reshape(values.shape)

    return jax.shard_map(per_device, mesh=mesh, in_specs=(seq_spec, seq_spec, seq_spec, seq_spec, id_spec),
                         out_specs=(seq_spec, seq_spec, seq_spec, seq_spec), check_vma=False)
```

```python
import functools

import jax
import jax.numpy as jnp
from jax import lax
from jax.experimental import pallas as pl
from jax.experimental.pallas import tpu as pltpu
from jax.sharding import PartitionSpec as P

NEG_BIG = -1e30
LOG2E = 1.4426950408889634
NS = 16
NJ = NS
AHEAD = 2
NG = 4
PLAN1 = 'RRRMFMRRFRFRRMMM'
PLAN0 = 'NNANANCCNCNNCNNA'
LAST2 = (8, 9, 11)
EARLY_X = {6: 0, 8: 1, 10: 3, 12: 5, 13: 6, 14: 7}
EARLY_Y = {5: 0, 7: 1, 9: 2, 10: 6, 13: 7, 14: 9, 15: 11}
LAG = (6, 8, 7)
LATE_CHIP = 2
VIA3 = (0, 1)


def where_plan(plan, kinds):
    return tuple(s for s in range(NS) if plan[s] in kinds)


ROUND, MERGE, FAR1 = (where_plan(PLAN1, x) for x in 'RMF')
HERE0, ON1, ON2 = (where_plan(PLAN0, x) for x in 'NAC')
OWN1 = where_plan(PLAN1, 'RM')
OWN2 = tuple(s for s in range(NS) if s not in LAST2)
OWN3 = tuple(range(NS))
PASS_X = where_plan(PLAN0, 'NC')
PASS_0 = where_plan(PLAN0, 'AC')


def dot_nt(a, b):
    return lax.dot_general(a, b, (((1,), (1,)), ((), ())), preferred_element_type=jnp.float32)


def dot_nn(a, b):
    return lax.dot_general(a, b, (((1,), (0,)), ((), ())), preferred_element_type=jnp.float32)


def dot_tn(a, b):
    return lax.dot_general(a, b, (((0,), (0,)), ((), ())), preferred_element_type=jnp.float32)


def remote(src, dst, send, recv, dev):
    return pltpu.make_async_remote_copy(src_ref=src, dst_ref=dst, send_sem=send, recv_sem=recv,
                                        device_id={'cp': dev}, device_id_type=pl.DeviceIdType.MESH)


def fused_kernel(scale, doc, q, g, k, v, o, dq, dk, dv, qgm, kvr, part, hold,
                 docs, kvs, qg, outb, dkv, sums, fin, e_scr, dp_scr, p_scr, l_scr, f_scr, t_scr, docr, o_acc,
                 doc_s, doc_r, isem, osem, gsem, osend_r, q_s, q_r, kv_s, kv_r, hop_s, part_r, fsem, dsend_r, lsem, xsem, rel_s, down_r):
    rank = lax.axis_index('cp')
    n_dev = docs.shape[0]
    c = rank // 2
    e = lax.rem(rank, 2)
    mate = 2 * c + 1 - e
    other = NS * (1 - e)
    mine = NS * e

    def dev(chip):
        return 2 * chip + e

    docs[rank] = doc[...]

    def doc_copy(i):
        return remote(doc, docs.at[rank], doc_s.at[i], doc_r.at[i], lax.rem(rank + i, n_dev))

    for i in range(1, n_dev):
        doc_copy(i).start()

    def kv_parts(chip, way, j, cols):
        out = []
        for col in cols:
            for which, ref in ((0, k), (1, v)):
                out.append(remote(ref.at[pl.ds(col * NS + j, 1)], kvr.at[c, pl.ds(j, 1), which, pl.ds(128 * e, 128)],
                                  kv_s.at[way, which], kv_r.at[c, j], 2 * chip + col))
        return out

    def send_kv(chip, way, j):
        for copy in kv_parts(chip, way, j, (0, 1)):
            copy.start()

    def kv_forward(a, chip, j):
        return remote(kvr.at[a, pl.ds(j, 1)], kvr.at[a, pl.ds(j, 1)], hop_s, kv_r.at[a, j], dev(chip))

    def stream_kv(j):
        @pl.when(c == 0)
        def _():
            send_kv(1, 0, j)
            send_kv(2, 1, j)

        if not isinstance(j, int) or j not in VIA3:
            @pl.when(c == 1)
            def _():
                send_kv(0, 1, j)

        @pl.when(c == 2)
        def _():
            send_kv(3, 0, j)

    def to_mate(j):
        for which, ref in ((0, k), (1, v)):
            remote(ref.at[pl.ds(other + j, 1)], kvr.at[c, pl.ds(j, 1), which, pl.ds(128 * e, 128)],
                   kv_s.at[2, which], kv_r.at[c, j], mate).start()

    def rows_to_mate(j):
        for which, ref in ((0, q), (1, g)):
            remote(ref.at[pl.ds(other + j, 1)], qgm.at[pl.ds(j, 1), which], q_s.at[which], q_r.at[j], mate).start()

    stream_kv(0)

    @pl.when(c == 1)
    def _():
        send_kv(3, 0, 0)
    to_mate(0)
    rows_to_mate(0)
    for j in range(1, AHEAD):
        stream_kv(j)
    for j in range(1, NJ):
        to_mate(j)
        rows_to_mate(j)
    for i in range(1, n_dev):
        doc_copy(i).wait()

    def member(s, group):
        out = jnp.bool_(False)
        for one in group:
            out = out | (s == one)
        return out

    def by_way_of_3(j):
        @pl.when(c == 3)
        def _():
            kv_forward(1, 1, j).wait_recv()
            kv_forward(1, 2, j).start()

    def arrive(j):
        remote(kvr.at[c, pl.ds(j, 1), :, pl.ds(0, 128)], kvr.at[c, pl.ds(j, 1), :, pl.ds(0, 128)],
               hop_s, kv_r.at[c, j], mate).wait_recv()
        remote(qgm.at[pl.ds(j, 1)], qgm.at[pl.ds(j, 1)], hop_s, q_r.at[j], mate).wait_recv()
        for a in range(3):
            need = a < c
            if a == 1:
                need = need & jnp.logical_not((c == 3) & member(j, VIA3))

            @pl.when(need)
            def _():
                kv_forward(a, a, j).wait_recv()

        @pl.when(c == 1)
        def _():
            kv_forward(0, 3, j).start()

            @pl.when(j + 1 < NJ)
            def _():
                send_kv(3, 0, j + 1)

        @pl.when((c == 0) & jnp.logical_not(member(j, VIA3)))
        def _():
            kv_forward(1, 1, j).wait_recv()
            kv_forward(1, 2, j).start()

        @pl.when(j + AHEAD < NJ)
        def _():
            stream_kv(j + AHEAD)

    def inputs(s, sl):
        row = mine + s
        rows = pl.ds(128 * e, 128)
        rest = pl.ds(128 - 128 * e, 128)
        pairs = [
            (q.at[row], qg.at[sl, 0]), (g.at[row], qg.at[sl, 2]), (qgm.at[s, 0], qg.at[sl, 1]), (qgm.at[s, 1], qg.at[sl, 3]),
            (k.at[row], kvs.at[sl, 0, 0, rows]), (v.at[row], kvs.at[sl, 0, 1, rows]),
            (kvr.at[c, s, :, rest], kvs.at[sl, 0, :, rest]),
        ]
        return [pltpu.make_async_copy(src, dst, isem.at[sl, i]) for i, (src, dst) in enumerate(pairs)]

    def far_input(s, sl, d):
        return pltpu.make_async_copy(kvr.at[c - d, s], kvs.at[sl, d], isem.at[sl, 6 + d])

    def fetch(s, sl):
        for copy in inputs(s, sl):
            copy.start()
        for d in range(1, 4):
            @pl.when(d <= c)
            def _():
                far_input(s, sl, d).start()

    def fetch_wait(s, sl):
        for copy in inputs(s, sl):
            copy.wait()
        for d in range(1, 4):
            @pl.when(d <= c)
            def _():
                far_input(s, sl, d).wait()

    def row_outputs(s, sl):
        row = mine + s
        here = [pltpu.make_async_copy(outb.at[sl, 0], o.at[row], osem.at[sl, 0]),
                pltpu.make_async_copy(outb.at[sl, 2], dq.at[row], osem.at[sl, 1])]
        there = [remote(outb.at[sl, 1], o.at[row], osem.at[sl, 2], osend_r.at[0], mate),
                 remote(outb.at[sl, 3], dq.at[row], osem.at[sl, 3], osend_r.at[1], mate)]
        return here, there

    def keep(sl, d, slot, s):
        return pltpu.make_async_copy(dkv.at[sl, d], hold.at[slot, s], gsem.at[sl, d])

    def give(sl, d, chip, slot, s):
        return remote(dkv.at[sl, d], part.at[slot, s], gsem.at[sl, d], part_r.at[slot, s], dev(chip))

    def rank_in(s, group):
        count = jnp.int32(0)
        for one in group:
            count = count + jnp.where(one < s, 1, 0)
        return count

    def choose(cond, yes, no):
        pl.when(cond)(yes)
        pl.when(jnp.logical_not(cond))(no)

    def grads_out(s, begin):
        sl = lax.rem(s, NG)

        def local(d, slot):
            copy = keep(sl, d, slot, s)
            copy.start() if begin else copy.wait()

        def away(d, chip, slot):
            copy = give(sl, d, chip, slot, s)
            copy.start() if begin else copy.wait_send()

        @pl.when(c == 0)
        def _():
            local(0, 1)

        @pl.when(c == 1)
        def _():
            choose(member(s, FAR1), lambda: away(0, 3, 2), lambda: local(0, 1))
            local(1, 0)

        @pl.when(c == 2)
        def _():
            choose(member(s, ROUND), lambda: local(1, 0), lambda: away(1, 3, 0))
            choose(member(s, LAST2), lambda: away(0, 3, 1), lambda: local(0, 1))
            pl.when(member(s, ON2))(lambda: local(2, 2))
            if not begin:
                pl.when(jnp.logical_not(member(s, ON2)))(lambda: away(2, 0, 1))

        if not begin:
            @pl.when(c == 3)
            def _():
                away(3, 1, 0)
                pl.when(member(s, ROUND))(lambda: away(2, 2, 0))
                pl.when(member(s, MERGE))(lambda: away(2, 1, 1))
                pl.when(jnp.logical_not(member(s, LAST2)))(lambda: away(1, 2, 1))

    def put(s, sl):
        here, there = row_outputs(s, sl)
        for copy in here + there:
            copy.start()
        grads_out(s, True)

    def put_wait(s, sl):
        here, there = row_outputs(s, sl)
        for copy in here:
            copy.wait()
        for copy in there:
            copy.wait_send()

    def final_copies(kind, sl, s, chip):
        row = mine + s
        out = []
        for which, ref in ((0, dk), (1, dv)):
            for far, rows in ((0, pl.ds(128 * e, 128)), (1, pl.ds(128 - 128 * e, 128))):
                src, sem = fin.at[kind, sl, which, rows], fsem.at[kind, sl, 2 * which + far]
                if far:
                    out.append(remote(src, ref.at[row], sem, dsend_r.at[which], mate if chip is None else 2 * chip + 1 - e))
                elif chip is None:
                    out.append(pltpu.make_async_copy(src, ref.at[row], sem))
                else:
                    out.append(remote(src, ref.at[row], sem, down_r.at[which], dev(chip)))
        return out

    def final_wait(kind, sl, chip):
        for i, copy in enumerate(final_copies(kind, sl, 0, chip)):
            if chip is None and i % 2 == 0:
                copy.wait()
            else:
                copy.wait_send()

    def finalize(kind, group, s, value, chip):
        count = rank_in(s, group)
        sl = lax.rem(count, 2)
        pl.when(count >= 2)(lambda: final_wait(kind, sl, chip))
        fin[kind, sl, 0] = (value[:, :256] * scale).astype(jnp.bfloat16)
        fin[kind, sl, 1] = value[:, 256:].astype(jnp.bfloat16)
        for copy in final_copies(kind, sl, s, chip):
            copy.start()

    def final_drain(kind, group, chip):
        for n in range(max(0, len(group) - 2), len(group)):
            final_wait(kind, n % 2, chip)

    row_tok = lax.broadcasted_iota(jnp.int32, (1024, 128), 0) >> 3
    lane = lax.broadcasted_iota(jnp.int32, (1024, 128), 1)
    cs = scale * LOG2E
    lo_half, hi_half = slice(0, 128), slice(128, 256)

    def attend(s, slot):
        row = mine + s
        gslot = lax.rem(s, NG)
        piece = (e, 1 - e)
        for role in range(2):
            dq_row = docs[2 * c + piece[role], pl.ds(row, 1), :]
            d_t = jnp.transpose(jnp.broadcast_to(dq_row, (128, 128)))
            docr[role] = jnp.broadcast_to(d_t[:, None, :], (128, 8, 128)).reshape(1024, 128)

        def g_of(role):
            return qg[slot, 2 + role]

        def far_loop(body, down=False):
            for chip in range(1, 4):
                @pl.when(c == chip)
                def _():
                    for d in (range(chip, 0, -1) if down else range(1, chip + 1)):
                        body(d, d == chip)

        def scores(role, d, causal):
            sc = dot_nt(qg[slot, role], kvs[slot, d, 0]) * cs
            xs = []
            for j in range(2):
                dk_row = docs[2 * (c - d) + j, pl.ds(row, 1), :]
                vis = docr[role] == dk_row
                if causal:
                    vis = vis & (lane + 128 * j <= row_tok + 128 * piece[role])
                xs.append(jnp.where(vis, sc[:, 128 * j:128 * (j + 1)], NEG_BIG))
            top = jnp.maximum(xs[0], xs[1])
            es = [jnp.exp2(x - top) for x in xs]
            e_scr[d, role, :, lo_half] = es[0]
            e_scr[d, role, :, hi_half] = es[1]
            f_scr[d, role] = top
            l_scr[d, role] = es[0] + es[1]
            return top

        def dprob(role, d):
            dp_scr[d, role] = dot_nt(g_of(role), kvs[slot, d, 1])

        for role in range(2):
            t_scr[role] = scores(role, 0, True)

        def far_scores(d, x):
            for role in range(2):
                t_scr[role] = jnp.maximum(t_scr[role], scores(role, d, False))
            for role in range(2):
                dprob(role, d)
            return x
        far_loop(far_scores)

        for role in range(2):
            t_scr[role] = jnp.broadcast_to(jnp.max(t_scr[role], axis=1, keepdims=True), (1024, 128))
        dprob(0, 0)

        for role in range(2):
            top = t_scr[role]
            norm = l_scr[0, role] * jnp.exp2(f_scr[0, role] - top)
            for d in range(1, 4):
                norm = norm + l_scr[d, role] * jnp.exp2(f_scr[d, role] - top)
            t_scr[role] = top + jnp.log2(jnp.broadcast_to(jnp.sum(norm, axis=1, keepdims=True), (1024, 128)))
        dprob(1, 0)

        def weighted(role, d):
            f = jnp.exp2(f_scr[d, role] - t_scr[role])
            f_scr[d, role] = f
            for half in (lo_half, hi_half):
                p_scr[d, role, :, half] = (e_scr[d, role, :, half] * f).astype(jnp.bfloat16)
            return dot_nn(p_scr[d, role], kvs[slot, d, 1])

        def value_grads(d):
            dkv[gslot, d, :, 256:] = dot_tn(p_scr[d, 0], g_of(0)) + dot_tn(p_scr[d, 1], g_of(1))

        for role in range(2):
            o_acc[role] = weighted(role, 0)

        def far_weighted(d, x):
            for role in range(2):
                o_acc[role] = o_acc[role] + weighted(role, d)
            value_grads(d)
            return x
        far_loop(far_weighted)

        for role in range(2):
            o_low = o_acc[role].astype(jnp.bfloat16)
            outb[slot, role] = o_low
            delta = jnp.sum(g_of(role).astype(jnp.float32) * o_low.astype(jnp.float32), axis=1, keepdims=True)
            t_scr[role] = jnp.broadcast_to(delta, (1024, 128))
        value_grads(0)

        def score_grads(d):
            out = []
            for role in range(2):
                ds = [
                    (e_scr[d, role, :, half] * f_scr[d, role] * (dp_scr[d, role, :, half] - t_scr[role])).astype(jnp.bfloat16)
                    for half in (lo_half, hi_half)
                ]
                out.append(jnp.concatenate(ds, axis=1))
            dkv[gslot, d, :, :256] = dot_tn(out[0], qg[slot, 0]) + dot_tn(out[1], qg[slot, 1])
            return [dot_nn(ds, kvs[slot, d, 0]) for ds in out]

        def far_grads(d, farthest):
            got = score_grads(d)
            for role in range(2):
                o_acc[role] = got[role] if farthest else o_acc[role] + got[role]
            if farthest and d == 3:
                give(gslot, 3, 1, 0, s).start()
            if farthest and d == 2:
                pl.when(jnp.logical_not(member(s, ON2)))(lambda: give(gslot, 2, 0, 1, s).start())
        far_loop(far_grads, down=True)

        @pl.when(c == 0)
        def _():
            o_acc[...] = jnp.zeros_like(o_acc)
        got = score_grads(0)
        for role in range(2):
            o_acc[role] = o_acc[role] + got[role]
        for role in range(2):
            outb[slot, 2 + role] = (o_acc[role] * scale).astype(jnp.bfloat16)

    def part_wait(slot, s):
        remote(part.at[slot, s], part.at[slot, s], hop_s, part_r.at[slot, s], mate).wait_recv()

    def load(src, i):
        return [pltpu.make_async_copy(src.at[pl.ds(64 * n, 64)], sums.at[i, pl.ds(64 * n, 64)], lsem.at[i, n]) for n in range(4)]

    def start(copies):
        for copy in copies:
            copy.start()

    def finish(copies):
        for copy in copies:
            copy.wait()

    def passed(s, sl, chip, slot):
        return remote(sums.at[4 + sl], part.at[slot, s], xsem.at[sl], part_r.at[slot, s], dev(chip))

    def relay(s):
        return remote(part.at[2, s], part.at[1, s], rel_s.at[s], part_r.at[1, s], dev(1))

    def pass_on(i, group, held, slot_in, chip, slot_out):
        count = rank_in(i, group)
        sl = lax.rem(count, 2)
        start(load(hold.at[held, i], 0))
        part_wait(slot_in, i)
        start(load(part.at[slot_in, i], 1))
        pl.when(count >= 2)(lambda: passed(i, sl, chip, slot_out).wait_send())
        finish(load(hold.at[held, i], 0))
        finish(load(part.at[slot_in, i], 1))
        sums[4 + sl] = sums[0] + sums[1]
        passed(i, sl, chip, slot_out).start()

    def pass_x(i):
        pass_on(i, PASS_X, 0, 0, 0, 0)

    def pass_y(i):
        pass_on(i, ROUND, 0, 0, 0, 2)

    def total(kind, group, s, held, slots, chip):
        terms = [hold.at[held, s]] + [part.at[slot, s] for slot in slots]
        for n, src in enumerate(terms):
            if n:
                part_wait(slots[n - 1], s)
            start(load(src, n))
        for n, src in enumerate(terms):
            finish(load(src, n))
        value = sums[0]
        for n in range(1, len(terms)):
            value = value + sums[n]
        finalize(kind, group, s, value, chip)

    for d in range(1, 4):
        f_scr[d] = jnp.full((2, 1024, 128), NEG_BIG, jnp.float32)
        l_scr[d] = jnp.zeros((2, 1024, 128), jnp.float32)
    by_way_of_3(VIA3[0])
    arrive(0)
    for j in VIA3[1:]:
        by_way_of_3(j)
    fetch(0, 0)

    def step(s, x):
        slot = lax.rem(s, 2)

        late = (c >= LATE_CHIP) & (s == 0)

        def ahead():
            arrive(s + 1)
            fetch(s + 1, 1 - slot)
        pl.when((s + 1 < NS) & jnp.logical_not(late))(ahead)

        @pl.when(s >= 2)
        def _():
            put_wait(s - 2, slot)

        @pl.when(s >= NG)
        def _():
            grads_out(s - NG, False)
        fetch_wait(s, slot)
        attend(s, slot)

        @pl.when(c == 3)
        def _():
            gslot = lax.rem(s, NG)
            pl.when(member(s, ROUND))(lambda: give(gslot, 2, 2, 0, s).start())

            @pl.when(member(s, MERGE))
            def _():
                part_wait(0, s)
                start(load(part.at[0, s], 0))
                finish(load(part.at[0, s], 0))
                dkv[gslot, 2] = dkv[gslot, 2] + sums[0]

            @pl.when(member(s, FAR1))
            def _():
                part_wait(0, s)
                start(load(part.at[0, s], 0))
                part_wait(2, s)
                start(load(part.at[2, s], 1))
                finish(load(part.at[0, s], 0))
                finish(load(part.at[2, s], 1))
                finalize(1, FAR1, s, dkv[gslot, 2] + sums[0] + sums[1], 1)
            finalize(0, OWN3, s, dkv[gslot, 0], None)
            pl.when(member(s, MERGE))(lambda: give(gslot, 2, 1, 1, s).start())

            def last_two():
                part_wait(1, s)
                start(load(part.at[1, s], 2))
                finish(load(part.at[1, s], 2))
                finalize(2, LAST2, s, dkv[gslot, 1] + sums[2], 2)
            choose(member(s, LAST2), last_two, lambda: give(gslot, 1, 2, 1, s).start())
        put(s, slot)
        for at, i in EARLY_X.items():
            pl.when((c == 1) & (s == at))(lambda: pass_x(i))
        for at, i in EARLY_Y.items():
            pl.when((c == 2) & (s == at))(lambda: pass_y(i))
        pl.when(late)(ahead)
        return x

    lax.fori_loop(0, NS, step, 0)
    put_wait(NS - 2, 0)
    put_wait(NS - 1, 1)
    for s in range(NS - NG, NS):
        grads_out(s, False)

    def home(i, x):
        def behind(lag, body):
            s = i - lag
            pl.when((s >= 0) & (s < NS))(lambda: body(s))

        @pl.when(c == 0)
        def _():
            @pl.when(member(i, ROUND))
            def _():
                part_wait(2, i)
                relay(i).start()
            pl.when(member(i, ON1))(lambda: pass_on(i, PASS_0, 1, 1, 1, 2))
            pl.when(member(i, ON2))(lambda: pass_on(i, PASS_0, 1, 0, 2, 2))
            behind(LAG[0], lambda s: pl.when(member(s, HERE0))(lambda: total(0, HERE0, s, 1, (1, 0), None)))

        @pl.when(c == 1)
        def _():
            later = tuple(s for s in PASS_X if s not in EARLY_X.values())
            pl.when(member(i, later))(lambda: pass_x(i))

            def body(s):
                pl.when(member(s, ON1))(lambda: total(1, ON1, s, 0, (0, 2), 0))
                pl.when(member(s, OWN1))(lambda: total(0, OWN1, s, 1, (1,), None))
            behind(LAG[1], body)

        @pl.when(c == 2)
        def _():
            later = tuple(s for s in ROUND if s not in EARLY_Y.values())
            pl.when(member(i, later))(lambda: pass_y(i))

            def body(s):
                pl.when(member(s, ON2))(lambda: total(1, ON2, s, 2, (2,), 0))
                pl.when(member(s, OWN2))(lambda: total(0, OWN2, s, 1, (1,), None))
            behind(LAG[2], body)
        return x

    @pl.when(c < 3)
    def _():
        lax.fori_loop(0, NS + max(LAG), home, 0)

    def down_wait(n):
        for which, ref in ((0, dk), (1, dv)):
            rows = ref.at[pl.ds(0, n)]
            remote(rows, rows, hop_s, down_r.at[which], mate).wait_recv()

    @pl.when(c == 0)
    def _():
        for s in ROUND:
            relay(s).wait_send()
        for sl in range(2):
            passed(0, sl, 1, 2).wait_send()
        sent = kvr.at[1, pl.ds(0, NS - len(VIA3))]
        remote(sent, sent, hop_s, kv_r.at[0, 0], mate).wait_send()
        final_drain(0, HERE0, None)
        down_wait(len(PASS_0))

    @pl.when(c == 1)
    def _():
        for sl in range(2):
            passed(0, sl, 0, 0).wait_send()
        remote(kvr.at[0], kvr.at[0], hop_s, kv_r.at[0, 0], mate).wait_send()
        final_drain(0, OWN1, None)
        final_drain(1, ON1, 0)
        down_wait(len(FAR1))

    @pl.when(c == 2)
    def _():
        for sl in range(2):
            passed(0, sl, 0, 2).wait_send()
        final_drain(0, OWN2, None)
        final_drain(1, ON2, 0)
        down_wait(len(LAST2))

    @pl.when(c == 3)
    def _():
        sent = kvr.at[1, pl.ds(0, len(VIA3))]
        remote(sent, sent, hop_s, kv_r.at[0, 0], mate).wait_send()
        final_drain(0, OWN3, None)
        final_drain(1, FAR1, 1)
        final_drain(2, LAST2, 2)
    for which, ref in ((0, k), (1, v)):
        some = ref.at[pl.ds(0, 2 * (NS - len(VIA3)))]
        for way, chips, sent in ((0, c < 3, ref), (1, c == 0, ref), (1, c == 1, some)):
            @pl.when(chips)
            def _():
                remote(sent, sent, kv_s.at[way, which], kv_r.at[0, 0], mate).wait_send()
        half = ref.at[pl.ds(other, NS)]
        remote(half, half, kv_s.at[2, which], kv_r.at[0, 0], mate).wait_send()
    for which, ref in ((0, q), (1, g)):
        half = ref.at[pl.ds(other, NS)]
        remote(half, half, q_s.at[which], q_r.at[0], mate).wait_send()
    for which, ref in ((0, o), (1, dq)):
        half = ref.at[pl.ds(other, NS)]
        remote(half, half, hop_s, osend_r.at[which], mate).wait_recv()
    for which, ref in ((0, dk), (1, dv)):
        half = ref.at[pl.ds(other, NS)]
        remote(half, half, hop_s, dsend_r.at[which], mate).wait_recv()


def place_kernel(slots, *refs):
    srcs, dsts, (buf, rsem, wsem) = refs[:4], refs[4:8], refs[8:]
    size = buf.shape[1]
    jobs = [(src.at[pl.ds(i, size)], dst.at[pl.ds(i, size)]) for src, dst in zip(srcs, dsts) for i in range(0, src.shape[0], size)]

    def read(j):
        return pltpu.make_async_copy(jobs[j][0], buf.at[j % slots], rsem.at[j % slots])

    def write(j):
        return pltpu.make_async_copy(buf.at[j % slots], jobs[j][1], wsem.at[j % slots])

    ahead = 10
    for j in range(min(ahead, len(jobs))):
        read(j).start()
    for j in range(len(jobs)):
        read(j).wait()
        write(j).start()
        if j + ahead < len(jobs):
            if j + ahead >= slots:
                write(j + ahead - slots).wait()
            read(j + ahead).start()
    for j in range(max(0, len(jobs) - slots), len(jobs)):
        write(j).wait()


ANY = pl.BlockSpec(memory_space=pl.ANY)
VMEM = pl.BlockSpec(memory_space=pltpu.VMEM)


def solution(mesh):
    n_dev = mesh.shape['cp']
    seq_spec = P('dp', 'cp', None, None)
    id_spec = P('dp', 'cp')
    bf, f32 = jnp.bfloat16, jnp.float32
    shape = jax.ShapeDtypeStruct
    dma = pltpu.SemaphoreType.DMA

    def per_device(query, keys, values, grad_out, doc_id):
        nb, piece, heads, hd = query.shape
        rows = piece * heads
        outs = pl.pallas_call(
            functools.partial(fused_kernel, hd ** -0.5),
            in_specs=[VMEM] + [ANY] * 4,
            out_specs=[ANY] * 8,
            out_shape=[
                shape((nb, rows, hd), bf), shape((nb, rows, hd), bf), shape((nb, piece, hd), bf), shape((nb, piece, hd), bf),
                shape((NS, 2, rows, hd), bf), shape((4, NS, 2, 256, 256), bf),
                shape((3, NS, 256, 512), f32), shape((3, NS, 256, 512), f32),
            ],
            scratch_shapes=[
                pltpu.VMEM((n_dev, nb, piece), jnp.int32), pltpu.VMEM((2, 4, 2, 256, 256), bf), pltpu.VMEM((2, 4, rows, hd), bf),
                pltpu.VMEM((2, 4, rows, hd), bf), pltpu.VMEM((NG, 4, 256, 512), f32), pltpu.VMEM((6, 256, 512), f32),
                pltpu.VMEM((3, 2, 2, 256, 256), bf),
                pltpu.VMEM((4, 2, rows, 256), f32), pltpu.VMEM((4, 2, rows, 256), f32), pltpu.VMEM((4, 2, rows, 256), bf),
                pltpu.VMEM((4, 2, rows, 128), f32), pltpu.VMEM((4, 2, rows, 128), f32), pltpu.VMEM((2, rows, 128), f32),
                pltpu.VMEM((2, rows, 128), jnp.int32), pltpu.VMEM((2, rows, hd), f32),
                dma((n_dev,)), dma((n_dev,)), dma((2, 10)), dma((2, 4)), dma((NG, 4)), dma((2,)), dma((2,)), dma((NJ,)), dma((3, 2)), dma((4, NJ)),
                dma, dma((3, NS)), dma((3, 2, 4)), dma((2,)), dma((3, 4)), dma((2,)), dma((NS,)), dma((2,)),
            ],
            compiler_params=pltpu.CompilerParams(has_side_effects=True, vmem_limit_bytes=62 * 1024 * 1024),
            name="attend",
        )(doc_id, query.reshape(nb, rows, hd), grad_out.reshape(nb, rows, hd), keys.reshape(nb, piece, hd), values.reshape(nb, piece, hd))
        outs = [x.reshape(-1, rows, hd) for x in outs[:4]]
        o, dq, dk, dv = pl.pallas_call(
            functools.partial(place_kernel, 14),
            in_specs=[ANY] * 4,
            out_specs=[ANY] * 4,
            out_shape=[shape(x.shape, bf) for x in outs],
            scratch_shapes=[pltpu.VMEM((14, 4, rows, hd), bf), dma((14,)), dma((14,))],
            compiler_params=pltpu.CompilerParams(vmem_limit_bytes=63 * 1024 * 1024),
            name="place",
        )(*outs)
        return o.reshape(query.shape), dq.reshape(query.shape), dk.reshape(keys.shape), dv.reshape(values.shape)

    return jax.shard_map(per_device, mesh=mesh, in_specs=(seq_spec, seq_spec, seq_spec, seq_spec, id_spec),
                         out_specs=(seq_spec, seq_spec, seq_spec, seq_spec), check_vma=False)
```
